32 devices in a mesh: ctx: 8 (over z, x), fsdp: 4 (over y, core).
Axes of the slice: x: 2, y: 2, z: 4, core: 2. Of those that a mesh axis runs over, the one named last changes fastest.
Arguments:
- tokens: bfloat16 [4, 1024, 1536], P('fsdp', 'ctx'), may hold values from -6 to 6
- cotangent: bfloat16 [4, 1024, 1536], P('fsdp', 'ctx'), may hold values from -6 to 6
- lengths: int32 [4, 4], P('fsdp'), may hold values from 1 to 512, 1024 in all within a row
- tile_order: int32 [4, 8], P('fsdp'), may hold values from 0 to 7, each once within a row
- routes: int32 [2, 4, 1024, 8], P(None, 'fsdp', 'ctx'), may hold values from 0 to 15, all different within a row; in each aligned block of 128 rows (0 to 127, 128 to 255, ..., all dimensions but the last counted through in order) at most 80 rows name the same one
- gates: float32 [2, 4, 1024, 8], P(None, 'fsdp', 'ctx'), may hold values from 0.1 to 1
- query_weight: float32 [2, 1536, 1536], P(None, ('ctx', 'fsdp')), may hold values from -0.15625 to 0.15625
- key_weight: float32 [2, 1536, 512], P(None, ('ctx', 'fsdp')), may hold values from -0.15625 to 0.15625
- value_weight: float32 [2, 1536, 512], P(None, ('ctx', 'fsdp')), may hold values from -0.15625 to 0.15625
- out_weight: float32 [2, 1536, 1536], P(None, ('ctx', 'fsdp')), may hold values from -0.625 to 0.625
- attn_gain: float32 [2, 1536], P(None, ('ctx', 'fsdp')), may hold values from 0.5 to 1.5
- moe_gain: float32 [2, 1536], P(None, ('ctx', 'fsdp')), may hold values from 0.5 to 1.5
- gate_weight: float32 [2, 16, 1536, 512], P(None, None, ('ctx', 'fsdp')), may hold values from -0.15625 to 0.15625
- up_weight: float32 [2, 16, 1536, 512], P(None, None, ('ctx', 'fsdp')), may hold values from -0.15625 to 0.15625
- down_weight: float32 [2, 16, 1536, 512], P(None, None, ('ctx', 'fsdp')), may hold values from -0.5 to 0.5
Outputs:
- output: bfloat16 [4, 1024, 1536], P('fsdp', 'ctx')
- grad_tokens: float32 [4, 1024, 1536], P('fsdp', 'ctx')
- grad_query_weight: float32 [2, 1536, 1536], P(None, ('ctx', 'fsdp'))
- grad_key_weight: float32 [2, 1536, 512], P(None, ('ctx', 'fsdp'))
- grad_value_weight: float32 [2, 1536, 512], P(None, ('ctx', 'fsdp'))
- grad_out_weight: float32 [2, 1536, 1536], P(None, ('ctx', 'fsdp'))
- grad_attn_gain: float32 [2, 1536], P(None, ('ctx', 'fsdp'))
- grad_moe_gain: float32 [2, 1536], P(None, ('ctx', 'fsdp'))
- grad_gate_weight: float32 [2, 16, 1536, 512], P(None, None, ('ctx', 'fsdp'))
- grad_up_weight: float32 [2, 16, 1536, 512], P(None, None, ('ctx', 'fsdp'))
- grad_down_weight: float32 [2, 16, 1536, 512], P(None, None, ('ctx', 'fsdp'))
The draws below stay inside these ranges and needn't reach their ends.
Inputs may be any that keep to these rules, and one draw needn't show every extreme that they name: The 4 lengths of a batch sum to 1024 and the longest is 512. `tile_order`: each batch's row holds every tile number once. `routes`: each token names 8 different experts; among the rows of one device in one layer (aligned blocks of 128 rows) no expert is named more than 80 times, and in some blocks one is named exactly 80 times.
All inputs are finite; a program needn't handle non-finite values.
Results may differ from the reference program's by a relative error of at most 0.028.
Values may be sent and summed in bfloat16 or wider, within the bound.
A program may use at most 384 MiB of HBM per device.

```python
import math
import jax
import jax.numpy as jnp
import numpy as np
from jax import lax

D = 1536
HEADS = 24
KV_HEADS = 8
HEAD_DIM = 64
FF = 512
TOPK = 8
EXPERTS = 16
LAYERS = 2
TILE = 128
TOK_DEV = 128
CAP = 80
GROUP = 1024
TILES = 8
BATCHES = 4
LONGEST = 512
SEQS = 4


def block_scale(key, shape, split, low, high):
    gain, own = 1.0, jax.random.fold_in(key, 6)
    for axis_at, parts in split:
        steps = jnp.exp(jax.random.uniform(jax.random.fold_in(own, axis_at), (parts,), jnp.float32, low / len(split), high / len(split)))
        gain = gain * jnp.repeat(steps, shape[axis_at] // parts).reshape([-1 if axis == axis_at else 1 for axis in range(len(shape))])
    return gain


def length_profile(count, total, most, lean):
    portions = [(1 << 20) // math.isqrt(grade ** lean) + 1 for grade in range(2, count + 1)]
    rest, given = total - most - (count - 1), [1] * (count - 1)
    while rest > 0:
        candidates = [i for i in range(count - 1) if given[i] < most]
        pool, remaining = sum([portions[i] for i in candidates]), rest
        for i in candidates:
            extra = min(most - given[i], max(1, remaining * portions[i] // pool), rest)
            given[i] = given[i] + extra
            rest = rest - extra
    return np.array([most] + given)


def uneven(rng, number_of, total, limit, lean):
    if number_of == 2:
        one = jax.random.randint(rng, (), max(1, total - limit), min(limit, total - 1) + 1)
        return jnp.stack([one, total - one])
    sizes = jnp.asarray(length_profile(number_of, total, limit, lean), jnp.int32)
    pairs = (number_of - 1) // 2
    donor, taker = sizes[1:1 + 2 * pairs:2], sizes[2:2 + 2 * pairs:2]
    slack = jnp.minimum(donor - 1, limit - taker)
    moved = jax.random.randint(jax.random.fold_in(rng, 1), (pairs,), 0, 1 << 20) % (slack + 1)
    sizes = sizes.at[1:1 + 2 * pairs:2].set(donor - moved).at[2:2 + 2 * pairs:2].set(taker + moved)
    return sizes[jax.random.permutation(jax.random.fold_in(rng, 2), number_of)]


def shared_out(stream_key, own, number, rows, amount, top, bound, lean):
    sequence = jax.random.permutation(stream_key, amount)
    heavy_load, usual = portions_of(amount, rows * top, bound, lean, True), portions_of(amount, rows * top, bound, lean, False)
    places = jnp.arange(amount)

    def named(sizes, turn):
        used = int((sizes > 0).sum())
        fixed = max(1, used // 4)
        moved = fixed + (places - fixed + turn * (used - fixed)) % max(1, amount - fixed)
        return jnp.zeros((amount,), jnp.int32).at[sequence[jnp.where(places < fixed, places, moved)]].set(jnp.asarray(sizes, jnp.int32))

    sizes = jnp.where(number % 4 == 0, named(heavy_load, number // 4), named(usual, number - number // 4 - 1))
    mixed = jax.random.permutation(jax.random.fold_in(own, 3), amount)
    giver, taker = mixed[0:amount // 2 * 2:2], mixed[1:amount // 2 * 2:2]
    margin = jnp.minimum(sizes[giver] - 1, bound - sizes[taker]) // 2
    margin = jnp.where((giver == sequence[0]) | (taker == sequence[0]) | (sizes[taker] == 0), 0, jnp.maximum(margin, 0))
    moved = jax.random.randint(jax.random.fold_in(own, 4), (amount // 2,), 0, 1 << 20) % (margin + 1)
    sizes = sizes.at[giver].add(-moved).at[taker].add(moved)
    members = jnp.searchsorted(jnp.cumsum(sizes), jnp.arange(rows * top), side="right").astype(jnp.int32)
    table = members.reshape(top, rows).T
    table = table[jax.random.permutation(jax.random.fold_in(own, 1), rows)]
    turn = jax.random.randint(jax.random.fold_in(own, 2), (rows, 1), 0, top)
    return jnp.take_along_axis(table, (jnp.arange(top)[None, :] + turn) % top, axis=1)


def portions_of(number_of, total, most, lean, full):
    weights = [(1 << 20) // math.isqrt(grade ** lean) + 1 for grade in range(1, number_of + 1)]
    largest = most if full else min(most, max(-(-total // number_of), total * weights[0] // sum(weights)))
    least = 1 if total - largest >= number_of - 1 else 0
    holding, surplus = [largest] + [least] * (number_of - 1), total - largest - least * (number_of - 1)
    while surplus > 0:
        movable = [i for i in range(1, number_of) if holding[i] < largest] or [i for i in range(1, number_of) if holding[i] < most]
        whole, left = sum([weights[i] for i in movable]), surplus
        for i in movable:
            extra = min(most - holding[i], max(1, left * weights[i] // whole), surplus)
            holding[i] = holding[i] + extra
            surplus = surplus - extra
    return np.array(holding)


def bell_draw(stream_key, dims, deviation, most, shards=(), held_as=jnp.bfloat16):
    gain = block_scale(stream_key, dims, shards, -0.22, 0.18) if shards else 1.0
    entries = jax.random.normal(stream_key, dims, jnp.float32) * deviation * gain
    return jnp.minimum(jnp.maximum(entries, -most), most).astype(held_as)


def setup_inputs(seed: int = 0) -> dict:
    arg_keys = jax.random.split(jax.random.key(seed), 16)
    tokens = bell_draw(arg_keys[0], (BATCHES, GROUP, D), 1.0, 6.0, ((0, 4), (1, 8)))
    cotangent = bell_draw(arg_keys[1], (BATCHES, GROUP, D), 1.0, 6.0, ((0, 4), (1, 8)))
    lengths = jax.vmap(lambda own: uneven(own, SEQS, GROUP, LONGEST, 2))(jax.random.split(arg_keys[2], BATCHES)).reshape((BATCHES, SEQS)).astype(jnp.int32)
    tile_order = jax.vmap(lambda own: jax.random.permutation(own, TILES))(jax.random.split(arg_keys[3], BATCHES)).reshape((BATCHES, TILES)).astype(jnp.int32)
    routes_keys = jax.random.split(jax.random.fold_in(arg_keys[4], 1), LAYERS * BATCHES * GROUP // TOK_DEV)
    routes_turns = jax.random.permutation(jax.random.fold_in(arg_keys[4], 3), LAYERS * BATCHES * GROUP // TOK_DEV)
    routes = jax.vmap(lambda own, number: shared_out(jax.random.fold_in(arg_keys[4], 2), own, number, TOK_DEV, EXPERTS, TOPK, CAP, 1))(routes_keys, routes_turns).reshape((LAYERS, BATCHES, GROUP, TOPK))
    gates = jnp.clip(jnp.exp(math.log(1.0) - 2.3025851 * jax.random.uniform(arg_keys[5], (LAYERS, BATCHES, GROUP, TOPK), jnp.float32) ** block_scale(arg_keys[5], (LAYERS, BATCHES, GROUP, TOPK), ((1, 4), (2, 8)), -0.2, 0.2)), 0.1, 1.0)
    query_weight = bell_draw(arg_keys[6], (LAYERS, D, HEADS * HEAD_DIM), D ** -0.5, 0.15625, ((1, 32),), jnp.float32)
    key_weight = bell_draw(arg_keys[7], (LAYERS, D, KV_HEADS * HEAD_DIM), D ** -0.5, 0.15625, ((1, 32),), jnp.float32)
    value_weight = bell_draw(arg_keys[8], (LAYERS, D, KV_HEADS * HEAD_DIM), D ** -0.5, 0.15625, ((1, 32),), jnp.float32)
    out_weight = bell_draw(arg_keys[9], (LAYERS, D, HEADS * HEAD_DIM), (HEADS * HEAD_DIM // 16) ** -0.5, 0.625, ((1, 32),), jnp.float32)
    attn_gain = jnp.clip(1.0 + 0.1 * jax.random.normal(arg_keys[10], (LAYERS, D), jnp.float32), 0.5, 1.5)
    moe_gain = jnp.clip(1.0 + 0.1 * jax.random.normal(arg_keys[11], (LAYERS, D), jnp.float32), 0.5, 1.5)
    gate_weight = bell_draw(arg_keys[12], (LAYERS, EXPERTS, D, FF), D ** -0.5, 0.15625, ((2, 32),), jnp.float32)
    up_weight = bell_draw(arg_keys[13], (LAYERS, EXPERTS, D, FF), D ** -0.5, 0.15625, ((2, 32),), jnp.float32)
    down_weight = bell_draw(arg_keys[14], (LAYERS, EXPERTS, D, FF), (FF // 4) ** -0.5, 0.5, ((2, 32),), jnp.float32)
    return dict(tokens=tokens, cotangent=cotangent, lengths=lengths, tile_order=tile_order, routes=routes, gates=gates, query_weight=query_weight, key_weight=key_weight, value_weight=value_weight, out_weight=out_weight, attn_gain=attn_gain, moe_gain=moe_gain, gate_weight=gate_weight, up_weight=up_weight, down_weight=down_weight)


EPSILON = 1e-06
NEGATIVE = -1e+30
HIGHEST = lax.Precision.HIGHEST

@jax.custom_vjp
def low(v):
    return lax.optimization_barrier(v.astype(jnp.bfloat16)).astype(jnp.float32)

@jax.custom_vjp
def low_back(v):
    return v

def low_keep(v):
    return (low(v), None)

def low_pass(kept, grad):
    return (grad,)

def back_keep(v):
    return (v, None)

def back_low(kept, grad):
    return (low(grad),)
low.defvjp(low_keep, low_pass)
low_back.defvjp(back_keep, back_low)

def layout(lengths, tile_order, group_rows):
    tile_count = tile_order.shape[0]
    row_ids = jnp.arange(group_rows, dtype=jnp.int32)
    in_tile = (row_ids // TILE)[:, None] == jnp.arange(tile_count, dtype=jnp.int32)[None, :]
    tile_of = lax.optimization_barrier(jnp.sum(jnp.where(in_tile, tile_order[None, :], 0), axis=1, dtype=jnp.int32))
    anchor = tile_of * TILE + row_ids % TILE
    seq_ends = jnp.cumsum(lengths, dtype=jnp.int32)
    seq_starts = seq_ends - lengths
    segment = lax.optimization_barrier(jnp.sum((anchor[:, None] >= seq_ends[None, :]).astype(jnp.int32), axis=1, dtype=jnp.int32))
    picked = segment[:, None] == jnp.arange(lengths.shape[0], dtype=jnp.int32)[None, :]
    offset = lax.optimization_barrier(jnp.sum(jnp.where(picked, seq_starts[None, :], 0), axis=1, dtype=jnp.int32))
    return (segment, anchor - offset)

def rms_norm(values, gain_vec):
    return values * lax.rsqrt(lax.optimization_barrier(jnp.mean(values * values, axis=-1, keepdims=True)) + EPSILON) * gain_vec

def rotate(values, places):
    half_dim = values.shape[-1] // 2
    freq_steps = jnp.arange(half_dim, dtype=jnp.float32)
    inverse = jnp.exp(freq_steps * (-2.0 * math.log(10000.0) / values.shape[-1]))
    angles = places[:, None] * inverse[None, :]
    cos_part = jnp.cos(angles)[:, None, :]
    sin_part = jnp.sin(angles)[:, None, :]
    first_half = values[..., :half_dim]
    second_half = values[..., half_dim:]
    return jnp.concatenate([first_half * cos_part - second_half * sin_part, second_half * cos_part + first_half * sin_part], axis=-1)

def attend(queries, key_rows, value_rows, segment, position, score_scale):
    block_count = GROUP // TOK_DEV
    heads_kv = key_rows.shape[1]
    groups = queries.shape[1] // heads_kv
    query_blocks = queries.reshape(block_count, TOK_DEV, heads_kv, groups, HEAD_DIM)
    seg_blocks = segment.reshape(block_count, TOK_DEV)
    pos_blocks = position.reshape(block_count, TOK_DEV)

    def one_block(block_item):
        query_part, seg_part, pos_part = block_item
        raw_scores = jnp.einsum('qhgd,khd->hgqk', query_part, key_rows, precision=HIGHEST) * score_scale
        raw_scores = low_back(raw_scores)
        visible = (seg_part[:, None] == segment[None, :]) & (position[None, :] <= pos_part[:, None])
        masked = jnp.where(visible[None, None], raw_scores, NEGATIVE)
        row_peak = lax.optimization_barrier(jnp.max(masked, axis=-1, keepdims=True))
        exp_scores = jnp.exp(masked - row_peak)
        attn_probs = exp_scores / lax.optimization_barrier(jnp.sum(exp_scores, axis=-1, keepdims=True))
        return jnp.einsum('hgqk,khd->qhgd', low(attn_probs), value_rows, precision=HIGHEST)
    outputs = lax.map(jax.checkpoint(one_block), (query_blocks, seg_blocks, pos_blocks))
    return outputs.reshape(GROUP, heads_kv * groups * HEAD_DIM)

def mixture(moe_in, gate_table, gate_full, up_full, down_full):

    def expert(running, expert_item):
        one_gate, one_up, one_down, gate_col = expert_item
        gate_act = low_back(jnp.dot(moe_in, one_gate, precision=HIGHEST))
        up_act = low_back(jnp.dot(moe_in, one_up, precision=HIGHEST))
        inner_act = low(jax.nn.silu(gate_act) * up_act)
        result = low_back(jnp.dot(inner_act, one_down.T, precision=HIGHEST))
        return (running + gate_col[:, None] * result, None)
    start_sum = jnp.zeros(moe_in.shape, jnp.float32)
    return lax.scan(expert, start_sum, (gate_full, up_full, down_full, gate_table.T))[0]

def forward(tokens_f, weight_set, segments, positions, gate_table):
    query_weight, key_weight, value_weight, out_weight, attn_gain, moe_gain, gate_weight, up_weight, down_weight = weight_set
    hidden = tokens_f
    score_scale = HEAD_DIM ** (-0.5)
    place_flat = positions.reshape(-1).astype(jnp.float32)
    for layer_index in range(LAYERS):
        query_full = low(query_weight[layer_index])
        key_full = low(key_weight[layer_index])
        value_full = low(value_weight[layer_index])
        out_full = low(out_weight[layer_index])
        attn_norm = low(attn_gain[layer_index])
        moe_norm = low(moe_gain[layer_index])
        gate_full = low(gate_weight[layer_index])
        up_full = low(up_weight[layer_index])
        down_full = low(down_weight[layer_index])
        normed = low(rms_norm(hidden, attn_norm)).reshape(-1, D)
        queries = low_back(jnp.dot(normed, query_full, precision=HIGHEST))
        key_rows = low_back(jnp.dot(normed, key_full, precision=HIGHEST))
        value_rows = low(low_back(jnp.dot(normed, value_full, precision=HIGHEST)))
        queries = low(rotate(queries.reshape(-1, HEADS, HEAD_DIM), place_flat))
        key_rows = low(rotate(key_rows.reshape(-1, KV_HEADS, HEAD_DIM), place_flat))
        value_rows = value_rows.reshape(-1, KV_HEADS, HEAD_DIM)
        pieces = []
        for batch_index in range(BATCHES):
            low_row = batch_index * GROUP
            pieces.append(attend(queries[low_row:low_row + GROUP], key_rows[low_row:low_row + GROUP], value_rows[low_row:low_row + GROUP], segments[batch_index], positions[batch_index], score_scale))
        attended = low(low_back(jnp.concatenate(pieces, axis=0)))
        middle = hidden + low_back(jnp.dot(attended, out_full.T, precision=HIGHEST)).reshape(hidden.shape)
        moe_in = low(rms_norm(middle, moe_norm)).reshape(-1, D)
        moe_out = mixture(moe_in, gate_table[layer_index].reshape(-1, EXPERTS), gate_full, up_full, down_full)
        hidden = middle + moe_out.reshape(hidden.shape)
    return hidden

def reference(tokens, cotangent, lengths, tile_order, routes, gates, query_weight, key_weight, value_weight, out_weight, attn_gain, moe_gain, gate_weight, up_weight, down_weight):
    seg_list = []
    pos_list = []
    for batch_index in range(BATCHES):
        segment, position = layout(lengths[batch_index], tile_order[batch_index], GROUP)
        seg_list.append(segment)
        pos_list.append(position)
    segments = jnp.stack(seg_list)
    positions = jnp.stack(pos_list)
    expert_ids = jnp.arange(EXPERTS, dtype=jnp.int32)
    gate_table = lax.optimization_barrier(jnp.sum(jnp.where(routes[..., None] == expert_ids, gates[..., None], 0.0), axis=-2))
    weight_set = (query_weight, key_weight, value_weight, out_weight, attn_gain, moe_gain, gate_weight, up_weight, down_weight)

    def run_layers(tokens_f, params_in):
        return forward(tokens_f, params_in, segments, positions, gate_table)
    result, pull_back = jax.vjp(run_layers, tokens.astype(jnp.float32), weight_set)
    grad_tokens, grad_set = pull_back(cotangent.astype(jnp.float32))
    return (result.astype(jnp.bfloat16), grad_tokens, grad_set[0], grad_set[1], grad_set[2], grad_set[3], grad_set[4], grad_set[5], grad_set[6], grad_set[7], grad_set[8])
```

```python
from functools import partial
import functools
import math

import jax
import jax.numpy as jnp
from jax import lax
from jax.experimental import pallas as pl
from jax.experimental.pallas import tpu as pltpu
from jax.sharding import PartitionSpec as P

HEAD_DIM = 64
EXPERTS = 16
LAYERS = 2
TILE = 128
CAP = 80


EPSILON = 1e-06
NEGATIVE = -1e30


def layout(lengths, tile_order, group_rows):
    tile_count = tile_order.shape[0]
    row_ids = jnp.arange(group_rows, dtype=jnp.int32)
    in_tile = (row_ids // TILE)[:, None] == jnp.arange(tile_count, dtype=jnp.int32)[None, :]
    tile_of = jnp.sum(jnp.where(in_tile, tile_order[None, :], 0), axis=1, dtype=jnp.int32)
    anchor = tile_of * TILE + row_ids % TILE
    seq_ends = jnp.cumsum(lengths, dtype=jnp.int32)
    seq_starts = seq_ends - lengths
    segment = jnp.sum(
        (anchor[:, None] >= seq_ends[None, :]).astype(jnp.int32), axis=1, dtype=jnp.int32
    )
    picked = segment[:, None] == jnp.arange(lengths.shape[0], dtype=jnp.int32)[None, :]
    offset = jnp.sum(jnp.where(picked, seq_starts[None, :], 0), axis=1, dtype=jnp.int32)
    return (segment, anchor - offset)


def rms_norm(values, gain_vec):
    return (
        values * lax.rsqrt(jnp.mean(values * values, axis=-1, keepdims=True) + EPSILON) * gain_vec
    )


def rotate(values, places):
    half_dim = values.shape[-1] // 2
    freq_steps = jnp.arange(half_dim, dtype=jnp.float32)
    inverse = jnp.exp(freq_steps * (-2.0 * math.log(10000.0) / values.shape[-1]))
    angles = places[:, None] * inverse[None, :]
    cos_part = jnp.cos(angles)[:, None, :]
    sin_part = jnp.sin(angles)[:, None, :]
    first_half = values[..., :half_dim]
    second_half = values[..., half_dim:]
    return jnp.concatenate(
        [
            first_half * cos_part - second_half * sin_part,
            second_half * cos_part + first_half * sin_part,
        ],
        axis=-1,
    )


def rotate_back(grads_in, places):
    return jax.vjp(partial(rotate, places=places), jnp.zeros(grads_in.shape, jnp.float32))[1](
        grads_in
    )[0]


def mix_inner(gate_act, up_act):
    return jax.nn.silu(gate_act) * up_act


def split_halves(master):
    experts_here, rows_here, hidden_units = master.shape
    return (
        master.astype(jnp.bfloat16)
        .reshape(experts_here, rows_here, 2, hidden_units // 2)
        .transpose(0, 2, 1, 3)
        .reshape(2 * experts_here, rows_here, hidden_units // 2)
    )


def merge_halves(grads_in):
    halves_all, rows_here, half_units = grads_in.shape
    return (
        grads_in.reshape(halves_all // 2, 2, rows_here, half_units)
        .transpose(0, 2, 1, 3)
        .reshape(halves_all // 2, rows_here, 2 * half_units)
    )


def doubled(slots):
    return jnp.broadcast_to(slots[:, None], (slots.shape[0], 2) + slots.shape[1:]).reshape(
        (2 * slots.shape[0],) + slots.shape[1:]
    )


def fold_halves(parts):
    return jnp.sum(parts.reshape((parts.shape[0] // 2, 2) + parts.shape[1:]), axis=1)


def send_out(slots):
    return lax.all_to_all(slots, "ctx", split_axis=0, concat_axis=1, tiled=True)


def send_back(parts):
    return lax.all_to_all(
        parts.astype(jnp.bfloat16), "ctx", split_axis=1, concat_axis=0, tiled=True
    ).astype(parts.dtype)


def routing(route_ids, gate_share, rows_here):
    expert_ids = jnp.arange(EXPERTS, dtype=jnp.int32)
    chosen = (route_ids[:, :, None] == expert_ids[None, None, :]).astype(jnp.int32)
    member = jnp.sum(chosen, axis=1, dtype=jnp.int32)
    before = jnp.cumsum(member, axis=0, dtype=jnp.int32) - member
    rank_of = jnp.sum(chosen * before[:, None, :], axis=2, dtype=jnp.int32)
    slot_of = route_ids * CAP + rank_of
    token_ids = jnp.broadcast_to(jnp.arange(rows_here, dtype=jnp.int32)[:, None], route_ids.shape)
    flat_slots = slot_of.reshape(-1)
    slot_token = (
        jnp.full((EXPERTS * CAP,), rows_here, jnp.int32).at[flat_slots].set(token_ids.reshape(-1))
    )
    slot_share = jnp.zeros((EXPERTS * CAP,), jnp.float32).at[flat_slots].set(gate_share.reshape(-1))
    return (slot_of, slot_token, slot_share)


def key_block(key_rows, value_rows, token_meta, block_index, block_rows):
    seg_local, pos_local, seg_all, pos_all = token_meta
    first_row = block_index * block_rows
    key_part = lax.dynamic_slice_in_dim(key_rows, first_row, block_rows, 0)
    value_part = lax.dynamic_slice_in_dim(value_rows, first_row, block_rows, 0)
    seg_part = lax.dynamic_slice_in_dim(seg_all, first_row, block_rows, 0)
    pos_part = lax.dynamic_slice_in_dim(pos_all, first_row, block_rows, 0)
    visible = (seg_local[:, None] == seg_part[None, :]) & (pos_part[None, :] <= pos_local[:, None])
    return (key_part, value_part, visible)


def scores(queries, key_part, visible, score_scale):
    raw_scores = (
        jnp.einsum("qhgd,khd->hgqk", queries, key_part, preferred_element_type=jnp.float32)
        * score_scale
    )
    return jnp.where(visible[None, None], raw_scores, NEGATIVE)


def keep_same(running):
    return running


def attention_forward(queries, key_rows, value_rows, token_meta, block_rows, score_scale):
    block_count = key_rows.shape[0] // block_rows
    rows_here, heads_kv, groups = (queries.shape[0], queries.shape[1], queries.shape[2])

    def stat_step(block_index, running):
        key_part, value_part, visible = key_block(
            key_rows, value_rows, token_meta, block_index, block_rows
        )

        def stat_update(current):
            row_peak, denom_sum = current
            logits = scores(queries, key_part, visible, score_scale)
            new_peak = jnp.maximum(row_peak, jnp.max(logits, axis=-1))
            denom_sum = denom_sum * jnp.exp(row_peak - new_peak) + jnp.sum(
                jnp.exp(logits - new_peak[..., None]), axis=-1
            )
            return (new_peak, denom_sum)

        return lax.cond(jnp.any(visible), stat_update, keep_same, running)

    start_stats = (
        jnp.full((heads_kv, groups, rows_here), NEGATIVE, jnp.float32),
        jnp.zeros((heads_kv, groups, rows_here), jnp.float32),
    )
    row_peak, denom_sum = lax.fori_loop(0, block_count, stat_step, start_stats)

    def out_step(block_index, partial_sum):
        key_part, value_part, visible = key_block(
            key_rows, value_rows, token_meta, block_index, block_rows
        )

        def out_update(current):
            attn_probs = (
                jnp.exp(scores(queries, key_part, visible, score_scale) - row_peak[..., None])
                / denom_sum[..., None]
            )
            return current + jnp.einsum(
                "hgqk,khd->qhgd",
                attn_probs.astype(jnp.bfloat16),
                value_part,
                preferred_element_type=jnp.float32,
            )

        return lax.cond(jnp.any(visible), out_update, keep_same, partial_sum)

    attended = lax.fori_loop(
        0, block_count, out_step, jnp.zeros((rows_here, heads_kv, groups, HEAD_DIM), jnp.float32)
    )
    return ((row_peak, denom_sum), attended)


def attention_backward(
    queries, key_rows, value_rows, token_meta, softmax_stats, grad_attended, block_rows, score_scale
):
    row_peak, denom_sum = softmax_stats
    block_count = key_rows.shape[0] // block_rows

    def probs_for(key_part, visible):
        return (
            jnp.exp(scores(queries, key_part, visible, score_scale) - row_peak[..., None])
            / denom_sum[..., None]
        )

    def delta_step(block_index, partial_sum):
        key_part, value_part, visible = key_block(
            key_rows, value_rows, token_meta, block_index, block_rows
        )

        def delta_update(current):
            attn_probs = probs_for(key_part, visible)
            grad_probs = jnp.einsum(
                "qhgd,khd->hgqk", grad_attended, value_part, preferred_element_type=jnp.float32
            )
            return current + jnp.sum(attn_probs * grad_probs, axis=-1)

        return lax.cond(jnp.any(visible), delta_update, keep_same, partial_sum)

    delta_sum = lax.fori_loop(0, block_count, delta_step, jnp.zeros(denom_sum.shape, jnp.float32))

    def grad_step(block_index, running):
        key_part, value_part, visible = key_block(
            key_rows, value_rows, token_meta, block_index, block_rows
        )
        first_row = block_index * block_rows

        def grad_update(current):
            grad_queries, grad_keys, grad_values = current
            attn_probs = probs_for(key_part, visible)
            grad_probs = jnp.einsum(
                "qhgd,khd->hgqk", grad_attended, value_part, preferred_element_type=jnp.float32
            )
            grad_scores = (attn_probs * (grad_probs - delta_sum[..., None])).astype(jnp.bfloat16)
            grad_queries = grad_queries + jnp.einsum(
                "hgqk,khd->qhgd", grad_scores, key_part, preferred_element_type=jnp.float32
            )
            key_term = jnp.einsum(
                "hgqk,qhgd->khd", grad_scores, queries, preferred_element_type=jnp.float32
            )
            value_term = jnp.einsum(
                "hgqk,qhgd->khd",
                attn_probs.astype(jnp.bfloat16),
                grad_attended,
                preferred_element_type=jnp.float32,
            )
            grad_keys = lax.dynamic_update_slice_in_dim(
                grad_keys,
                lax.dynamic_slice_in_dim(grad_keys, first_row, block_rows, 0) + key_term,
                first_row,
                0,
            )
            grad_values = lax.dynamic_update_slice_in_dim(
                grad_values,
                lax.dynamic_slice_in_dim(grad_values, first_row, block_rows, 0) + value_term,
                first_row,
                0,
            )
            return (grad_queries, grad_keys, grad_values)

        return lax.cond(jnp.any(visible), grad_update, keep_same, running)

    start_grads = (
        jnp.zeros(queries.shape, jnp.float32),
        jnp.zeros(key_rows.shape, jnp.float32),
        jnp.zeros(value_rows.shape, jnp.float32),
    )
    return lax.fori_loop(0, block_count, grad_step, start_grads)


def fetch_layer(master_set, layer_index):
    (
        query_weight,
        key_weight,
        value_weight,
        out_weight,
        attn_gain,
        moe_gain,
        gate_weight,
        up_weight,
        down_weight,
    ) = master_set
    attn_set = (
        lax.all_gather(
            query_weight[layer_index].astype(jnp.bfloat16), ("ctx", "fsdp"), axis=0, tiled=True
        ),
        lax.all_gather(
            key_weight[layer_index].astype(jnp.bfloat16), ("ctx", "fsdp"), axis=0, tiled=True
        ),
        lax.all_gather(
            value_weight[layer_index].astype(jnp.bfloat16), ("ctx", "fsdp"), axis=0, tiled=True
        ),
        lax.all_gather(
            out_weight[layer_index].astype(jnp.bfloat16), ("ctx", "fsdp"), axis=0, tiled=True
        ),
        lax.all_gather(
            attn_gain[layer_index].astype(jnp.bfloat16), ("ctx", "fsdp"), axis=0, tiled=True
        ),
        lax.all_gather(
            moe_gain[layer_index].astype(jnp.bfloat16), ("ctx", "fsdp"), axis=0, tiled=True
        ),
    )
    row_set = (
        lax.all_gather(split_halves(gate_weight[layer_index]), "fsdp", axis=1, tiled=True),
        lax.all_gather(split_halves(up_weight[layer_index]), "fsdp", axis=1, tiled=True),
        lax.all_gather(split_halves(down_weight[layer_index]), "fsdp", axis=1, tiled=True),
    )
    expert_set = (
        lax.all_to_all(row_set[0], "ctx", split_axis=0, concat_axis=1, tiled=True),
        lax.all_to_all(row_set[1], "ctx", split_axis=0, concat_axis=1, tiled=True),
        lax.all_to_all(row_set[2], "ctx", split_axis=0, concat_axis=1, tiled=True),
    )
    return tuple(attn_set) + tuple(expert_set)


def layer_forward(hidden, weights, route_ids, gate_share, token_meta, places, block_rows):
    (
        query_full,
        key_full,
        value_full,
        out_full,
        attn_norm,
        moe_norm,
        gate_full,
        up_full,
        down_full,
    ) = weights
    rows_here, model_width = hidden.shape
    heads_all = query_full.shape[1] // HEAD_DIM
    heads_kv = key_full.shape[1] // HEAD_DIM
    groups = heads_all // heads_kv
    score_scale = HEAD_DIM ** (-0.5)
    normed = rms_norm(hidden, attn_norm.astype(jnp.float32)).astype(jnp.bfloat16)
    queries = rotate(
        jnp.dot(normed, query_full, preferred_element_type=jnp.float32).reshape(
            rows_here, heads_all, HEAD_DIM
        ),
        places,
    ).astype(jnp.bfloat16)
    key_new = (
        rotate(
            jnp.dot(normed, key_full, preferred_element_type=jnp.float32).reshape(
                rows_here, heads_kv, HEAD_DIM
            ),
            places,
        )
        .astype(jnp.bfloat16)
        .reshape(rows_here, heads_kv * HEAD_DIM)
    )
    value_new = jnp.dot(normed, value_full, preferred_element_type=jnp.float32).astype(jnp.bfloat16)
    key_rows, value_rows = (
        lax.all_gather(key_new, "ctx", axis=0, tiled=True),
        lax.all_gather(value_new, "ctx", axis=0, tiled=True),
    )
    key_rows = key_rows.reshape(-1, heads_kv, HEAD_DIM)
    value_rows = value_rows.reshape(-1, heads_kv, HEAD_DIM)
    queries = queries.reshape(rows_here, heads_kv, groups, HEAD_DIM)
    softmax_stats, attended = attention_forward(
        queries, key_rows, value_rows, token_meta, block_rows, score_scale
    )
    attended = attended.reshape(rows_here, heads_all * HEAD_DIM).astype(jnp.bfloat16)
    middle = hidden + jnp.einsum(
        "tx,dx->td", attended, out_full, preferred_element_type=jnp.float32
    )
    moe_in = rms_norm(middle, moe_norm.astype(jnp.float32)).astype(jnp.bfloat16)
    slot_of, slot_token, slot_share = routing(route_ids, gate_share, rows_here)
    padded = jnp.concatenate([moe_in, jnp.zeros((1, model_width), jnp.bfloat16)], axis=0)
    dispatched = jnp.take(padded, slot_token, axis=0).reshape(EXPERTS, CAP, model_width)
    owner_rows = send_out(doubled(dispatched))
    gate_act = jnp.einsum("ecd,edf->ecf", owner_rows, gate_full, preferred_element_type=jnp.float32)
    up_act = jnp.einsum("ecd,edf->ecf", owner_rows, up_full, preferred_element_type=jnp.float32)
    inner_act = mix_inner(gate_act, up_act).astype(jnp.bfloat16)
    expert_part = jnp.einsum(
        "ecf,edf->ecd", inner_act, down_full, preferred_element_type=jnp.float32
    )
    expert_out = fold_halves(send_back(expert_part))
    expert_out = expert_out.reshape(EXPERTS * CAP, model_width)
    moe_out = jnp.sum(jnp.take(expert_out, slot_of, axis=0) * gate_share[..., None], axis=1)
    record = (
        hidden,
        normed,
        queries,
        key_rows,
        value_rows,
        softmax_stats,
        attended,
        middle,
        moe_in,
        slot_of,
        slot_token,
        slot_share,
        owner_rows,
        gate_act,
        up_act,
        inner_act,
    )
    return (record, middle + moe_out)


def layer_backward(grad_hidden, record, weights, token_meta, places, block_rows):
    (
        hidden,
        normed,
        queries,
        key_rows,
        value_rows,
        softmax_stats,
        attended,
        middle,
        moe_in,
        slot_of,
        slot_token,
        slot_share,
        owner_rows,
        gate_act,
        up_act,
        inner_act,
    ) = record
    (
        query_full,
        key_full,
        value_full,
        out_full,
        attn_norm,
        moe_norm,
        gate_full,
        up_full,
        down_full,
    ) = weights
    rows_here, model_width = hidden.shape
    heads_kv, groups = (queries.shape[1], queries.shape[2])
    group_rows = key_rows.shape[0]
    score_scale = HEAD_DIM ** (-0.5)
    grad_padded = jnp.concatenate([grad_hidden, jnp.zeros((1, model_width), jnp.float32)], axis=0)
    grad_expert = (
        (jnp.take(grad_padded, slot_token, axis=0) * slot_share[:, None])
        .astype(jnp.bfloat16)
        .reshape(EXPERTS, CAP, model_width)
    )
    grad_owner = send_out(doubled(grad_expert))
    grad_down = jnp.einsum(
        "ecd,ecf->edf", grad_owner, inner_act, preferred_element_type=jnp.float32
    )
    grad_inner = jnp.einsum(
        "ecd,edf->ecf", grad_owner, down_full, preferred_element_type=jnp.float32
    )
    grad_gate_act, grad_up_act = jax.vjp(mix_inner, gate_act, up_act)[1](grad_inner)
    grad_gate_act = grad_gate_act.astype(jnp.bfloat16)
    grad_up_act = grad_up_act.astype(jnp.bfloat16)
    grad_gate = jnp.einsum(
        "ecd,ecf->edf", owner_rows, grad_gate_act, preferred_element_type=jnp.float32
    )
    grad_up = jnp.einsum(
        "ecd,ecf->edf", owner_rows, grad_up_act, preferred_element_type=jnp.float32
    )
    grad_owner_rows = jnp.einsum(
        "ecf,edf->ecd", grad_gate_act, gate_full, preferred_element_type=jnp.float32
    ) + jnp.einsum("ecf,edf->ecd", grad_up_act, up_full, preferred_element_type=jnp.float32)
    grad_dispatched = fold_halves(send_back(grad_owner_rows))
    home_set = (
        lax.all_to_all(
            grad_gate.astype(jnp.bfloat16), "ctx", split_axis=1, concat_axis=0, tiled=True
        ).astype(grad_gate.dtype),
        lax.all_to_all(
            grad_up.astype(jnp.bfloat16), "ctx", split_axis=1, concat_axis=0, tiled=True
        ).astype(grad_up.dtype),
        lax.all_to_all(
            grad_down.astype(jnp.bfloat16), "ctx", split_axis=1, concat_axis=0, tiled=True
        ).astype(grad_down.dtype),
    )
    summed_set = (
        lax.psum_scatter(
            home_set[0].astype(jnp.bfloat16), "fsdp", scatter_dimension=1, tiled=True
        ).astype(jnp.float32),
        lax.psum_scatter(
            home_set[1].astype(jnp.bfloat16), "fsdp", scatter_dimension=1, tiled=True
        ).astype(jnp.float32),
        lax.psum_scatter(
            home_set[2].astype(jnp.bfloat16), "fsdp", scatter_dimension=1, tiled=True
        ).astype(jnp.float32),
    )
    expert_grads = (
        merge_halves(summed_set[0]),
        merge_halves(summed_set[1]),
        merge_halves(summed_set[2]),
    )
    grad_moe_in = jnp.sum(
        jnp.take(grad_dispatched.reshape(EXPERTS * CAP, model_width), slot_of, axis=0), axis=1
    )
    grad_middle_part, grad_moe_norm = jax.vjp(rms_norm, middle, moe_norm.astype(jnp.float32))[1](
        grad_moe_in
    )
    grad_middle = grad_hidden + grad_middle_part
    grad_rounded = grad_middle.astype(jnp.bfloat16)
    grad_out_full = jnp.einsum(
        "td,tx->dx", grad_rounded, attended, preferred_element_type=jnp.float32
    )
    grad_attended = (
        jnp.dot(grad_rounded, out_full, preferred_element_type=jnp.float32)
        .astype(jnp.bfloat16)
        .reshape(rows_here, heads_kv, groups, HEAD_DIM)
    )
    grad_queries, grad_keys, grad_values = attention_backward(
        queries,
        key_rows,
        value_rows,
        token_meta,
        softmax_stats,
        grad_attended,
        block_rows,
        score_scale,
    )
    key_sums, value_sums = (
        lax.psum_scatter(
            grad_keys.reshape(group_rows, heads_kv * HEAD_DIM).astype(jnp.bfloat16),
            "ctx",
            scatter_dimension=0,
            tiled=True,
        ).astype(jnp.float32),
        lax.psum_scatter(
            grad_values.reshape(group_rows, heads_kv * HEAD_DIM).astype(jnp.bfloat16),
            "ctx",
            scatter_dimension=0,
            tiled=True,
        ).astype(jnp.float32),
    )
    grad_query_rows = (
        rotate_back(
            grad_queries.reshape(rows_here, heads_kv * groups, HEAD_DIM) * score_scale, places
        )
        .astype(jnp.bfloat16)
        .reshape(rows_here, heads_kv * groups * HEAD_DIM)
    )
    grad_key_rows = (
        rotate_back(key_sums.reshape(rows_here, heads_kv, HEAD_DIM) * score_scale, places)
        .astype(jnp.bfloat16)
        .reshape(rows_here, heads_kv * HEAD_DIM)
    )
    grad_value_rows = value_sums.astype(jnp.bfloat16)
    grad_query_full = jnp.einsum(
        "td,tx->dx", normed, grad_query_rows, preferred_element_type=jnp.float32
    )
    grad_key_full = jnp.einsum(
        "td,tx->dx", normed, grad_key_rows, preferred_element_type=jnp.float32
    )
    grad_value_full = jnp.einsum(
        "td,tx->dx", normed, grad_value_rows, preferred_element_type=jnp.float32
    )
    grad_normed = jnp.einsum(
        "tx,dx->td", grad_query_rows, query_full, preferred_element_type=jnp.float32
    )
    grad_normed = grad_normed + jnp.einsum(
        "tx,dx->td", grad_key_rows, key_full, preferred_element_type=jnp.float32
    )
    grad_normed = grad_normed + jnp.einsum(
        "tx,dx->td", grad_value_rows, value_full, preferred_element_type=jnp.float32
    )
    grad_hidden_part, grad_attn_norm = jax.vjp(rms_norm, hidden, attn_norm.astype(jnp.float32))[1](
        grad_normed
    )
    attn_grads = (
        lax.psum_scatter(grad_query_full, ("ctx", "fsdp"), scatter_dimension=0, tiled=True),
        lax.psum_scatter(grad_key_full, ("ctx", "fsdp"), scatter_dimension=0, tiled=True),
        lax.psum_scatter(grad_value_full, ("ctx", "fsdp"), scatter_dimension=0, tiled=True),
        lax.psum_scatter(grad_out_full, ("ctx", "fsdp"), scatter_dimension=0, tiled=True),
        lax.psum_scatter(grad_attn_norm, ("ctx", "fsdp"), scatter_dimension=0, tiled=True),
        lax.psum_scatter(grad_moe_norm, ("ctx", "fsdp"), scatter_dimension=0, tiled=True),
    )
    return (grad_middle + grad_hidden_part, attn_grads, expert_grads)


def body(
    tokens,
    cotangent,
    lengths,
    tile_order,
    routes,
    gates,
    query_weight,
    key_weight,
    value_weight,
    out_weight,
    attn_gain,
    moe_gain,
    gate_weight,
    up_weight,
    down_weight,
):
    rows_here = tokens.shape[1]
    group_rows = rows_here * lax.axis_size("ctx")
    seg_all, pos_all = layout(lengths[0], tile_order[0], group_rows)
    first_row = lax.axis_index("ctx") * rows_here
    seg_local = lax.dynamic_slice_in_dim(seg_all, first_row, rows_here, 0)
    pos_local = lax.dynamic_slice_in_dim(pos_all, first_row, rows_here, 0)
    token_meta = (seg_local, pos_local, seg_all, pos_all)
    places = pos_local.astype(jnp.float32)
    block_rows = math.gcd(group_rows, 512)
    master_set = (
        query_weight,
        key_weight,
        value_weight,
        out_weight,
        attn_gain,
        moe_gain,
        gate_weight,
        up_weight,
        down_weight,
    )
    hidden = tokens[0].astype(jnp.float32)
    records = []
    for layer_index in range(LAYERS):
        weights = fetch_layer(master_set, layer_index)
        record, hidden = layer_forward(
            hidden,
            weights,
            routes[layer_index, 0],
            gates[layer_index, 0],
            token_meta,
            places,
            block_rows,
        )
        records.append(record)
    grad_hidden = cotangent[0].astype(jnp.float32)
    attn_layers = []
    expert_layers = []
    for layer_index in reversed(range(LAYERS)):
        weights = fetch_layer(master_set, layer_index)
        grad_hidden, attn_grads, expert_grads = layer_backward(
            grad_hidden, records[layer_index], weights, token_meta, places, block_rows
        )
        attn_layers.insert(0, attn_grads)
        expert_layers.insert(0, expert_grads)
    grad_query_weight = jnp.stack([layer_grads[0] for layer_grads in attn_layers])
    grad_key_weight = jnp.stack([layer_grads[1] for layer_grads in attn_layers])
    grad_value_weight = jnp.stack([layer_grads[2] for layer_grads in attn_layers])
    grad_out_weight = jnp.stack([layer_grads[3] for layer_grads in attn_layers])
    grad_attn_gain = jnp.stack([layer_grads[4] for layer_grads in attn_layers])
    grad_moe_gain = jnp.stack([layer_grads[5] for layer_grads in attn_layers])
    grad_gate_weight = jnp.stack([layer_grads[0] for layer_grads in expert_layers])
    grad_up_weight = jnp.stack([layer_grads[1] for layer_grads in expert_layers])
    grad_down_weight = jnp.stack([layer_grads[2] for layer_grads in expert_layers])
    return (
        hidden.astype(jnp.bfloat16)[None],
        grad_hidden[None],
        grad_query_weight,
        grad_key_weight,
        grad_value_weight,
        grad_out_weight,
        grad_attn_gain,
        grad_moe_gain,
        grad_gate_weight,
        grad_up_weight,
        grad_down_weight,
    )


BF = jnp.bfloat16
F32 = jnp.float32
NX = 2
NCORE = 2


def at_device(ctx, fsdp):
    return {"ctx": ctx, "fsdp": fsdp}


def remote(src, dst, send_sem, recv_sem, ctx, fsdp):
    return pltpu.make_async_remote_copy(
        src_ref=src, dst_ref=dst, send_sem=send_sem, recv_sem=recv_sem,
        device_id={"ctx": ctx, "fsdp": fsdp}, device_id_type=pl.DeviceIdType.MESH,
    )


def greet_line(nz, z, x, fsdp):
    barrier = pltpu.get_barrier_semaphore()
    pl.semaphore_signal(barrier, inc=1, device_id={"ctx": z * NX + 1 - x, "fsdp": fsdp}, device_id_type=pl.DeviceIdType.MESH)

    @pl.when(z > 0)
    def _():
        pl.semaphore_signal(barrier, inc=1, device_id={"ctx": (z - 1) * NX + x, "fsdp": fsdp}, device_id_type=pl.DeviceIdType.MESH)

    @pl.when(z < nz - 1)
    def _():
        pl.semaphore_signal(barrier, inc=1, device_id={"ctx": (z + 1) * NX + x, "fsdp": fsdp}, device_id_type=pl.DeviceIdType.MESH)

    pl.semaphore_wait(barrier, 1 + jnp.where(z > 0, 1, 0) + jnp.where(z < nz - 1, 1, 0))


def gather_kernel(nz, x_ref, o_ref, own_sem, up_send, up_recv, down_send, down_recv, x_send, x_recv):
    ctx, fsdp = lax.axis_index("ctx"), lax.axis_index("fsdp")
    z, x = ctx // NX, ctx % NX
    greet_line(nz, z, x, fsdp)
    other = 1 - x

    def up(t):
        src = x_ref if t == 0 else o_ref.at[(z - t) * NX + x]
        return remote(src, o_ref.at[(z - t) * NX + x], up_send.at[t], up_recv.at[t], (z + 1) * NX + x, fsdp)

    def down(t):
        src = x_ref if t == 0 else o_ref.at[(z + t) * NX + x]
        return remote(src, o_ref.at[(z + t) * NX + x], down_send.at[t], down_recv.at[t], (z - 1) * NX + x, fsdp)

    def up_in(t):
        return remote(x_ref, o_ref.at[(z - 1 - t) * NX + x], up_send.at[t], up_recv.at[t], (z + 1) * NX + x, fsdp)

    def down_in(t):
        return remote(x_ref, o_ref.at[(z + 1 + t) * NX + x], down_send.at[t], down_recv.at[t], (z - 1) * NX + x, fsdp)

    def across(row, src=None):
        return remote(o_ref.at[row * NX + x] if src is None else src, o_ref.at[row * NX + x], x_send.at[row], x_recv.at[row], z * NX + other, fsdp)

    def across_in(row):
        return remote(x_ref, o_ref.at[row * NX + other], x_send.at[row], x_recv.at[row], z * NX + other, fsdp)

    own = pltpu.make_async_copy(x_ref, o_ref.at[ctx], own_sem)

    @pl.when(z < nz - 1)
    def _():
        up(0).start()

    @pl.when(z > 0)
    def _():
        down(0).start()

    across(z, x_ref).start()
    own.start()
    for t in range(nz - 1):
        @pl.when(z - 1 - t >= 0)
        def _():
            up_in(t).wait_recv()

            @pl.when(z < nz - 1)
            def _():
                up(t + 1).start()

            across(z - 1 - t).start()

        @pl.when(z + 1 + t < nz)
        def _():
            down_in(t).wait_recv()

            @pl.when(z > 0)
            def _():
                down(t + 1).start()

            across(z + 1 + t).start()

    own.wait()
    for t in range(nz - 1):
        @pl.when((z - t >= 0) & (z < nz - 1))
        def _():
            up(t).wait_send()

        @pl.when((z + t < nz) & (z > 0))
        def _():
            down(t).wait_send()

    for row in range(nz):
        across(row).wait_send()
        across_in(row).wait_recv()


def gather_rows(block, nz):
    rows, width = block.shape
    return pl.pallas_call(
        functools.partial(gather_kernel, nz),
        out_shape=jax.ShapeDtypeStruct((nz * NX, rows, width), block.dtype),
        in_specs=[pl.BlockSpec(memory_space=pltpu.VMEM)],
        out_specs=pl.BlockSpec(memory_space=pl.ANY),
        scratch_shapes=[
            pltpu.SemaphoreType.DMA,
            pltpu.SemaphoreType.DMA((nz,)),
            pltpu.SemaphoreType.DMA((nz,)),
            pltpu.SemaphoreType.DMA((nz,)),
            pltpu.SemaphoreType.DMA((nz,)),
            pltpu.SemaphoreType.DMA((nz,)),
            pltpu.SemaphoreType.DMA((nz,)),
        ],
        compiler_params=pltpu.CompilerParams(collective_id=1, has_side_effects=True),
        name="gather_rows",
    )(block)


def scatter_kernel(nz, p_ref, o_ref, xin, acc, up_in, down_in, x_send, x_recv, up_send, up_recv, down_send, down_recv):
    ctx, fsdp = lax.axis_index("ctx"), lax.axis_index("fsdp")
    z, x = ctx // NX, ctx % NX
    greet_line(nz, z, x, fsdp)
    other = 1 - x

    def across(row):
        return remote(p_ref.at[row * NX + other], xin.at[row], x_send.at[row], x_recv.at[row], z * NX + other, fsdp)

    def up(row):
        return remote(acc.at[row], up_in.at[row], up_send.at[row], up_recv.at[row], (z + 1) * NX + x, fsdp)

    def down(row):
        return remote(acc.at[row], down_in.at[row], down_send.at[row], down_recv.at[row], (z - 1) * NX + x, fsdp)

    far_up = [nz - 1 - i for i in range(nz)]

    def order(i):
        low = jnp.where(z == 0, nz - 1 - i, jnp.where(z == nz - 1, i, 0))
        if nz == 4:
            mid1 = (3, 0, 2, 1)[i]
            mid2 = (0, 3, 1, 2)[i]
            return jnp.where((z == 0) | (z == 3), low, jnp.where(z == 1, mid1, mid2))
        return low

    for i in range(nz):
        across(order(i)).start()
    for i in range(nz):
        row = order(i)
        across(row).wait_recv()
        mine = p_ref[row * NX + x].astype(F32) + xin[row].astype(F32)

        @pl.when(row > z)
        def _():
            @pl.when(z == 0)
            def _():
                acc[row] = mine.astype(BF)

            @pl.when(z > 0)
            def _():
                up(row).wait_recv()
                acc[row] = (mine + up_in[row].astype(F32)).astype(BF)

            up(row).start()

        @pl.when(row < z)
        def _():
            @pl.when(z == nz - 1)
            def _():
                acc[row] = mine.astype(BF)

            @pl.when(z < nz - 1)
            def _():
                down(row).wait_recv()
                acc[row] = (mine + down_in[row].astype(F32)).astype(BF)

            down(row).start()

        @pl.when(row == z)
        def _():
            o_ref[...] = mine

    @pl.when(z > 0)
    def _():
        up(z).wait_recv()
        o_ref[...] += up_in[z].astype(F32)

    @pl.when(z < nz - 1)
    def _():
        down(z).wait_recv()
        o_ref[...] += down_in[z].astype(F32)

    for row in range(nz):
        across(row).wait_send()

        @pl.when(row > z)
        def _():
            up(row).wait_send()

        @pl.when(row < z)
        def _():
            down(row).wait_send()


def scatter_rows(parts, nz):
    _, rows, width = parts.shape
    return pl.pallas_call(
        functools.partial(scatter_kernel, nz),
        out_shape=jax.ShapeDtypeStruct((rows, width), F32),
        in_specs=[pl.BlockSpec(memory_space=pltpu.VMEM)],
        out_specs=pl.BlockSpec(memory_space=pltpu.VMEM),
        scratch_shapes=[
            pltpu.VMEM((nz, rows, width), BF),
            pltpu.VMEM((nz, rows, width), BF),
            pltpu.VMEM((nz, rows, width), BF),
            pltpu.VMEM((nz, rows, width), BF),
            pltpu.SemaphoreType.DMA((nz,)),
            pltpu.SemaphoreType.DMA((nz,)),
            pltpu.SemaphoreType.DMA((nz,)),
            pltpu.SemaphoreType.DMA((nz,)),
            pltpu.SemaphoreType.DMA((nz,)),
            pltpu.SemaphoreType.DMA((nz,)),
        ],
        compiler_params=pltpu.CompilerParams(collective_id=2, has_side_effects=True, vmem_limit_bytes=60 << 20),
        name="scatter_rows",
    )(parts)


def weights_kernel(nctx, nfs, rows, w_ref, g_ref, o_ref, go_ref, own_sem, p_send, p_recv, y_send, y_recv, c_send, c_recv,
                   gown_sem, gp_send, gp_recv, gy_send, gy_recv, gc_send, gc_recv):
    ctx, fsdp = lax.axis_index("ctx"), lax.axis_index("fsdp")
    y, core = fsdp // NCORE, fsdp % NCORE
    y_mate = (1 - y) * NCORE + core
    c_mate = y * NCORE + 1 - core
    barrier = pltpu.get_barrier_semaphore()
    for step in range(1, nctx):
        pl.semaphore_signal(barrier, inc=1, device_id={"ctx": (ctx + step) % nctx, "fsdp": fsdp}, device_id_type=pl.DeviceIdType.MESH)
    for mate in (y_mate, c_mate):
        pl.semaphore_signal(barrier, inc=1, device_id={"ctx": ctx, "fsdp": mate}, device_id_type=pl.DeviceIdType.MESH)
    pl.semaphore_wait(barrier, nctx + 1)

    def place(s, f):
        return o_ref.at[:, pl.ds(pl.multiple_of((s * nfs + f) * rows, rows), rows), :]

    def gplace(s, f):
        return go_ref.at[s * nfs + f]

    def direct(step):
        to = (ctx + step) % nctx
        return (remote(w_ref.at[to], place(ctx, fsdp), p_send.at[step], p_recv.at[step], to, fsdp),
                remote(g_ref, gplace(ctx, fsdp), gp_send.at[step], gp_recv.at[step], to, fsdp))

    def direct_in(step):
        frm = (ctx + nctx - step) % nctx
        return (remote(w_ref.at[ctx], place(frm, fsdp), p_send.at[step], p_recv.at[step], frm, fsdp),
                remote(g_ref, gplace(frm, fsdp), gp_send.at[step], gp_recv.at[step], frm, fsdp))

    def to_y(step, own=False):
        frm = (ctx + nctx - step) % nctx
        return (remote(w_ref.at[ctx] if own else place(frm, fsdp), place(frm, fsdp), y_send.at[step], y_recv.at[step], ctx, y_mate),
                remote(g_ref if own else gplace(frm, fsdp), gplace(frm, fsdp), gy_send.at[step], gy_recv.at[step], ctx, y_mate))

    def from_y(step):
        frm = (ctx + nctx - step) % nctx
        return (remote(w_ref.at[ctx], place(frm, y_mate), y_send.at[step], y_recv.at[step], ctx, y_mate),
                remote(g_ref, gplace(frm, y_mate), gy_send.at[step], gy_recv.at[step], ctx, y_mate))

    def to_c(step, f, k, own=False):
        frm = (ctx + nctx - step) % nctx
        return (remote(w_ref.at[ctx] if own else place(frm, f), place(frm, f), c_send.at[k, step], c_recv.at[k, step], ctx, c_mate),
                remote(g_ref if own else gplace(frm, f), gplace(frm, f), gc_send.at[k, step], gc_recv.at[k, step], ctx, c_mate))

    def from_c(step, k):
        frm = (ctx + nctx - step) % nctx
        f = (c_mate, (1 - y) * NCORE + 1 - core)[k]
        return (remote(w_ref.at[ctx], place(frm, f), c_send.at[k, step], c_recv.at[k, step], ctx, c_mate),
                remote(g_ref, gplace(frm, f), gc_send.at[k, step], gc_recv.at[k, step], ctx, c_mate))

    def start(pair):
        for copy in pair:
            copy.start()

    own = (pltpu.make_async_copy(w_ref.at[ctx], place(ctx, fsdp), own_sem),
           pltpu.make_async_copy(g_ref, gplace(ctx, fsdp), gown_sem))
    for step in range(1, nctx):
        start(direct(step))
    start(to_y(0, own=True))
    start(to_c(0, fsdp, 0, own=True))
    start(own)
    for step in range(1, nctx):
        for copy in direct_in(step):
            copy.wait_recv()
        start(to_y(step))
        start(to_c(step, fsdp, 0))
    for step in range(nctx):
        for copy in from_y(step):
            copy.wait_recv()
        start(to_c(step, y_mate, 1))
    for copy in own:
        copy.wait()
    for step in range(nctx):
        for k in range(2):
            for copy in from_c(step, k):
                copy.wait_recv()
            for copy in to_c(step, fsdp, k):
                copy.wait_send()
        for copy in to_y(step):
            copy.wait_send()
        if step:
            for copy in direct(step):
                copy.wait_send()


def spread_weights(send, gains, nfs):
    nctx, mats, rows, width = send.shape
    return pl.pallas_call(
        functools.partial(weights_kernel, nctx, nfs, rows),
        out_shape=(jax.ShapeDtypeStruct((mats, nctx * nfs * rows, width), send.dtype),
                   jax.ShapeDtypeStruct((nctx * nfs,) + gains.shape, gains.dtype)),
        in_specs=[pl.BlockSpec(memory_space=pltpu.VMEM), pl.BlockSpec(memory_space=pltpu.VMEM)],
        out_specs=(pl.BlockSpec(memory_space=pl.ANY), pl.BlockSpec(memory_space=pl.ANY)),
        scratch_shapes=[
            pltpu.SemaphoreType.DMA,
            pltpu.SemaphoreType.DMA((nctx,)), pltpu.SemaphoreType.DMA((nctx,)),
            pltpu.SemaphoreType.DMA((nctx,)), pltpu.SemaphoreType.DMA((nctx,)),
            pltpu.SemaphoreType.DMA((2, nctx)), pltpu.SemaphoreType.DMA((2, nctx)),
        ] * 2,
        compiler_params=pltpu.CompilerParams(collective_id=3, has_side_effects=True, vmem_limit_bytes=40 << 20),
        name="spread_weights",
    )(send, gains)


def grads_kernel(nctx, nfs, rows, g_ref, e_ref, o_ref, eo_ref, cin, yin, half, full, e_cin, e_half, e_yin, e_full,
                 own_sem, c_send, c_recv, y_send, y_recv, p_send, p_recv, eown_sem, ec_sem, ey_sem, ep_send, ep_recv):
    ctx, fsdp = lax.axis_index("ctx"), lax.axis_index("fsdp")
    y, core = fsdp // NCORE, fsdp % NCORE
    y_mate = (1 - y) * NCORE + core
    c_mate = y * NCORE + 1 - core
    mats = g_ref.shape[0]
    barrier = pltpu.get_barrier_semaphore()
    for step in range(1, nctx):
        pl.semaphore_signal(barrier, inc=1, device_id={"ctx": (ctx + step) % nctx, "fsdp": fsdp}, device_id_type=pl.DeviceIdType.MESH)
    for mate in (y_mate, c_mate):
        pl.semaphore_signal(barrier, inc=1, device_id={"ctx": ctx, "fsdp": mate}, device_id_type=pl.DeviceIdType.MESH)
    pl.semaphore_wait(barrier, nctx + 1)

    def span(s, f):
        return pl.ds(pl.multiple_of((s * nfs + f) * rows, rows), rows)

    def to_c(step, k):
        s = (ctx + step) % nctx
        f = (1 - y if k == 0 else y) * NCORE + 1 - core
        return remote(g_ref.at[:, span(s, f), :], cin.at[k, step], c_send.at[k, step], c_recv.at[k, step], ctx, c_mate)

    def to_y(step):
        return remote(half.at[step], yin.at[step], y_send.at[step], y_recv.at[step], ctx, y_mate)

    def out(step):
        s = (ctx + step) % nctx
        return remote(full.at[step], o_ref.at[ctx], p_send.at[step], p_recv.at[step], s, fsdp)

    def out_in(step):
        s = (ctx + nctx - step) % nctx
        return remote(full.at[step], o_ref.at[s], p_send.at[step], p_recv.at[step], s, fsdp)

    e_to_c = remote(e_ref.at[1 - core], e_cin, ec_sem.at[0], ec_sem.at[1], ctx, c_mate)
    e_to_y = remote(e_half.at[1 - y], e_yin, ey_sem.at[0], ey_sem.at[1], ctx, y_mate)

    def e_out(step):
        s = (ctx + step) % nctx
        return remote(e_full.at[s], eo_ref.at[ctx], ep_send.at[step], ep_recv.at[step], s, fsdp)

    def e_out_in(step):
        s = (ctx + nctx - step) % nctx
        return remote(e_full.at[s], eo_ref.at[s], ep_send.at[step], ep_recv.at[step], s, fsdp)

    e_to_c.start()
    for step in range(nctx):
        to_c((step + 1) % nctx, 0).start()
    for step in range(nctx):
        to_c((step + 1) % nctx, 1).start()
    e_to_c.wait_recv()
    e_half[...] = e_ref[core] + e_cin[...]
    e_to_y.start()
    e_own = pltpu.make_async_copy(e_full.at[ctx], eo_ref.at[ctx], eown_sem)
    own = pltpu.make_async_copy(full.at[0], o_ref.at[ctx], own_sem)

    def first(i, _):
        step = (i + 1) % nctx
        s = (ctx + step) % nctx
        to_c(step, 0).wait_recv()

        def one(m, _):
            half[step, m] = (g_ref[m, span(s, y_mate), :].astype(F32) + cin[0, step, m].astype(F32)).astype(BF)
            return 0

        lax.fori_loop(0, mats, one, 0)
        to_y(step).start()
        return 0

    lax.fori_loop(0, nctx, first, 0)
    e_to_y.wait_recv()
    e_full[...] = e_half[y] + e_yin[...]
    e_own.start()
    for step in range(1, nctx):
        e_out(step).start()

    def second(i, _):
        step = (i + 1) % nctx
        s = (ctx + step) % nctx
        to_c(step, 1).wait_recv()
        to_y(step).wait_recv()

        def one(m, _):
            full[step, m] = (g_ref[m, span(s, fsdp), :].astype(F32) + cin[1, step, m].astype(F32) + yin[step, m].astype(F32)).astype(BF)
            return 0

        lax.fori_loop(0, mats, one, 0)

        @pl.when(step > 0)
        def _():
            out(step).start()

        return 0

    lax.fori_loop(0, nctx, second, 0)
    own.start()
    for step in range(nctx):
        for k in range(2):
            to_c(step, k).wait_send()
        to_y(step).wait_send()
        if step:
            out(step).wait_send()
            out_in(step).wait_recv()
            e_out(step).wait_send()
            e_out_in(step).wait_recv()
    e_to_c.wait_send()
    e_to_y.wait_send()
    e_own.wait()
    own.wait()


def collect_grads(grads, extra, nctx, nfs):
    mats, total, width = grads.shape
    rows = total // (nctx * nfs)
    blk = (mats, rows, width)
    return pl.pallas_call(
        functools.partial(grads_kernel, nctx, nfs, rows),
        out_shape=(jax.ShapeDtypeStruct((nctx,) + blk, BF), jax.ShapeDtypeStruct((nctx, 8, 128), F32)),
        in_specs=[pl.BlockSpec(memory_space=pltpu.VMEM), pl.BlockSpec(memory_space=pltpu.VMEM)],
        out_specs=(pl.BlockSpec(memory_space=pl.ANY), pl.BlockSpec(memory_space=pl.ANY)),
        scratch_shapes=[
            pltpu.VMEM((2, nctx) + blk, BF),
            pltpu.VMEM((nctx,) + blk, BF),
            pltpu.VMEM((nctx,) + blk, BF),
            pltpu.VMEM((nctx,) + blk, BF),
            pltpu.VMEM((2, nctx, 8, 128), F32),
            pltpu.VMEM((2, nctx, 8, 128), F32),
            pltpu.VMEM((nctx, 8, 128), F32),
            pltpu.VMEM((nctx, 8, 128), F32),
            pltpu.SemaphoreType.DMA,
            pltpu.SemaphoreType.DMA((2, nctx)), pltpu.SemaphoreType.DMA((2, nctx)),
            pltpu.SemaphoreType.DMA((nctx,)), pltpu.SemaphoreType.DMA((nctx,)),
            pltpu.SemaphoreType.DMA((nctx,)), pltpu.SemaphoreType.DMA((nctx,)),
            pltpu.SemaphoreType.DMA,
            pltpu.SemaphoreType.DMA((2,)), pltpu.SemaphoreType.DMA((2,)),
            pltpu.SemaphoreType.DMA((nctx,)), pltpu.SemaphoreType.DMA((nctx,)),
        ],
        compiler_params=pltpu.CompilerParams(collective_id=4, has_side_effects=True, vmem_limit_bytes=60 << 20),
        name="collect_grads",
    )(grads, extra)


def rope_tables(places):
    half_dim = HEAD_DIM // 2
    freq_steps = jnp.arange(half_dim, dtype=jnp.float32)
    inverse = jnp.exp(freq_steps * (-2.0 * math.log(10000.0) / HEAD_DIM))
    angles = places[:, None] * inverse[None, :]
    return jnp.cos(angles), jnp.sin(angles)


def turn(values, cos_part, sin_part):
    half_dim = HEAD_DIM // 2
    first_half = values[..., :half_dim]
    second_half = values[..., half_dim:]
    cos_part, sin_part = cos_part[:, None, :], sin_part[:, None, :]
    return jnp.concatenate(
        [first_half * cos_part - second_half * sin_part, second_half * cos_part + first_half * sin_part],
        axis=-1,
    )


def dot(left, right, dims):
    return lax.dot_general(left, right, (dims, ((), ())), preferred_element_type=jnp.float32)


NN = ((1,), (0,))
NT = ((1,), (1,))
TN = ((0,), (0,))


def pack_weights(master_set, layer, nctx):
    query_weight, key_weight, value_weight, out_weight, attn_gain, moe_gain, gate_weight, up_weight, down_weight = master_set
    rows = query_weight.shape[1]

    def columns(master):
        low = master[layer].astype(BF).reshape(rows, nctx, -1)
        return low.transpose(1, 0, 2)

    attn = jnp.concatenate(
        [columns(query_weight), columns(key_weight), columns(value_weight), columns(out_weight)], axis=-1
    )

    def experts(master):
        low = master[layer].astype(BF)
        return low.reshape(nctx, -1, rows, low.shape[-1])

    send = jnp.concatenate(
        [attn[:, None], experts(gate_weight), experts(up_weight), experts(down_weight)], axis=1
    )
    gains = jnp.stack([attn_gain[layer], moe_gain[layer]]).astype(BF).astype(F32)
    gains = jnp.pad(gains, ((0, 6), (0, 128 - rows)))
    return send, gains


def norm_back(values, gain, grad):
    scale = lax.rsqrt(jnp.mean(values * values, axis=-1, keepdims=True) + EPSILON)
    unit = values * scale
    grad_gain = jnp.sum(grad * unit, axis=0)
    pulled = grad * gain
    return scale * (pulled - unit * jnp.mean(pulled * unit, axis=-1, keepdims=True)), grad_gain


def fast_body(nctx, nfs, *args):
    (tokens, cotangent, lengths, tile_order, routes, gates), master_set = args[:6], args[6:]
    nz = nctx // NX
    rows_here, model_width = tokens.shape[1], tokens.shape[2]
    group_rows = rows_here * nctx
    ctx = lax.axis_index("ctx")
    seg_all, pos_all = layout(lengths[0], tile_order[0], group_rows)
    visible = (seg_all[:, None] == seg_all[None, :]) & (pos_all[None, :] <= pos_all[:, None])
    cos_part, sin_part = rope_tables(pos_all.astype(jnp.float32))
    score_scale = HEAD_DIM ** (-0.5)
    q_width = 3 * HEAD_DIM
    kv_at, v_at, o_at = q_width, q_width + HEAD_DIM, q_width + 2 * HEAD_DIM

    expert_ids = jnp.arange(EXPERTS, dtype=jnp.int32)
    table = jnp.sum(
        jnp.where(routes[:, 0, :, :, None] == expert_ids, gates[:, 0, :, :, None], 0.0), axis=-2
    )
    table_all = lax.all_gather(
        table.transpose(1, 0, 2).reshape(rows_here, LAYERS * EXPERTS), "ctx", axis=0, tiled=True
    ).reshape(group_rows, LAYERS, EXPERTS // 2, 2)
    table_mine = lax.dynamic_index_in_dim(table_all, ctx, 2, keepdims=False)

    fetched = []
    for layer in range(LAYERS):
        send, gains = pack_weights(master_set, layer, nctx)
        mats, gain_all = spread_weights(send, gains, nfs)
        rows = send.shape[2]
        fetched.append((mats, gain_all[:, 0, :rows].reshape(-1), gain_all[:, 1, :rows].reshape(-1)))

    hidden = tokens[0].astype(jnp.float32)
    records = []
    for layer in range(LAYERS):
        mats, attn_gain, moe_gain = fetched[layer]
        attn = mats[0]
        normed = rms_norm(hidden, attn_gain).astype(BF)
        normed_all = gather_rows(normed, nz).reshape(group_rows, model_width)
        proj = dot(normed_all, attn[:, :o_at], NN)
        turned = turn(proj[:, :v_at].reshape(group_rows, 4, HEAD_DIM), cos_part, sin_part).astype(BF)
        queries, keys = turned[:, :3], turned[:, 3]
        values = proj[:, v_at:].astype(BF)
        raw = jnp.einsum("qhd,kd->hqk", queries, keys, preferred_element_type=jnp.float32) * score_scale
        raw = jnp.where(visible[None], raw, NEGATIVE)
        peak = jnp.max(raw, axis=-1, keepdims=True)
        powers = jnp.exp(raw - peak)
        probs = powers / jnp.sum(powers, axis=-1, keepdims=True)
        attended = jnp.einsum("hqk,kd->qhd", probs.astype(BF), values, preferred_element_type=jnp.float32)
        attended = attended.reshape(group_rows, q_width).astype(BF)
        part = dot(attended, attn[:, o_at:], NT).astype(BF)
        middle = hidden + scatter_rows(part.reshape(nctx, rows_here, model_width), nz)

        moe_in = rms_norm(middle, moe_gain).astype(BF)
        moe_all = gather_rows(moe_in, nz).reshape(group_rows, model_width)
        acts = []
        total = 0.0
        for e in range(2):
            gate_act = dot(moe_all, mats[1 + e], NN)
            up_act = dot(moe_all, mats[3 + e], NN)
            inner = (table_mine[:, layer, e][:, None] * (jax.nn.silu(gate_act) * up_act)).astype(BF)
            acts.append((gate_act, up_act, inner))
            total = total + dot(inner, mats[5 + e], NT)
        moved = scatter_rows(total.astype(BF).reshape(nctx, rows_here, model_width), nz)
        records.append((hidden, normed_all, queries, keys, values, probs, attended, middle, moe_all, acts))
        hidden = middle + moved

    output = hidden.astype(BF)
    grad = cotangent[0].astype(jnp.float32)
    collected = [None] * LAYERS
    for layer in reversed(range(LAYERS)):
        mats, attn_gain, moe_gain = fetched[layer]
        attn = mats[0]
        hidden, normed_all, queries, keys, values, probs, attended, middle, moe_all, acts = records[layer]
        grad_all = gather_rows(grad.astype(BF), nz).reshape(group_rows, model_width)
        grad_gate, grad_up, grad_down = [], [], []
        total = 0.0
        for e in range(2):
            gate_act, up_act, inner = acts[e]
            grad_down.append(dot(grad_all, inner, TN).astype(BF))
            grad_inner = table_mine[:, layer, e][:, None] * dot(grad_all, mats[5 + e], NN)
            sigmoid = jax.nn.sigmoid(gate_act)
            d_gate = (grad_inner * up_act * sigmoid * (1.0 + gate_act * (1.0 - sigmoid))).astype(BF)
            d_up = (grad_inner * gate_act * sigmoid).astype(BF)
            grad_gate.append(dot(moe_all, d_gate, TN).astype(BF))
            grad_up.append(dot(moe_all, d_up, TN).astype(BF))
            total = total + dot(d_gate, mats[1 + e], NT) + dot(d_up, mats[3 + e], NT)
        grad_moe_in = scatter_rows(total.astype(BF).reshape(nctx, rows_here, model_width), nz)
        through, grad_moe_gain = norm_back(middle, moe_gain, grad_moe_in)
        grad_middle = grad + through

        middle_all = gather_rows(grad_middle.astype(BF), nz).reshape(group_rows, model_width)
        grad_out = dot(middle_all, attended, TN).astype(BF)
        grad_att = dot(middle_all, attn[:, o_at:], NN).astype(BF).reshape(group_rows, 3, HEAD_DIM)
        dp = jnp.einsum("qhd,kd->hqk", grad_att, values, preferred_element_type=jnp.float32)
        delta = jnp.sum(probs * dp, axis=-1, keepdims=True)
        d_scores = (probs * (dp - delta)).astype(BF)
        dq = jnp.einsum("hqk,kd->qhd", d_scores, keys, preferred_element_type=jnp.float32) * score_scale
        dk = jnp.einsum("hqk,qhd->kd", d_scores, queries, preferred_element_type=jnp.float32) * score_scale
        dv = jnp.einsum("hqk,qhd->kd", probs.astype(BF), grad_att, preferred_element_type=jnp.float32)
        back = turn(jnp.concatenate([dq, dk[:, None]], axis=1), cos_part, -sin_part)
        d_proj = jnp.concatenate([back.reshape(group_rows, v_at), dv], axis=1).astype(BF)
        grad_proj = dot(normed_all, d_proj, TN).astype(BF)
        part = dot(d_proj, attn[:, :o_at], NT).astype(BF)
        grad_normed = scatter_rows(part.reshape(nctx, rows_here, model_width), nz)
        through, grad_attn_gain = norm_back(hidden, attn_gain, grad_normed)
        grad = grad_middle + through

        grads = jnp.stack([jnp.concatenate([grad_proj, grad_out], axis=1)] + grad_gate + grad_up + grad_down)
        rows = model_width // (nctx * nfs)
        extra = jnp.stack([grad_attn_gain, grad_moe_gain]).reshape(2, nctx, nfs // NCORE, NCORE, rows)
        extra = jnp.pad(extra.transpose(3, 2, 1, 0, 4), ((0, 0), (0, 0), (0, 0), (0, 6), (0, 128 - rows)))
        collected[layer] = collect_grads(grads, extra, nctx, nfs)

    def attn_part(low, high):
        return jnp.stack(
            [
                c[0][:, 0, :, low:high].transpose(1, 0, 2).reshape(c[0].shape[2], -1).astype(F32)
                for c in collected
            ]
        )

    def expert_part(first):
        return jnp.stack(
            [
                c[0][:, first : first + 2].reshape((EXPERTS,) + c[0].shape[2:]).astype(F32)
                for c in collected
            ]
        )

    def gain_part(kind):
        return jnp.stack([jnp.sum(c[1][:, kind, :rows], axis=0) for c in collected])

    return (
        output[None],
        grad[None],
        attn_part(0, kv_at),
        attn_part(kv_at, v_at),
        attn_part(v_at, o_at),
        attn_part(o_at, o_at + q_width),
        gain_part(0),
        gain_part(1),
        expert_part(1),
        expert_part(3),
        expert_part(5),
    )


def solution(mesh):
    placed = (
        P("fsdp", "ctx", None),
        P("fsdp", "ctx", None),
        P("fsdp", None),
        P("fsdp", None),
        P(None, "fsdp", "ctx", None),
        P(None, "fsdp", "ctx", None),
        P(None, ("ctx", "fsdp"), None),
        P(None, ("ctx", "fsdp"), None),
        P(None, ("ctx", "fsdp"), None),
        P(None, ("ctx", "fsdp"), None),
        P(None, ("ctx", "fsdp")),
        P(None, ("ctx", "fsdp")),
        P(None, None, ("ctx", "fsdp"), None),
        P(None, None, ("ctx", "fsdp"), None),
        P(None, None, ("ctx", "fsdp"), None),
    )
    nctx, nfs = mesh.shape["ctx"], mesh.shape["fsdp"]
    chosen = partial(fast_body, nctx, nfs) if (nctx, nfs) == (8, 4) else body
    return jax.shard_map(
        chosen,
        mesh=mesh,
        in_specs=placed,
        out_specs=(
            P("fsdp", "ctx", None),
            P("fsdp", "ctx", None),
            P(None, ("ctx", "fsdp"), None),
            P(None, ("ctx", "fsdp"), None),
            P(None, ("ctx", "fsdp"), None),
            P(None, ("ctx", "fsdp"), None),
            P(None, ("ctx", "fsdp")),
            P(None, ("ctx", "fsdp")),
            P(None, None, ("ctx", "fsdp"), None),
            P(None, None, ("ctx", "fsdp"), None),
            P(None, None, ("ctx", "fsdp"), None),
        ),
        check_vma=False,
    )
```

```python
from functools import partial
import functools
import math

import jax
import jax.numpy as jnp
from jax import lax
from jax.experimental import pallas as pl
from jax.experimental.pallas import tpu as pltpu
from jax.sharding import PartitionSpec as P

HEAD_DIM = 64
EXPERTS = 16
LAYERS = 2
TILE = 128
CAP = 80


EPSILON = 1e-06
NEGATIVE = -1e30


def layout(lengths, tile_order, group_rows):
    tile_count = tile_order.shape[0]
    row_ids = jnp.arange(group_rows, dtype=jnp.int32)
    in_tile = (row_ids // TILE)[:, None] == jnp.arange(tile_count, dtype=jnp.int32)[None, :]
    tile_of = jnp.sum(jnp.where(in_tile, tile_order[None, :], 0), axis=1, dtype=jnp.int32)
    anchor = tile_of * TILE + row_ids % TILE
    seq_ends = jnp.cumsum(lengths, dtype=jnp.int32)
    seq_starts = seq_ends - lengths
    segment = jnp.sum(
        (anchor[:, None] >= seq_ends[None, :]).astype(jnp.int32), axis=1, dtype=jnp.int32
    )
    picked = segment[:, None] == jnp.arange(lengths.shape[0], dtype=jnp.int32)[None, :]
    offset = jnp.sum(jnp.where(picked, seq_starts[None, :], 0), axis=1, dtype=jnp.int32)
    return (segment, anchor - offset)


def rms_norm(values, gain_vec):
    return (
        values * lax.rsqrt(jnp.mean(values * values, axis=-1, keepdims=True) + EPSILON) * gain_vec
    )


def rotate(values, places):
    half_dim = values.shape[-1] // 2
    freq_steps = jnp.arange(half_dim, dtype=jnp.float32)
    inverse = jnp.exp(freq_steps * (-2.0 * math.log(10000.0) / values.shape[-1]))
    angles = places[:, None] * inverse[None, :]
    cos_part = jnp.cos(angles)[:, None, :]
    sin_part = jnp.sin(angles)[:, None, :]
    first_half = values[..., :half_dim]
    second_half = values[..., half_dim:]
    return jnp.concatenate(
        [
            first_half * cos_part - second_half * sin_part,
            second_half * cos_part + first_half * sin_part,
        ],
        axis=-1,
    )


def rotate_back(grads_in, places):
    return jax.vjp(partial(rotate, places=places), jnp.zeros(grads_in.shape, jnp.float32))[1](
        grads_in
    )[0]


def mix_inner(gate_act, up_act):
    return jax.nn.silu(gate_act) * up_act


def split_halves(master):
    experts_here, rows_here, hidden_units = master.shape
    return (
        master.astype(jnp.bfloat16)
        .reshape(experts_here, rows_here, 2, hidden_units // 2)
        .transpose(0, 2, 1, 3)
        .reshape(2 * experts_here, rows_here, hidden_units // 2)
    )


def merge_halves(grads_in):
    halves_all, rows_here, half_units = grads_in.shape
    return (
        grads_in.reshape(halves_all // 2, 2, rows_here, half_units)
        .transpose(0, 2, 1, 3)
        .reshape(halves_all // 2, rows_here, 2 * half_units)
    )


def doubled(slots):
    return jnp.broadcast_to(slots[:, None], (slots.shape[0], 2) + slots.shape[1:]).reshape(
        (2 * slots.shape[0],) + slots.shape[1:]
    )


def fold_halves(parts):
    return jnp.sum(parts.reshape((parts.shape[0] // 2, 2) + parts.shape[1:]), axis=1)


def send_out(slots):
    return lax.all_to_all(slots, "ctx", split_axis=0, concat_axis=1, tiled=True)


def send_back(parts):
    return lax.all_to_all(
        parts.astype(jnp.bfloat16), "ctx", split_axis=1, concat_axis=0, tiled=True
    ).astype(parts.dtype)


def routing(route_ids, gate_share, rows_here):
    expert_ids = jnp.arange(EXPERTS, dtype=jnp.int32)
    chosen = (route_ids[:, :, None] == expert_ids[None, None, :]).astype(jnp.int32)
    member = jnp.sum(chosen, axis=1, dtype=jnp.int32)
    before = jnp.cumsum(member, axis=0, dtype=jnp.int32) - member
    rank_of = jnp.sum(chosen * before[:, None, :], axis=2, dtype=jnp.int32)
    slot_of = route_ids * CAP + rank_of
    token_ids = jnp.broadcast_to(jnp.arange(rows_here, dtype=jnp.int32)[:, None], route_ids.shape)
    flat_slots = slot_of.reshape(-1)
    slot_token = (
        jnp.full((EXPERTS * CAP,), rows_here, jnp.int32).at[flat_slots].set(token_ids.reshape(-1))
    )
    slot_share = jnp.zeros((EXPERTS * CAP,), jnp.float32).at[flat_slots].set(gate_share.reshape(-1))
    return (slot_of, slot_token, slot_share)


def key_block(key_rows, value_rows, token_meta, block_index, block_rows):
    seg_local, pos_local, seg_all, pos_all = token_meta
    first_row = block_index * block_rows
    key_part = lax.dynamic_slice_in_dim(key_rows, first_row, block_rows, 0)
    value_part = lax.dynamic_slice_in_dim(value_rows, first_row, block_rows, 0)
    seg_part = lax.dynamic_slice_in_dim(seg_all, first_row, block_rows, 0)
    pos_part = lax.dynamic_slice_in_dim(pos_all, first_row, block_rows, 0)
    visible = (seg_local[:, None] == seg_part[None, :]) & (pos_part[None, :] <= pos_local[:, None])
    return (key_part, value_part, visible)


def scores(queries, key_part, visible, score_scale):
    raw_scores = (
        jnp.einsum("qhgd,khd->hgqk", queries, key_part, preferred_element_type=jnp.float32)
        * score_scale
    )
    return jnp.where(visible[None, None], raw_scores, NEGATIVE)


def keep_same(running):
    return running


def attention_forward(queries, key_rows, value_rows, token_meta, block_rows, score_scale):
    block_count = key_rows.shape[0] // block_rows
    rows_here, heads_kv, groups = (queries.shape[0], queries.shape[1], queries.shape[2])

    def stat_step(block_index, running):
        key_part, value_part, visible = key_block(
            key_rows, value_rows, token_meta, block_index, block_rows
        )

        def stat_update(current):
            row_peak, denom_sum = current
            logits = scores(queries, key_part, visible, score_scale)
            new_peak = jnp.maximum(row_peak, jnp.max(logits, axis=-1))
            denom_sum = denom_sum * jnp.exp(row_peak - new_peak) + jnp.sum(
                jnp.exp(logits - new_peak[..., None]), axis=-1
            )
            return (new_peak, denom_sum)

        return lax.cond(jnp.any(visible), stat_update, keep_same, running)

    start_stats = (
        jnp.full((heads_kv, groups, rows_here), NEGATIVE, jnp.float32),
        jnp.zeros((heads_kv, groups, rows_here), jnp.float32),
    )
    row_peak, denom_sum = lax.fori_loop(0, block_count, stat_step, start_stats)

    def out_step(block_index, partial_sum):
        key_part, value_part, visible = key_block(
            key_rows, value_rows, token_meta, block_index, block_rows
        )

        def out_update(current):
            attn_probs = (
                jnp.exp(scores(queries, key_part, visible, score_scale) - row_peak[..., None])
                / denom_sum[..., None]
            )
            return current + jnp.einsum(
                "hgqk,khd->qhgd",
                attn_probs.astype(jnp.bfloat16),
                value_part,
                preferred_element_type=jnp.float32,
            )

        return lax.cond(jnp.any(visible), out_update, keep_same, partial_sum)

    attended = lax.fori_loop(
        0, block_count, out_step, jnp.zeros((rows_here, heads_kv, groups, HEAD_DIM), jnp.float32)
    )
    return ((row_peak, denom_sum), attended)


def attention_backward(
    queries, key_rows, value_rows, token_meta, softmax_stats, grad_attended, block_rows, score_scale
):
    row_peak, denom_sum = softmax_stats
    block_count = key_rows.shape[0] // block_rows

    def probs_for(key_part, visible):
        return (
            jnp.exp(scores(queries, key_part, visible, score_scale) - row_peak[..., None])
            / denom_sum[..., None]
        )

    def delta_step(block_index, partial_sum):
        key_part, value_part, visible = key_block(
            key_rows, value_rows, token_meta, block_index, block_rows
        )

        def delta_update(current):
            attn_probs = probs_for(key_part, visible)
            grad_probs = jnp.einsum(
                "qhgd,khd->hgqk", grad_attended, value_part, preferred_element_type=jnp.float32
            )
            return current + jnp.sum(attn_probs * grad_probs, axis=-1)

        return lax.cond(jnp.any(visible), delta_update, keep_same, partial_sum)

    delta_sum = lax.fori_loop(0, block_count, delta_step, jnp.zeros(denom_sum.shape, jnp.float32))

    def grad_step(block_index, running):
        key_part, value_part, visible = key_block(
            key_rows, value_rows, token_meta, block_index, block_rows
        )
        first_row = block_index * block_rows

        def grad_update(current):
            grad_queries, grad_keys, grad_values = current
            attn_probs = probs_for(key_part, visible)
            grad_probs = jnp.einsum(
                "qhgd,khd->hgqk", grad_attended, value_part, preferred_element_type=jnp.float32
            )
            grad_scores = (attn_probs * (grad_probs - delta_sum[..., None])).astype(jnp.bfloat16)
            grad_queries = grad_queries + jnp.einsum(
                "hgqk,khd->qhgd", grad_scores, key_part, preferred_element_type=jnp.float32
            )
            key_term = jnp.einsum(
                "hgqk,qhgd->khd", grad_scores, queries, preferred_element_type=jnp.float32
            )
            value_term = jnp.einsum(
                "hgqk,qhgd->khd",
                attn_probs.astype(jnp.bfloat16),
                grad_attended,
                preferred_element_type=jnp.float32,
            )
            grad_keys = lax.dynamic_update_slice_in_dim(
                grad_keys,
                lax.dynamic_slice_in_dim(grad_keys, first_row, block_rows, 0) + key_term,
                first_row,
                0,
            )
            grad_values = lax.dynamic_update_slice_in_dim(
                grad_values,
                lax.dynamic_slice_in_dim(grad_values, first_row, block_rows, 0) + value_term,
                first_row,
                0,
            )
            return (grad_queries, grad_keys, grad_values)

        return lax.cond(jnp.any(visible), grad_update, keep_same, running)

    start_grads = (
        jnp.zeros(queries.shape, jnp.float32),
        jnp.zeros(key_rows.shape, jnp.float32),
        jnp.zeros(value_rows.shape, jnp.float32),
    )
    return lax.fori_loop(0, block_count, grad_step, start_grads)


def fetch_layer(master_set, layer_index):
    (
        query_weight,
        key_weight,
        value_weight,
        out_weight,
        attn_gain,
        moe_gain,
        gate_weight,
        up_weight,
        down_weight,
    ) = master_set
    attn_set = (
        lax.all_gather(
            query_weight[layer_index].astype(jnp.bfloat16), ("ctx", "fsdp"), axis=0, tiled=True
        ),
        lax.all_gather(
            key_weight[layer_index].astype(jnp.bfloat16), ("ctx", "fsdp"), axis=0, tiled=True
        ),
        lax.all_gather(
            value_weight[layer_index].astype(jnp.bfloat16), ("ctx", "fsdp"), axis=0, tiled=True
        ),
        lax.all_gather(
            out_weight[layer_index].astype(jnp.bfloat16), ("ctx", "fsdp"), axis=0, tiled=True
        ),
        lax.all_gather(
            attn_gain[layer_index].astype(jnp.bfloat16), ("ctx", "fsdp"), axis=0, tiled=True
        ),
        lax.all_gather(
            moe_gain[layer_index].astype(jnp.bfloat16), ("ctx", "fsdp"), axis=0, tiled=True
        ),
    )
    row_set = (
        lax.all_gather(split_halves(gate_weight[layer_index]), "fsdp", axis=1, tiled=True),
        lax.all_gather(split_halves(up_weight[layer_index]), "fsdp", axis=1, tiled=True),
        lax.all_gather(split_halves(down_weight[layer_index]), "fsdp", axis=1, tiled=True),
    )
    expert_set = (
        lax.all_to_all(row_set[0], "ctx", split_axis=0, concat_axis=1, tiled=True),
        lax.all_to_all(row_set[1], "ctx", split_axis=0, concat_axis=1, tiled=True),
        lax.all_to_all(row_set[2], "ctx", split_axis=0, concat_axis=1, tiled=True),
    )
    return tuple(attn_set) + tuple(expert_set)


def layer_forward(hidden, weights, route_ids, gate_share, token_meta, places, block_rows):
    (
        query_full,
        key_full,
        value_full,
        out_full,
        attn_norm,
        moe_norm,
        gate_full,
        up_full,
        down_full,
    ) = weights
    rows_here, model_width = hidden.shape
    heads_all = query_full.shape[1] // HEAD_DIM
    heads_kv = key_full.shape[1] // HEAD_DIM
    groups = heads_all // heads_kv
    score_scale = HEAD_DIM ** (-0.5)
    normed = rms_norm(hidden, attn_norm.astype(jnp.float32)).astype(jnp.bfloat16)
    queries = rotate(
        jnp.dot(normed, query_full, preferred_element_type=jnp.float32).reshape(
            rows_here, heads_all, HEAD_DIM
        ),
        places,
    ).astype(jnp.bfloat16)
    key_new = (
        rotate(
            jnp.dot(normed, key_full, preferred_element_type=jnp.float32).reshape(
                rows_here, heads_kv, HEAD_DIM
            ),
            places,
        )
        .astype(jnp.bfloat16)
        .reshape(rows_here, heads_kv * HEAD_DIM)
    )
    value_new = jnp.dot(normed, value_full, preferred_element_type=jnp.float32).astype(jnp.bfloat16)
    key_rows, value_rows = (
        lax.all_gather(key_new, "ctx", axis=0, tiled=True),
        lax.all_gather(value_new, "ctx", axis=0, tiled=True),
    )
    key_rows = key_rows.reshape(-1, heads_kv, HEAD_DIM)
    value_rows = value_rows.reshape(-1, heads_kv, HEAD_DIM)
    queries = queries.reshape(rows_here, heads_kv, groups, HEAD_DIM)
    softmax_stats, attended = attention_forward(
        queries, key_rows, value_rows, token_meta, block_rows, score_scale
    )
    attended = attended.reshape(rows_here, heads_all * HEAD_DIM).astype(jnp.bfloat16)
    middle = hidden + jnp.einsum(
        "tx,dx->td", attended, out_full, preferred_element_type=jnp.float32
    )
    moe_in = rms_norm(middle, moe_norm.astype(jnp.float32)).astype(jnp.bfloat16)
    slot_of, slot_token, slot_share = routing(route_ids, gate_share, rows_here)
    padded = jnp.concatenate([moe_in, jnp.zeros((1, model_width), jnp.bfloat16)], axis=0)
    dispatched = jnp.take(padded, slot_token, axis=0).reshape(EXPERTS, CAP, model_width)
    owner_rows = send_out(doubled(dispatched))
    gate_act = jnp.einsum("ecd,edf->ecf", owner_rows, gate_full, preferred_element_type=jnp.float32)
    up_act = jnp.einsum("ecd,edf->ecf", owner_rows, up_full, preferred_element_type=jnp.float32)
    inner_act = mix_inner(gate_act, up_act).astype(jnp.bfloat16)
    expert_part = jnp.einsum(
        "ecf,edf->ecd", inner_act, down_full, preferred_element_type=jnp.float32
    )
    expert_out = fold_halves(send_back(expert_part))
    expert_out = expert_out.reshape(EXPERTS * CAP, model_width)
    moe_out = jnp.sum(jnp.take(expert_out, slot_of, axis=0) * gate_share[..., None], axis=1)
    record = (
        hidden,
        normed,
        queries,
        key_rows,
        value_rows,
        softmax_stats,
        attended,
        middle,
        moe_in,
        slot_of,
        slot_token,
        slot_share,
        owner_rows,
        gate_act,
        up_act,
        inner_act,
    )
    return (record, middle + moe_out)


def layer_backward(grad_hidden, record, weights, token_meta, places, block_rows):
    (
        hidden,
        normed,
        queries,
        key_rows,
        value_rows,
        softmax_stats,
        attended,
        middle,
        moe_in,
        slot_of,
        slot_token,
        slot_share,
        owner_rows,
        gate_act,
        up_act,
        inner_act,
    ) = record
    (
        query_full,
        key_full,
        value_full,
        out_full,
        attn_norm,
        moe_norm,
        gate_full,
        up_full,
        down_full,
    ) = weights
    rows_here, model_width = hidden.shape
    heads_kv, groups = (queries.shape[1], queries.shape[2])
    group_rows = key_rows.shape[0]
    score_scale = HEAD_DIM ** (-0.5)
    grad_padded = jnp.concatenate([grad_hidden, jnp.zeros((1, model_width), jnp.float32)], axis=0)
    grad_expert = (
        (jnp.take(grad_padded, slot_token, axis=0) * slot_share[:, None])
        .astype(jnp.bfloat16)
        .reshape(EXPERTS, CAP, model_width)
    )
    grad_owner = send_out(doubled(grad_expert))
    grad_down = jnp.einsum(
        "ecd,ecf->edf", grad_owner, inner_act, preferred_element_type=jnp.float32
    )
    grad_inner = jnp.einsum(
        "ecd,edf->ecf", grad_owner, down_full, preferred_element_type=jnp.float32
    )
    grad_gate_act, grad_up_act = jax.vjp(mix_inner, gate_act, up_act)[1](grad_inner)
    grad_gate_act = grad_gate_act.astype(jnp.bfloat16)
    grad_up_act = grad_up_act.astype(jnp.bfloat16)
    grad_gate = jnp.einsum(
        "ecd,ecf->edf", owner_rows, grad_gate_act, preferred_element_type=jnp.float32
    )
    grad_up = jnp.einsum(
        "ecd,ecf->edf", owner_rows, grad_up_act, preferred_element_type=jnp.float32
    )
    grad_owner_rows = jnp.einsum(
        "ecf,edf->ecd", grad_gate_act, gate_full, preferred_element_type=jnp.float32
    ) + jnp.einsum("ecf,edf->ecd", grad_up_act, up_full, preferred_element_type=jnp.float32)
    grad_dispatched = fold_halves(send_back(grad_owner_rows))
    home_set = (
        lax.all_to_all(
            grad_gate.astype(jnp.bfloat16), "ctx", split_axis=1, concat_axis=0, tiled=True
        ).astype(grad_gate.dtype),
        lax.all_to_all(
            grad_up.astype(jnp.bfloat16), "ctx", split_axis=1, concat_axis=0, tiled=True
        ).astype(grad_up.dtype),
        lax.all_to_all(
            grad_down.astype(jnp.bfloat16), "ctx", split_axis=1, concat_axis=0, tiled=True
        ).astype(grad_down.dtype),
    )
    summed_set = (
        lax.psum_scatter(
            home_set[0].astype(jnp.bfloat16), "fsdp", scatter_dimension=1, tiled=True
        ).astype(jnp.float32),
        lax.psum_scatter(
            home_set[1].astype(jnp.bfloat16), "fsdp", scatter_dimension=1, tiled=True
        ).astype(jnp.float32),
        lax.psum_scatter(
            home_set[2].astype(jnp.bfloat16), "fsdp", scatter_dimension=1, tiled=True
        ).astype(jnp.float32),
    )
    expert_grads = (
        merge_halves(summed_set[0]),
        merge_halves(summed_set[1]),
        merge_halves(summed_set[2]),
    )
    grad_moe_in = jnp.sum(
        jnp.take(grad_dispatched.reshape(EXPERTS * CAP, model_width), slot_of, axis=0), axis=1
    )
    grad_middle_part, grad_moe_norm = jax.vjp(rms_norm, middle, moe_norm.astype(jnp.float32))[1](
        grad_moe_in
    )
    grad_middle = grad_hidden + grad_middle_part
    grad_rounded = grad_middle.astype(jnp.bfloat16)
    grad_out_full = jnp.einsum(
        "td,tx->dx", grad_rounded, attended, preferred_element_type=jnp.float32
    )
    grad_attended = (
        jnp.dot(grad_rounded, out_full, preferred_element_type=jnp.float32)
        .astype(jnp.bfloat16)
        .reshape(rows_here, heads_kv, groups, HEAD_DIM)
    )
    grad_queries, grad_keys, grad_values = attention_backward(
        queries,
        key_rows,
        value_rows,
        token_meta,
        softmax_stats,
        grad_attended,
        block_rows,
        score_scale,
    )
    key_sums, value_sums = (
        lax.psum_scatter(
            grad_keys.reshape(group_rows, heads_kv * HEAD_DIM).astype(jnp.bfloat16),
            "ctx",
            scatter_dimension=0,
            tiled=True,
        ).astype(jnp.float32),
        lax.psum_scatter(
            grad_values.reshape(group_rows, heads_kv * HEAD_DIM).astype(jnp.bfloat16),
            "ctx",
            scatter_dimension=0,
            tiled=True,
        ).astype(jnp.float32),
    )
    grad_query_rows = (
        rotate_back(
            grad_queries.reshape(rows_here, heads_kv * groups, HEAD_DIM) * score_scale, places
        )
        .astype(jnp.bfloat16)
        .reshape(rows_here, heads_kv * groups * HEAD_DIM)
    )
    grad_key_rows = (
        rotate_back(key_sums.reshape(rows_here, heads_kv, HEAD_DIM) * score_scale, places)
        .astype(jnp.bfloat16)
        .reshape(rows_here, heads_kv * HEAD_DIM)
    )
    grad_value_rows = value_sums.astype(jnp.bfloat16)
    grad_query_full = jnp.einsum(
        "td,tx->dx", normed, grad_query_rows, preferred_element_type=jnp.float32
    )
    grad_key_full = jnp.einsum(
        "td,tx->dx", normed, grad_key_rows, preferred_element_type=jnp.float32
    )
    grad_value_full = jnp.einsum(
        "td,tx->dx", normed, grad_value_rows, preferred_element_type=jnp.float32
    )
    grad_normed = jnp.einsum(
        "tx,dx->td", grad_query_rows, query_full, preferred_element_type=jnp.float32
    )
    grad_normed = grad_normed + jnp.einsum(
        "tx,dx->td", grad_key_rows, key_full, preferred_element_type=jnp.float32
    )
    grad_normed = grad_normed + jnp.einsum(
        "tx,dx->td", grad_value_rows, value_full, preferred_element_type=jnp.float32
    )
    grad_hidden_part, grad_attn_norm = jax.vjp(rms_norm, hidden, attn_norm.astype(jnp.float32))[1](
        grad_normed
    )
    attn_grads = (
        lax.psum_scatter(grad_query_full, ("ctx", "fsdp"), scatter_dimension=0, tiled=True),
        lax.psum_scatter(grad_key_full, ("ctx", "fsdp"), scatter_dimension=0, tiled=True),
        lax.psum_scatter(grad_value_full, ("ctx", "fsdp"), scatter_dimension=0, tiled=True),
        lax.psum_scatter(grad_out_full, ("ctx", "fsdp"), scatter_dimension=0, tiled=True),
        lax.psum_scatter(grad_attn_norm, ("ctx", "fsdp"), scatter_dimension=0, tiled=True),
        lax.psum_scatter(grad_moe_norm, ("ctx", "fsdp"), scatter_dimension=0, tiled=True),
    )
    return (grad_middle + grad_hidden_part, attn_grads, expert_grads)


def body(
    tokens,
    cotangent,
    lengths,
    tile_order,
    routes,
    gates,
    query_weight,
    key_weight,
    value_weight,
    out_weight,
    attn_gain,
    moe_gain,
    gate_weight,
    up_weight,
    down_weight,
):
    rows_here = tokens.shape[1]
    group_rows = rows_here * lax.axis_size("ctx")
    seg_all, pos_all = layout(lengths[0], tile_order[0], group_rows)
    first_row = lax.axis_index("ctx") * rows_here
    seg_local = lax.dynamic_slice_in_dim(seg_all, first_row, rows_here, 0)
    pos_local = lax.dynamic_slice_in_dim(pos_all, first_row, rows_here, 0)
    token_meta = (seg_local, pos_local, seg_all, pos_all)
    places = pos_local.astype(jnp.float32)
    block_rows = math.gcd(group_rows, 512)
    master_set = (
        query_weight,
        key_weight,
        value_weight,
        out_weight,
        attn_gain,
        moe_gain,
        gate_weight,
        up_weight,
        down_weight,
    )
    hidden = tokens[0].astype(jnp.float32)
    records = []
    for layer_index in range(LAYERS):
        weights = fetch_layer(master_set, layer_index)
        record, hidden = layer_forward(
            hidden,
            weights,
            routes[layer_index, 0],
            gates[layer_index, 0],
            token_meta,
            places,
            block_rows,
        )
        records.append(record)
    grad_hidden = cotangent[0].astype(jnp.float32)
    attn_layers = []
    expert_layers = []
    for layer_index in reversed(range(LAYERS)):
        weights = fetch_layer(master_set, layer_index)
        grad_hidden, attn_grads, expert_grads = layer_backward(
            grad_hidden, records[layer_index], weights, token_meta, places, block_rows
        )
        attn_layers.insert(0, attn_grads)
        expert_layers.insert(0, expert_grads)
    grad_query_weight = jnp.stack([layer_grads[0] for layer_grads in attn_layers])
    grad_key_weight = jnp.stack([layer_grads[1] for layer_grads in attn_layers])
    grad_value_weight = jnp.stack([layer_grads[2] for layer_grads in attn_layers])
    grad_out_weight = jnp.stack([layer_grads[3] for layer_grads in attn_layers])
    grad_attn_gain = jnp.stack([layer_grads[4] for layer_grads in attn_layers])
    grad_moe_gain = jnp.stack([layer_grads[5] for layer_grads in attn_layers])
    grad_gate_weight = jnp.stack([layer_grads[0] for layer_grads in expert_layers])
    grad_up_weight = jnp.stack([layer_grads[1] for layer_grads in expert_layers])
    grad_down_weight = jnp.stack([layer_grads[2] for layer_grads in expert_layers])
    return (
        hidden.astype(jnp.bfloat16)[None],
        grad_hidden[None],
        grad_query_weight,
        grad_key_weight,
        grad_value_weight,
        grad_out_weight,
        grad_attn_gain,
        grad_moe_gain,
        grad_gate_weight,
        grad_up_weight,
        grad_down_weight,
    )


BF = jnp.bfloat16
F32 = jnp.float32
NX = 2
NCORE = 2
ANY = pl.BlockSpec(memory_space=pl.ANY)
VM = pl.BlockSpec(memory_space=pltpu.VMEM)
DMA = pltpu.SemaphoreType.DMA

NN = ((1,), (0,))
NT = ((1,), (1,))
TN = ((0,), (0,))


def dot(left, right, dims):
    return lax.dot_general(left, right, (dims, ((), ())), preferred_element_type=jnp.float32)


def remote(src, dst, send_sem, recv_sem, ctx, fsdp):
    return pltpu.make_async_remote_copy(
        src_ref=src,
        dst_ref=dst,
        send_sem=send_sem,
        recv_sem=recv_sem,
        device_id={"ctx": ctx, "fsdp": fsdp},
        device_id_type=pl.DeviceIdType.MESH,
    )


def greet(barrier, ctx, fsdp):
    pl.semaphore_signal(
        barrier, inc=1, device_id={"ctx": ctx, "fsdp": fsdp}, device_id_type=pl.DeviceIdType.MESH
    )


class Line:
    def __init__(self, nz):
        self.nz = nz
        self.ctx, self.fsdp = lax.axis_index("ctx"), lax.axis_index("fsdp")
        self.z, self.x = self.ctx // NX, self.ctx % NX
        self.mate = self.z * NX + 1 - self.x
        self.above = (self.z + 1) * NX + self.x
        self.below = (self.z - 1) * NX + self.x

    def greet(self):
        barrier = pltpu.get_barrier_semaphore()
        greet(barrier, self.mate, self.fsdp)

        @pl.when(self.z > 0)
        def _():
            greet(barrier, self.below, self.fsdp)

        @pl.when(self.z < self.nz - 1)
        def _():
            greet(barrier, self.above, self.fsdp)

        ends = jnp.where(self.z > 0, 1, 0) + jnp.where(self.z < self.nz - 1, 1, 0)
        pl.semaphore_wait(barrier, 1 + ends)

    def near(self, i):
        z, nz = self.z, self.nz
        mid1 = jnp.where(i == 0, 1, jnp.where(i == 1, 0, i))
        mid2 = jnp.where(i == 0, 2, jnp.where(i == 1, 1, jnp.where(i == 2, 3, 0)))
        return jnp.where(z == 0, i, jnp.where(z == nz - 1, nz - 1 - i, jnp.where(z == 1, mid1, mid2)))

    def far(self, i):
        z, nz = self.z, self.nz
        mid1 = jnp.where(i == 0, 3, jnp.where(i == 1, 0, jnp.where(i == 2, 2, 1)))
        mid2 = jnp.where(i == 0, 0, jnp.where(i == 1, 3, jnp.where(i == 2, 1, 2)))
        return jnp.where(z == 0, nz - 1 - i, jnp.where(z == nz - 1, i, jnp.where(z == 1, mid1, mid2)))


class Gather:
    @staticmethod
    def scratch(nz):
        return [DMA((6, nz))]

    def __init__(self, line, own_ref, all_ref, sems):
        self.line, self.own, self.all, self.sems = line, own_ref, all_ref, sems

    def block(self, row):
        return self.all.at[row * NX + self.line.x]

    def up(self, t, src=None):
        line = self.line
        block = self.block(line.z - t)
        return remote(block if src is None else src, block, self.sems.at[0, t], self.sems.at[1, t], line.above, line.fsdp)

    def down(self, t, src=None):
        line = self.line
        block = self.block(line.z + t)
        return remote(block if src is None else src, block, self.sems.at[2, t], self.sems.at[3, t], line.below, line.fsdp)

    def across(self, row, src=None):
        line = self.line
        block = self.block(row)
        return remote(block if src is None else src, block, self.sems.at[4, row], self.sems.at[5, row], line.mate, line.fsdp)

    def start(self):
        line = self.line

        @pl.when(line.z < line.nz - 1)
        def _():
            self.up(0, self.own).start()

        @pl.when(line.z > 0)
        def _():
            self.down(0, self.own).start()

        self.across(line.z, self.own).start()

    def forward(self, t):
        line = self.line

        @pl.when(line.z - 1 - t >= 0)
        def _():
            remote(self.own, self.block(line.z - 1 - t), self.sems.at[0, t], self.sems.at[1, t], line.above, line.fsdp).wait_recv()

            @pl.when(line.z < line.nz - 1)
            def _():
                self.up(t + 1).start()

            self.across(line.z - 1 - t).start()

        @pl.when(line.z + 1 + t < line.nz)
        def _():
            remote(self.own, self.block(line.z + 1 + t), self.sems.at[2, t], self.sems.at[3, t], line.below, line.fsdp).wait_recv()

            @pl.when(line.z > 0)
            def _():
                self.down(t + 1).start()

            self.across(line.z + 1 + t).start()

    def wait_pair(self, row):
        line = self.line
        remote(self.own, self.all.at[row * NX + 1 - line.x], self.sems.at[4, row], self.sems.at[5, row], line.mate, line.fsdp).wait_recv()

    def finish(self):
        line = self.line
        for t in range(line.nz - 1):

            @pl.when((line.z - t >= 0) & (line.z < line.nz - 1))
            def _():
                self.up(t).wait_send()

            @pl.when((line.z + t < line.nz) & (line.z > 0))
            def _():
                self.down(t).wait_send()

        for row in range(line.nz):
            self.across(row).wait_send()


class Scatter:
    @staticmethod
    def scratch(nz, rows, width):
        return [pltpu.VMEM((4, nz, rows, width), BF), DMA((6, nz))]

    def __init__(self, line, part_ref, out_ref, work, sems):
        self.line, self.part, self.out, self.sems = line, part_ref, out_ref, sems
        self.xin, self.acc, self.upin, self.downin = (work.at[i] for i in range(4))

    def across(self, row):
        line = self.line
        return remote(self.part.at[row * NX + 1 - line.x], self.xin.at[row], self.sems.at[0, row], self.sems.at[1, row], line.mate, line.fsdp)

    def up(self, row):
        line = self.line
        return remote(self.acc.at[row], self.upin.at[row], self.sems.at[2, row], self.sems.at[3, row], line.above, line.fsdp)

    def down(self, row):
        line = self.line
        return remote(self.acc.at[row], self.downin.at[row], self.sems.at[4, row], self.sems.at[5, row], line.below, line.fsdp)

    def add(self, i):
        line = self.line
        row = line.far(i)
        self.across(row).wait_recv()
        mine = self.part[row * NX + line.x].astype(F32) + self.xin[row].astype(F32)

        @pl.when(row > line.z)
        def _():
            @pl.when(line.z == 0)
            def _():
                self.acc[row] = mine.astype(BF)

            @pl.when(line.z > 0)
            def _():
                self.up(row).wait_recv()
                self.acc[row] = (mine + self.upin[row].astype(F32)).astype(BF)

            self.up(row).start()

        @pl.when(row < line.z)
        def _():
            @pl.when(line.z == line.nz - 1)
            def _():
                self.acc[row] = mine.astype(BF)

            @pl.when(line.z < line.nz - 1)
            def _():
                self.down(row).wait_recv()
                self.acc[row] = (mine + self.downin[row].astype(F32)).astype(BF)

            self.down(row).start()

        @pl.when(row == line.z)
        def _():
            self.out[...] = mine

    def finish(self):
        line = self.line

        @pl.when(line.z > 0)
        def _():
            self.up(line.z).wait_recv()
            self.out[...] += self.upin[line.z].astype(F32)

        @pl.when(line.z < line.nz - 1)
        def _():
            self.down(line.z).wait_recv()
            self.out[...] += self.downin[line.z].astype(F32)

        for row in range(line.nz):
            self.across(row).wait_send()

            @pl.when(row > line.z)
            def _():
                self.up(row).wait_send()

            @pl.when(row < line.z)
            def _():
                self.down(row).wait_send()


def params(collective, vmem_mib):
    return pltpu.CompilerParams(collective_id=collective, has_side_effects=True, vmem_limit_bytes=vmem_mib << 20)


def gather_kernel(nz, x_ref, o_ref, own_sem, sems):
    line = Line(nz)
    line.greet()
    ring = Gather(line, x_ref, o_ref, sems)
    ring.start()
    own = pltpu.make_async_copy(x_ref, o_ref.at[line.ctx], own_sem)
    own.start()
    for t in range(nz - 1):
        ring.forward(t)
    for row in range(nz):
        ring.wait_pair(row)
    ring.finish()
    own.wait()


def gather_rows(block, nz):
    rows, width = block.shape
    return pl.pallas_call(
        functools.partial(gather_kernel, nz),
        out_shape=jax.ShapeDtypeStruct((nz * NX, rows, width), block.dtype),
        in_specs=[VM],
        out_specs=ANY,
        scratch_shapes=[DMA] + Gather.scratch(nz),
        compiler_params=params(1, 16),
        name="gather_rows",
    )(block)


def scatter_kernel(nz, p_ref, o_ref, work, sems):
    line = Line(nz)
    line.greet()
    ring = Scatter(line, p_ref, o_ref, work, sems)
    for i in range(nz):
        ring.across(line.far(i)).start()
    for i in range(nz):
        ring.add(i)
    ring.finish()


def scatter_rows(parts, nz):
    _, rows, width = parts.shape
    return pl.pallas_call(
        functools.partial(scatter_kernel, nz),
        out_shape=jax.ShapeDtypeStruct((rows, width), F32),
        in_specs=[VM],
        out_specs=VM,
        scratch_shapes=Scatter.scratch(nz, rows, width),
        compiler_params=params(2, 32),
        name="scatter_rows",
    )(parts)


def experts_kernel(nz, layer, x_ref, share_ref, mats_ref, o_ref, all_out, gate_out, up_out,
                   mats, blocks, part, gate, up, load_sem, save_sem, gsems, work, ssems):
    line = Line(nz)
    rows, width = x_ref.shape
    load = pltpu.make_async_copy(mats_ref.at[layer, pl.ds(1, 6)], mats, load_sem)
    load.start()
    line.greet()
    ring = Gather(line, x_ref, blocks, gsems)
    ring.start()
    blocks[line.ctx] = x_ref[...]
    load.wait()

    def saves(row):
        pair = pl.ds(row * NX, NX)
        return (
            pltpu.make_async_copy(blocks.at[pair], all_out.at[pair], save_sem.at[0, row]),
            pltpu.make_async_copy(gate.at[pair], gate_out.at[pair], save_sem.at[1, row]),
            pltpu.make_async_copy(up.at[pair], up_out.at[pair], save_sem.at[2, row]),
        )

    def step(i, carry):
        @pl.when(i < nz - 1)
        def _():
            ring.forward(i)

        row = line.near(i)
        ring.wait_pair(row)
        pair = pl.ds(row * NX, NX)
        block = blocks[pair].reshape(NX * rows, width)
        share = share_ref[pair].reshape(NX * rows, 2)
        total = None
        for e in range(2):
            gate_act = dot(block, mats[e], NN)
            up_act = dot(block, mats[2 + e], NN)
            units = gate_act.shape[1]
            gate[pair, :, pl.ds(e * units, units)] = gate_act.astype(BF).reshape(NX, rows, units)
            up[pair, :, pl.ds(e * units, units)] = up_act.astype(BF).reshape(NX, rows, units)
            inner = gate_act / (1.0 + jnp.exp(-gate_act)) * up_act * share[:, e : e + 1]
            term = dot(inner.astype(BF), mats[4 + e], NT)
            total = term if total is None else total + term
        part[pair] = total.astype(BF).reshape(NX, rows, width)
        for save in saves(row):
            save.start()
        return carry

    lax.fori_loop(0, nz, step, 0)
    sums = Scatter(line, part, o_ref, work, ssems)
    for i in range(nz):
        sums.across(line.far(i)).start()
    ring.finish()
    for i in range(nz):
        sums.add(i)
    sums.finish()
    for row in range(nz):
        for save in saves(row):
            save.wait()


def experts_forward(block, share, mats, layer, nz):
    rows, width = block.shape
    units = mats.shape[3]
    group = nz * NX
    acts = jax.ShapeDtypeStruct((group, rows, 2 * units), BF)
    return pl.pallas_call(
        functools.partial(experts_kernel, nz, layer),
        out_shape=(
            jax.ShapeDtypeStruct((rows, width), F32),
            jax.ShapeDtypeStruct((group, rows, width), BF),
            acts,
            acts,
        ),
        in_specs=[VM, VM, ANY],
        out_specs=(VM, ANY, ANY, ANY),
        scratch_shapes=[
            pltpu.VMEM((6, width, units), BF),
            pltpu.VMEM((group, rows, width), BF),
            pltpu.VMEM((group, rows, width), BF),
            pltpu.VMEM((group, rows, 2 * units), BF),
            pltpu.VMEM((group, rows, 2 * units), BF),
            DMA,
            DMA((3, nz)),
        ]
        + Gather.scratch(nz)
        + Scatter.scratch(nz, rows, width),
        compiler_params=params(5 + 2 * layer, 60),
        name="experts_forward",
    )(block, share, mats)


def experts_back_kernel(nz, layer, x_ref, share_ref, mats_ref, gate_ref, up_ref, o_ref, all_out, dgate_out, dup_out, inner_out,
                        mats, blocks, part, gate, up, inners, load_sem, save_sem, gsems, work, ssems):
    line = Line(nz)
    rows, width = x_ref.shape
    loads = (
        pltpu.make_async_copy(mats_ref.at[layer, pl.ds(1, 6)], mats, load_sem.at[0]),
        pltpu.make_async_copy(gate_ref, gate, load_sem.at[1]),
        pltpu.make_async_copy(up_ref, up, load_sem.at[2]),
    )
    for load in loads:
        load.start()
    line.greet()
    ring = Gather(line, x_ref, blocks, gsems)
    ring.start()
    blocks[line.ctx] = x_ref[...]
    for load in loads:
        load.wait()

    def saves(row):
        pair = pl.ds(row * NX, NX)
        return (
            pltpu.make_async_copy(blocks.at[pair], all_out.at[pair], save_sem.at[0, row]),
            pltpu.make_async_copy(gate.at[pair], dgate_out.at[pair], save_sem.at[1, row]),
            pltpu.make_async_copy(up.at[pair], dup_out.at[pair], save_sem.at[2, row]),
            pltpu.make_async_copy(inners.at[pair], inner_out.at[pair], save_sem.at[3, row]),
        )

    def step(i, carry):
        @pl.when(i < nz - 1)
        def _():
            ring.forward(i)

        row = line.near(i)
        ring.wait_pair(row)
        pair = pl.ds(row * NX, NX)
        block = blocks[pair].reshape(NX * rows, width)
        share = share_ref[pair].reshape(NX * rows, 2)
        total = None
        units = mats.shape[2]
        for e in range(2):
            part_of = pl.ds(e * units, units)
            gate_act = gate[pair, :, part_of].reshape(NX * rows, units).astype(F32)
            up_act = up[pair, :, part_of].reshape(NX * rows, units).astype(F32)
            grad_inner = dot(block, mats[4 + e], NN) * share[:, e : e + 1]
            sigmoid = 1.0 / (1.0 + jnp.exp(-gate_act))
            silu = gate_act * sigmoid
            d_gate = (grad_inner * up_act * (sigmoid + silu * (1.0 - sigmoid))).astype(BF)
            d_up = (grad_inner * silu).astype(BF)
            inners[pair, :, part_of] = (silu * up_act * share[:, e : e + 1]).astype(BF).reshape(NX, rows, units)
            gate[pair, :, part_of] = d_gate.reshape(NX, rows, units)
            up[pair, :, part_of] = d_up.reshape(NX, rows, units)
            term = dot(d_gate, mats[e], NT) + dot(d_up, mats[2 + e], NT)
            total = term if total is None else total + term
        part[pair] = total.astype(BF).reshape(NX, rows, width)
        for save in saves(row):
            save.start()
        return carry

    lax.fori_loop(0, nz, step, 0)
    sums = Scatter(line, part, o_ref, work, ssems)
    for i in range(nz):
        sums.across(line.far(i)).start()
    ring.finish()
    for i in range(nz):
        sums.add(i)
    sums.finish()
    for row in range(nz):
        for save in saves(row):
            save.wait()


def experts_backward(block, share, mats, layer, gate_act, up_act, nz):
    rows, width = block.shape
    units = mats.shape[3]
    group = nz * NX
    acts = jax.ShapeDtypeStruct((group, rows, 2 * units), BF)
    held = pltpu.VMEM((group, rows, 2 * units), BF)
    return pl.pallas_call(
        functools.partial(experts_back_kernel, nz, layer),
        out_shape=(
            jax.ShapeDtypeStruct((rows, width), F32),
            jax.ShapeDtypeStruct((group, rows, width), BF),
            acts,
            acts,
            acts,
        ),
        in_specs=[VM, VM, ANY, ANY, ANY],
        out_specs=(VM, ANY, ANY, ANY, ANY),
        scratch_shapes=[
            pltpu.VMEM((6, width, units), BF),
            pltpu.VMEM((group, rows, width), BF),
            pltpu.VMEM((group, rows, width), BF),
            held,
            held,
            held,
            DMA((3,)),
            DMA((4, nz)),
        ]
        + Gather.scratch(nz)
        + Scatter.scratch(nz, rows, width),
        compiler_params=params(6 + 2 * layer, 60),
        name="experts_backward",
    )(block, share, mats, gate_act, up_act)


def far_of(nz, z, i):
    mid1 = jnp.where(i == 0, 3, jnp.where(i == 1, 0, jnp.where(i == 2, 2, 1)))
    mid2 = jnp.where(i == 0, 0, jnp.where(i == 1, 3, jnp.where(i == 2, 1, 2)))
    return jnp.where(z == 0, nz - 1 - i, jnp.where(z == nz - 1, i, jnp.where(z == 1, mid1, mid2)))


class Exchange:
    @staticmethod
    def scratch(nz, blk, lead=()):
        return [
            pltpu.VMEM(lead + (2, 2, 2) + blk, BF),
            pltpu.VMEM(lead + (nz,) + blk, BF),
            DMA(lead + (2, nz, nz, 2)),
            DMA(lead + (2, nz)),
        ]

    def __init__(self, line, src_at, dst_at, passing, for_mate, zs, xs, lead=()):
        self.line, self.src_at, self.dst_at, self.lead = line, src_at, dst_at, lead
        self.passing, self.for_mate, self.zs, self.xs = passing, for_mate, zs, xs

    def held(self, way, src, dest, side, at):
        last = self.line.nz - 1
        slot = (dest - at - 1) + src if way == 0 else (at - dest - 1) + last - src
        return self.passing.at[self.lead + (way, slot, side)]

    def zsem(self, kind, src, dest, side):
        return self.zs.at[self.lead + (kind, src, dest, side)]

    def hop(self, way, src, dest, side, ref):
        line = self.line
        to = line.z + 1 if way == 0 else line.z - 1
        sems = self.zsem(0, src, dest, side), self.zsem(1, src, dest, side)
        target = to * NX + line.x

        @pl.when(dest == to)
        def _():
            land = self.dst_at(src * NX + line.x) if side == 0 else self.for_mate.at[self.lead + (src,)]
            remote(ref, land, *sems, target, line.fsdp).start()

        @pl.when(dest != to)
        def _():
            remote(ref, self.held(way, src, dest, side, to), *sems, target, line.fsdp).start()

    def to_mate(self, src, ref=None):
        line = self.line
        ref = self.for_mate.at[self.lead + (src,)] if ref is None else ref
        return remote(ref, self.dst_at(src * NX + line.x), self.xs.at[self.lead + (0, src)], self.xs.at[self.lead + (1, src)], line.mate, line.fsdp)

    def send(self, dest):
        line = self.line
        for side, column in ((0, line.x), (1, 1 - line.x)):
            ref = self.src_at(dest * NX + column)

            @pl.when(dest > line.z)
            def _():
                self.hop(0, line.z, dest, side, ref)

            @pl.when(dest < line.z)
            def _():
                self.hop(1, line.z, dest, side, ref)

        @pl.when(dest == line.z)
        def _():
            self.to_mate(line.z, self.src_at(line.mate)).start()

    def events(self, i):
        line = self.line
        found = []
        for k in range(1, line.nz):
            j = i - k
            for way in range(2):
                src = line.z - k if way == 0 else line.z + k
                dest = far_of(line.nz, src, j)
                here = (dest >= line.z) if way == 0 else (dest <= line.z)
                found.append((way, src, dest, (src >= 0) & (src < line.nz) & (j >= 0) & (j < line.nz - 1) & here))
        return found

    def handle(self, way, src, dest, arrived):
        line = self.line
        for side in range(2):
            wait = self.held(way, 0 if way == 0 else line.nz - 1, line.z + 1 if way == 0 else line.z - 1, side, line.z)
            remote(wait, wait, self.zsem(0, src, dest, side), self.zsem(1, src, dest, side), line.mate, line.fsdp).wait_recv()

            @pl.when(dest != line.z)
            def _():
                self.hop(way, src, dest, side, self.held(way, src, dest, side, line.z))

        @pl.when(dest == line.z)
        def _():
            self.to_mate(src).start()
            arrived(src * NX + line.x)

    def mate_arrived(self, src):
        line = self.line
        wait = self.for_mate.at[self.lead + (src,)]
        remote(wait, wait, self.xs.at[self.lead + (0, src)], self.xs.at[self.lead + (1, src)], line.mate, line.fsdp).wait_recv()

    def finish(self):
        line = self.line
        wait = self.for_mate.at[self.lead + (0,)]
        for src in range(line.nz):
            for dest in range(line.nz):
                if src != dest:
                    passes = (line.z >= src) & (line.z < dest) if src < dest else (line.z <= src) & (line.z > dest)

                    @pl.when(passes)
                    def _():
                        for side in range(2):
                            remote(wait, wait, self.zsem(0, src, dest, side), self.zsem(1, src, dest, side), line.mate, line.fsdp).wait_send()

            self.to_mate(src).wait_send()


LAG = 3


def weights_kernel(nctx, nfs, rows, w_ref, g_ref, o_ref, go_ref, passing, for_mate, zs, xs, own_sem, y_sem, c_sem, gown_sem, gp_sem, gy_sem, gc_sem):
    nz = nctx // NX
    line = Line(nz)
    ctx, fsdp = line.ctx, line.fsdp
    layers = w_ref.shape[0]
    y, core = fsdp // NCORE, fsdp % NCORE
    y_mate = (1 - y) * NCORE + core
    c_mate = y * NCORE + 1 - core
    y_c_mate = (1 - y) * NCORE + 1 - core
    barrier = pltpu.get_barrier_semaphore()
    for step in range(1, nctx):
        greet(barrier, (ctx + step) % nctx, fsdp)
    for other in (y_mate, c_mate):
        greet(barrier, ctx, other)
    pl.semaphore_wait(barrier, nctx + 1)

    def place(layer, s, f):
        return o_ref.at[layer, :, pl.ds(pl.multiple_of((s * nfs + f) * rows, rows), rows), :]

    def swap(layer):
        return Exchange(
            line,
            lambda to: w_ref.at[layer, to],
            lambda frm: place(layer, frm, fsdp),
            passing, for_mate, zs, xs,
            (layer,),
        )

    def over_y(layer, frm, f, ref=None):
        return remote(place(layer, frm, f) if ref is None else ref, place(layer, frm, f), y_sem.at[0, layer, frm], y_sem.at[1, layer, frm], ctx, y_mate)

    def over_c(layer, frm, f, k, ref=None):
        return remote(place(layer, frm, f) if ref is None else ref, place(layer, frm, f), c_sem.at[0, k, layer, frm], c_sem.at[1, k, layer, frm], ctx, c_mate)

    def own(layer):
        return pltpu.make_async_copy(w_ref.at[layer, ctx], place(layer, ctx, fsdp), own_sem.at[layer])

    def begin(layer):
        exchange = swap(layer)
        for i in range(nz - 1):
            exchange.send(line.far(i))
        exchange.send(line.z)
        over_y(layer, ctx, fsdp, w_ref.at[layer, ctx]).start()
        over_c(layer, ctx, fsdp, 0, w_ref.at[layer, ctx]).start()
        own(layer).start()

    def arrived(layer, frm):
        over_y(layer, frm, fsdp).start()
        over_c(layer, frm, fsdp, 0).start()

    def from_y(layer, frm):
        over_y(layer, frm, y_mate).wait_recv()
        over_c(layer, frm, y_mate, 1).start()

    def take(layer, i):
        exchange = swap(layer)
        for way, src, dest, real in exchange.events(i):

            @pl.when(real)
            def _():
                exchange.handle(way, src, dest, lambda frm: arrived(layer, frm))

        def mine(late, then):
            @pl.when(i == late)
            def _():
                then(line.z)

            for way, src, dest, real in exchange.events(i - late):

                @pl.when(real & (dest == line.z))
                def _():
                    then(src)

        def mates(src):
            exchange.mate_arrived(src)
            arrived(layer, src * NX + 1 - line.x)

        mine(1, mates)
        mine(2, lambda src: from_y(layer, src * NX + line.x))
        mine(3, lambda src: from_y(layer, src * NX + 1 - line.x))

    def small(to):
        return remote(g_ref.at[to], go_ref.at[ctx * nfs + fsdp], gp_sem.at[0, to], gp_sem.at[1, ctx], to, fsdp)

    def small_in(frm):
        return remote(g_ref.at[ctx], go_ref.at[frm * nfs + fsdp], gp_sem.at[0, frm], gp_sem.at[1, frm], frm, fsdp)

    def small_y(frm, f):
        return remote(go_ref.at[frm * nfs + f], go_ref.at[frm * nfs + f], gy_sem.at[0, frm], gy_sem.at[1, frm], ctx, y_mate)

    def small_c(frm, f, k):
        return remote(go_ref.at[frm * nfs + f], go_ref.at[frm * nfs + f], gc_sem.at[0, k, frm], gc_sem.at[1, k, frm], ctx, c_mate)

    small_own = pltpu.make_async_copy(g_ref.at[ctx], go_ref.at[ctx * nfs + fsdp], gown_sem)
    small_own.start()
    for step in range(1, nctx):
        small((ctx + step) % nctx).start()
    steps = 2 * nz - 3 + 3

    def step(i, carry):
        for layer in range(layers):
            at = i - LAG * layer

            @pl.when(at == 0)
            def _():
                begin(layer)

        def each(layer, carry):
            at = i - LAG * layer

            @pl.when((at > 0) & (at <= steps))
            def _():
                take(layer, at)

            return carry

        lax.fori_loop(0, layers, each, 0)
        return carry

    lax.fori_loop(0, steps + 1 + LAG * (layers - 1), step, 0)
    small_own.wait()
    for k in range(nctx):
        if k:
            small_in((ctx + k) % nctx).wait_recv()
        small_y((ctx + k) % nctx, fsdp).start()
        small_c((ctx + k) % nctx, fsdp, 0).start()
    for k in range(nctx):
        small_y((ctx + k) % nctx, y_mate).wait_recv()
        small_c((ctx + k) % nctx, y_mate, 1).start()
    for frm in range(nctx):
        small_c(frm, c_mate, 0).wait_recv()
        small_c(frm, y_c_mate, 1).wait_recv()
        small_c(frm, fsdp, 0).wait_send()
        small_c(frm, y_mate, 1).wait_send()
        small_y(frm, fsdp).wait_send()
    for step_ in range(1, nctx):
        small((ctx + step_) % nctx).wait_send()

    def close(layer, carry):
        own(layer).wait()
        for frm in range(nctx):
            over_c(layer, frm, c_mate, 0).wait_recv()
            over_c(layer, frm, y_c_mate, 1).wait_recv()
            over_c(layer, frm, fsdp, 0).wait_send()
            over_c(layer, frm, y_mate, 1).wait_send()
            over_y(layer, frm, fsdp).wait_send()
        swap(layer).finish()
        return carry

    lax.fori_loop(0, layers, close, 0)


def spread_weights(send, small, nfs):
    layers, nctx, mats, rows, width = send.shape
    return pl.pallas_call(
        functools.partial(weights_kernel, nctx, nfs, rows),
        out_shape=(
            jax.ShapeDtypeStruct((layers, mats, nctx * nfs * rows, width), send.dtype),
            jax.ShapeDtypeStruct((nctx * nfs,) + small.shape[1:], small.dtype),
        ),
        in_specs=[VM, VM],
        out_specs=(ANY, ANY),
        scratch_shapes=Exchange.scratch(nctx // NX, (mats, rows, width), (layers,))
        + [
            DMA((layers,)),
            DMA((2, layers, nctx)),
            DMA((2, 2, layers, nctx)),
            DMA,
            DMA((2, nctx)),
            DMA((2, nctx)),
            DMA((2, 2, nctx)),
        ],
        compiler_params=params(3, 40),
        name="spread_weights",
    )(send, small)


def grads_kernel(nctx, nfs, rows, normed_ref, dproj_ref, middle_ref, attended_ref, moe_ref, dgate_ref, dup_ref, grad_ref, inner_ref, e_ref,
                 o_ref, eo_ref, mine, cin, yin, half, full, e_cin, e_half, e_yin, e_full,
                 own_sem, c_sem, y_sem, p_sem, eown_sem, ec_sem, ey_sem, ep_sem):
    nz = nctx // NX
    line = Line(nz)
    ctx, fsdp = line.ctx, line.fsdp
    y, core = fsdp // NCORE, fsdp % NCORE
    y_mate = (1 - y) * NCORE + core
    c_mate = y * NCORE + 1 - core
    mats = mine.shape[0]
    proj = dproj_ref.shape[1]
    units = dgate_ref.shape[1] // 2
    slab = NX * nfs * rows
    barrier = pltpu.get_barrier_semaphore()
    for step in range(1, nctx):
        greet(barrier, (ctx + step) % nctx, fsdp)
    for other in (y_mate, c_mate):
        greet(barrier, ctx, other)
    pl.semaphore_wait(barrier, nctx + 1)

    def span(s, f):
        return pl.ds(pl.multiple_of((s * nfs + f) * rows, rows), rows)

    def to_c(s, k):
        f = (1 - y if k == 0 else y) * NCORE + 1 - core
        return remote(mine.at[:, span(s, f), :], cin.at[k, s], c_sem.at[0, k, s], c_sem.at[1, k, s], ctx, c_mate)

    def to_y(s):
        return remote(half.at[s], yin.at[s], y_sem.at[0, s], y_sem.at[1, s], ctx, y_mate)

    def out(s):
        return remote(full.at[s], o_ref.at[ctx], p_sem.at[0, s], p_sem.at[1, ctx], s, fsdp)

    def out_in(s):
        return remote(full.at[s], o_ref.at[s], p_sem.at[0, s], p_sem.at[1, s], s, fsdp)

    e_to_c = remote(e_ref.at[1 - core], e_cin, ec_sem.at[0], ec_sem.at[1], ctx, c_mate)
    e_to_y = remote(e_half.at[1 - y], e_yin, ey_sem.at[0], ey_sem.at[1], ctx, y_mate)

    def e_out(s):
        return remote(e_full.at[s], eo_ref.at[ctx], ep_sem.at[0, s], ep_sem.at[1, ctx], s, fsdp)

    def e_out_in(s):
        return remote(e_full.at[s], eo_ref.at[s], ep_sem.at[0, s], ep_sem.at[1, s], s, fsdp)

    e_to_c.start()
    own = pltpu.make_async_copy(full.at[ctx], o_ref.at[ctx], own_sem)
    e_own = pltpu.make_async_copy(e_full.at[ctx], eo_ref.at[ctx], eown_sem)

    turn_of = line.far

    def compute(row):
        lanes = pl.ds(pl.multiple_of(row * slab, 128), slab)
        tall = pl.ds(pl.multiple_of(row * slab, 16), slab)
        mine[0, tall, pl.ds(0, proj)] = dot(normed_ref[:, lanes], dproj_ref[...], TN).astype(BF)
        mine[0, tall, pl.ds(proj, mine.shape[2] - proj)] = dot(middle_ref[:, lanes], attended_ref[...], TN).astype(BF)
        moe = moe_ref[:, lanes]
        for e in range(2):
            part_of = pl.ds(e * units, units)
            mine[1 + e, tall, :] = dot(moe, dgate_ref[:, part_of], TN).astype(BF)
            mine[3 + e, tall, :] = dot(moe, dup_ref[:, part_of], TN).astype(BF)
            mine[5 + e, tall, :] = dot(grad_ref[:, lanes], inner_ref[:, part_of], TN).astype(BF)

    def first(s):
        to_c(s, 0).wait_recv()

        def one(m, _):
            half[s, m] = (mine[m, span(s, y_mate), :].astype(F32) + cin[0, s, m].astype(F32)).astype(BF)
            return 0

        lax.fori_loop(0, mats, one, 0)
        to_y(s).start()

    def second(s):
        to_c(s, 1).wait_recv()
        to_y(s).wait_recv()

        def one(m, _):
            full[s, m] = (mine[m, span(s, fsdp), :].astype(F32) + cin[1, s, m].astype(F32) + yin[s, m].astype(F32)).astype(BF)
            return 0

        lax.fori_loop(0, mats, one, 0)

        @pl.when(s != ctx)
        def _():
            out(s).start()

    def step(i, carry):
        @pl.when(i < nz)
        def _():
            row = turn_of(i)
            compute(row)
            for k in range(2):
                for side in range(NX):
                    to_c(row * NX + side, k).start()

        @pl.when((i >= 1) & (i < nz + 1))
        def _():
            for side in range(NX):
                first(turn_of(i - 1) * NX + side)

        @pl.when((i >= 2) & (i < nz + 2))
        def _():
            row = turn_of(i - 2)
            for side in range(NX):
                second(row * NX + side)

        return carry

    lax.fori_loop(0, nz + 2, step, 0)
    own.start()
    e_to_c.wait_recv()
    e_half[...] = e_ref[core] + e_cin[...]
    e_to_y.start()
    e_to_y.wait_recv()
    e_full[...] = e_half[y] + e_yin[...]
    e_own.start()
    for step_ in range(1, nctx):
        e_out((ctx + step_) % nctx).start()
    for s in range(nctx):
        for k in range(2):
            to_c(s, k).wait_send()
        to_y(s).wait_send()

        @pl.when(s != ctx)
        def _():
            out(s).wait_send()
            out_in(s).wait_recv()
            e_out(s).wait_send()
            e_out_in(s).wait_recv()

    e_to_c.wait_send()
    e_to_y.wait_send()
    e_own.wait()
    own.wait()


def collect_grads(nctx, nfs, normed, dproj, middle, attended, moe, dgate, dup, grad, inner, extra):
    width = normed.shape[1]
    rows = width // (nctx * nfs)
    mats, cols = 7, dproj.shape[1] + attended.shape[1]
    blk = (mats, rows, cols)
    tile = extra.shape[3:]
    return pl.pallas_call(
        functools.partial(grads_kernel, nctx, nfs, rows),
        out_shape=(jax.ShapeDtypeStruct((nctx,) + blk, BF), jax.ShapeDtypeStruct((nctx,) + tile, F32)),
        in_specs=[VM] * 10,
        out_specs=(ANY, ANY),
        scratch_shapes=[
            pltpu.VMEM((mats, width, cols), BF),
            pltpu.VMEM((2, nctx) + blk, BF),
            pltpu.VMEM((nctx,) + blk, BF),
            pltpu.VMEM((nctx,) + blk, BF),
            pltpu.VMEM((nctx,) + blk, BF),
            pltpu.VMEM((2, nctx) + tile, F32),
            pltpu.VMEM((2, nctx) + tile, F32),
            pltpu.VMEM((nctx,) + tile, F32),
            pltpu.VMEM((nctx,) + tile, F32),
            DMA,
            DMA((2, 2, nctx)),
            DMA((2, nctx)),
            DMA((2, nctx)),
            DMA,
            DMA((2,)),
            DMA((2,)),
            DMA((2, nctx)),
        ],
        compiler_params=params(4, 63),
        name="collect_grads",
    )(normed, dproj, middle, attended, moe, dgate, dup, grad, inner, extra)


def rope_tables(places):
    half_dim = HEAD_DIM // 2
    freq_steps = jnp.arange(half_dim, dtype=jnp.float32)
    inverse = jnp.exp(freq_steps * (-2.0 * math.log(10000.0) / HEAD_DIM))
    angles = places[:, None] * inverse[None, :]
    return jnp.cos(angles), jnp.sin(angles)


def turn(values, cos_part, sin_part):
    half_dim = HEAD_DIM // 2
    first_half = values[..., :half_dim]
    second_half = values[..., half_dim:]
    cos_part, sin_part = cos_part[:, None, :], sin_part[:, None, :]
    return jnp.concatenate(
        [first_half * cos_part - second_half * sin_part, second_half * cos_part + first_half * sin_part],
        axis=-1,
    )


def pack_weights(master_set, layer, nctx):
    query_weight, key_weight, value_weight, out_weight, attn_gain, moe_gain, gate_weight, up_weight, down_weight = master_set
    rows = query_weight.shape[1]

    def columns(master):
        low = master[layer].astype(BF).reshape(rows, nctx, -1)
        return low.transpose(1, 0, 2)

    attn = jnp.concatenate(
        [columns(query_weight), columns(key_weight), columns(value_weight), columns(out_weight)], axis=-1
    )

    def experts(master):
        low = master[layer].astype(BF)
        return low.reshape(nctx, -1, rows, low.shape[-1])

    send = jnp.concatenate(
        [attn[:, None], experts(gate_weight), experts(up_weight), experts(down_weight)], axis=1
    )
    gains = jnp.stack([attn_gain[layer], moe_gain[layer]]).astype(BF).astype(F32)
    return send, jnp.pad(gains, ((0, 0), (0, 128 - rows)))


def norm_back(values, gain, grad):
    scale = lax.rsqrt(jnp.mean(values * values, axis=-1, keepdims=True) + EPSILON)
    unit = values * scale
    grad_gain = jnp.sum(grad * unit, axis=0)
    pulled = grad * gain
    return scale * (pulled - unit * jnp.mean(pulled * unit, axis=-1, keepdims=True)), grad_gain


def fast_body(nctx, nfs, *args):
    (tokens, cotangent, lengths, tile_order, routes, gates), master_set = args[:6], args[6:]
    nz = nctx // NX
    rows_here, model_width = tokens.shape[1], tokens.shape[2]
    group_rows = rows_here * nctx
    ctx = lax.axis_index("ctx")
    seg_all, pos_all = layout(lengths[0], tile_order[0], group_rows)
    visible = (seg_all[:, None] == seg_all[None, :]) & (pos_all[None, :] <= pos_all[:, None])
    cos_part, sin_part = rope_tables(pos_all.astype(jnp.float32))
    score_scale = HEAD_DIM ** (-0.5)
    q_width = 3 * HEAD_DIM
    kv_at, v_at, o_at = q_width, q_width + HEAD_DIM, q_width + 2 * HEAD_DIM

    expert_ids = jnp.arange(EXPERTS, dtype=jnp.int32)
    table = jnp.sum(
        jnp.where(routes[:, 0, :, :, None] == expert_ids, gates[:, 0, :, :, None], 0.0), axis=-2
    )
    packed = [pack_weights(master_set, layer, nctx) for layer in range(LAYERS)]
    rows = packed[0][0].shape[2]
    gains = jnp.broadcast_to(jnp.concatenate([gain for _, gain in packed])[None], (nctx, 2 * LAYERS, 128))
    shares = table.transpose(2, 0, 1).reshape(nctx, 2, LAYERS, rows_here).transpose(0, 2, 1, 3)
    shares = shares.reshape(nctx, 2 * LAYERS, rows_here)
    pad = jnp.zeros((nctx, 8 - 2 * LAYERS, 128), F32)
    small = jnp.concatenate([gains, pad, shares, pad], axis=1)
    mats_all, small_all = spread_weights(jnp.stack([send for send, _ in packed]), small, nfs)
    shares = lax.dynamic_index_in_dim(
        small_all.reshape(nctx, nfs, 16, 128), lax.axis_index("fsdp"), 1, keepdims=False
    )
    fetched = [
        (
            mats_all[layer, 0],
            small_all[:, 2 * layer, :rows].reshape(-1),
            small_all[:, 2 * layer + 1, :rows].reshape(-1),
            shares[:, 8 + 2 * layer : 10 + 2 * layer].transpose(0, 2, 1),
        )
        for layer in range(LAYERS)
    ]

    hidden = tokens[0].astype(jnp.float32)
    records = []
    for layer in range(LAYERS):
        attn, attn_gain, moe_gain, share = fetched[layer]
        normed = rms_norm(hidden, attn_gain).astype(BF)
        normed_all = gather_rows(normed, nz).reshape(group_rows, model_width)
        proj = dot(normed_all, attn[:, :o_at], NN)
        turned = turn(proj[:, :v_at].reshape(group_rows, 4, HEAD_DIM), cos_part, sin_part).astype(BF)
        queries, keys = turned[:, :3], turned[:, 3]
        values = proj[:, v_at:].astype(BF)
        raw = jnp.einsum("qhd,kd->hqk", queries, keys, preferred_element_type=jnp.float32) * score_scale
        raw = jnp.where(visible[None], raw, NEGATIVE)
        peak = jnp.max(raw, axis=-1, keepdims=True)
        powers = jnp.exp(raw - peak)
        probs = powers / jnp.sum(powers, axis=-1, keepdims=True)
        attended = jnp.einsum("hqk,kd->qhd", probs.astype(BF), values, preferred_element_type=jnp.float32)
        attended = attended.reshape(group_rows, q_width).astype(BF)
        part = dot(attended, attn[:, o_at:], NT).astype(BF)
        middle = hidden + scatter_rows(part.reshape(nctx, rows_here, model_width), nz)

        moe_in = rms_norm(middle, moe_gain).astype(BF)
        moved, moe_all, gate_act, up_act = experts_forward(moe_in, share, mats_all, layer, nz)
        records.append((hidden, normed_all, queries, keys, values, probs, attended, middle, moe_all, gate_act, up_act))
        hidden = middle + moved

    output = hidden.astype(BF)
    grad = cotangent[0].astype(jnp.float32)
    collected = [None] * LAYERS
    for layer in reversed(range(LAYERS)):
        attn, attn_gain, moe_gain, share = fetched[layer]
        hidden, normed_all, queries, keys, values, probs, attended, middle, moe_all, gate_act, up_act = records[layer]
        grad_moe_in, grad_all, d_gate, d_up, inner = experts_backward(grad.astype(BF), share, mats_all, layer, gate_act, up_act, nz)
        through, grad_moe_gain = norm_back(middle, moe_gain, grad_moe_in)
        grad_middle = grad + through

        middle_all = gather_rows(grad_middle.astype(BF), nz).reshape(group_rows, model_width)
        grad_att = dot(middle_all, attn[:, o_at:], NN).astype(BF).reshape(group_rows, 3, HEAD_DIM)
        dp = jnp.einsum("qhd,kd->hqk", grad_att, values, preferred_element_type=jnp.float32)
        delta = jnp.sum(probs * dp, axis=-1, keepdims=True)
        d_scores = (probs * (dp - delta)).astype(BF)
        dq = jnp.einsum("hqk,kd->qhd", d_scores, keys, preferred_element_type=jnp.float32) * score_scale
        dk = jnp.einsum("hqk,qhd->kd", d_scores, queries, preferred_element_type=jnp.float32) * score_scale
        dv = jnp.einsum("hqk,qhd->kd", probs.astype(BF), grad_att, preferred_element_type=jnp.float32)
        back = turn(jnp.concatenate([dq, dk[:, None]], axis=1), cos_part, -sin_part)
        d_proj = jnp.concatenate([back.reshape(group_rows, v_at), dv], axis=1).astype(BF)
        part = dot(d_proj, attn[:, :o_at], NT).astype(BF)
        grad_normed = scatter_rows(part.reshape(nctx, rows_here, model_width), nz)
        through, grad_attn_gain = norm_back(hidden, attn_gain, grad_normed)
        grad = grad_middle + through

        extra = jnp.stack([grad_attn_gain, grad_moe_gain]).reshape(2, nctx, nfs // NCORE, NCORE, rows)
        extra = jnp.pad(extra.transpose(3, 2, 1, 0, 4), ((0, 0), (0, 0), (0, 0), (0, 6), (0, 128 - rows)))
        flat = [part.reshape(group_rows, -1) for part in (moe_all, d_gate, d_up, grad_all, inner)]
        collected[layer] = collect_grads(nctx, nfs, normed_all, d_proj, middle_all, attended, *flat, extra)

    def attn_part(low, high):
        return jnp.stack(
            [
                c[0][:, 0, :, low:high].transpose(1, 0, 2).reshape(c[0].shape[2], -1).astype(F32)
                for c in collected
            ]
        )

    def expert_part(first):
        return jnp.stack(
            [
                c[0][:, first : first + 2].reshape((EXPERTS,) + c[0].shape[2:]).astype(F32)
                for c in collected
            ]
        )

    def gain_part(kind):
        return jnp.stack([jnp.sum(c[1][:, kind, :rows], axis=0) for c in collected])

    return (
        output[None],
        grad[None],
        attn_part(0, kv_at),
        attn_part(kv_at, v_at),
        attn_part(v_at, o_at),
        attn_part(o_at, o_at + q_width),
        gain_part(0),
        gain_part(1),
        expert_part(1),
        expert_part(3),
        expert_part(5),
    )


def solution(mesh):
    placed = (
        P("fsdp", "ctx", None),
        P("fsdp", "ctx", None),
        P("fsdp", None),
        P("fsdp", None),
        P(None, "fsdp", "ctx", None),
        P(None, "fsdp", "ctx", None),
        P(None, ("ctx", "fsdp"), None),
        P(None, ("ctx", "fsdp"), None),
        P(None, ("ctx", "fsdp"), None),
        P(None, ("ctx", "fsdp"), None),
        P(None, ("ctx", "fsdp")),
        P(None, ("ctx", "fsdp")),
        P(None, None, ("ctx", "fsdp"), None),
        P(None, None, ("ctx", "fsdp"), None),
        P(None, None, ("ctx", "fsdp"), None),
    )
    nctx, nfs = mesh.shape["ctx"], mesh.shape["fsdp"]
    chosen = partial(fast_body, nctx, nfs) if (nctx, nfs) == (8, 4) else body
    return jax.shard_map(
        chosen,
        mesh=mesh,
        in_specs=placed,
        out_specs=(
            P("fsdp", "ctx", None),
            P("fsdp", "ctx", None),
            P(None, ("ctx", "fsdp"), None),
            P(None, ("ctx", "fsdp"), None),
            P(None, ("ctx", "fsdp"), None),
            P(None, ("ctx", "fsdp"), None),
            P(None, ("ctx", "fsdp")),
            P(None, ("ctx", "fsdp")),
            P(None, None, ("ctx", "fsdp"), None),
            P(None, None, ("ctx", "fsdp"), None),
            P(None, None, ("ctx", "fsdp"), None),
        ),
        check_vma=False,
    )
```

```python
from functools import partial
import functools
import math

import jax
import jax.numpy as jnp
from jax import lax
from jax.experimental import pallas as pl
from jax.experimental.pallas import tpu as pltpu
from jax.sharding import PartitionSpec as P

HEAD_DIM = 64
EXPERTS = 16
LAYERS = 2
TILE = 128
CAP = 80


EPSILON = 1e-06
NEGATIVE = -1e30


def layout(lengths, tile_order, group_rows):
    tile_count = tile_order.shape[0]
    row_ids = jnp.arange(group_rows, dtype=jnp.int32)
    in_tile = (row_ids // TILE)[:, None] == jnp.arange(tile_count, dtype=jnp.int32)[None, :]
    tile_of = jnp.sum(jnp.where(in_tile, tile_order[None, :], 0), axis=1, dtype=jnp.int32)
    anchor = tile_of * TILE + row_ids % TILE
    seq_ends = jnp.cumsum(lengths, dtype=jnp.int32)
    seq_starts = seq_ends - lengths
    segment = jnp.sum(
        (anchor[:, None] >= seq_ends[None, :]).astype(jnp.int32), axis=1, dtype=jnp.int32
    )
    picked = segment[:, None] == jnp.arange(lengths.shape[0], dtype=jnp.int32)[None, :]
    offset = jnp.sum(jnp.where(picked, seq_starts[None, :], 0), axis=1, dtype=jnp.int32)
    return (segment, anchor - offset)


def rms_norm(values, gain_vec):
    return (
        values * lax.rsqrt(jnp.mean(values * values, axis=-1, keepdims=True) + EPSILON) * gain_vec
    )


def rotate(values, places):
    half_dim = values.shape[-1] // 2
    freq_steps = jnp.arange(half_dim, dtype=jnp.float32)
    inverse = jnp.exp(freq_steps * (-2.0 * math.log(10000.0) / values.shape[-1]))
    angles = places[:, None] * inverse[None, :]
    cos_part = jnp.cos(angles)[:, None, :]
    sin_part = jnp.sin(angles)[:, None, :]
    first_half = values[..., :half_dim]
    second_half = values[..., half_dim:]
    return jnp.concatenate(
        [
            first_half * cos_part - second_half * sin_part,
            second_half * cos_part + first_half * sin_part,
        ],
        axis=-1,
    )


def rotate_back(grads_in, places):
    return jax.vjp(partial(rotate, places=places), jnp.zeros(grads_in.shape, jnp.float32))[1](
        grads_in
    )[0]


def mix_inner(gate_act, up_act):
    return jax.nn.silu(gate_act) * up_act


def split_halves(master):
    experts_here, rows_here, hidden_units = master.shape
    return (
        master.astype(jnp.bfloat16)
        .reshape(experts_here, rows_here, 2, hidden_units // 2)
        .transpose(0, 2, 1, 3)
        .reshape(2 * experts_here, rows_here, hidden_units // 2)
    )


def merge_halves(grads_in):
    halves_all, rows_here, half_units = grads_in.shape
    return (
        grads_in.reshape(halves_all // 2, 2, rows_here, half_units)
        .transpose(0, 2, 1, 3)
        .reshape(halves_all // 2, rows_here, 2 * half_units)
    )


def doubled(slots):
    return jnp.broadcast_to(slots[:, None], (slots.shape[0], 2) + slots.shape[1:]).reshape(
        (2 * slots.shape[0],) + slots.shape[1:]
    )


def fold_halves(parts):
    return jnp.sum(parts.reshape((parts.shape[0] // 2, 2) + parts.shape[1:]), axis=1)


def send_out(slots):
    return lax.all_to_all(slots, "ctx", split_axis=0, concat_axis=1, tiled=True)


def send_back(parts):
    return lax.all_to_all(
        parts.astype(jnp.bfloat16), "ctx", split_axis=1, concat_axis=0, tiled=True
    ).astype(parts.dtype)


def routing(route_ids, gate_share, rows_here):
    expert_ids = jnp.arange(EXPERTS, dtype=jnp.int32)
    chosen = (route_ids[:, :, None] == expert_ids[None, None, :]).astype(jnp.int32)
    member = jnp.sum(chosen, axis=1, dtype=jnp.int32)
    before = jnp.cumsum(member, axis=0, dtype=jnp.int32) - member
    rank_of = jnp.sum(chosen * before[:, None, :], axis=2, dtype=jnp.int32)
    slot_of = route_ids * CAP + rank_of
    token_ids = jnp.broadcast_to(jnp.arange(rows_here, dtype=jnp.int32)[:, None], route_ids.shape)
    flat_slots = slot_of.reshape(-1)
    slot_token = (
        jnp.full((EXPERTS * CAP,), rows_here, jnp.int32).at[flat_slots].set(token_ids.reshape(-1))
    )
    slot_share = jnp.zeros((EXPERTS * CAP,), jnp.float32).at[flat_slots].set(gate_share.reshape(-1))
    return (slot_of, slot_token, slot_share)


def key_block(key_rows, value_rows, token_meta, block_index, block_rows):
    seg_local, pos_local, seg_all, pos_all = token_meta
    first_row = block_index * block_rows
    key_part = lax.dynamic_slice_in_dim(key_rows, first_row, block_rows, 0)
    value_part = lax.dynamic_slice_in_dim(value_rows, first_row, block_rows, 0)
    seg_part = lax.dynamic_slice_in_dim(seg_all, first_row, block_rows, 0)
    pos_part = lax.dynamic_slice_in_dim(pos_all, first_row, block_rows, 0)
    visible = (seg_local[:, None] == seg_part[None, :]) & (pos_part[None, :] <= pos_local[:, None])
    return (key_part, value_part, visible)


def scores(queries, key_part, visible, score_scale):
    raw_scores = (
        jnp.einsum("qhgd,khd->hgqk", queries, key_part, preferred_element_type=jnp.float32)
        * score_scale
    )
    return jnp.where(visible[None, None], raw_scores, NEGATIVE)


def keep_same(running):
    return running


def attention_forward(queries, key_rows, value_rows, token_meta, block_rows, score_scale):
    block_count = key_rows.shape[0] // block_rows
    rows_here, heads_kv, groups = (queries.shape[0], queries.shape[1], queries.shape[2])

    def stat_step(block_index, running):
        key_part, value_part, visible = key_block(
            key_rows, value_rows, token_meta, block_index, block_rows
        )

        def stat_update(current):
            row_peak, denom_sum = current
            logits = scores(queries, key_part, visible, score_scale)
            new_peak = jnp.maximum(row_peak, jnp.max(logits, axis=-1))
            denom_sum = denom_sum * jnp.exp(row_peak - new_peak) + jnp.sum(
                jnp.exp(logits - new_peak[..., None]), axis=-1
            )
            return (new_peak, denom_sum)

        return lax.cond(jnp.any(visible), stat_update, keep_same, running)

    start_stats = (
        jnp.full((heads_kv, groups, rows_here), NEGATIVE, jnp.float32),
        jnp.zeros((heads_kv, groups, rows_here), jnp.float32),
    )
    row_peak, denom_sum = lax.fori_loop(0, block_count, stat_step, start_stats)

    def out_step(block_index, partial_sum):
        key_part, value_part, visible = key_block(
            key_rows, value_rows, token_meta, block_index, block_rows
        )

        def out_update(current):
            attn_probs = (
                jnp.exp(scores(queries, key_part, visible, score_scale) - row_peak[..., None])
                / denom_sum[..., None]
            )
            return current + jnp.einsum(
                "hgqk,khd->qhgd",
                attn_probs.astype(jnp.bfloat16),
                value_part,
                preferred_element_type=jnp.float32,
            )

        return lax.cond(jnp.any(visible), out_update, keep_same, partial_sum)

    attended = lax.fori_loop(
        0, block_count, out_step, jnp.zeros((rows_here, heads_kv, groups, HEAD_DIM), jnp.float32)
    )
    return ((row_peak, denom_sum), attended)


def attention_backward(
    queries, key_rows, value_rows, token_meta, softmax_stats, grad_attended, block_rows, score_scale
):
    row_peak, denom_sum = softmax_stats
    block_count = key_rows.shape[0] // block_rows

    def probs_for(key_part, visible):
        return (
            jnp.exp(scores(queries, key_part, visible, score_scale) - row_peak[..., None])
            / denom_sum[..., None]
        )

    def delta_step(block_index, partial_sum):
        key_part, value_part, visible = key_block(
            key_rows, value_rows, token_meta, block_index, block_rows
        )

        def delta_update(current):
            attn_probs = probs_for(key_part, visible)
            grad_probs = jnp.einsum(
                "qhgd,khd->hgqk", grad_attended, value_part, preferred_element_type=jnp.float32
            )
            return current + jnp.sum(attn_probs * grad_probs, axis=-1)

        return lax.cond(jnp.any(visible), delta_update, keep_same, partial_sum)

    delta_sum = lax.fori_loop(0, block_count, delta_step, jnp.zeros(denom_sum.shape, jnp.float32))

    def grad_step(block_index, running):
        key_part, value_part, visible = key_block(
            key_rows, value_rows, token_meta, block_index, block_rows
        )
        first_row = block_index * block_rows

        def grad_update(current):
            grad_queries, grad_keys, grad_values = current
            attn_probs = probs_for(key_part, visible)
            grad_probs = jnp.einsum(
                "qhgd,khd->hgqk", grad_attended, value_part, preferred_element_type=jnp.float32
            )
            grad_scores = (attn_probs * (grad_probs - delta_sum[..., None])).astype(jnp.bfloat16)
            grad_queries = grad_queries + jnp.einsum(
                "hgqk,khd->qhgd", grad_scores, key_part, preferred_element_type=jnp.float32
            )
            key_term = jnp.einsum(
                "hgqk,qhgd->khd", grad_scores, queries, preferred_element_type=jnp.float32
            )
            value_term = jnp.einsum(
                "hgqk,qhgd->khd",
                attn_probs.astype(jnp.bfloat16),
                grad_attended,
                preferred_element_type=jnp.float32,
            )
            grad_keys = lax.dynamic_update_slice_in_dim(
                grad_keys,
                lax.dynamic_slice_in_dim(grad_keys, first_row, block_rows, 0) + key_term,
                first_row,
                0,
            )
            grad_values = lax.dynamic_update_slice_in_dim(
                grad_values,
                lax.dynamic_slice_in_dim(grad_values, first_row, block_rows, 0) + value_term,
                first_row,
                0,
            )
            return (grad_queries, grad_keys, grad_values)

        return lax.cond(jnp.any(visible), grad_update, keep_same, running)

    start_grads = (
        jnp.zeros(queries.shape, jnp.float32),
        jnp.zeros(key_rows.shape, jnp.float32),
        jnp.zeros(value_rows.shape, jnp.float32),
    )
    return lax.fori_loop(0, block_count, grad_step, start_grads)


def fetch_layer(master_set, layer_index):
    (
        query_weight,
        key_weight,
        value_weight,
        out_weight,
        attn_gain,
        moe_gain,
        gate_weight,
        up_weight,
        down_weight,
    ) = master_set
    attn_set = (
        lax.all_gather(
            query_weight[layer_index].astype(jnp.bfloat16), ("ctx", "fsdp"), axis=0, tiled=True
        ),
        lax.all_gather(
            key_weight[layer_index].astype(jnp.bfloat16), ("ctx", "fsdp"), axis=0, tiled=True
        ),
        lax.all_gather(
            value_weight[layer_index].astype(jnp.bfloat16), ("ctx", "fsdp"), axis=0, tiled=True
        ),
        lax.all_gather(
            out_weight[layer_index].astype(jnp.bfloat16), ("ctx", "fsdp"), axis=0, tiled=True
        ),
        lax.all_gather(
            attn_gain[layer_index].astype(jnp.bfloat16), ("ctx", "fsdp"), axis=0, tiled=True
        ),
        lax.all_gather(
            moe_gain[layer_index].astype(jnp.bfloat16), ("ctx", "fsdp"), axis=0, tiled=True
        ),
    )
    row_set = (
        lax.all_gather(split_halves(gate_weight[layer_index]), "fsdp", axis=1, tiled=True),
        lax.all_gather(split_halves(up_weight[layer_index]), "fsdp", axis=1, tiled=True),
        lax.all_gather(split_halves(down_weight[layer_index]), "fsdp", axis=1, tiled=True),
    )
    expert_set = (
        lax.all_to_all(row_set[0], "ctx", split_axis=0, concat_axis=1, tiled=True),
        lax.all_to_all(row_set[1], "ctx", split_axis=0, concat_axis=1, tiled=True),
        lax.all_to_all(row_set[2], "ctx", split_axis=0, concat_axis=1, tiled=True),
    )
    return tuple(attn_set) + tuple(expert_set)


def layer_forward(hidden, weights, route_ids, gate_share, token_meta, places, block_rows):
    (
        query_full,
        key_full,
        value_full,
        out_full,
        attn_norm,
        moe_norm,
        gate_full,
        up_full,
        down_full,
    ) = weights
    rows_here, model_width = hidden.shape
    heads_all = query_full.shape[1] // HEAD_DIM
    heads_kv = key_full.shape[1] // HEAD_DIM
    groups = heads_all // heads_kv
    score_scale = HEAD_DIM ** (-0.5)
    normed = rms_norm(hidden, attn_norm.astype(jnp.float32)).astype(jnp.bfloat16)
    queries = rotate(
        jnp.dot(normed, query_full, preferred_element_type=jnp.float32).reshape(
            rows_here, heads_all, HEAD_DIM
        ),
        places,
    ).astype(jnp.bfloat16)
    key_new = (
        rotate(
            jnp.dot(normed, key_full, preferred_element_type=jnp.float32).reshape(
                rows_here, heads_kv, HEAD_DIM
            ),
            places,
        )
        .astype(jnp.bfloat16)
        .reshape(rows_here, heads_kv * HEAD_DIM)
    )
    value_new = jnp.dot(normed, value_full, preferred_element_type=jnp.float32).astype(jnp.bfloat16)
    key_rows, value_rows = (
        lax.all_gather(key_new, "ctx", axis=0, tiled=True),
        lax.all_gather(value_new, "ctx", axis=0, tiled=True),
    )
    key_rows = key_rows.reshape(-1, heads_kv, HEAD_DIM)
    value_rows = value_rows.reshape(-1, heads_kv, HEAD_DIM)
    queries = queries.reshape(rows_here, heads_kv, groups, HEAD_DIM)
    softmax_stats, attended = attention_forward(
        queries, key_rows, value_rows, token_meta, block_rows, score_scale
    )
    attended = attended.reshape(rows_here, heads_all * HEAD_DIM).astype(jnp.bfloat16)
    middle = hidden + jnp.einsum(
        "tx,dx->td", attended, out_full, preferred_element_type=jnp.float32
    )
    moe_in = rms_norm(middle, moe_norm.astype(jnp.float32)).astype(jnp.bfloat16)
    slot_of, slot_token, slot_share = routing(route_ids, gate_share, rows_here)
    padded = jnp.concatenate([moe_in, jnp.zeros((1, model_width), jnp.bfloat16)], axis=0)
    dispatched = jnp.take(padded, slot_token, axis=0).reshape(EXPERTS, CAP, model_width)
    owner_rows = send_out(doubled(dispatched))
    gate_act = jnp.einsum("ecd,edf->ecf", owner_rows, gate_full, preferred_element_type=jnp.float32)
    up_act = jnp.einsum("ecd,edf->ecf", owner_rows, up_full, preferred_element_type=jnp.float32)
    inner_act = mix_inner(gate_act, up_act).astype(jnp.bfloat16)
    expert_part = jnp.einsum(
        "ecf,edf->ecd", inner_act, down_full, preferred_element_type=jnp.float32
    )
    expert_out = fold_halves(send_back(expert_part))
    expert_out = expert_out.reshape(EXPERTS * CAP, model_width)
    moe_out = jnp.sum(jnp.take(expert_out, slot_of, axis=0) * gate_share[..., None], axis=1)
    record = (
        hidden,
        normed,
        queries,
        key_rows,
        value_rows,
        softmax_stats,
        attended,
        middle,
        moe_in,
        slot_of,
        slot_token,
        slot_share,
        owner_rows,
        gate_act,
        up_act,
        inner_act,
    )
    return (record, middle + moe_out)


def layer_backward(grad_hidden, record, weights, token_meta, places, block_rows):
    (
        hidden,
        normed,
        queries,
        key_rows,
        value_rows,
        softmax_stats,
        attended,
        middle,
        moe_in,
        slot_of,
        slot_token,
        slot_share,
        owner_rows,
        gate_act,
        up_act,
        inner_act,
    ) = record
    (
        query_full,
        key_full,
        value_full,
        out_full,
        attn_norm,
        moe_norm,
        gate_full,
        up_full,
        down_full,
    ) = weights
    rows_here, model_width = hidden.shape
    heads_kv, groups = (queries.shape[1], queries.shape[2])
    group_rows = key_rows.shape[0]
    score_scale = HEAD_DIM ** (-0.5)
    grad_padded = jnp.concatenate([grad_hidden, jnp.zeros((1, model_width), jnp.float32)], axis=0)
    grad_expert = (
        (jnp.take(grad_padded, slot_token, axis=0) * slot_share[:, None])
        .astype(jnp.bfloat16)
        .reshape(EXPERTS, CAP, model_width)
    )
    grad_owner = send_out(doubled(grad_expert))
    grad_down = jnp.einsum(
        "ecd,ecf->edf", grad_owner, inner_act, preferred_element_type=jnp.float32
    )
    grad_inner = jnp.einsum(
        "ecd,edf->ecf", grad_owner, down_full, preferred_element_type=jnp.float32
    )
    grad_gate_act, grad_up_act = jax.vjp(mix_inner, gate_act, up_act)[1](grad_inner)
    grad_gate_act = grad_gate_act.astype(jnp.bfloat16)
    grad_up_act = grad_up_act.astype(jnp.bfloat16)
    grad_gate = jnp.einsum(
        "ecd,ecf->edf", owner_rows, grad_gate_act, preferred_element_type=jnp.float32
    )
    grad_up = jnp.einsum(
        "ecd,ecf->edf", owner_rows, grad_up_act, preferred_element_type=jnp.float32
    )
    grad_owner_rows = jnp.einsum(
        "ecf,edf->ecd", grad_gate_act, gate_full, preferred_element_type=jnp.float32
    ) + jnp.einsum("ecf,edf->ecd", grad_up_act, up_full, preferred_element_type=jnp.float32)
    grad_dispatched = fold_halves(send_back(grad_owner_rows))
    home_set = (
        lax.all_to_all(
            grad_gate.astype(jnp.bfloat16), "ctx", split_axis=1, concat_axis=0, tiled=True
        ).astype(grad_gate.dtype),
        lax.all_to_all(
            grad_up.astype(jnp.bfloat16), "ctx", split_axis=1, concat_axis=0, tiled=True
        ).astype(grad_up.dtype),
        lax.all_to_all(
            grad_down.astype(jnp.bfloat16), "ctx", split_axis=1, concat_axis=0, tiled=True
        ).astype(grad_down.dtype),
    )
    summed_set = (
        lax.psum_scatter(
            home_set[0].astype(jnp.bfloat16), "fsdp", scatter_dimension=1, tiled=True
        ).astype(jnp.float32),
        lax.psum_scatter(
            home_set[1].astype(jnp.bfloat16), "fsdp", scatter_dimension=1, tiled=True
        ).astype(jnp.float32),
        lax.psum_scatter(
            home_set[2].astype(jnp.bfloat16), "fsdp", scatter_dimension=1, tiled=True
        ).astype(jnp.float32),
    )
    expert_grads = (
        merge_halves(summed_set[0]),
        merge_halves(summed_set[1]),
        merge_halves(summed_set[2]),
    )
    grad_moe_in = jnp.sum(
        jnp.take(grad_dispatched.reshape(EXPERTS * CAP, model_width), slot_of, axis=0), axis=1
    )
    grad_middle_part, grad_moe_norm = jax.vjp(rms_norm, middle, moe_norm.astype(jnp.float32))[1](
        grad_moe_in
    )
    grad_middle = grad_hidden + grad_middle_part
    grad_rounded = grad_middle.astype(jnp.bfloat16)
    grad_out_full = jnp.einsum(
        "td,tx->dx", grad_rounded, attended, preferred_element_type=jnp.float32
    )
    grad_attended = (
        jnp.dot(grad_rounded, out_full, preferred_element_type=jnp.float32)
        .astype(jnp.bfloat16)
        .reshape(rows_here, heads_kv, groups, HEAD_DIM)
    )
    grad_queries, grad_keys, grad_values = attention_backward(
        queries,
        key_rows,
        value_rows,
        token_meta,
        softmax_stats,
        grad_attended,
        block_rows,
        score_scale,
    )
    key_sums, value_sums = (
        lax.psum_scatter(
            grad_keys.reshape(group_rows, heads_kv * HEAD_DIM).astype(jnp.bfloat16),
            "ctx",
            scatter_dimension=0,
            tiled=True,
        ).astype(jnp.float32),
        lax.psum_scatter(
            grad_values.reshape(group_rows, heads_kv * HEAD_DIM).astype(jnp.bfloat16),
            "ctx",
            scatter_dimension=0,
            tiled=True,
        ).astype(jnp.float32),
    )
    grad_query_rows = (
        rotate_back(
            grad_queries.reshape(rows_here, heads_kv * groups, HEAD_DIM) * score_scale, places
        )
        .astype(jnp.bfloat16)
        .reshape(rows_here, heads_kv * groups * HEAD_DIM)
    )
    grad_key_rows = (
        rotate_back(key_sums.reshape(rows_here, heads_kv, HEAD_DIM) * score_scale, places)
        .astype(jnp.bfloat16)
        .reshape(rows_here, heads_kv * HEAD_DIM)
    )
    grad_value_rows = value_sums.astype(jnp.bfloat16)
    grad_query_full = jnp.einsum(
        "td,tx->dx", normed, grad_query_rows, preferred_element_type=jnp.float32
    )
    grad_key_full = jnp.einsum(
        "td,tx->dx", normed, grad_key_rows, preferred_element_type=jnp.float32
    )
    grad_value_full = jnp.einsum(
        "td,tx->dx", normed, grad_value_rows, preferred_element_type=jnp.float32
    )
    grad_normed = jnp.einsum(
        "tx,dx->td", grad_query_rows, query_full, preferred_element_type=jnp.float32
    )
    grad_normed = grad_normed + jnp.einsum(
        "tx,dx->td", grad_key_rows, key_full, preferred_element_type=jnp.float32
    )
    grad_normed = grad_normed + jnp.einsum(
        "tx,dx->td", grad_value_rows, value_full, preferred_element_type=jnp.float32
    )
    grad_hidden_part, grad_attn_norm = jax.vjp(rms_norm, hidden, attn_norm.astype(jnp.float32))[1](
        grad_normed
    )
    attn_grads = (
        lax.psum_scatter(grad_query_full, ("ctx", "fsdp"), scatter_dimension=0, tiled=True),
        lax.psum_scatter(grad_key_full, ("ctx", "fsdp"), scatter_dimension=0, tiled=True),
        lax.psum_scatter(grad_value_full, ("ctx", "fsdp"), scatter_dimension=0, tiled=True),
        lax.psum_scatter(grad_out_full, ("ctx", "fsdp"), scatter_dimension=0, tiled=True),
        lax.psum_scatter(grad_attn_norm, ("ctx", "fsdp"), scatter_dimension=0, tiled=True),
        lax.psum_scatter(grad_moe_norm, ("ctx", "fsdp"), scatter_dimension=0, tiled=True),
    )
    return (grad_middle + grad_hidden_part, attn_grads, expert_grads)


def body(
    tokens,
    cotangent,
    lengths,
    tile_order,
    routes,
    gates,
    query_weight,
    key_weight,
    value_weight,
    out_weight,
    attn_gain,
    moe_gain,
    gate_weight,
    up_weight,
    down_weight,
):
    rows_here = tokens.shape[1]
    group_rows = rows_here * lax.axis_size("ctx")
    seg_all, pos_all = layout(lengths[0], tile_order[0], group_rows)
    first_row = lax.axis_index("ctx") * rows_here
    seg_local = lax.dynamic_slice_in_dim(seg_all, first_row, rows_here, 0)
    pos_local = lax.dynamic_slice_in_dim(pos_all, first_row, rows_here, 0)
    token_meta = (seg_local, pos_local, seg_all, pos_all)
    places = pos_local.astype(jnp.float32)
    block_rows = math.gcd(group_rows, 512)
    master_set = (
        query_weight,
        key_weight,
        value_weight,
        out_weight,
        attn_gain,
        moe_gain,
        gate_weight,
        up_weight,
        down_weight,
    )
    hidden = tokens[0].astype(jnp.float32)
    records = []
    for layer_index in range(LAYERS):
        weights = fetch_layer(master_set, layer_index)
        record, hidden = layer_forward(
            hidden,
            weights,
            routes[layer_index, 0],
            gates[layer_index, 0],
            token_meta,
            places,
            block_rows,
        )
        records.append(record)
    grad_hidden = cotangent[0].astype(jnp.float32)
    attn_layers = []
    expert_layers = []
    for layer_index in reversed(range(LAYERS)):
        weights = fetch_layer(master_set, layer_index)
        grad_hidden, attn_grads, expert_grads = layer_backward(
            grad_hidden, records[layer_index], weights, token_meta, places, block_rows
        )
        attn_layers.insert(0, attn_grads)
        expert_layers.insert(0, expert_grads)
    grad_query_weight = jnp.stack([layer_grads[0] for layer_grads in attn_layers])
    grad_key_weight = jnp.stack([layer_grads[1] for layer_grads in attn_layers])
    grad_value_weight = jnp.stack([layer_grads[2] for layer_grads in attn_layers])
    grad_out_weight = jnp.stack([layer_grads[3] for layer_grads in attn_layers])
    grad_attn_gain = jnp.stack([layer_grads[4] for layer_grads in attn_layers])
    grad_moe_gain = jnp.stack([layer_grads[5] for layer_grads in attn_layers])
    grad_gate_weight = jnp.stack([layer_grads[0] for layer_grads in expert_layers])
    grad_up_weight = jnp.stack([layer_grads[1] for layer_grads in expert_layers])
    grad_down_weight = jnp.stack([layer_grads[2] for layer_grads in expert_layers])
    return (
        hidden.astype(jnp.bfloat16)[None],
        grad_hidden[None],
        grad_query_weight,
        grad_key_weight,
        grad_value_weight,
        grad_out_weight,
        grad_attn_gain,
        grad_moe_gain,
        grad_gate_weight,
        grad_up_weight,
        grad_down_weight,
    )


BF = jnp.bfloat16
F32 = jnp.float32
NX = 2
NCORE = 2
ANY = pl.BlockSpec(memory_space=pl.ANY)
VM = pl.BlockSpec(memory_space=pltpu.VMEM)
DMA = pltpu.SemaphoreType.DMA

NN = ((1,), (0,))
NT = ((1,), (1,))
TN = ((0,), (0,))


def dot(left, right, dims):
    return lax.dot_general(left, right, (dims, ((), ())), preferred_element_type=jnp.float32)


def remote(src, dst, send_sem, recv_sem, ctx, fsdp):
    return pltpu.make_async_remote_copy(
        src_ref=src,
        dst_ref=dst,
        send_sem=send_sem,
        recv_sem=recv_sem,
        device_id={"ctx": ctx, "fsdp": fsdp},
        device_id_type=pl.DeviceIdType.MESH,
    )


def greet(barrier, ctx, fsdp):
    pl.semaphore_signal(
        barrier, inc=1, device_id={"ctx": ctx, "fsdp": fsdp}, device_id_type=pl.DeviceIdType.MESH
    )


class Line:
    def __init__(self, nz):
        self.nz = nz
        self.ctx, self.fsdp = lax.axis_index("ctx"), lax.axis_index("fsdp")
        self.z, self.x = self.ctx // NX, self.ctx % NX
        self.mate = self.z * NX + 1 - self.x
        self.above = (self.z + 1) * NX + self.x
        self.below = (self.z - 1) * NX + self.x

    def greet(self):
        barrier = pltpu.get_barrier_semaphore()
        greet(barrier, self.mate, self.fsdp)

        @pl.when(self.z > 0)
        def _():
            greet(barrier, self.below, self.fsdp)

        @pl.when(self.z < self.nz - 1)
        def _():
            greet(barrier, self.above, self.fsdp)

        ends = jnp.where(self.z > 0, 1, 0) + jnp.where(self.z < self.nz - 1, 1, 0)
        pl.semaphore_wait(barrier, 1 + ends)

    def near(self, i):
        z, nz = self.z, self.nz
        mid1 = jnp.where(i == 0, 1, jnp.where(i == 1, 0, i))
        mid2 = jnp.where(i == 0, 2, jnp.where(i == 1, 1, jnp.where(i == 2, 3, 0)))
        return jnp.where(z == 0, i, jnp.where(z == nz - 1, nz - 1 - i, jnp.where(z == 1, mid1, mid2)))

    def far(self, i):
        z, nz = self.z, self.nz
        mid1 = jnp.where(i == 0, 3, jnp.where(i == 1, 0, jnp.where(i == 2, 2, 1)))
        mid2 = jnp.where(i == 0, 0, jnp.where(i == 1, 3, jnp.where(i == 2, 1, 2)))
        return jnp.where(z == 0, nz - 1 - i, jnp.where(z == nz - 1, i, jnp.where(z == 1, mid1, mid2)))


class Gather:
    @staticmethod
    def scratch(nz):
        return [DMA((6, nz))]

    def __init__(self, line, own_ref, all_ref, sems):
        self.line, self.own, self.all, self.sems = line, own_ref, all_ref, sems

    def block(self, row):
        return self.all.at[row * NX + self.line.x]

    def up(self, t, src=None):
        line = self.line
        block = self.block(line.z - t)
        return remote(block if src is None else src, block, self.sems.at[0, t], self.sems.at[1, t], line.above, line.fsdp)

    def down(self, t, src=None):
        line = self.line
        block = self.block(line.z + t)
        return remote(block if src is None else src, block, self.sems.at[2, t], self.sems.at[3, t], line.below, line.fsdp)

    def across(self, row, src=None):
        line = self.line
        block = self.block(row)
        return remote(block if src is None else src, block, self.sems.at[4, row], self.sems.at[5, row], line.mate, line.fsdp)

    def start(self):
        line = self.line

        @pl.when(line.z < line.nz - 1)
        def _():
            self.up(0, self.own).start()

        @pl.when(line.z > 0)
        def _():
            self.down(0, self.own).start()

        self.across(line.z, self.own).start()

    def forward(self, t):
        line = self.line

        @pl.when(line.z - 1 - t >= 0)
        def _():
            remote(self.own, self.block(line.z - 1 - t), self.sems.at[0, t], self.sems.at[1, t], line.above, line.fsdp).wait_recv()

            @pl.when(line.z < line.nz - 1)
            def _():
                self.up(t + 1).start()

            self.across(line.z - 1 - t).start()

        @pl.when(line.z + 1 + t < line.nz)
        def _():
            remote(self.own, self.block(line.z + 1 + t), self.sems.at[2, t], self.sems.at[3, t], line.below, line.fsdp).wait_recv()

            @pl.when(line.z > 0)
            def _():
                self.down(t + 1).start()

            self.across(line.z + 1 + t).start()

    def wait_pair(self, row):
        line = self.line
        remote(self.own, self.all.at[row * NX + 1 - line.x], self.sems.at[4, row], self.sems.at[5, row], line.mate, line.fsdp).wait_recv()

    def finish(self):
        line = self.line
        for t in range(line.nz - 1):

            @pl.when((line.z - t >= 0) & (line.z < line.nz - 1))
            def _():
                self.up(t).wait_send()

            @pl.when((line.z + t < line.nz) & (line.z > 0))
            def _():
                self.down(t).wait_send()

        for row in range(line.nz):
            self.across(row).wait_send()


class Scatter:
    @staticmethod
    def scratch(nz, rows, width):
        return [pltpu.VMEM((4, nz, rows, width), BF), DMA((6, nz))]

    def __init__(self, line, part_ref, out_ref, work, sems):
        self.line, self.part, self.out, self.sems = line, part_ref, out_ref, sems
        self.xin, self.acc, self.upin, self.downin = (work.at[i] for i in range(4))

    def across(self, row):
        line = self.line
        return remote(self.part.at[row * NX + 1 - line.x], self.xin.at[row], self.sems.at[0, row], self.sems.at[1, row], line.mate, line.fsdp)

    def up(self, row):
        line = self.line
        return remote(self.acc.at[row], self.upin.at[row], self.sems.at[2, row], self.sems.at[3, row], line.above, line.fsdp)

    def down(self, row):
        line = self.line
        return remote(self.acc.at[row], self.downin.at[row], self.sems.at[4, row], self.sems.at[5, row], line.below, line.fsdp)

    def add(self, i):
        line = self.line
        row = line.far(i)
        self.across(row).wait_recv()
        mine = self.part[row * NX + line.x].astype(F32) + self.xin[row].astype(F32)

        @pl.when(row > line.z)
        def _():
            @pl.when(line.z == 0)
            def _():
                self.acc[row] = mine.astype(BF)

            @pl.when(line.z > 0)
            def _():
                self.up(row).wait_recv()
                self.acc[row] = (mine + self.upin[row].astype(F32)).astype(BF)

            self.up(row).start()

        @pl.when(row < line.z)
        def _():
            @pl.when(line.z == line.nz - 1)
            def _():
                self.acc[row] = mine.astype(BF)

            @pl.when(line.z < line.nz - 1)
            def _():
                self.down(row).wait_recv()
                self.acc[row] = (mine + self.downin[row].astype(F32)).astype(BF)

            self.down(row).start()

        @pl.when(row == line.z)
        def _():
            self.out[...] = mine

    def finish(self):
        line = self.line

        @pl.when(line.z > 0)
        def _():
            self.up(line.z).wait_recv()
            self.out[...] += self.upin[line.z].astype(F32)

        @pl.when(line.z < line.nz - 1)
        def _():
            self.down(line.z).wait_recv()
            self.out[...] += self.downin[line.z].astype(F32)

        for row in range(line.nz):
            self.across(row).wait_send()

            @pl.when(row > line.z)
            def _():
                self.up(row).wait_send()

            @pl.when(row < line.z)
            def _():
                self.down(row).wait_send()


def params(collective, vmem_mib):
    return pltpu.CompilerParams(collective_id=collective, has_side_effects=True, vmem_limit_bytes=vmem_mib << 20)


def gather_kernel(nz, x_ref, o_ref, own_sem, sems):
    line = Line(nz)
    line.greet()
    ring = Gather(line, x_ref, o_ref, sems)
    ring.start()
    own = pltpu.make_async_copy(x_ref, o_ref.at[line.ctx], own_sem)
    own.start()
    for t in range(nz - 1):
        ring.forward(t)
    for row in range(nz):
        ring.wait_pair(row)
    ring.finish()
    own.wait()


def gather_rows(block, nz):
    rows, width = block.shape
    return pl.pallas_call(
        functools.partial(gather_kernel, nz),
        out_shape=jax.ShapeDtypeStruct((nz * NX, rows, width), block.dtype),
        in_specs=[VM],
        out_specs=ANY,
        scratch_shapes=[DMA] + Gather.scratch(nz),
        compiler_params=params(1, 16),
        name="gather_rows",
    )(block)


def scatter_kernel(nz, p_ref, o_ref, work, sems):
    line = Line(nz)
    line.greet()
    ring = Scatter(line, p_ref, o_ref, work, sems)
    for i in range(nz):
        ring.across(line.far(i)).start()
    for i in range(nz):
        ring.add(i)
    ring.finish()


def scatter_rows(parts, nz):
    _, rows, width = parts.shape
    return pl.pallas_call(
        functools.partial(scatter_kernel, nz),
        out_shape=jax.ShapeDtypeStruct((rows, width), F32),
        in_specs=[VM],
        out_specs=VM,
        scratch_shapes=Scatter.scratch(nz, rows, width),
        compiler_params=params(2, 32),
        name="scatter_rows",
    )(parts)


def experts_kernel(nz, layer, x_ref, share_ref, mats_ref, o_ref, all_out, gate_out, up_out,
                   mats, blocks, part, gate, up, load_sem, save_sem, gsems, work, ssems):
    line = Line(nz)
    rows, width = x_ref.shape
    load = pltpu.make_async_copy(mats_ref.at[layer, pl.ds(1, 6)], mats, load_sem)
    load.start()
    line.greet()
    ring = Gather(line, x_ref, blocks, gsems)
    ring.start()
    blocks[line.ctx] = x_ref[...]
    load.wait()

    def saves(row):
        pair = pl.ds(row * NX, NX)
        return (
            pltpu.make_async_copy(blocks.at[pair], all_out.at[pair], save_sem.at[0, row]),
            pltpu.make_async_copy(gate.at[pair], gate_out.at[pair], save_sem.at[1, row]),
            pltpu.make_async_copy(up.at[pair], up_out.at[pair], save_sem.at[2, row]),
        )

    def step(i, carry):
        @pl.when(i < nz - 1)
        def _():
            ring.forward(i)

        row = line.near(i)
        ring.wait_pair(row)
        pair = pl.ds(row * NX, NX)
        block = blocks[pair].reshape(NX * rows, width)
        share = share_ref[pair].reshape(NX * rows, 2)
        total = None
        for e in range(2):
            gate_act = dot(block, mats[e], NN)
            up_act = dot(block, mats[2 + e], NN)
            units = gate_act.shape[1]
            gate[pair, :, pl.ds(e * units, units)] = gate_act.astype(BF).reshape(NX, rows, units)
            up[pair, :, pl.ds(e * units, units)] = up_act.astype(BF).reshape(NX, rows, units)
            inner = gate_act / (1.0 + jnp.exp(-gate_act)) * up_act * share[:, e : e + 1]
            term = dot(inner.astype(BF), mats[4 + e], NT)
            total = term if total is None else total + term
        part[pair] = total.astype(BF).reshape(NX, rows, width)
        for save in saves(row):
            save.start()
        return carry

    lax.fori_loop(0, nz, step, 0)
    sums = Scatter(line, part, o_ref, work, ssems)
    for i in range(nz):
        sums.across(line.far(i)).start()
    ring.finish()
    for i in range(nz):
        sums.add(i)
    sums.finish()
    for row in range(nz):
        for save in saves(row):
            save.wait()


def experts_forward(block, share, mats, layer, nz):
    rows, width = block.shape
    units = mats.shape[3]
    group = nz * NX
    acts = jax.ShapeDtypeStruct((group, rows, 2 * units), BF)
    return pl.pallas_call(
        functools.partial(experts_kernel, nz, layer),
        out_shape=(
            jax.ShapeDtypeStruct((rows, width), F32),
            jax.ShapeDtypeStruct((group, rows, width), BF),
            acts,
            acts,
        ),
        in_specs=[VM, VM, ANY],
        out_specs=(VM, ANY, ANY, ANY),
        scratch_shapes=[
            pltpu.VMEM((6, width, units), BF),
            pltpu.VMEM((group, rows, width), BF),
            pltpu.VMEM((group, rows, width), BF),
            pltpu.VMEM((group, rows, 2 * units), BF),
            pltpu.VMEM((group, rows, 2 * units), BF),
            DMA,
            DMA((3, nz)),
        ]
        + Gather.scratch(nz)
        + Scatter.scratch(nz, rows, width),
        compiler_params=params(5 + 2 * layer, 60),
        name="experts_forward",
    )(block, share, mats)


def experts_back_kernel(nz, layer, x_ref, share_ref, mats_ref, gate_ref, up_ref, o_ref, all_out, dgate_out, dup_out, inner_out,
                        mats, blocks, part, gate, up, inners, load_sem, save_sem, gsems, work, ssems):
    line = Line(nz)
    rows, width = x_ref.shape
    loads = (
        pltpu.make_async_copy(mats_ref.at[layer, pl.ds(1, 6)], mats, load_sem.at[0]),
        pltpu.make_async_copy(gate_ref, gate, load_sem.at[1]),
        pltpu.make_async_copy(up_ref, up, load_sem.at[2]),
    )
    for load in loads:
        load.start()
    line.greet()
    ring = Gather(line, x_ref, blocks, gsems)
    ring.start()
    blocks[line.ctx] = x_ref[...]
    for load in loads:
        load.wait()

    def saves(row):
        pair = pl.ds(row * NX, NX)
        return (
            pltpu.make_async_copy(blocks.at[pair], all_out.at[pair], save_sem.at[0, row]),
            pltpu.make_async_copy(gate.at[pair], dgate_out.at[pair], save_sem.at[1, row]),
            pltpu.make_async_copy(up.at[pair], dup_out.at[pair], save_sem.at[2, row]),
            pltpu.make_async_copy(inners.at[pair], inner_out.at[pair], save_sem.at[3, row]),
        )

    def step(i, carry):
        @pl.when(i < nz - 1)
        def _():
            ring.forward(i)

        row = line.near(i)
        ring.wait_pair(row)
        pair = pl.ds(row * NX, NX)
        block = blocks[pair].reshape(NX * rows, width)
        share = share_ref[pair].reshape(NX * rows, 2)
        total = None
        units = mats.shape[2]
        for e in range(2):
            part_of = pl.ds(e * units, units)
            gate_act = gate[pair, :, part_of].reshape(NX * rows, units).astype(F32)
            up_act = up[pair, :, part_of].reshape(NX * rows, units).astype(F32)
            grad_inner = dot(block, mats[4 + e], NN) * share[:, e : e + 1]
            sigmoid = 1.0 / (1.0 + jnp.exp(-gate_act))
            silu = gate_act * sigmoid
            d_gate = (grad_inner * up_act * (sigmoid + silu * (1.0 - sigmoid))).astype(BF)
            d_up = (grad_inner * silu).astype(BF)
            inners[pair, :, part_of] = (silu * up_act * share[:, e : e + 1]).astype(BF).reshape(NX, rows, units)
            gate[pair, :, part_of] = d_gate.reshape(NX, rows, units)
            up[pair, :, part_of] = d_up.reshape(NX, rows, units)
            term = dot(d_gate, mats[e], NT) + dot(d_up, mats[2 + e], NT)
            total = term if total is None else total + term
        part[pair] = total.astype(BF).reshape(NX, rows, width)
        for save in saves(row):
            save.start()
        return carry

    lax.fori_loop(0, nz, step, 0)
    sums = Scatter(line, part, o_ref, work, ssems)
    for i in range(nz):
        sums.across(line.far(i)).start()
    ring.finish()
    for i in range(nz):
        sums.add(i)
    sums.finish()
    for row in range(nz):
        for save in saves(row):
            save.wait()


def experts_backward(block, share, mats, layer, gate_act, up_act, nz):
    rows, width = block.shape
    units = mats.shape[3]
    group = nz * NX
    acts = jax.ShapeDtypeStruct((group, rows, 2 * units), BF)
    held = pltpu.VMEM((group, rows, 2 * units), BF)
    return pl.pallas_call(
        functools.partial(experts_back_kernel, nz, layer),
        out_shape=(
            jax.ShapeDtypeStruct((rows, width), F32),
            jax.ShapeDtypeStruct((group, rows, width), BF),
            acts,
            acts,
            acts,
        ),
        in_specs=[VM, VM, ANY, ANY, ANY],
        out_specs=(VM, ANY, ANY, ANY, ANY),
        scratch_shapes=[
            pltpu.VMEM((6, width, units), BF),
            pltpu.VMEM((group, rows, width), BF),
            pltpu.VMEM((group, rows, width), BF),
            held,
            held,
            held,
            DMA((3,)),
            DMA((4, nz)),
        ]
        + Gather.scratch(nz)
        + Scatter.scratch(nz, rows, width),
        compiler_params=params(6 + 2 * layer, 60),
        name="experts_backward",
    )(block, share, mats, gate_act, up_act)


def far_of(nz, z, i):
    mid1 = jnp.where(i == 0, 3, jnp.where(i == 1, 0, jnp.where(i == 2, 2, 1)))
    mid2 = jnp.where(i == 0, 0, jnp.where(i == 1, 3, jnp.where(i == 2, 1, 2)))
    return jnp.where(z == 0, nz - 1 - i, jnp.where(z == nz - 1, i, jnp.where(z == 1, mid1, mid2)))


class Exchange:
    @staticmethod
    def scratch(nz, blk, lead=()):
        return [
            pltpu.VMEM(lead + (2, 2, 2) + blk, BF),
            pltpu.VMEM(lead + (nz,) + blk, BF),
            DMA(lead + (2, nz, nz, 2)),
            DMA(lead + (2, nz)),
        ]

    def __init__(self, line, src_at, dst_at, passing, for_mate, zs, xs, lead=()):
        self.line, self.src_at, self.dst_at, self.lead = line, src_at, dst_at, lead
        self.passing, self.for_mate, self.zs, self.xs = passing, for_mate, zs, xs

    def held(self, way, src, dest, side, at):
        last = self.line.nz - 1
        slot = (dest - at - 1) + src if way == 0 else (at - dest - 1) + last - src
        return self.passing.at[self.lead + (way, slot, side)]

    def zsem(self, kind, src, dest, side):
        return self.zs.at[self.lead + (kind, src, dest, side)]

    def hop(self, way, src, dest, side, ref):
        line = self.line
        to = line.z + 1 if way == 0 else line.z - 1
        sems = self.zsem(0, src, dest, side), self.zsem(1, src, dest, side)
        target = to * NX + line.x

        @pl.when(dest == to)
        def _():
            land = self.dst_at(src * NX + line.x) if side == 0 else self.for_mate.at[self.lead + (src,)]
            remote(ref, land, *sems, target, line.fsdp).start()

        @pl.when(dest != to)
        def _():
            remote(ref, self.held(way, src, dest, side, to), *sems, target, line.fsdp).start()

    def to_mate(self, src, ref=None):
        line = self.line
        ref = self.for_mate.at[self.lead + (src,)] if ref is None else ref
        return remote(ref, self.dst_at(src * NX + line.x), self.xs.at[self.lead + (0, src)], self.xs.at[self.lead + (1, src)], line.mate, line.fsdp)

    def send(self, dest):
        line = self.line
        for side, column in ((0, line.x), (1, 1 - line.x)):
            ref = self.src_at(dest * NX + column)

            @pl.when(dest > line.z)
            def _():
                self.hop(0, line.z, dest, side, ref)

            @pl.when(dest < line.z)
            def _():
                self.hop(1, line.z, dest, side, ref)

        @pl.when(dest == line.z)
        def _():
            self.to_mate(line.z, self.src_at(line.mate)).start()

    def events(self, i):
        line = self.line
        found = []
        for k in range(1, line.nz):
            j = i - k
            for way in range(2):
                src = line.z - k if way == 0 else line.z + k
                dest = far_of(line.nz, src, j)
                here = (dest >= line.z) if way == 0 else (dest <= line.z)
                found.append((way, src, dest, (src >= 0) & (src < line.nz) & (j >= 0) & (j < line.nz - 1) & here))
        return found

    def handle(self, way, src, dest, arrived):
        line = self.line
        for side in range(2):
            wait = self.held(way, 0 if way == 0 else line.nz - 1, line.z + 1 if way == 0 else line.z - 1, side, line.z)
            remote(wait, wait, self.zsem(0, src, dest, side), self.zsem(1, src, dest, side), line.mate, line.fsdp).wait_recv()

            @pl.when(dest != line.z)
            def _():
                self.hop(way, src, dest, side, self.held(way, src, dest, side, line.z))

        @pl.when(dest == line.z)
        def _():
            self.to_mate(src).start()
            arrived(src * NX + line.x)

    def mate_arrived(self, src):
        line = self.line
        wait = self.for_mate.at[self.lead + (src,)]
        remote(wait, wait, self.xs.at[self.lead + (0, src)], self.xs.at[self.lead + (1, src)], line.mate, line.fsdp).wait_recv()

    def finish(self):
        line = self.line
        wait = self.for_mate.at[self.lead + (0,)]
        for src in range(line.nz):
            for dest in range(line.nz):
                if src != dest:
                    passes = (line.z >= src) & (line.z < dest) if src < dest else (line.z <= src) & (line.z > dest)

                    @pl.when(passes)
                    def _():
                        for side in range(2):
                            remote(wait, wait, self.zsem(0, src, dest, side), self.zsem(1, src, dest, side), line.mate, line.fsdp).wait_send()

            self.to_mate(src).wait_send()


LAG = 3


def weights_kernel(nctx, nfs, rows, w_ref, g_ref, o_ref, go_ref, passing, for_mate, zs, xs, own_sem, y_sem, c_sem, gown_sem, gp_sem, gy_sem, gc_sem):
    nz = nctx // NX
    line = Line(nz)
    ctx, fsdp = line.ctx, line.fsdp
    layers = w_ref.shape[0]
    y, core = fsdp // NCORE, fsdp % NCORE
    y_mate = (1 - y) * NCORE + core
    c_mate = y * NCORE + 1 - core
    y_c_mate = (1 - y) * NCORE + 1 - core
    barrier = pltpu.get_barrier_semaphore()
    for step in range(1, nctx):
        greet(barrier, (ctx + step) % nctx, fsdp)
    for other in (y_mate, c_mate):
        greet(barrier, ctx, other)
    pl.semaphore_wait(barrier, nctx + 1)

    def place(layer, s, f):
        return o_ref.at[layer, :, pl.ds(pl.multiple_of((s * nfs + f) * rows, rows), rows), :]

    def swap(layer):
        return Exchange(
            line,
            lambda to: w_ref.at[layer, to],
            lambda frm: place(layer, frm, fsdp),
            passing, for_mate, zs, xs,
            (layer,),
        )

    def over_y(layer, frm, f, ref=None):
        return remote(place(layer, frm, f) if ref is None else ref, place(layer, frm, f), y_sem.at[0, layer, frm], y_sem.at[1, layer, frm], ctx, y_mate)

    def over_c(layer, frm, f, k, ref=None):
        return remote(place(layer, frm, f) if ref is None else ref, place(layer, frm, f), c_sem.at[0, k, layer, frm], c_sem.at[1, k, layer, frm], ctx, c_mate)

    def own(layer):
        return pltpu.make_async_copy(w_ref.at[layer, ctx], place(layer, ctx, fsdp), own_sem.at[layer])

    def begin(layer):
        exchange = swap(layer)
        for i in range(nz - 1):
            exchange.send(line.far(i))
        exchange.send(line.z)
        over_y(layer, ctx, fsdp, w_ref.at[layer, ctx]).start()
        over_c(layer, ctx, fsdp, 0, w_ref.at[layer, ctx]).start()
        own(layer).start()

    def arrived(layer, frm):
        over_y(layer, frm, fsdp).start()
        over_c(layer, frm, fsdp, 0).start()

    def from_y(layer, frm):
        over_y(layer, frm, y_mate).wait_recv()
        over_c(layer, frm, y_mate, 1).start()

    def take(layer, i):
        exchange = swap(layer)
        for way, src, dest, real in exchange.events(i):

            @pl.when(real)
            def _():
                exchange.handle(way, src, dest, lambda frm: arrived(layer, frm))

        def mine(late, then):
            @pl.when(i == late)
            def _():
                then(line.z)

            for way, src, dest, real in exchange.events(i - late):

                @pl.when(real & (dest == line.z))
                def _():
                    then(src)

        def mates(src):
            exchange.mate_arrived(src)
            arrived(layer, src * NX + 1 - line.x)

        mine(1, mates)
        mine(2, lambda src: from_y(layer, src * NX + line.x))
        mine(3, lambda src: from_y(layer, src * NX + 1 - line.x))

    def small(to):
        return remote(g_ref.at[to], go_ref.at[ctx * nfs + fsdp], gp_sem.at[0, to], gp_sem.at[1, ctx], to, fsdp)

    def small_in(frm):
        return remote(g_ref.at[ctx], go_ref.at[frm * nfs + fsdp], gp_sem.at[0, frm], gp_sem.at[1, frm], frm, fsdp)

    def small_y(frm, f):
        return remote(go_ref.at[frm * nfs + f], go_ref.at[frm * nfs + f], gy_sem.at[0, frm], gy_sem.at[1, frm], ctx, y_mate)

    def small_c(frm, f, k):
        return remote(go_ref.at[frm * nfs + f], go_ref.at[frm * nfs + f], gc_sem.at[0, k, frm], gc_sem.at[1, k, frm], ctx, c_mate)

    small_own = pltpu.make_async_copy(g_ref.at[ctx], go_ref.at[ctx * nfs + fsdp], gown_sem)
    small_own.start()
    for step in range(1, nctx):
        small((ctx + step) % nctx).start()
    steps = 2 * nz - 3 + 3

    def step(i, carry):
        for layer in range(layers):
            at = i - LAG * layer

            @pl.when(at == 0)
            def _():
                begin(layer)

        def each(layer, carry):
            at = i - LAG * layer

            @pl.when((at > 0) & (at <= steps))
            def _():
                take(layer, at)

            return carry

        lax.fori_loop(0, layers, each, 0)
        return carry

    lax.fori_loop(0, steps + 1 + LAG * (layers - 1), step, 0)
    small_own.wait()
    for k in range(nctx):
        if k:
            small_in((ctx + k) % nctx).wait_recv()
        small_y((ctx + k) % nctx, fsdp).start()
        small_c((ctx + k) % nctx, fsdp, 0).start()
    for k in range(nctx):
        small_y((ctx + k) % nctx, y_mate).wait_recv()
        small_c((ctx + k) % nctx, y_mate, 1).start()
    for frm in range(nctx):
        small_c(frm, c_mate, 0).wait_recv()
        small_c(frm, y_c_mate, 1).wait_recv()
        small_c(frm, fsdp, 0).wait_send()
        small_c(frm, y_mate, 1).wait_send()
        small_y(frm, fsdp).wait_send()
    for step_ in range(1, nctx):
        small((ctx + step_) % nctx).wait_send()

    def close(layer, carry):
        own(layer).wait()
        for frm in range(nctx):
            over_c(layer, frm, c_mate, 0).wait_recv()
            over_c(layer, frm, y_c_mate, 1).wait_recv()
            over_c(layer, frm, fsdp, 0).wait_send()
            over_c(layer, frm, y_mate, 1).wait_send()
            over_y(layer, frm, fsdp).wait_send()
        swap(layer).finish()
        return carry

    lax.fori_loop(0, layers, close, 0)


def spread_weights(send, small, nfs):
    layers, nctx, mats, rows, width = send.shape
    return pl.pallas_call(
        functools.partial(weights_kernel, nctx, nfs, rows),
        out_shape=(
            jax.ShapeDtypeStruct((layers, mats, nctx * nfs * rows, width), send.dtype),
            jax.ShapeDtypeStruct((nctx * nfs,) + small.shape[1:], small.dtype),
        ),
        in_specs=[VM, VM],
        out_specs=(ANY, ANY),
        scratch_shapes=Exchange.scratch(nctx // NX, (mats, rows, width), (layers,))
        + [
            DMA((layers,)),
            DMA((2, layers, nctx)),
            DMA((2, 2, layers, nctx)),
            DMA,
            DMA((2, nctx)),
            DMA((2, nctx)),
            DMA((2, 2, nctx)),
        ],
        compiler_params=params(3, 40),
        name="spread_weights",
    )(send, small)


def grads_kernel(nctx, nfs, rows, normed_ref, dproj_ref, middle_ref, attended_ref, moe_ref, dgate_ref, dup_ref, grad_ref, inner_ref, e_ref,
                 o_ref, eo_ref, mine, cin, yin, half, full, e_cin, e_half, e_yin, e_full,
                 own_sem, c_sem, y_sem, p_sem, eown_sem, ec_sem, ey_sem, ep_sem):
    nz = nctx // NX
    line = Line(nz)
    ctx, fsdp = line.ctx, line.fsdp
    y, core = fsdp // NCORE, fsdp % NCORE
    y_mate = (1 - y) * NCORE + core
    c_mate = y * NCORE + 1 - core
    mats = mine.shape[0]
    proj = mine.shape[2] - attended_ref.shape[1]
    units = dgate_ref.shape[1] // 2
    slab = NX * nfs * rows
    barrier = pltpu.get_barrier_semaphore()
    for step in range(1, nctx):
        greet(barrier, (ctx + step) % nctx, fsdp)
    for other in (y_mate, c_mate):
        greet(barrier, ctx, other)
    pl.semaphore_wait(barrier, nctx + 1)

    def span(s, f):
        return pl.ds(pl.multiple_of((s * nfs + f) * rows, rows), rows)

    def to_c(s, k):
        f = (1 - y if k == 0 else y) * NCORE + 1 - core
        return remote(mine.at[:, span(s, f), :], cin.at[k, s], c_sem.at[0, k, s], c_sem.at[1, k, s], ctx, c_mate)

    def to_y(s):
        return remote(half.at[s], yin.at[s], y_sem.at[0, s], y_sem.at[1, s], ctx, y_mate)

    def out(s):
        return remote(full.at[s], o_ref.at[ctx], p_sem.at[0, s], p_sem.at[1, ctx], s, fsdp)

    def out_in(s):
        return remote(full.at[s], o_ref.at[s], p_sem.at[0, s], p_sem.at[1, s], s, fsdp)

    e_to_c = remote(e_ref.at[1 - core], e_cin, ec_sem.at[0], ec_sem.at[1], ctx, c_mate)
    e_to_y = remote(e_half.at[1 - y], e_yin, ey_sem.at[0], ey_sem.at[1], ctx, y_mate)

    def e_out(s):
        return remote(e_full.at[s], eo_ref.at[ctx], ep_sem.at[0, s], ep_sem.at[1, ctx], s, fsdp)

    def e_out_in(s):
        return remote(e_full.at[s], eo_ref.at[s], ep_sem.at[0, s], ep_sem.at[1, s], s, fsdp)

    e_to_c.start()
    own = pltpu.make_async_copy(full.at[ctx], o_ref.at[ctx], own_sem)
    e_own = pltpu.make_async_copy(e_full.at[ctx], eo_ref.at[ctx], eown_sem)

    turn_of = line.far

    def compute(row):
        lanes = pl.ds(pl.multiple_of(row * slab, 128), slab)
        tall = pl.ds(pl.multiple_of(row * slab, 16), slab)
        mine[0, tall, pl.ds(0, proj)] = dot(normed_ref[:, lanes], dproj_ref[...], TN)[:, :proj].astype(BF)
        mine[0, tall, pl.ds(proj, mine.shape[2] - proj)] = dot(middle_ref[:, lanes], attended_ref[...], TN).astype(BF)
        moe = moe_ref[:, lanes]
        for e in range(2):
            part_of = pl.ds(e * units, units)
            mine[1 + e, tall, :] = dot(moe, dgate_ref[:, part_of], TN).astype(BF)
            mine[3 + e, tall, :] = dot(moe, dup_ref[:, part_of], TN).astype(BF)
            mine[5 + e, tall, :] = dot(grad_ref[:, lanes], inner_ref[:, part_of], TN).astype(BF)

    def first(s):
        to_c(s, 0).wait_recv()

        def one(m, _):
            half[s, m] = (mine[m, span(s, y_mate), :].astype(F32) + cin[0, s, m].astype(F32)).astype(BF)
            return 0

        lax.fori_loop(0, mats, one, 0)
        to_y(s).start()

    def second(s):
        to_c(s, 1).wait_recv()
        to_y(s).wait_recv()

        def one(m, _):
            full[s, m] = (mine[m, span(s, fsdp), :].astype(F32) + cin[1, s, m].astype(F32) + yin[s, m].astype(F32)).astype(BF)
            return 0

        lax.fori_loop(0, mats, one, 0)

        @pl.when(s != ctx)
        def _():
            out(s).start()

    def step(i, carry):
        @pl.when(i < nz)
        def _():
            row = turn_of(i)
            compute(row)
            for k in range(2):
                for side in range(NX):
                    to_c(row * NX + side, k).start()

        @pl.when((i >= 1) & (i < nz + 1))
        def _():
            for side in range(NX):
                first(turn_of(i - 1) * NX + side)

        @pl.when((i >= 2) & (i < nz + 2))
        def _():
            row = turn_of(i - 2)
            for side in range(NX):
                second(row * NX + side)

        return carry

    lax.fori_loop(0, nz + 2, step, 0)
    own.start()
    e_to_c.wait_recv()
    e_half[...] = e_ref[core] + e_cin[...]
    e_to_y.start()
    e_to_y.wait_recv()
    e_full[...] = e_half[y] + e_yin[...]
    e_own.start()
    for step_ in range(1, nctx):
        e_out((ctx + step_) % nctx).start()
    for s in range(nctx):
        for k in range(2):
            to_c(s, k).wait_send()
        to_y(s).wait_send()

        @pl.when(s != ctx)
        def _():
            out(s).wait_send()
            out_in(s).wait_recv()
            e_out(s).wait_send()
            e_out_in(s).wait_recv()

    e_to_c.wait_send()
    e_to_y.wait_send()
    e_own.wait()
    own.wait()


def collect_grads(nctx, nfs, normed, dproj, middle, attended, moe, dgate, dup, grad, inner, extra):
    width = normed.shape[1]
    rows = width // (nctx * nfs)
    mats, cols = 7, dgate.shape[1] // 2
    blk = (mats, rows, cols)
    tile = extra.shape[3:]
    return pl.pallas_call(
        functools.partial(grads_kernel, nctx, nfs, rows),
        out_shape=(jax.ShapeDtypeStruct((nctx,) + blk, BF), jax.ShapeDtypeStruct((nctx,) + tile, F32)),
        in_specs=[VM] * 10,
        out_specs=(ANY, ANY),
        scratch_shapes=[
            pltpu.VMEM((mats, width, cols), BF),
            pltpu.VMEM((2, nctx) + blk, BF),
            pltpu.VMEM((nctx,) + blk, BF),
            pltpu.VMEM((nctx,) + blk, BF),
            pltpu.VMEM((nctx,) + blk, BF),
            pltpu.VMEM((2, nctx) + tile, F32),
            pltpu.VMEM((2, nctx) + tile, F32),
            pltpu.VMEM((nctx,) + tile, F32),
            pltpu.VMEM((nctx,) + tile, F32),
            DMA,
            DMA((2, 2, nctx)),
            DMA((2, nctx)),
            DMA((2, nctx)),
            DMA,
            DMA((2,)),
            DMA((2,)),
            DMA((2, nctx)),
        ],
        compiler_params=params(4, 63),
        name="collect_grads",
    )(normed, dproj, middle, attended, moe, dgate, dup, grad, inner, extra)


def spin(values, cos_part, sin_part):
    lane = lax.broadcasted_iota(jnp.int32, values.shape, 1) % HEAD_DIM
    half_dim = HEAD_DIM // 2
    swapped = jnp.where(
        lane < half_dim,
        pltpu.roll(values, values.shape[1] - half_dim, 1),
        pltpu.roll(values, half_dim, 1),
    )
    return values * cos_part + swapped * sin_part


def attention_kernel(nz, layer, x_ref, mats_ref, cos_ref, sin_ref, key_at_ref, query_at_ref,
                     o_ref, all_out, q_ref, k_ref, v_ref, peak_ref, share_ref, att_ref,
                     attn, out_w, blocks, part, v_turned, probs, load_sem, save_sem, gsems, work, ssems):
    line = Line(nz)
    rows, width = x_ref.shape
    pair_rows = NX * rows
    heads = q_ref.shape[1] // rows
    o_at = (heads + 2) * HEAD_DIM
    wide = -(-o_at // 128) * 128
    load = pltpu.make_async_copy(mats_ref.at[layer, 0], attn, load_sem)
    load.start()
    line.greet()
    ring = Gather(line, x_ref, blocks, gsems)
    ring.start()
    blocks[line.ctx] = x_ref[...]
    load.wait()
    out_w[...] = attn[:, o_at:]

    def save(row):
        pair = pl.ds(row * NX, NX)
        return pltpu.make_async_copy(blocks.at[pair], all_out.at[pair], save_sem.at[row])

    def project(i, carry):
        @pl.when(i < nz - 1)
        def _():
            ring.forward(i)

        row = line.near(i)
        ring.wait_pair(row)
        pair = pl.ds(row * NX, NX)
        tall = pl.ds(pl.multiple_of(row * pair_rows, pair_rows), pair_rows)
        block = blocks[pair].reshape(pair_rows, width)
        save(row).start()
        proj = dot(block, attn[:, :wide], NN)
        cos_part, sin_part = cos_ref[tall, :], sin_ref[tall, :]
        first = spin(proj[:, :128], cos_part, sin_part)
        second = spin(proj[:, 128:256], cos_part, sin_part)
        values = proj[:, 256 : 256 + HEAD_DIM]
        for side in range(NX):
            at = slice(side * rows, (side + 1) * rows)
            q_ref[row * NX + side, 0:rows, :] = first[at, :HEAD_DIM].astype(BF)
            q_ref[row * NX + side, rows : 2 * rows, :] = first[at, HEAD_DIM:].astype(BF)
            q_ref[row * NX + side, 2 * rows : 3 * rows, :] = second[at, :HEAD_DIM].astype(BF)
        k_ref[tall, :] = second[:, HEAD_DIM:].astype(BF)
        v_ref[tall, :] = values.astype(BF)
        v_turned[:, tall] = values.T.astype(BF)
        return carry

    lax.fori_loop(0, nz, project, 0)
    ring.finish()
    sums = Scatter(line, part, o_ref, work, ssems)

    def attend(at):
        scores = dot(k_ref[...], q_ref[at], NT)
        key_at = key_at_ref[...]
        visible = (key_at >= query_at_ref[at, 0:1, :]) & (key_at <= query_at_ref[at, 1:2, :])
        for head in range(heads):
            lanes = slice(head * rows, (head + 1) * rows)
            raw = jnp.where(visible, scores[:, lanes] * HEAD_DIM**-0.5, NEGATIVE)
            peak = jnp.max(raw, axis=0, keepdims=True)
            powers = jnp.exp(raw - peak)
            peak_ref[at, :, lanes] = peak
            share_ref[at, :, lanes] = 1.0 / jnp.sum(powers, axis=0, keepdims=True)
            probs[:, lanes] = powers.astype(BF)
        turned = dot(v_turned[...], probs[...], NN) * share_ref[at]
        stacked = turned.T.astype(BF)
        for head in range(heads):
            att_ref[at, :, head * HEAD_DIM : (head + 1) * HEAD_DIM] = stacked[head * rows : (head + 1) * rows]
        part[at] = dot(att_ref[at], out_w[...], NT).astype(BF)

    def step(i, carry):
        row = line.far(i)
        attend(row * NX + 1 - line.x)
        sums.across(row).start()
        attend(row * NX + line.x)

        @pl.when(i > 0)
        def _():
            sums.add(i - 1)

        return carry

    lax.fori_loop(0, nz, step, 0)
    sums.add(nz - 1)
    sums.finish()
    for row in range(nz):
        save(row).wait()


def attention_rows(block, mats, layer, cos_part, sin_part, key_at, query_at, nz):
    rows, width = block.shape
    group = nz * NX
    group_rows = group * rows
    heads = 3
    return pl.pallas_call(
        functools.partial(attention_kernel, nz, layer),
        out_shape=(
            jax.ShapeDtypeStruct((rows, width), F32),
            jax.ShapeDtypeStruct((group, rows, width), BF),
            jax.ShapeDtypeStruct((group, heads * rows, HEAD_DIM), BF),
            jax.ShapeDtypeStruct((group_rows, HEAD_DIM), BF),
            jax.ShapeDtypeStruct((group_rows, HEAD_DIM), BF),
            jax.ShapeDtypeStruct((group, 1, heads * rows), F32),
            jax.ShapeDtypeStruct((group, 1, heads * rows), F32),
            jax.ShapeDtypeStruct((group, rows, heads * HEAD_DIM), BF),
        ),
        in_specs=[VM, ANY, VM, VM, VM, VM],
        out_specs=(VM, ANY, VM, VM, VM, VM, VM, VM),
        scratch_shapes=[
            pltpu.VMEM(mats.shape[2:], BF),
            pltpu.VMEM((width, heads * HEAD_DIM), BF),
            pltpu.VMEM((group, rows, width), BF),
            pltpu.VMEM((group, rows, width), BF),
            pltpu.VMEM((HEAD_DIM, group_rows), BF),
            pltpu.VMEM((group_rows, heads * rows), BF),
            DMA,
            DMA((nz,)),
        ]
        + Gather.scratch(nz)
        + Scatter.scratch(nz, rows, width),
        compiler_params=params(9 + 2 * layer, 60),
        name="attention_forward",
    )(block, mats, cos_part, sin_part, key_at, query_at)


def attention_back_kernel(nz, layer, x_ref, mats_ref, cos_ref, sin_ref, key_at_ref, query_at_ref, q_ref, k_ref, v_ref, peak_ref, share_ref,
                          o_ref, all_out, dproj_ref,
                          attn, out_w, blocks, part, k_turned, probs, slopes, dq, dk, dv, load_sem, save_sem, gsems, work, ssems):
    line = Line(nz)
    rows, width = x_ref.shape
    pair_rows = NX * rows
    heads = q_ref.shape[1] // rows
    o_at = (heads + 2) * HEAD_DIM
    wide = dproj_ref.shape[2]
    scale = HEAD_DIM**-0.5
    load = pltpu.make_async_copy(mats_ref.at[layer, 0], attn, load_sem)
    load.start()
    line.greet()
    ring = Gather(line, x_ref, blocks, gsems)
    ring.start()
    blocks[line.ctx] = x_ref[...]
    k_turned[...] = k_ref[...].astype(F32).T.astype(BF)
    dk[...] = jnp.zeros(dk.shape, F32)
    dv[...] = jnp.zeros(dv.shape, F32)
    load.wait()
    out_w[...] = attn[:, o_at:]

    def save(row):
        pair = pl.ds(row * NX, NX)
        return pltpu.make_async_copy(blocks.at[pair], all_out.at[pair], save_sem.at[row])

    def back(at):
        d_att = dot(blocks[at], out_w[...], NN)
        d_heads = jnp.concatenate(
            [d_att[:, head * HEAD_DIM : (head + 1) * HEAD_DIM] for head in range(heads)], axis=0
        ).astype(BF)
        scores = dot(k_ref[...], q_ref[at], NT)
        d_probs = dot(v_ref[...], d_heads, NT)
        key_at = key_at_ref[...]
        visible = (key_at >= query_at_ref[at, 0:1, :]) & (key_at <= query_at_ref[at, 1:2, :])
        for head in range(heads):
            lanes = slice(head * rows, (head + 1) * rows)
            raw = jnp.where(visible, scores[:, lanes] * scale, NEGATIVE)
            prob = jnp.exp(raw - peak_ref[at, :, lanes]) * share_ref[at, :, lanes]
            grad = d_probs[:, lanes]
            delta = jnp.sum(prob * grad, axis=0, keepdims=True)
            probs[:, lanes] = prob.astype(BF)
            slopes[:, lanes] = (prob * (grad - delta)).astype(BF)
        dv[...] += dot(probs[...], d_heads, NN)
        dk[...] += dot(slopes[...], q_ref[at], NN)
        stacked = dot(k_turned[...], slopes[...], NN).T * scale
        for head in range(heads):
            dq[at, :, head * HEAD_DIM : (head + 1) * HEAD_DIM] = stacked[head * rows : (head + 1) * rows]

    def take(i, carry):
        @pl.when(i < nz - 1)
        def _():
            ring.forward(i)

        row = line.near(i)
        back(row * NX + line.x)
        ring.wait_pair(row)
        save(row).start()
        back(row * NX + 1 - line.x)
        return carry

    lax.fori_loop(0, nz, take, 0)
    ring.finish()
    sums = Scatter(line, part, o_ref, work, ssems)

    def project(at):
        tall = pl.ds(pl.multiple_of(at * rows, rows), rows)
        cos_part, sin_part = cos_ref[tall, :], -sin_ref[tall, :]
        block_dq = dq[at]
        second = jnp.concatenate([block_dq[:, 128:], dk[tall, :] * scale], axis=1)
        dproj_ref[at, :, 0:128] = spin(block_dq[:, :128], cos_part, sin_part).astype(BF)
        dproj_ref[at, :, 128:256] = spin(second, cos_part, sin_part).astype(BF)
        last = jnp.concatenate([dv[tall, :], jnp.zeros((rows, wide - 256 - HEAD_DIM), F32)], axis=1)
        dproj_ref[at, :, 256:wide] = last.astype(BF)
        part[at] = dot(dproj_ref[at], attn[:, :wide], NT).astype(BF)

    def step(i, carry):
        row = line.far(i)
        project(row * NX + 1 - line.x)
        sums.across(row).start()
        project(row * NX + line.x)

        @pl.when(i > 0)
        def _():
            sums.add(i - 1)

        return carry

    lax.fori_loop(0, nz, step, 0)
    sums.add(nz - 1)
    sums.finish()
    for row in range(nz):
        save(row).wait()


def attention_rows_back(block, mats, layer, cos_part, sin_part, key_at, query_at, queries, keys, values, peaks, shares, nz):
    rows, width = block.shape
    group = nz * NX
    group_rows = group * rows
    heads = 3
    wide = 384
    return pl.pallas_call(
        functools.partial(attention_back_kernel, nz, layer),
        out_shape=(
            jax.ShapeDtypeStruct((rows, width), F32),
            jax.ShapeDtypeStruct((group, rows, width), BF),
            jax.ShapeDtypeStruct((group, rows, wide), BF),
        ),
        in_specs=[VM, ANY] + [VM] * 9,
        out_specs=(VM, ANY, VM),
        scratch_shapes=[
            pltpu.VMEM(mats.shape[2:], BF),
            pltpu.VMEM((width, heads * HEAD_DIM), BF),
            pltpu.VMEM((group, rows, width), BF),
            pltpu.VMEM((group, rows, width), BF),
            pltpu.VMEM((HEAD_DIM, group_rows), BF),
            pltpu.VMEM((group_rows, heads * rows), BF),
            pltpu.VMEM((group_rows, heads * rows), BF),
            pltpu.VMEM((group, rows, heads * HEAD_DIM), F32),
            pltpu.VMEM((group_rows, HEAD_DIM), F32),
            pltpu.VMEM((group_rows, HEAD_DIM), F32),
            DMA,
            DMA((nz,)),
        ]
        + Gather.scratch(nz)
        + Scatter.scratch(nz, rows, width),
        compiler_params=params(10 + 2 * layer, 60),
        name="attention_backward",
    )(block, mats, cos_part, sin_part, key_at, query_at, queries, keys, values, peaks, shares)


def rope_tables(places):
    half_dim = HEAD_DIM // 2
    freq_steps = jnp.arange(half_dim, dtype=jnp.float32)
    inverse = jnp.exp(freq_steps * (-2.0 * math.log(10000.0) / HEAD_DIM))
    angles = places[:, None] * inverse[None, :]
    return jnp.cos(angles), jnp.sin(angles)


def pack_weights(master_set, layer, nctx):
    query_weight, key_weight, value_weight, out_weight, attn_gain, moe_gain, gate_weight, up_weight, down_weight = master_set
    rows = query_weight.shape[1]

    def columns(master):
        low = master[layer].astype(BF).reshape(rows, nctx, -1)
        return low.transpose(1, 0, 2)

    attn = jnp.concatenate(
        [columns(query_weight), columns(key_weight), columns(value_weight), columns(out_weight)], axis=-1
    )

    def experts(master):
        low = master[layer].astype(BF)
        return low.reshape(nctx, -1, rows, low.shape[-1])

    send = jnp.concatenate(
        [attn[:, None], experts(gate_weight), experts(up_weight), experts(down_weight)], axis=1
    )
    gains = jnp.stack([attn_gain[layer], moe_gain[layer]]).astype(BF).astype(F32)
    return send, jnp.pad(gains, ((0, 0), (0, 128 - rows)))


def norm_back(values, gain, grad):
    scale = lax.rsqrt(jnp.mean(values * values, axis=-1, keepdims=True) + EPSILON)
    unit = values * scale
    grad_gain = jnp.sum(grad * unit, axis=0)
    pulled = grad * gain
    return scale * (pulled - unit * jnp.mean(pulled * unit, axis=-1, keepdims=True)), grad_gain


def fast_body(nctx, nfs, *args):
    (tokens, cotangent, lengths, tile_order, routes, gates), master_set = args[:6], args[6:]
    nz = nctx // NX
    rows_here, model_width = tokens.shape[1], tokens.shape[2]
    group_rows = rows_here * nctx
    ctx = lax.axis_index("ctx")
    _, pos_all = layout(lengths[0], tile_order[0], group_rows)
    cos_half, sin_half = rope_tables(pos_all.astype(jnp.float32))
    cos_part = jnp.concatenate([cos_half] * 4, axis=1)
    sin_part = jnp.concatenate([-sin_half, sin_half] * 2, axis=1)
    row_ids = jnp.arange(rows_here, dtype=jnp.int32)
    first_at = (tile_order[0][:, None] * TILE + row_ids[None, :]).reshape(group_rows)
    key_at = first_at[:, None]
    query_at = jnp.stack(
        [(first_at - pos_all).reshape(nctx, rows_here), first_at.reshape(nctx, rows_here)], axis=1
    )
    q_width = 3 * HEAD_DIM
    kv_at, v_at, o_at = q_width, q_width + HEAD_DIM, q_width + 2 * HEAD_DIM

    expert_ids = jnp.arange(EXPERTS, dtype=jnp.int32)
    table = jnp.sum(
        jnp.where(routes[:, 0, :, :, None] == expert_ids, gates[:, 0, :, :, None], 0.0), axis=-2
    )
    packed = [pack_weights(master_set, layer, nctx) for layer in range(LAYERS)]
    rows = packed[0][0].shape[2]
    gains = jnp.broadcast_to(jnp.concatenate([gain for _, gain in packed])[None], (nctx, 2 * LAYERS, 128))
    shares = table.transpose(2, 0, 1).reshape(nctx, 2, LAYERS, rows_here).transpose(0, 2, 1, 3)
    shares = shares.reshape(nctx, 2 * LAYERS, rows_here)
    pad = jnp.zeros((nctx, 8 - 2 * LAYERS, 128), F32)
    small = jnp.concatenate([gains, pad, shares, pad], axis=1)
    mats_all, small_all = spread_weights(jnp.stack([send for send, _ in packed]), small, nfs)
    shares = lax.dynamic_index_in_dim(
        small_all.reshape(nctx, nfs, 16, 128), lax.axis_index("fsdp"), 1, keepdims=False
    )
    fetched = [
        (
            small_all[:, 2 * layer, :rows].reshape(-1),
            small_all[:, 2 * layer + 1, :rows].reshape(-1),
            shares[:, 8 + 2 * layer : 10 + 2 * layer].transpose(0, 2, 1),
        )
        for layer in range(LAYERS)
    ]

    hidden = tokens[0].astype(jnp.float32)
    records = []
    for layer in range(LAYERS):
        attn_gain, moe_gain, share = fetched[layer]
        normed = rms_norm(hidden, attn_gain).astype(BF)
        mixed, normed_all, queries, keys, values, peaks, sums, attended = attention_rows(
            normed, mats_all, layer, cos_part, sin_part, key_at, query_at, nz
        )
        middle = hidden + mixed

        moe_in = rms_norm(middle, moe_gain).astype(BF)
        moved, moe_all, gate_act, up_act = experts_forward(moe_in, share, mats_all, layer, nz)
        records.append((hidden, normed_all, queries, keys, values, peaks, sums, attended, middle, moe_all, gate_act, up_act))
        hidden = middle + moved

    output = hidden.astype(BF)
    grad = cotangent[0].astype(jnp.float32)
    collected = [None] * LAYERS
    for layer in reversed(range(LAYERS)):
        attn_gain, moe_gain, share = fetched[layer]
        hidden, normed_all, queries, keys, values, peaks, sums, attended, middle, moe_all, gate_act, up_act = records[layer]
        grad_moe_in, grad_all, d_gate, d_up, inner = experts_backward(grad.astype(BF), share, mats_all, layer, gate_act, up_act, nz)
        through, grad_moe_gain = norm_back(middle, moe_gain, grad_moe_in)
        grad_middle = grad + through

        grad_normed, middle_all, d_proj = attention_rows_back(
            grad_middle.astype(BF), mats_all, layer, cos_part, sin_part, key_at, query_at, queries, keys, values, peaks, sums, nz
        )
        through, grad_attn_gain = norm_back(hidden, attn_gain, grad_normed)
        grad = grad_middle + through

        extra = jnp.stack([grad_attn_gain, grad_moe_gain]).reshape(2, nctx, nfs // NCORE, NCORE, rows)
        extra = jnp.pad(extra.transpose(3, 2, 1, 0, 4), ((0, 0), (0, 0), (0, 0), (0, 6), (0, 128 - rows)))
        flat = [part.reshape(group_rows, -1) for part in (normed_all, d_proj, middle_all, attended, moe_all, d_gate, d_up, grad_all, inner)]
        collected[layer] = collect_grads(nctx, nfs, *flat, extra)

    def attn_part(low, high):
        return jnp.stack(
            [
                c[0][:, 0, :, low:high].transpose(1, 0, 2).reshape(c[0].shape[2], -1).astype(F32)
                for c in collected
            ]
        )

    def expert_part(first):
        return jnp.stack(
            [
                c[0][:, first : first + 2].reshape((EXPERTS,) + c[0].shape[2:]).astype(F32)
                for c in collected
            ]
        )

    def gain_part(kind):
        return jnp.stack([jnp.sum(c[1][:, kind, :rows], axis=0) for c in collected])

    return (
        output[None],
        grad[None],
        attn_part(0, kv_at),
        attn_part(kv_at, v_at),
        attn_part(v_at, o_at),
        attn_part(o_at, o_at + q_width),
        gain_part(0),
        gain_part(1),
        expert_part(1),
        expert_part(3),
        expert_part(5),
    )


def solution(mesh):
    placed = (
        P("fsdp", "ctx", None),
        P("fsdp", "ctx", None),
        P("fsdp", None),
        P("fsdp", None),
        P(None, "fsdp", "ctx", None),
        P(None, "fsdp", "ctx", None),
        P(None, ("ctx", "fsdp"), None),
        P(None, ("ctx", "fsdp"), None),
        P(None, ("ctx", "fsdp"), None),
        P(None, ("ctx", "fsdp"), None),
        P(None, ("ctx", "fsdp")),
        P(None, ("ctx", "fsdp")),
        P(None, None, ("ctx", "fsdp"), None),
        P(None, None, ("ctx", "fsdp"), None),
        P(None, None, ("ctx", "fsdp"), None),
    )
    nctx, nfs = mesh.shape["ctx"], mesh.shape["fsdp"]
    chosen = partial(fast_body, nctx, nfs) if (nctx, nfs) == (8, 4) else body
    return jax.shard_map(
        chosen,
        mesh=mesh,
        in_specs=placed,
        out_specs=(
            P("fsdp", "ctx", None),
            P("fsdp", "ctx", None),
            P(None, ("ctx", "fsdp"), None),
            P(None, ("ctx", "fsdp"), None),
            P(None, ("ctx", "fsdp"), None),
            P(None, ("ctx", "fsdp"), None),
            P(None, ("ctx", "fsdp")),
            P(None, ("ctx", "fsdp")),
            P(None, None, ("ctx", "fsdp"), None),
            P(None, None, ("ctx", "fsdp"), None),
            P(None, None, ("ctx", "fsdp"), None),
        ),
        check_vma=False,
    )
```

```python
from functools import partial
import functools
import math

import jax
import jax.numpy as jnp
from jax import lax
from jax.experimental import pallas as pl
from jax.experimental.pallas import tpu as pltpu
from jax.sharding import PartitionSpec as P

HEAD_DIM = 64
EXPERTS = 16
LAYERS = 2
TILE = 128
CAP = 80


EPSILON = 1e-06
NEGATIVE = -1e30


def layout(lengths, tile_order, group_rows):
    tile_count = tile_order.shape[0]
    row_ids = jnp.arange(group_rows, dtype=jnp.int32)
    in_tile = (row_ids // TILE)[:, None] == jnp.arange(tile_count, dtype=jnp.int32)[None, :]
    tile_of = jnp.sum(jnp.where(in_tile, tile_order[None, :], 0), axis=1, dtype=jnp.int32)
    anchor = tile_of * TILE + row_ids % TILE
    seq_ends = jnp.cumsum(lengths, dtype=jnp.int32)
    seq_starts = seq_ends - lengths
    segment = jnp.sum(
        (anchor[:, None] >= seq_ends[None, :]).astype(jnp.int32), axis=1, dtype=jnp.int32
    )
    picked = segment[:, None] == jnp.arange(lengths.shape[0], dtype=jnp.int32)[None, :]
    offset = jnp.sum(jnp.where(picked, seq_starts[None, :], 0), axis=1, dtype=jnp.int32)
    return (segment, anchor - offset)


def rms_norm(values, gain_vec):
    return (
        values * lax.rsqrt(jnp.mean(values * values, axis=-1, keepdims=True) + EPSILON) * gain_vec
    )


def rotate(values, places):
    half_dim = values.shape[-1] // 2
    freq_steps = jnp.arange(half_dim, dtype=jnp.float32)
    inverse = jnp.exp(freq_steps * (-2.0 * math.log(10000.0) / values.shape[-1]))
    angles = places[:, None] * inverse[None, :]
    cos_part = jnp.cos(angles)[:, None, :]
    sin_part = jnp.sin(angles)[:, None, :]
    first_half = values[..., :half_dim]
    second_half = values[..., half_dim:]
    return jnp.concatenate(
        [
            first_half * cos_part - second_half * sin_part,
            second_half * cos_part + first_half * sin_part,
        ],
        axis=-1,
    )


def rotate_back(grads_in, places):
    return jax.vjp(partial(rotate, places=places), jnp.zeros(grads_in.shape, jnp.float32))[1](
        grads_in
    )[0]


def mix_inner(gate_act, up_act):
    return jax.nn.silu(gate_act) * up_act


def split_halves(master):
    experts_here, rows_here, hidden_units = master.shape
    return (
        master.astype(jnp.bfloat16)
        .reshape(experts_here, rows_here, 2, hidden_units // 2)
        .transpose(0, 2, 1, 3)
        .reshape(2 * experts_here, rows_here, hidden_units // 2)
    )


def merge_halves(grads_in):
    halves_all, rows_here, half_units = grads_in.shape
    return (
        grads_in.reshape(halves_all // 2, 2, rows_here, half_units)
        .transpose(0, 2, 1, 3)
        .reshape(halves_all // 2, rows_here, 2 * half_units)
    )


def doubled(slots):
    return jnp.broadcast_to(slots[:, None], (slots.shape[0], 2) + slots.shape[1:]).reshape(
        (2 * slots.shape[0],) + slots.shape[1:]
    )


def fold_halves(parts):
    return jnp.sum(parts.reshape((parts.shape[0] // 2, 2) + parts.shape[1:]), axis=1)


def send_out(slots):
    return lax.all_to_all(slots, "ctx", split_axis=0, concat_axis=1, tiled=True)


def send_back(parts):
    return lax.all_to_all(
        parts.astype(jnp.bfloat16), "ctx", split_axis=1, concat_axis=0, tiled=True
    ).astype(parts.dtype)


def routing(route_ids, gate_share, rows_here):
    expert_ids = jnp.arange(EXPERTS, dtype=jnp.int32)
    chosen = (route_ids[:, :, None] == expert_ids[None, None, :]).astype(jnp.int32)
    member = jnp.sum(chosen, axis=1, dtype=jnp.int32)
    before = jnp.cumsum(member, axis=0, dtype=jnp.int32) - member
    rank_of = jnp.sum(chosen * before[:, None, :], axis=2, dtype=jnp.int32)
    slot_of = route_ids * CAP + rank_of
    token_ids = jnp.broadcast_to(jnp.arange(rows_here, dtype=jnp.int32)[:, None], route_ids.shape)
    flat_slots = slot_of.reshape(-1)
    slot_token = (
        jnp.full((EXPERTS * CAP,), rows_here, jnp.int32).at[flat_slots].set(token_ids.reshape(-1))
    )
    slot_share = jnp.zeros((EXPERTS * CAP,), jnp.float32).at[flat_slots].set(gate_share.reshape(-1))
    return (slot_of, slot_token, slot_share)


def key_block(key_rows, value_rows, token_meta, block_index, block_rows):
    seg_local, pos_local, seg_all, pos_all = token_meta
    first_row = block_index * block_rows
    key_part = lax.dynamic_slice_in_dim(key_rows, first_row, block_rows, 0)
    value_part = lax.dynamic_slice_in_dim(value_rows, first_row, block_rows, 0)
    seg_part = lax.dynamic_slice_in_dim(seg_all, first_row, block_rows, 0)
    pos_part = lax.dynamic_slice_in_dim(pos_all, first_row, block_rows, 0)
    visible = (seg_local[:, None] == seg_part[None, :]) & (pos_part[None, :] <= pos_local[:, None])
    return (key_part, value_part, visible)


def scores(queries, key_part, visible, score_scale):
    raw_scores = (
        jnp.einsum("qhgd,khd->hgqk", queries, key_part, preferred_element_type=jnp.float32)
        * score_scale
    )
    return jnp.where(visible[None, None], raw_scores, NEGATIVE)


def keep_same(running):
    return running


def attention_forward(queries, key_rows, value_rows, token_meta, block_rows, score_scale):
    block_count = key_rows.shape[0] // block_rows
    rows_here, heads_kv, groups = (queries.shape[0], queries.shape[1], queries.shape[2])

    def stat_step(block_index, running):
        key_part, value_part, visible = key_block(
            key_rows, value_rows, token_meta, block_index, block_rows
        )

        def stat_update(current):
            row_peak, denom_sum = current
            logits = scores(queries, key_part, visible, score_scale)
            new_peak = jnp.maximum(row_peak, jnp.max(logits, axis=-1))
            denom_sum = denom_sum * jnp.exp(row_peak - new_peak) + jnp.sum(
                jnp.exp(logits - new_peak[..., None]), axis=-1
            )
            return (new_peak, denom_sum)

        return lax.cond(jnp.any(visible), stat_update, keep_same, running)

    start_stats = (
        jnp.full((heads_kv, groups, rows_here), NEGATIVE, jnp.float32),
        jnp.zeros((heads_kv, groups, rows_here), jnp.float32),
    )
    row_peak, denom_sum = lax.fori_loop(0, block_count, stat_step, start_stats)

    def out_step(block_index, partial_sum):
        key_part, value_part, visible = key_block(
            key_rows, value_rows, token_meta, block_index, block_rows
        )

        def out_update(current):
            attn_probs = (
                jnp.exp(scores(queries, key_part, visible, score_scale) - row_peak[..., None])
                / denom_sum[..., None]
            )
            return current + jnp.einsum(
                "hgqk,khd->qhgd",
                attn_probs.astype(jnp.bfloat16),
                value_part,
                preferred_element_type=jnp.float32,
            )

        return lax.cond(jnp.any(visible), out_update, keep_same, partial_sum)

    attended = lax.fori_loop(
        0, block_count, out_step, jnp.zeros((rows_here, heads_kv, groups, HEAD_DIM), jnp.float32)
    )
    return ((row_peak, denom_sum), attended)


def attention_backward(
    queries, key_rows, value_rows, token_meta, softmax_stats, grad_attended, block_rows, score_scale
):
    row_peak, denom_sum = softmax_stats
    block_count = key_rows.shape[0] // block_rows

    def probs_for(key_part, visible):
        return (
            jnp.exp(scores(queries, key_part, visible, score_scale) - row_peak[..., None])
            / denom_sum[..., None]
        )

    def delta_step(block_index, partial_sum):
        key_part, value_part, visible = key_block(
            key_rows, value_rows, token_meta, block_index, block_rows
        )

        def delta_update(current):
            attn_probs = probs_for(key_part, visible)
            grad_probs = jnp.einsum(
                "qhgd,khd->hgqk", grad_attended, value_part, preferred_element_type=jnp.float32
            )
            return current + jnp.sum(attn_probs * grad_probs, axis=-1)

        return lax.cond(jnp.any(visible), delta_update, keep_same, partial_sum)

    delta_sum = lax.fori_loop(0, block_count, delta_step, jnp.zeros(denom_sum.shape, jnp.float32))

    def grad_step(block_index, running):
        key_part, value_part, visible = key_block(
            key_rows, value_rows, token_meta, block_index, block_rows
        )
        first_row = block_index * block_rows

        def grad_update(current):
            grad_queries, grad_keys, grad_values = current
            attn_probs = probs_for(key_part, visible)
            grad_probs = jnp.einsum(
                "qhgd,khd->hgqk", grad_attended, value_part, preferred_element_type=jnp.float32
            )
            grad_scores = (attn_probs * (grad_probs - delta_sum[..., None])).astype(jnp.bfloat16)
            grad_queries = grad_queries + jnp.einsum(
                "hgqk,khd->qhgd", grad_scores, key_part, preferred_element_type=jnp.float32
            )
            key_term = jnp.einsum(
                "hgqk,qhgd->khd", grad_scores, queries, preferred_element_type=jnp.float32
            )
            value_term = jnp.einsum(
                "hgqk,qhgd->khd",
                attn_probs.astype(jnp.bfloat16),
                grad_attended,
                preferred_element_type=jnp.float32,
            )
            grad_keys = lax.dynamic_update_slice_in_dim(
                grad_keys,
                lax.dynamic_slice_in_dim(grad_keys, first_row, block_rows, 0) + key_term,
                first_row,
                0,
            )
            grad_values = lax.dynamic_update_slice_in_dim(
                grad_values,
                lax.dynamic_slice_in_dim(grad_values, first_row, block_rows, 0) + value_term,
                first_row,
                0,
            )
            return (grad_queries, grad_keys, grad_values)

        return lax.cond(jnp.any(visible), grad_update, keep_same, running)

    start_grads = (
        jnp.zeros(queries.shape, jnp.float32),
        jnp.zeros(key_rows.shape, jnp.float32),
        jnp.zeros(value_rows.shape, jnp.float32),
    )
    return lax.fori_loop(0, block_count, grad_step, start_grads)


def fetch_layer(master_set, layer_index):
    (
        query_weight,
        key_weight,
        value_weight,
        out_weight,
        attn_gain,
        moe_gain,
        gate_weight,
        up_weight,
        down_weight,
    ) = master_set
    attn_set = (
        lax.all_gather(
            query_weight[layer_index].astype(jnp.bfloat16), ("ctx", "fsdp"), axis=0, tiled=True
        ),
        lax.all_gather(
            key_weight[layer_index].astype(jnp.bfloat16), ("ctx", "fsdp"), axis=0, tiled=True
        ),
        lax.all_gather(
            value_weight[layer_index].astype(jnp.bfloat16), ("ctx", "fsdp"), axis=0, tiled=True
        ),
        lax.all_gather(
            out_weight[layer_index].astype(jnp.bfloat16), ("ctx", "fsdp"), axis=0, tiled=True
        ),
        lax.all_gather(
            attn_gain[layer_index].astype(jnp.bfloat16), ("ctx", "fsdp"), axis=0, tiled=True
        ),
        lax.all_gather(
            moe_gain[layer_index].astype(jnp.bfloat16), ("ctx", "fsdp"), axis=0, tiled=True
        ),
    )
    row_set = (
        lax.all_gather(split_halves(gate_weight[layer_index]), "fsdp", axis=1, tiled=True),
        lax.all_gather(split_halves(up_weight[layer_index]), "fsdp", axis=1, tiled=True),
        lax.all_gather(split_halves(down_weight[layer_index]), "fsdp", axis=1, tiled=True),
    )
    expert_set = (
        lax.all_to_all(row_set[0], "ctx", split_axis=0, concat_axis=1, tiled=True),
        lax.all_to_all(row_set[1], "ctx", split_axis=0, concat_axis=1, tiled=True),
        lax.all_to_all(row_set[2], "ctx", split_axis=0, concat_axis=1, tiled=True),
    )
    return tuple(attn_set) + tuple(expert_set)


def layer_forward(hidden, weights, route_ids, gate_share, token_meta, places, block_rows):
    (
        query_full,
        key_full,
        value_full,
        out_full,
        attn_norm,
        moe_norm,
        gate_full,
        up_full,
        down_full,
    ) = weights
    rows_here, model_width = hidden.shape
    heads_all = query_full.shape[1] // HEAD_DIM
    heads_kv = key_full.shape[1] // HEAD_DIM
    groups = heads_all // heads_kv
    score_scale = HEAD_DIM ** (-0.5)
    normed = rms_norm(hidden, attn_norm.astype(jnp.float32)).astype(jnp.bfloat16)
    queries = rotate(
        jnp.dot(normed, query_full, preferred_element_type=jnp.float32).reshape(
            rows_here, heads_all, HEAD_DIM
        ),
        places,
    ).astype(jnp.bfloat16)
    key_new = (
        rotate(
            jnp.dot(normed, key_full, preferred_element_type=jnp.float32).reshape(
                rows_here, heads_kv, HEAD_DIM
            ),
            places,
        )
        .astype(jnp.bfloat16)
        .reshape(rows_here, heads_kv * HEAD_DIM)
    )
    value_new = jnp.dot(normed, value_full, preferred_element_type=jnp.float32).astype(jnp.bfloat16)
    key_rows, value_rows = (
        lax.all_gather(key_new, "ctx", axis=0, tiled=True),
        lax.all_gather(value_new, "ctx", axis=0, tiled=True),
    )
    key_rows = key_rows.reshape(-1, heads_kv, HEAD_DIM)
    value_rows = value_rows.reshape(-1, heads_kv, HEAD_DIM)
    queries = queries.reshape(rows_here, heads_kv, groups, HEAD_DIM)
    softmax_stats, attended = attention_forward(
        queries, key_rows, value_rows, token_meta, block_rows, score_scale
    )
    attended = attended.reshape(rows_here, heads_all * HEAD_DIM).astype(jnp.bfloat16)
    middle = hidden + jnp.einsum(
        "tx,dx->td", attended, out_full, preferred_element_type=jnp.float32
    )
    moe_in = rms_norm(middle, moe_norm.astype(jnp.float32)).astype(jnp.bfloat16)
    slot_of, slot_token, slot_share = routing(route_ids, gate_share, rows_here)
    padded = jnp.concatenate([moe_in, jnp.zeros((1, model_width), jnp.bfloat16)], axis=0)
    dispatched = jnp.take(padded, slot_token, axis=0).reshape(EXPERTS, CAP, model_width)
    owner_rows = send_out(doubled(dispatched))
    gate_act = jnp.einsum("ecd,edf->ecf", owner_rows, gate_full, preferred_element_type=jnp.float32)
    up_act = jnp.einsum("ecd,edf->ecf", owner_rows, up_full, preferred_element_type=jnp.float32)
    inner_act = mix_inner(gate_act, up_act).astype(jnp.bfloat16)
    expert_part = jnp.einsum(
        "ecf,edf->ecd", inner_act, down_full, preferred_element_type=jnp.float32
    )
    expert_out = fold_halves(send_back(expert_part))
    expert_out = expert_out.reshape(EXPERTS * CAP, model_width)
    moe_out = jnp.sum(jnp.take(expert_out, slot_of, axis=0) * gate_share[..., None], axis=1)
    record = (
        hidden,
        normed,
        queries,
        key_rows,
        value_rows,
        softmax_stats,
        attended,
        middle,
        moe_in,
        slot_of,
        slot_token,
        slot_share,
        owner_rows,
        gate_act,
        up_act,
        inner_act,
    )
    return (record, middle + moe_out)


def layer_backward(grad_hidden, record, weights, token_meta, places, block_rows):
    (
        hidden,
        normed,
        queries,
        key_rows,
        value_rows,
        softmax_stats,
        attended,
        middle,
        moe_in,
        slot_of,
        slot_token,
        slot_share,
        owner_rows,
        gate_act,
        up_act,
        inner_act,
    ) = record
    (
        query_full,
        key_full,
        value_full,
        out_full,
        attn_norm,
        moe_norm,
        gate_full,
        up_full,
        down_full,
    ) = weights
    rows_here, model_width = hidden.shape
    heads_kv, groups = (queries.shape[1], queries.shape[2])
    group_rows = key_rows.shape[0]
    score_scale = HEAD_DIM ** (-0.5)
    grad_padded = jnp.concatenate([grad_hidden, jnp.zeros((1, model_width), jnp.float32)], axis=0)
    grad_expert = (
        (jnp.take(grad_padded, slot_token, axis=0) * slot_share[:, None])
        .astype(jnp.bfloat16)
        .reshape(EXPERTS, CAP, model_width)
    )
    grad_owner = send_out(doubled(grad_expert))
    grad_down = jnp.einsum(
        "ecd,ecf->edf", grad_owner, inner_act, preferred_element_type=jnp.float32
    )
    grad_inner = jnp.einsum(
        "ecd,edf->ecf", grad_owner, down_full, preferred_element_type=jnp.float32
    )
    grad_gate_act, grad_up_act = jax.vjp(mix_inner, gate_act, up_act)[1](grad_inner)
    grad_gate_act = grad_gate_act.astype(jnp.bfloat16)
    grad_up_act = grad_up_act.astype(jnp.bfloat16)
    grad_gate = jnp.einsum(
        "ecd,ecf->edf", owner_rows, grad_gate_act, preferred_element_type=jnp.float32
    )
    grad_up = jnp.einsum(
        "ecd,ecf->edf", owner_rows, grad_up_act, preferred_element_type=jnp.float32
    )
    grad_owner_rows = jnp.einsum(
        "ecf,edf->ecd", grad_gate_act, gate_full, preferred_element_type=jnp.float32
    ) + jnp.einsum("ecf,edf->ecd", grad_up_act, up_full, preferred_element_type=jnp.float32)
    grad_dispatched = fold_halves(send_back(grad_owner_rows))
    home_set = (
        lax.all_to_all(
            grad_gate.astype(jnp.bfloat16), "ctx", split_axis=1, concat_axis=0, tiled=True
        ).astype(grad_gate.dtype),
        lax.all_to_all(
            grad_up.astype(jnp.bfloat16), "ctx", split_axis=1, concat_axis=0, tiled=True
        ).astype(grad_up.dtype),
        lax.all_to_all(
            grad_down.astype(jnp.bfloat16), "ctx", split_axis=1, concat_axis=0, tiled=True
        ).astype(grad_down.dtype),
    )
    summed_set = (
        lax.psum_scatter(
            home_set[0].astype(jnp.bfloat16), "fsdp", scatter_dimension=1, tiled=True
        ).astype(jnp.float32),
        lax.psum_scatter(
            home_set[1].astype(jnp.bfloat16), "fsdp", scatter_dimension=1, tiled=True
        ).astype(jnp.float32),
        lax.psum_scatter(
            home_set[2].astype(jnp.bfloat16), "fsdp", scatter_dimension=1, tiled=True
        ).astype(jnp.float32),
    )
    expert_grads = (
        merge_halves(summed_set[0]),
        merge_halves(summed_set[1]),
        merge_halves(summed_set[2]),
    )
    grad_moe_in = jnp.sum(
        jnp.take(grad_dispatched.reshape(EXPERTS * CAP, model_width), slot_of, axis=0), axis=1
    )
    grad_middle_part, grad_moe_norm = jax.vjp(rms_norm, middle, moe_norm.astype(jnp.float32))[1](
        grad_moe_in
    )
    grad_middle = grad_hidden + grad_middle_part
    grad_rounded = grad_middle.astype(jnp.bfloat16)
    grad_out_full = jnp.einsum(
        "td,tx->dx", grad_rounded, attended, preferred_element_type=jnp.float32
    )
    grad_attended = (
        jnp.dot(grad_rounded, out_full, preferred_element_type=jnp.float32)
        .astype(jnp.bfloat16)
        .reshape(rows_here, heads_kv, groups, HEAD_DIM)
    )
    grad_queries, grad_keys, grad_values = attention_backward(
        queries,
        key_rows,
        value_rows,
        token_meta,
        softmax_stats,
        grad_attended,
        block_rows,
        score_scale,
    )
    key_sums, value_sums = (
        lax.psum_scatter(
            grad_keys.reshape(group_rows, heads_kv * HEAD_DIM).astype(jnp.bfloat16),
            "ctx",
            scatter_dimension=0,
            tiled=True,
        ).astype(jnp.float32),
        lax.psum_scatter(
            grad_values.reshape(group_rows, heads_kv * HEAD_DIM).astype(jnp.bfloat16),
            "ctx",
            scatter_dimension=0,
            tiled=True,
        ).astype(jnp.float32),
    )
    grad_query_rows = (
        rotate_back(
            grad_queries.reshape(rows_here, heads_kv * groups, HEAD_DIM) * score_scale, places
        )
        .astype(jnp.bfloat16)
        .reshape(rows_here, heads_kv * groups * HEAD_DIM)
    )
    grad_key_rows = (
        rotate_back(key_sums.reshape(rows_here, heads_kv, HEAD_DIM) * score_scale, places)
        .astype(jnp.bfloat16)
        .reshape(rows_here, heads_kv * HEAD_DIM)
    )
    grad_value_rows = value_sums.astype(jnp.bfloat16)
    grad_query_full = jnp.einsum(
        "td,tx->dx", normed, grad_query_rows, preferred_element_type=jnp.float32
    )
    grad_key_full = jnp.einsum(
        "td,tx->dx", normed, grad_key_rows, preferred_element_type=jnp.float32
    )
    grad_value_full = jnp.einsum(
        "td,tx->dx", normed, grad_value_rows, preferred_element_type=jnp.float32
    )
    grad_normed = jnp.einsum(
        "tx,dx->td", grad_query_rows, query_full, preferred_element_type=jnp.float32
    )
    grad_normed = grad_normed + jnp.einsum(
        "tx,dx->td", grad_key_rows, key_full, preferred_element_type=jnp.float32
    )
    grad_normed = grad_normed + jnp.einsum(
        "tx,dx->td", grad_value_rows, value_full, preferred_element_type=jnp.float32
    )
    grad_hidden_part, grad_attn_norm = jax.vjp(rms_norm, hidden, attn_norm.astype(jnp.float32))[1](
        grad_normed
    )
    attn_grads = (
        lax.psum_scatter(grad_query_full, ("ctx", "fsdp"), scatter_dimension=0, tiled=True),
        lax.psum_scatter(grad_key_full, ("ctx", "fsdp"), scatter_dimension=0, tiled=True),
        lax.psum_scatter(grad_value_full, ("ctx", "fsdp"), scatter_dimension=0, tiled=True),
        lax.psum_scatter(grad_out_full, ("ctx", "fsdp"), scatter_dimension=0, tiled=True),
        lax.psum_scatter(grad_attn_norm, ("ctx", "fsdp"), scatter_dimension=0, tiled=True),
        lax.psum_scatter(grad_moe_norm, ("ctx", "fsdp"), scatter_dimension=0, tiled=True),
    )
    return (grad_middle + grad_hidden_part, attn_grads, expert_grads)


def body(
    tokens,
    cotangent,
    lengths,
    tile_order,
    routes,
    gates,
    query_weight,
    key_weight,
    value_weight,
    out_weight,
    attn_gain,
    moe_gain,
    gate_weight,
    up_weight,
    down_weight,
):
    rows_here = tokens.shape[1]
    group_rows = rows_here * lax.axis_size("ctx")
    seg_all, pos_all = layout(lengths[0], tile_order[0], group_rows)
    first_row = lax.axis_index("ctx") * rows_here
    seg_local = lax.dynamic_slice_in_dim(seg_all, first_row, rows_here, 0)
    pos_local = lax.dynamic_slice_in_dim(pos_all, first_row, rows_here, 0)
    token_meta = (seg_local, pos_local, seg_all, pos_all)
    places = pos_local.astype(jnp.float32)
    block_rows = math.gcd(group_rows, 512)
    master_set = (
        query_weight,
        key_weight,
        value_weight,
        out_weight,
        attn_gain,
        moe_gain,
        gate_weight,
        up_weight,
        down_weight,
    )
    hidden = tokens[0].astype(jnp.float32)
    records = []
    for layer_index in range(LAYERS):
        weights = fetch_layer(master_set, layer_index)
        record, hidden = layer_forward(
            hidden,
            weights,
            routes[layer_index, 0],
            gates[layer_index, 0],
            token_meta,
            places,
            block_rows,
        )
        records.append(record)
    grad_hidden = cotangent[0].astype(jnp.float32)
    attn_layers = []
    expert_layers = []
    for layer_index in reversed(range(LAYERS)):
        weights = fetch_layer(master_set, layer_index)
        grad_hidden, attn_grads, expert_grads = layer_backward(
            grad_hidden, records[layer_index], weights, token_meta, places, block_rows
        )
        attn_layers.insert(0, attn_grads)
        expert_layers.insert(0, expert_grads)
    grad_query_weight = jnp.stack([layer_grads[0] for layer_grads in attn_layers])
    grad_key_weight = jnp.stack([layer_grads[1] for layer_grads in attn_layers])
    grad_value_weight = jnp.stack([layer_grads[2] for layer_grads in attn_layers])
    grad_out_weight = jnp.stack([layer_grads[3] for layer_grads in attn_layers])
    grad_attn_gain = jnp.stack([layer_grads[4] for layer_grads in attn_layers])
    grad_moe_gain = jnp.stack([layer_grads[5] for layer_grads in attn_layers])
    grad_gate_weight = jnp.stack([layer_grads[0] for layer_grads in expert_layers])
    grad_up_weight = jnp.stack([layer_grads[1] for layer_grads in expert_layers])
    grad_down_weight = jnp.stack([layer_grads[2] for layer_grads in expert_layers])
    return (
        hidden.astype(jnp.bfloat16)[None],
        grad_hidden[None],
        grad_query_weight,
        grad_key_weight,
        grad_value_weight,
        grad_out_weight,
        grad_attn_gain,
        grad_moe_gain,
        grad_gate_weight,
        grad_up_weight,
        grad_down_weight,
    )


BF = jnp.bfloat16
F32 = jnp.float32
NX = 2
NCORE = 2
ANY = pl.BlockSpec(memory_space=pl.ANY)
VM = pl.BlockSpec(memory_space=pltpu.VMEM)
DMA = pltpu.SemaphoreType.DMA

NN = ((1,), (0,))
NT = ((1,), (1,))
TN = ((0,), (0,))


def dot(left, right, dims):
    return lax.dot_general(left, right, (dims, ((), ())), preferred_element_type=jnp.float32)


def remote(src, dst, send_sem, recv_sem, ctx, fsdp):
    return pltpu.make_async_remote_copy(
        src_ref=src,
        dst_ref=dst,
        send_sem=send_sem,
        recv_sem=recv_sem,
        device_id={"ctx": ctx, "fsdp": fsdp},
        device_id_type=pl.DeviceIdType.MESH,
    )


def greet(barrier, ctx, fsdp):
    pl.semaphore_signal(
        barrier, inc=1, device_id={"ctx": ctx, "fsdp": fsdp}, device_id_type=pl.DeviceIdType.MESH
    )


class Line:
    def __init__(self, nz):
        self.nz = nz
        self.ctx, self.fsdp = lax.axis_index("ctx"), lax.axis_index("fsdp")
        self.z, self.x = self.ctx // NX, self.ctx % NX
        self.mate = self.z * NX + 1 - self.x
        self.above = (self.z + 1) * NX + self.x
        self.below = (self.z - 1) * NX + self.x

    def greet(self):
        barrier = pltpu.get_barrier_semaphore()
        greet(barrier, self.mate, self.fsdp)

        @pl.when(self.z > 0)
        def _():
            greet(barrier, self.below, self.fsdp)

        @pl.when(self.z < self.nz - 1)
        def _():
            greet(barrier, self.above, self.fsdp)

        ends = jnp.where(self.z > 0, 1, 0) + jnp.where(self.z < self.nz - 1, 1, 0)
        pl.semaphore_wait(barrier, 1 + ends)

    def near(self, i):
        z, nz = self.z, self.nz
        mid1 = jnp.where(i == 0, 1, jnp.where(i == 1, 0, i))
        mid2 = jnp.where(i == 0, 2, jnp.where(i == 1, 1, jnp.where(i == 2, 3, 0)))
        return jnp.where(z == 0, i, jnp.where(z == nz - 1, nz - 1 - i, jnp.where(z == 1, mid1, mid2)))

    def far(self, i):
        z, nz = self.z, self.nz
        mid1 = jnp.where(i == 0, 3, jnp.where(i == 1, 0, jnp.where(i == 2, 2, 1)))
        mid2 = jnp.where(i == 0, 0, jnp.where(i == 1, 3, jnp.where(i == 2, 1, 2)))
        return jnp.where(z == 0, nz - 1 - i, jnp.where(z == nz - 1, i, jnp.where(z == 1, mid1, mid2)))


EXTRA = 16


class Gather:
    @staticmethod
    def scratch(nz):
        return [DMA((10, nz))]

    def __init__(self, line, own_ref, all_ref, sems):
        self.line, self.own, self.all, self.sems = line, own_ref, all_ref, sems
        self.main = own_ref.shape[0] - EXTRA

    def block(self, row, column=None):
        column = self.line.x if column is None else column
        return self.all.at[row * NX + column, pl.ds(0, self.main)]

    def extras(self, row):
        return self.all.at[pl.ds(row * NX, NX), pl.ds(self.main, EXTRA)]

    def own_main(self):
        return self.own.at[pl.ds(0, self.main)]

    def move(self, kind, t, src, dst, ctx):
        return remote(src, dst, self.sems.at[kind, t], self.sems.at[kind + 1, t], ctx, self.line.fsdp)

    def up(self, t, src=None):
        block = self.block(self.line.z - t)
        return self.move(0, t, block if src is None else src, block, self.line.above)

    def down(self, t, src=None):
        block = self.block(self.line.z + t)
        return self.move(2, t, block if src is None else src, block, self.line.below)

    def across(self, row, src=None):
        block = self.block(row)
        return self.move(4, row, block if src is None else src, block, self.line.mate)

    def extra_up(self, t):
        return self.move(6, t, self.extras(self.line.z - t), self.extras(self.line.z - t), self.line.above)

    def extra_down(self, t):
        return self.move(8, t, self.extras(self.line.z + t), self.extras(self.line.z + t), self.line.below)

    def extra_across(self, column):
        own = self.own.at[pl.ds(self.main, EXTRA)]
        there = self.all.at[self.line.z * NX + column, pl.ds(self.main, EXTRA)]
        last = self.line.nz - 1
        return remote(own, there, self.sems.at[6, last], self.sems.at[7, last], self.line.mate, self.line.fsdp)

    def start(self):
        line = self.line
        self.extra_across(line.x).start()

        @pl.when(line.z < line.nz - 1)
        def _():
            self.up(0, self.own_main()).start()

        @pl.when(line.z > 0)
        def _():
            self.down(0, self.own_main()).start()

        self.across(line.z, self.own_main()).start()

    def start_extras(self):
        line = self.line
        self.extra_across(1 - line.x).wait_recv()

        @pl.when(line.z < line.nz - 1)
        def _():
            self.extra_up(0).start()

        @pl.when(line.z > 0)
        def _():
            self.extra_down(0).start()

    def forward(self, t):
        line = self.line

        @pl.when(line.z - 1 - t >= 0)
        def _():
            row = line.z - 1 - t
            self.move(0, t, self.own_main(), self.block(row), line.above).wait_recv()

            @pl.when(line.z < line.nz - 1)
            def _():
                self.up(t + 1).start()

            self.across(row).start()
            self.move(6, t, self.extras(row), self.extras(row), line.above).wait_recv()

            @pl.when(line.z < line.nz - 1)
            def _():
                self.extra_up(t + 1).start()

        @pl.when(line.z + 1 + t < line.nz)
        def _():
            row = line.z + 1 + t
            self.move(2, t, self.own_main(), self.block(row), line.below).wait_recv()

            @pl.when(line.z > 0)
            def _():
                self.down(t + 1).start()

            self.across(row).start()
            self.move(8, t, self.extras(row), self.extras(row), line.below).wait_recv()

            @pl.when(line.z > 0)
            def _():
                self.extra_down(t + 1).start()

    def wait_pair(self, row):
        self.move(4, row, self.own_main(), self.block(row, 1 - self.line.x), self.line.mate).wait_recv()

    def finish(self):
        line = self.line
        self.extra_across(line.x).wait_send()
        for t in range(line.nz - 1):

            @pl.when((line.z - t >= 0) & (line.z < line.nz - 1))
            def _():
                self.up(t).wait_send()
                self.extra_up(t).wait_send()

            @pl.when((line.z + t < line.nz) & (line.z > 0))
            def _():
                self.down(t).wait_send()
                self.extra_down(t).wait_send()

        for row in range(line.nz):
            self.across(row).wait_send()


class Scatter:
    @staticmethod
    def scratch(nz, rows, width):
        return [
            pltpu.VMEM((4, nz, rows - EXTRA, width), BF),
            pltpu.VMEM((4, nz, NX, EXTRA, width), BF),
            DMA((10, nz)),
            DMA((2,)),
        ]

    def __init__(self, line, part_ref, out_ref, work, extra, sems, mate_sems):
        self.line, self.part, self.out, self.sems, self.mate_sems = line, part_ref, out_ref, sems, mate_sems
        self.xin, self.acc, self.upin, self.downin = (work.at[i] for i in range(4))
        self.eacc, self.eup, self.edown, self.emate = (extra.at[i] for i in range(4))
        self.main = part_ref.shape[1] - EXTRA

    def move(self, kind, row, src, dst, ctx):
        return remote(src, dst, self.sems.at[kind, row], self.sems.at[kind + 1, row], ctx, self.line.fsdp)

    def across(self, row):
        mates = self.part.at[row * NX + 1 - self.line.x, pl.ds(0, self.main)]
        return self.move(0, row, mates, self.xin.at[row], self.line.mate)

    def up(self, row):
        return self.move(2, row, self.acc.at[row], self.upin.at[row], self.line.above)

    def down(self, row):
        return self.move(4, row, self.acc.at[row], self.downin.at[row], self.line.below)

    def extra_up(self, row):
        return self.move(6, row, self.eacc.at[row], self.eup.at[row], self.line.above)

    def extra_down(self, row):
        return self.move(8, row, self.eacc.at[row], self.edown.at[row], self.line.below)

    def extra_across(self):
        return remote(
            self.emate.at[0, 0], self.emate.at[1, 0], self.mate_sems.at[0], self.mate_sems.at[1], self.line.mate, self.line.fsdp
        )

    def extras(self, row):
        return self.part[pl.ds(row * NX, NX), pl.ds(self.main, EXTRA), :].astype(F32)

    def add(self, i):
        line = self.line
        row = line.far(i)

        @pl.when(row > line.z)
        def _():
            @pl.when(line.z == 0)
            def _():
                self.eacc[row] = self.extras(row).astype(BF)

            @pl.when(line.z > 0)
            def _():
                self.extra_up(row).wait_recv()
                self.eacc[row] = (self.extras(row) + self.eup[row].astype(F32)).astype(BF)

            self.extra_up(row).start()

        @pl.when(row < line.z)
        def _():
            @pl.when(line.z == line.nz - 1)
            def _():
                self.eacc[row] = self.extras(row).astype(BF)

            @pl.when(line.z < line.nz - 1)
            def _():
                self.extra_down(row).wait_recv()
                self.eacc[row] = (self.extras(row) + self.edown[row].astype(F32)).astype(BF)

            self.extra_down(row).start()

        self.across(row).wait_recv()
        mine = self.part[row * NX + line.x, 0 : self.main, :].astype(F32) + self.xin[row].astype(F32)

        @pl.when(row > line.z)
        def _():
            @pl.when(line.z == 0)
            def _():
                self.acc[row] = mine.astype(BF)

            @pl.when(line.z > 0)
            def _():
                self.up(row).wait_recv()
                self.acc[row] = (mine + self.upin[row].astype(F32)).astype(BF)

            self.up(row).start()

        @pl.when(row < line.z)
        def _():
            @pl.when(line.z == line.nz - 1)
            def _():
                self.acc[row] = mine.astype(BF)

            @pl.when(line.z < line.nz - 1)
            def _():
                self.down(row).wait_recv()
                self.acc[row] = (mine + self.downin[row].astype(F32)).astype(BF)

            self.down(row).start()

        @pl.when(row == line.z)
        def _():
            self.out[0 : self.main, :] = mine

    def extra_sum(self, column):
        at = self.line.z * NX + column
        return self.part[at, self.main : self.main + EXTRA, :].astype(F32)

    def finish(self):
        line = self.line
        self.out[self.main : self.main + EXTRA, :] = self.extra_sum(line.x)
        others = self.extra_sum(1 - line.x)

        def more(ref):
            self.out[self.main : self.main + EXTRA, :] += ref[line.z, line.x].astype(F32)

        @pl.when(line.z > 0)
        def _():
            self.extra_up(line.z).wait_recv()
            more(self.eup)

        @pl.when(line.z < line.nz - 1)
        def _():
            self.extra_down(line.z).wait_recv()
            more(self.edown)

        @pl.when(line.z == 0)
        def _():
            self.emate[0, 0] = (others + self.edown[line.z, 1 - line.x].astype(F32)).astype(BF)

        @pl.when(line.z == line.nz - 1)
        def _():
            self.emate[0, 0] = (others + self.eup[line.z, 1 - line.x].astype(F32)).astype(BF)

        @pl.when((line.z > 0) & (line.z < line.nz - 1))
        def _():
            self.emate[0, 0] = (
                others + self.eup[line.z, 1 - line.x].astype(F32) + self.edown[line.z, 1 - line.x].astype(F32)
            ).astype(BF)

        self.extra_across().start()

        @pl.when(line.z > 0)
        def _():
            self.up(line.z).wait_recv()
            self.out[0 : self.main, :] += self.upin[line.z].astype(F32)

        @pl.when(line.z < line.nz - 1)
        def _():
            self.down(line.z).wait_recv()
            self.out[0 : self.main, :] += self.downin[line.z].astype(F32)

        self.extra_across().wait_recv()
        self.out[self.main : self.main + EXTRA, :] += self.emate[1, 0].astype(F32)
        self.extra_across().wait_send()
        for row in range(line.nz):
            self.across(row).wait_send()

            @pl.when(row > line.z)
            def _():
                self.up(row).wait_send()
                self.extra_up(row).wait_send()

            @pl.when(row < line.z)
            def _():
                self.down(row).wait_send()
                self.extra_down(row).wait_send()


def params(collective, vmem_mib):
    return pltpu.CompilerParams(collective_id=collective, has_side_effects=True, vmem_limit_bytes=vmem_mib << 20)


def experts_kernel(nz, layer, x_ref, share_ref, mats_ref, o_ref, all_out, gate_out, up_out,
                   mats, blocks, part, gate, up, load_sem, save_sem, gsems, work, ework, ssems, msems):
    line = Line(nz)
    rows, width = x_ref.shape
    load = pltpu.make_async_copy(mats_ref.at[layer, pl.ds(1, 6)], mats, load_sem)
    load.start()
    line.greet()
    ring = Gather(line, x_ref, blocks, gsems)
    blocks[line.ctx] = x_ref[...]
    ring.start()
    load.wait()
    ring.start_extras()

    def saves(row):
        pair = pl.ds(row * NX, NX)
        return (
            pltpu.make_async_copy(blocks.at[pair], all_out.at[pair], save_sem.at[0, row]),
            pltpu.make_async_copy(gate.at[pair], gate_out.at[pair], save_sem.at[1, row]),
            pltpu.make_async_copy(up.at[pair], up_out.at[pair], save_sem.at[2, row]),
        )

    def step(i, carry):
        @pl.when(i < nz - 1)
        def _():
            ring.forward(i)

        row = line.near(i)
        ring.wait_pair(row)
        pair = pl.ds(row * NX, NX)
        block = blocks[pair].reshape(NX * rows, width)
        share = share_ref[pair].reshape(NX * rows, 2)
        total = None
        for e in range(2):
            gate_act = dot(block, mats[e], NN)
            up_act = dot(block, mats[2 + e], NN)
            units = gate_act.shape[1]
            gate[pair, :, pl.ds(e * units, units)] = gate_act.astype(BF).reshape(NX, rows, units)
            up[pair, :, pl.ds(e * units, units)] = up_act.astype(BF).reshape(NX, rows, units)
            inner = gate_act / (1.0 + jnp.exp(-gate_act)) * up_act * share[:, e : e + 1]
            term = dot(inner.astype(BF), mats[4 + e], NT)
            total = term if total is None else total + term
        part[pair] = total.astype(BF).reshape(NX, rows, width)
        for save in saves(row):
            save.start()
        return carry

    lax.fori_loop(0, nz, step, 0)
    sums = Scatter(line, part, o_ref, work, ework, ssems, msems)
    for i in range(nz):
        sums.across(line.far(i)).start()
    ring.finish()
    for i in range(nz):
        sums.add(i)
    sums.finish()
    for row in range(nz):
        for save in saves(row):
            save.wait()


def experts_forward(block, share, mats, layer, nz):
    rows, width = block.shape
    units = mats.shape[3]
    group = nz * NX
    acts = jax.ShapeDtypeStruct((group, rows, 2 * units), BF)
    return pl.pallas_call(
        functools.partial(experts_kernel, nz, layer),
        out_shape=(
            jax.ShapeDtypeStruct((rows, width), F32),
            jax.ShapeDtypeStruct((group, rows, width), BF),
            acts,
            acts,
        ),
        in_specs=[VM, VM, ANY],
        out_specs=(VM, ANY, ANY, ANY),
        scratch_shapes=[
            pltpu.VMEM((6, width, units), BF),
            pltpu.VMEM((group, rows, width), BF),
            pltpu.VMEM((group, rows, width), BF),
            pltpu.VMEM((group, rows, 2 * units), BF),
            pltpu.VMEM((group, rows, 2 * units), BF),
            DMA,
            DMA((3, nz)),
        ]
        + Gather.scratch(nz)
        + Scatter.scratch(nz, rows, width),
        compiler_params=params(5 + 2 * layer, 60),
        name="experts_forward",
    )(block, share, mats)


def experts_back_kernel(nz, layer, x_ref, share_ref, mats_ref, gate_ref, up_ref, o_ref, all_out, dgate_out, dup_out, inner_out,
                        mats, blocks, part, gate, up, inners, load_sem, save_sem, gsems, work, ework, ssems, msems):
    line = Line(nz)
    rows, width = x_ref.shape
    loads = (
        pltpu.make_async_copy(mats_ref.at[layer, pl.ds(1, 6)], mats, load_sem.at[0]),
        pltpu.make_async_copy(gate_ref, gate, load_sem.at[1]),
        pltpu.make_async_copy(up_ref, up, load_sem.at[2]),
    )
    for load in loads:
        load.start()
    line.greet()
    ring = Gather(line, x_ref, blocks, gsems)
    blocks[line.ctx] = x_ref[...]
    ring.start()
    for load in loads:
        load.wait()
    ring.start_extras()

    def saves(row):
        pair = pl.ds(row * NX, NX)
        return (
            pltpu.make_async_copy(blocks.at[pair], all_out.at[pair], save_sem.at[0, row]),
            pltpu.make_async_copy(gate.at[pair], dgate_out.at[pair], save_sem.at[1, row]),
            pltpu.make_async_copy(up.at[pair], dup_out.at[pair], save_sem.at[2, row]),
            pltpu.make_async_copy(inners.at[pair], inner_out.at[pair], save_sem.at[3, row]),
        )

    def step(i, carry):
        @pl.when(i < nz - 1)
        def _():
            ring.forward(i)

        row = line.near(i)
        ring.wait_pair(row)
        pair = pl.ds(row * NX, NX)
        block = blocks[pair].reshape(NX * rows, width)
        share = share_ref[pair].reshape(NX * rows, 2)
        total = None
        units = mats.shape[2]
        for e in range(2):
            part_of = pl.ds(e * units, units)
            gate_act = gate[pair, :, part_of].reshape(NX * rows, units).astype(F32)
            up_act = up[pair, :, part_of].reshape(NX * rows, units).astype(F32)
            grad_inner = dot(block, mats[4 + e], NN) * share[:, e : e + 1]
            sigmoid = 1.0 / (1.0 + jnp.exp(-gate_act))
            silu = gate_act * sigmoid
            d_gate = (grad_inner * up_act * (sigmoid + silu * (1.0 - sigmoid))).astype(BF)
            d_up = (grad_inner * silu).astype(BF)
            inners[pair, :, part_of] = (silu * up_act * share[:, e : e + 1]).astype(BF).reshape(NX, rows, units)
            gate[pair, :, part_of] = d_gate.reshape(NX, rows, units)
            up[pair, :, part_of] = d_up.reshape(NX, rows, units)
            term = dot(d_gate, mats[e], NT) + dot(d_up, mats[2 + e], NT)
            total = term if total is None else total + term
        part[pair] = total.astype(BF).reshape(NX, rows, width)
        for save in saves(row):
            save.start()
        return carry

    lax.fori_loop(0, nz, step, 0)
    sums = Scatter(line, part, o_ref, work, ework, ssems, msems)
    for i in range(nz):
        sums.across(line.far(i)).start()
    ring.finish()
    for i in range(nz):
        sums.add(i)
    sums.finish()
    for row in range(nz):
        for save in saves(row):
            save.wait()


def experts_backward(block, share, mats, layer, gate_act, up_act, nz):
    rows, width = block.shape
    units = mats.shape[3]
    group = nz * NX
    acts = jax.ShapeDtypeStruct((group, rows, 2 * units), BF)
    held = pltpu.VMEM((group, rows, 2 * units), BF)
    return pl.pallas_call(
        functools.partial(experts_back_kernel, nz, layer),
        out_shape=(
            jax.ShapeDtypeStruct((rows, width), F32),
            jax.ShapeDtypeStruct((group, rows, width), BF),
            acts,
            acts,
            acts,
        ),
        in_specs=[VM, VM, ANY, ANY, ANY],
        out_specs=(VM, ANY, ANY, ANY, ANY),
        scratch_shapes=[
            pltpu.VMEM((6, width, units), BF),
            pltpu.VMEM((group, rows, width), BF),
            pltpu.VMEM((group, rows, width), BF),
            held,
            held,
            held,
            DMA((3,)),
            DMA((4, nz)),
        ]
        + Gather.scratch(nz)
        + Scatter.scratch(nz, rows, width),
        compiler_params=params(6 + 2 * layer, 60),
        name="experts_backward",
    )(block, share, mats, gate_act, up_act)


def far_of(nz, z, i):
    mid1 = jnp.where(i == 0, 3, jnp.where(i == 1, 0, jnp.where(i == 2, 2, 1)))
    mid2 = jnp.where(i == 0, 0, jnp.where(i == 1, 3, jnp.where(i == 2, 1, 2)))
    return jnp.where(z == 0, nz - 1 - i, jnp.where(z == nz - 1, i, jnp.where(z == 1, mid1, mid2)))


class Exchange:
    @staticmethod
    def scratch(nz, blk, lead=()):
        return [
            pltpu.VMEM(lead + (2, 2, 2) + blk, BF),
            pltpu.VMEM(lead + (nz,) + blk, BF),
            DMA(lead + (2, nz, nz, 2)),
            DMA(lead + (2, nz)),
        ]

    def __init__(self, line, src_at, dst_at, passing, for_mate, zs, xs, lead=()):
        self.line, self.src_at, self.dst_at, self.lead = line, src_at, dst_at, lead
        self.passing, self.for_mate, self.zs, self.xs = passing, for_mate, zs, xs

    def held(self, way, src, dest, side, at):
        last = self.line.nz - 1
        slot = (dest - at - 1) + src if way == 0 else (at - dest - 1) + last - src
        return self.passing.at[self.lead + (way, slot, side)]

    def zsem(self, kind, src, dest, side):
        return self.zs.at[self.lead + (kind, src, dest, side)]

    def hop(self, way, src, dest, side, ref):
        line = self.line
        to = line.z + 1 if way == 0 else line.z - 1
        sems = self.zsem(0, src, dest, side), self.zsem(1, src, dest, side)
        target = to * NX + line.x

        @pl.when(dest == to)
        def _():
            land = self.dst_at(src * NX + line.x) if side == 0 else self.for_mate.at[self.lead + (src,)]
            remote(ref, land, *sems, target, line.fsdp).start()

        @pl.when(dest != to)
        def _():
            remote(ref, self.held(way, src, dest, side, to), *sems, target, line.fsdp).start()

    def to_mate(self, src, ref=None):
        line = self.line
        ref = self.for_mate.at[self.lead + (src,)] if ref is None else ref
        return remote(ref, self.dst_at(src * NX + line.x), self.xs.at[self.lead + (0, src)], self.xs.at[self.lead + (1, src)], line.mate, line.fsdp)

    def send(self, dest):
        line = self.line
        for side, column in ((0, line.x), (1, 1 - line.x)):
            ref = self.src_at(dest * NX + column)

            @pl.when(dest > line.z)
            def _():
                self.hop(0, line.z, dest, side, ref)

            @pl.when(dest < line.z)
            def _():
                self.hop(1, line.z, dest, side, ref)

        @pl.when(dest == line.z)
        def _():
            self.to_mate(line.z, self.src_at(line.mate)).start()

    def events(self, i):
        line = self.line
        found = []
        for k in range(1, line.nz):
            j = i - k
            for way in range(2):
                src = line.z - k if way == 0 else line.z + k
                dest = far_of(line.nz, src, j)
                here = (dest >= line.z) if way == 0 else (dest <= line.z)
                found.append((way, src, dest, (src >= 0) & (src < line.nz) & (j >= 0) & (j < line.nz - 1) & here))
        return found

    def handle(self, way, src, dest, arrived):
        line = self.line
        for side in range(2):
            wait = self.held(way, 0 if way == 0 else line.nz - 1, line.z + 1 if way == 0 else line.z - 1, side, line.z)
            remote(wait, wait, self.zsem(0, src, dest, side), self.zsem(1, src, dest, side), line.mate, line.fsdp).wait_recv()

            @pl.when(dest != line.z)
            def _():
                self.hop(way, src, dest, side, self.held(way, src, dest, side, line.z))

        @pl.when(dest == line.z)
        def _():
            self.to_mate(src).start()
            arrived(src * NX + line.x)

    def mate_arrived(self, src):
        line = self.line
        wait = self.for_mate.at[self.lead + (src,)]
        remote(wait, wait, self.xs.at[self.lead + (0, src)], self.xs.at[self.lead + (1, src)], line.mate, line.fsdp).wait_recv()

    def finish(self):
        line = self.line
        wait = self.for_mate.at[self.lead + (0,)]
        for src in range(line.nz):
            for dest in range(line.nz):
                if src != dest:
                    passes = (line.z >= src) & (line.z < dest) if src < dest else (line.z <= src) & (line.z > dest)

                    @pl.when(passes)
                    def _():
                        for side in range(2):
                            remote(wait, wait, self.zsem(0, src, dest, side), self.zsem(1, src, dest, side), line.mate, line.fsdp).wait_send()

            self.to_mate(src).wait_send()


LAG = 3


def weights_kernel(nctx, nfs, rows, w_ref, g_ref, o_ref, go_ref, passing, for_mate, zs, xs, own_sem, y_sem, c_sem, gown_sem, gp_sem, gy_sem, gc_sem):
    nz = nctx // NX
    line = Line(nz)
    ctx, fsdp = line.ctx, line.fsdp
    layers = w_ref.shape[0]
    y, core = fsdp // NCORE, fsdp % NCORE
    y_mate = (1 - y) * NCORE + core
    c_mate = y * NCORE + 1 - core
    y_c_mate = (1 - y) * NCORE + 1 - core
    barrier = pltpu.get_barrier_semaphore()
    for step in range(1, nctx):
        greet(barrier, (ctx + step) % nctx, fsdp)
    for other in (y_mate, c_mate):
        greet(barrier, ctx, other)
    pl.semaphore_wait(barrier, nctx + 1)

    def place(layer, s, f):
        return o_ref.at[layer, :, pl.ds(pl.multiple_of((s * nfs + f) * rows, rows), rows), :]

    def swap(layer):
        return Exchange(
            line,
            lambda to: w_ref.at[layer, to],
            lambda frm: place(layer, frm, fsdp),
            passing, for_mate, zs, xs,
            (layer,),
        )

    def over_y(layer, frm, f, ref=None):
        return remote(place(layer, frm, f) if ref is None else ref, place(layer, frm, f), y_sem.at[0, layer, frm], y_sem.at[1, layer, frm], ctx, y_mate)

    def over_c(layer, frm, f, k, ref=None):
        return remote(place(layer, frm, f) if ref is None else ref, place(layer, frm, f), c_sem.at[0, k, layer, frm], c_sem.at[1, k, layer, frm], ctx, c_mate)

    def own(layer):
        return pltpu.make_async_copy(w_ref.at[layer, ctx], place(layer, ctx, fsdp), own_sem.at[layer])

    def begin(layer):
        exchange = swap(layer)
        for i in range(nz - 1):
            exchange.send(line.far(i))
        exchange.send(line.z)
        over_y(layer, ctx, fsdp, w_ref.at[layer, ctx]).start()
        over_c(layer, ctx, fsdp, 0, w_ref.at[layer, ctx]).start()
        own(layer).start()

    def arrived(layer, frm):
        over_y(layer, frm, fsdp).start()
        over_c(layer, frm, fsdp, 0).start()

    def from_y(layer, frm):
        over_y(layer, frm, y_mate).wait_recv()
        over_c(layer, frm, y_mate, 1).start()

    def take(layer, i):
        exchange = swap(layer)
        for way, src, dest, real in exchange.events(i):

            @pl.when(real)
            def _():
                exchange.handle(way, src, dest, lambda frm: arrived(layer, frm))

        def mine(late, then):
            @pl.when(i == late)
            def _():
                then(line.z)

            for way, src, dest, real in exchange.events(i - late):

                @pl.when(real & (dest == line.z))
                def _():
                    then(src)

        def mates(src):
            exchange.mate_arrived(src)
            arrived(layer, src * NX + 1 - line.x)

        mine(1, mates)
        mine(2, lambda src: from_y(layer, src * NX + line.x))
        mine(3, lambda src: from_y(layer, src * NX + 1 - line.x))

    def small(to):
        return remote(g_ref.at[to], go_ref.at[ctx * nfs + fsdp], gp_sem.at[0, to], gp_sem.at[1, ctx], to, fsdp)

    def small_in(frm):
        return remote(g_ref.at[ctx], go_ref.at[frm * nfs + fsdp], gp_sem.at[0, frm], gp_sem.at[1, frm], frm, fsdp)

    def small_y(frm, f):
        return remote(go_ref.at[frm * nfs + f], go_ref.at[frm * nfs + f], gy_sem.at[0, frm], gy_sem.at[1, frm], ctx, y_mate)

    def small_c(frm, f, k):
        return remote(go_ref.at[frm * nfs + f], go_ref.at[frm * nfs + f], gc_sem.at[0, k, frm], gc_sem.at[1, k, frm], ctx, c_mate)

    small_own = pltpu.make_async_copy(g_ref.at[ctx], go_ref.at[ctx * nfs + fsdp], gown_sem)
    small_own.start()
    for step in range(1, nctx):
        small((ctx + step) % nctx).start()
    steps = 2 * nz - 3 + 3

    def step(i, carry):
        for layer in range(layers):
            at = i - LAG * layer

            @pl.when(at == 0)
            def _():
                begin(layer)

        def each(layer, carry):
            at = i - LAG * layer

            @pl.when((at > 0) & (at <= steps))
            def _():
                take(layer, at)

            return carry

        lax.fori_loop(0, layers, each, 0)
        return carry

    lax.fori_loop(0, steps + 1 + LAG * (layers - 1), step, 0)
    small_own.wait()
    for k in range(nctx):
        if k:
            small_in((ctx + k) % nctx).wait_recv()
        small_y((ctx + k) % nctx, fsdp).start()
        small_c((ctx + k) % nctx, fsdp, 0).start()
    for k in range(nctx):
        small_y((ctx + k) % nctx, y_mate).wait_recv()
        small_c((ctx + k) % nctx, y_mate, 1).start()
    for frm in range(nctx):
        small_c(frm, c_mate, 0).wait_recv()
        small_c(frm, y_c_mate, 1).wait_recv()
        small_c(frm, fsdp, 0).wait_send()
        small_c(frm, y_mate, 1).wait_send()
        small_y(frm, fsdp).wait_send()
    for step_ in range(1, nctx):
        small((ctx + step_) % nctx).wait_send()

    def close(layer, carry):
        own(layer).wait()
        for frm in range(nctx):
            over_c(layer, frm, c_mate, 0).wait_recv()
            over_c(layer, frm, y_c_mate, 1).wait_recv()
            over_c(layer, frm, fsdp, 0).wait_send()
            over_c(layer, frm, y_mate, 1).wait_send()
            over_y(layer, frm, fsdp).wait_send()
        swap(layer).finish()
        return carry

    lax.fori_loop(0, layers, close, 0)


def spread_weights(send, small, nfs):
    layers, nctx, mats, rows, width = send.shape
    return pl.pallas_call(
        functools.partial(weights_kernel, nctx, nfs, rows),
        out_shape=(
            jax.ShapeDtypeStruct((layers, mats, nctx * nfs * rows, width), send.dtype),
            jax.ShapeDtypeStruct((nctx * nfs,) + small.shape[1:], small.dtype),
        ),
        in_specs=[VM, VM],
        out_specs=(ANY, ANY),
        scratch_shapes=Exchange.scratch(nctx // NX, (mats, rows, width), (layers,))
        + [
            DMA((layers,)),
            DMA((2, layers, nctx)),
            DMA((2, 2, layers, nctx)),
            DMA,
            DMA((2, nctx)),
            DMA((2, nctx)),
            DMA((2, 2, nctx)),
        ],
        compiler_params=params(3, 40),
        name="spread_weights",
    )(send, small)


def grads_kernel(nctx, nfs, rows, layers, *refs):
    count = 9 * layers
    ins, (e_ref, o_ref, eo_ref), refs = refs[:count], refs[count : count + 3], refs[count + 3 :]
    tall, dproj, attended, dgate, dup, inner, mine, cin, yin, e_cin, e_half, e_yin, e_full = refs[:13]
    tall_sem, wide_sem, own_sem, c_sem, y_sem, p_sem, eown_sem, ec_sem, ey_sem, ep_sem = refs[13:]
    nz = nctx // NX
    line = Line(nz)
    ctx, fsdp = line.ctx, line.fsdp
    y, core = fsdp // NCORE, fsdp % NCORE
    y_mate = (1 - y) * NCORE + core
    c_mate = y * NCORE + 1 - core
    mats, slab = mine.shape[1], mine.shape[2]
    proj = mine.shape[3] - attended.shape[2]
    units = dgate.shape[2] // 2
    items = layers * nz

    def layer_of(i):
        return layers - 1 - i // nz

    def row_of(i):
        return line.far(i % nz)

    def wide_loads(layer):
        _, dproj_in, _, attended_in, _, dgate_in, dup_in, _, inner_in = ins[9 * layer : 9 * layer + 9]
        pairs = ((dproj_in, dproj), (attended_in, attended), (dgate_in, dgate), (dup_in, dup), (inner_in, inner))
        return [pltpu.make_async_copy(src, dst.at[layer], wide_sem.at[k, layer]) for k, (src, dst) in enumerate(pairs)]

    def tall_loads(i, layer):
        normed_in, _, middle_in, _, moe_in, _, _, grad_in, _ = ins[9 * layer : 9 * layer + 9]
        lanes = pl.ds(pl.multiple_of(row_of(i) * slab, 128), slab)
        return [
            pltpu.make_async_copy(src.at[:, lanes], tall.at[i % 2, k], tall_sem.at[i % 2, k])
            for k, src in enumerate((normed_in, middle_in, moe_in, grad_in))
        ]

    def load(i):
        for layer in range(layers):

            @pl.when(layer_of(i) == layer)
            def _():
                for copy in tall_loads(i, layer):
                    copy.start()

    for layer in reversed(range(layers)):
        for copy in wide_loads(layer):
            copy.start()
        if layer == layers - 1:
            load(0)
    barrier = pltpu.get_barrier_semaphore()
    for step in range(1, nctx):
        greet(barrier, (ctx + step) % nctx, fsdp)
    for other in (y_mate, c_mate):
        greet(barrier, ctx, other)
    pl.semaphore_wait(barrier, nctx + 1)

    def span(side, f):
        return pl.ds(pl.multiple_of((side * nfs + f) * rows, rows), rows)

    def to_c(i, side, k):
        layer, s = layer_of(i), row_of(i) * NX + side
        f = (1 - y if k == 0 else y) * NCORE + 1 - core
        return remote(mine.at[i % 3, :, span(side, f), :], cin.at[layer, k, s], c_sem.at[0, layer, k, s], c_sem.at[1, layer, k, s], ctx, c_mate)

    def to_y(layer, s):
        return remote(cin.at[layer, 0, s], yin.at[layer, s], y_sem.at[0, layer, s], y_sem.at[1, layer, s], ctx, y_mate)

    def out(layer, s):
        return remote(cin.at[layer, 1, s], o_ref.at[layer, ctx], p_sem.at[0, layer, s], p_sem.at[1, layer, ctx], s, fsdp)

    def out_in(layer, s):
        return remote(cin.at[layer, 1, s], o_ref.at[layer, s], p_sem.at[0, layer, s], p_sem.at[1, layer, s], s, fsdp)

    def own(layer):
        return pltpu.make_async_copy(cin.at[layer, 1, ctx], o_ref.at[layer, ctx], own_sem.at[layer])

    e_to_c = remote(e_ref.at[1 - core], e_cin, ec_sem.at[0], ec_sem.at[1], ctx, c_mate)
    e_to_y = remote(e_half.at[1 - y], e_yin, ey_sem.at[0], ey_sem.at[1], ctx, y_mate)
    e_own = pltpu.make_async_copy(e_full.at[ctx], eo_ref.at[ctx], eown_sem)

    def e_out(s):
        return remote(e_full.at[s], eo_ref.at[ctx], ep_sem.at[0, s], ep_sem.at[1, ctx], s, fsdp)

    def e_out_in(s):
        return remote(e_full.at[s], eo_ref.at[s], ep_sem.at[0, s], ep_sem.at[1, s], s, fsdp)

    e_to_c.start()

    def compute(i):
        layer, slot, here = layer_of(i), i % 2, i % 3
        mine[here, 0, :, pl.ds(0, proj)] = dot(tall[slot, 0], dproj[layer], TN)[:, :proj].astype(BF)
        mine[here, 0, :, pl.ds(proj, mine.shape[3] - proj)] = dot(tall[slot, 1], attended[layer], TN).astype(BF)
        for e in range(2):
            part_of = pl.ds(e * units, units)
            mine[here, 1 + e] = dot(tall[slot, 2], dgate[layer, :, part_of], TN).astype(BF)
            mine[here, 3 + e] = dot(tall[slot, 2], dup[layer, :, part_of], TN).astype(BF)
            mine[here, 5 + e] = dot(tall[slot, 3], inner[layer, :, part_of], TN).astype(BF)

    def first(i, side):
        layer, s = layer_of(i), row_of(i) * NX + side
        to_c(i, side, 0).wait_recv()

        def one(m, _):
            term = mine[i % 3, m, span(side, y_mate), :].astype(F32)
            cin[layer, 0, s, m] = (term + cin[layer, 0, s, m].astype(F32)).astype(BF)
            return 0

        lax.fori_loop(0, mats, one, 0)
        to_y(layer, s).start()

    def second(i, side):
        layer, s = layer_of(i), row_of(i) * NX + side
        to_c(i, side, 1).wait_recv()
        to_y(layer, s).wait_recv()

        def one(m, _):
            term = mine[i % 3, m, span(side, fsdp), :].astype(F32) + yin[layer, s, m].astype(F32)
            cin[layer, 1, s, m] = (term + cin[layer, 1, s, m].astype(F32)).astype(BF)
            return 0

        lax.fori_loop(0, mats, one, 0)
        for k in range(2):
            to_c(i, side, k).wait_send()

        @pl.when(s != ctx)
        def _():
            out(layer, s).start()

        @pl.when(s == ctx)
        def _():
            own(layer).start()

    def step(i, carry):
        @pl.when(i < items)
        def _():
            for layer in range(layers):

                @pl.when(i == (layers - 1 - layer) * nz)
                def _():
                    for copy in wide_loads(layer):
                        copy.wait()

            for copy in tall_loads(i, 0):
                copy.wait()

            @pl.when(i + 1 < items)
            def _():
                load(i + 1)

            compute(i)
            for k in range(2):
                for side in range(NX):
                    to_c(i, side, k).start()

        @pl.when((i >= 1) & (i < items + 1))
        def _():
            for side in range(NX):
                first(i - 1, side)

        @pl.when(i >= 2)
        def _():
            for side in range(NX):
                second(i - 2, side)

        @pl.when(i == 1)
        def _():
            e_to_c.wait_recv()
            e_half[...] = e_ref[core] + e_cin[...]
            e_to_y.start()

        @pl.when(i == 3)
        def _():
            e_to_y.wait_recv()
            e_full[...] = e_half[y] + e_yin[...]
            e_own.start()
            for step_ in range(1, nctx):
                e_out((ctx + step_) % nctx).start()

        return carry

    lax.fori_loop(0, items + 2, step, 0)
    for layer in range(layers):
        own(layer).wait()
        for s in range(nctx):
            to_y(layer, s).wait_send()

            @pl.when(s != ctx)
            def _():
                out(layer, s).wait_send()
                out_in(layer, s).wait_recv()

    for s in range(nctx):

        @pl.when(s != ctx)
        def _():
            e_out(s).wait_send()
            e_out_in(s).wait_recv()

    e_to_c.wait_send()
    e_to_y.wait_send()
    e_own.wait()


def collect_grads(nctx, nfs, layer_args, extra):
    layers = len(layer_args)
    normed, dproj, middle, attended, moe, dgate, dup, grad, inner = layer_args[0]
    group_rows, width = normed.shape
    rows = width // (nctx * nfs)
    slab = NX * nfs * rows
    mats, cols = 7, dgate.shape[1] // 2
    blk = (mats, rows, cols)
    tile = extra.shape[3:]
    held = [pltpu.VMEM((layers,) + part.shape, BF) for part in (dproj, attended, dgate, dup, inner)]
    return pl.pallas_call(
        functools.partial(grads_kernel, nctx, nfs, rows, layers),
        out_shape=(jax.ShapeDtypeStruct((layers, nctx) + blk, BF), jax.ShapeDtypeStruct((nctx,) + tile, F32)),
        in_specs=[ANY] * (9 * layers) + [VM],
        out_specs=(ANY, ANY),
        scratch_shapes=[pltpu.VMEM((2, 4, group_rows, slab), BF)]
        + held
        + [
            pltpu.VMEM((3, mats, slab, cols), BF),
            pltpu.VMEM((layers, 2, nctx) + blk, BF),
            pltpu.VMEM((layers, nctx) + blk, BF),
            pltpu.VMEM((2, nctx) + tile, F32),
            pltpu.VMEM((2, nctx) + tile, F32),
            pltpu.VMEM((nctx,) + tile, F32),
            pltpu.VMEM((nctx,) + tile, F32),
            DMA((2, 4)),
            DMA((5, layers)),
            DMA((layers,)),
            DMA((2, layers, 2, nctx)),
            DMA((2, layers, nctx)),
            DMA((2, layers, nctx)),
            DMA,
            DMA((2,)),
            DMA((2,)),
            DMA((2, nctx)),
        ],
        compiler_params=params(4, 63),
        name="collect_grads",
    )(*[part for args in layer_args for part in args], extra)


def spin(values, cos_part, sin_part):
    lane = lax.broadcasted_iota(jnp.int32, values.shape, 1) % HEAD_DIM
    half_dim = HEAD_DIM // 2
    swapped = jnp.where(
        lane < half_dim,
        pltpu.roll(values, values.shape[1] - half_dim, 1),
        pltpu.roll(values, half_dim, 1),
    )
    return values * cos_part + swapped * sin_part


def attention_kernel(nz, layer, x_ref, mats_ref, cos_ref, sin_ref, key_at_ref, query_at_ref,
                     o_ref, all_out, q_ref, k_ref, v_ref, peak_ref, share_ref, att_ref,
                     attn, out_w, blocks, part, v_turned, probs, load_sem, save_sem, gsems, work, ework, ssems, msems):
    line = Line(nz)
    rows, width = x_ref.shape
    pair_rows = NX * rows
    heads = q_ref.shape[1] // rows
    o_at = (heads + 2) * HEAD_DIM
    wide = -(-o_at // 128) * 128
    load = pltpu.make_async_copy(mats_ref.at[layer, 0], attn, load_sem)
    load.start()
    line.greet()
    ring = Gather(line, x_ref, blocks, gsems)
    blocks[line.ctx] = x_ref[...]
    ring.start()
    load.wait()
    out_w[...] = attn[:, o_at:]
    ring.start_extras()

    def save(row):
        pair = pl.ds(row * NX, NX)
        return pltpu.make_async_copy(blocks.at[pair], all_out.at[pair], save_sem.at[row])

    def project(i, carry):
        @pl.when(i < nz - 1)
        def _():
            ring.forward(i)

        row = line.near(i)
        ring.wait_pair(row)
        pair = pl.ds(row * NX, NX)
        tall = pl.ds(pl.multiple_of(row * pair_rows, pair_rows), pair_rows)
        block = blocks[pair].reshape(pair_rows, width)
        save(row).start()
        proj = dot(block, attn[:, :wide], NN)
        cos_part, sin_part = cos_ref[tall, :], sin_ref[tall, :]
        first = spin(proj[:, :128], cos_part, sin_part)
        second = spin(proj[:, 128:256], cos_part, sin_part)
        values = proj[:, 256 : 256 + HEAD_DIM]
        for side in range(NX):
            at = slice(side * rows, (side + 1) * rows)
            q_ref[row * NX + side, 0:rows, :] = first[at, :HEAD_DIM].astype(BF)
            q_ref[row * NX + side, rows : 2 * rows, :] = first[at, HEAD_DIM:].astype(BF)
            q_ref[row * NX + side, 2 * rows : 3 * rows, :] = second[at, :HEAD_DIM].astype(BF)
        k_ref[tall, :] = second[:, HEAD_DIM:].astype(BF)
        v_ref[tall, :] = values.astype(BF)
        v_turned[:, tall] = values.T.astype(BF)
        return carry

    lax.fori_loop(0, nz, project, 0)
    ring.finish()
    sums = Scatter(line, part, o_ref, work, ework, ssems, msems)

    def attend(at):
        scores = dot(k_ref[...], q_ref[at], NT)
        key_at = key_at_ref[...]
        visible = (key_at >= query_at_ref[at, 0:1, :]) & (key_at <= query_at_ref[at, 1:2, :])
        for head in range(heads):
            lanes = slice(head * rows, (head + 1) * rows)
            raw = jnp.where(visible, scores[:, lanes] * HEAD_DIM**-0.5, NEGATIVE)
            peak = jnp.max(raw, axis=0, keepdims=True)
            powers = jnp.exp(raw - peak)
            peak_ref[at, :, lanes] = peak
            share_ref[at, :, lanes] = 1.0 / jnp.sum(powers, axis=0, keepdims=True)
            probs[:, lanes] = powers.astype(BF)
        turned = dot(v_turned[...], probs[...], NN) * share_ref[at]
        stacked = turned.T.astype(BF)
        for head in range(heads):
            att_ref[at, :, head * HEAD_DIM : (head + 1) * HEAD_DIM] = stacked[head * rows : (head + 1) * rows]
        part[at] = dot(att_ref[at], out_w[...], NT).astype(BF)

    def step(i, carry):
        row = line.far(i)
        attend(row * NX + 1 - line.x)
        sums.across(row).start()
        attend(row * NX + line.x)

        @pl.when(i > 0)
        def _():
            sums.add(i - 1)

        return carry

    lax.fori_loop(0, nz, step, 0)
    sums.add(nz - 1)
    sums.finish()
    for row in range(nz):
        save(row).wait()


def attention_rows(block, mats, layer, cos_part, sin_part, key_at, query_at, nz):
    rows, width = block.shape
    group = nz * NX
    group_rows = group * rows
    heads = 3
    return pl.pallas_call(
        functools.partial(attention_kernel, nz, layer),
        out_shape=(
            jax.ShapeDtypeStruct((rows, width), F32),
            jax.ShapeDtypeStruct((group, rows, width), BF),
            jax.ShapeDtypeStruct((group, heads * rows, HEAD_DIM), BF),
            jax.ShapeDtypeStruct((group_rows, HEAD_DIM), BF),
            jax.ShapeDtypeStruct((group_rows, HEAD_DIM), BF),
            jax.ShapeDtypeStruct((group, 1, heads * rows), F32),
            jax.ShapeDtypeStruct((group, 1, heads * rows), F32),
            jax.ShapeDtypeStruct((group, rows, heads * HEAD_DIM), BF),
        ),
        in_specs=[VM, ANY, VM, VM, VM, VM],
        out_specs=(VM, ANY, VM, VM, VM, VM, VM, VM),
        scratch_shapes=[
            pltpu.VMEM(mats.shape[2:], BF),
            pltpu.VMEM((width, heads * HEAD_DIM), BF),
            pltpu.VMEM((group, rows, width), BF),
            pltpu.VMEM((group, rows, width), BF),
            pltpu.VMEM((HEAD_DIM, group_rows), BF),
            pltpu.VMEM((group_rows, heads * rows), BF),
            DMA,
            DMA((nz,)),
        ]
        + Gather.scratch(nz)
        + Scatter.scratch(nz, rows, width),
        compiler_params=params(9 + 2 * layer, 60),
        name="attention_forward",
    )(block, mats, cos_part, sin_part, key_at, query_at)


def attention_back_kernel(nz, layer, x_ref, mats_ref, cos_ref, sin_ref, key_at_ref, query_at_ref, q_ref, k_ref, v_ref, peak_ref, share_ref,
                          o_ref, all_out, dproj_ref,
                          attn, out_w, blocks, part, k_turned, probs, slopes, dq, dk, dv, load_sem, save_sem, gsems, work, ework, ssems, msems):
    line = Line(nz)
    rows, width = x_ref.shape
    pair_rows = NX * rows
    heads = q_ref.shape[1] // rows
    o_at = (heads + 2) * HEAD_DIM
    wide = dproj_ref.shape[2]
    scale = HEAD_DIM**-0.5
    load = pltpu.make_async_copy(mats_ref.at[layer, 0], attn, load_sem)
    load.start()
    line.greet()
    ring = Gather(line, x_ref, blocks, gsems)
    blocks[line.ctx] = x_ref[...]
    ring.start()
    k_turned[...] = k_ref[...].astype(F32).T.astype(BF)
    dk[...] = jnp.zeros(dk.shape, F32)
    dv[...] = jnp.zeros(dv.shape, F32)
    load.wait()
    out_w[...] = attn[:, o_at:]
    ring.start_extras()

    def save(row):
        pair = pl.ds(row * NX, NX)
        return pltpu.make_async_copy(blocks.at[pair], all_out.at[pair], save_sem.at[row])

    def back(at):
        d_att = dot(blocks[at], out_w[...], NN)
        d_heads = jnp.concatenate(
            [d_att[:, head * HEAD_DIM : (head + 1) * HEAD_DIM] for head in range(heads)], axis=0
        ).astype(BF)
        scores = dot(k_ref[...], q_ref[at], NT)
        d_probs = dot(v_ref[...], d_heads, NT)
        key_at = key_at_ref[...]
        visible = (key_at >= query_at_ref[at, 0:1, :]) & (key_at <= query_at_ref[at, 1:2, :])
        for head in range(heads):
            lanes = slice(head * rows, (head + 1) * rows)
            raw = jnp.where(visible, scores[:, lanes] * scale, NEGATIVE)
            prob = jnp.exp(raw - peak_ref[at, :, lanes]) * share_ref[at, :, lanes]
            grad = d_probs[:, lanes]
            delta = jnp.sum(prob * grad, axis=0, keepdims=True)
            probs[:, lanes] = prob.astype(BF)
            slopes[:, lanes] = (prob * (grad - delta)).astype(BF)
        dv[...] += dot(probs[...], d_heads, NN)
        dk[...] += dot(slopes[...], q_ref[at], NN)
        stacked = dot(k_turned[...], slopes[...], NN).T * scale
        for head in range(heads):
            dq[at, :, head * HEAD_DIM : (head + 1) * HEAD_DIM] = stacked[head * rows : (head + 1) * rows]

    def take(i, carry):
        @pl.when(i < nz - 1)
        def _():
            ring.forward(i)

        row = line.near(i)
        back(row * NX + line.x)
        ring.wait_pair(row)
        save(row).start()
        back(row * NX + 1 - line.x)
        return carry

    lax.fori_loop(0, nz, take, 0)
    ring.finish()
    sums = Scatter(line, part, o_ref, work, ework, ssems, msems)

    def project(at):
        tall = pl.ds(pl.multiple_of(at * rows, rows), rows)
        cos_part, sin_part = cos_ref[tall, :], -sin_ref[tall, :]
        block_dq = dq[at]
        second = jnp.concatenate([block_dq[:, 128:], dk[tall, :] * scale], axis=1)
        dproj_ref[at, :, 0:128] = spin(block_dq[:, :128], cos_part, sin_part).astype(BF)
        dproj_ref[at, :, 128:256] = spin(second, cos_part, sin_part).astype(BF)
        last = jnp.concatenate([dv[tall, :], jnp.zeros((rows, wide - 256 - HEAD_DIM), F32)], axis=1)
        dproj_ref[at, :, 256:wide] = last.astype(BF)
        part[at] = dot(dproj_ref[at], attn[:, :wide], NT).astype(BF)

    def step(i, carry):
        row = line.far(i)
        project(row * NX + 1 - line.x)
        sums.across(row).start()
        project(row * NX + line.x)

        @pl.when(i > 0)
        def _():
            sums.add(i - 1)

        return carry

    lax.fori_loop(0, nz, step, 0)
    sums.add(nz - 1)
    sums.finish()
    for row in range(nz):
        save(row).wait()


def attention_rows_back(block, mats, layer, cos_part, sin_part, key_at, query_at, queries, keys, values, peaks, shares, nz):
    rows, width = block.shape
    group = nz * NX
    group_rows = group * rows
    heads = 3
    wide = 384
    return pl.pallas_call(
        functools.partial(attention_back_kernel, nz, layer),
        out_shape=(
            jax.ShapeDtypeStruct((rows, width), F32),
            jax.ShapeDtypeStruct((group, rows, width), BF),
            jax.ShapeDtypeStruct((group, rows, wide), BF),
        ),
        in_specs=[VM, ANY] + [VM] * 9,
        out_specs=(VM, ANY, VM),
        scratch_shapes=[
            pltpu.VMEM(mats.shape[2:], BF),
            pltpu.VMEM((width, heads * HEAD_DIM), BF),
            pltpu.VMEM((group, rows, width), BF),
            pltpu.VMEM((group, rows, width), BF),
            pltpu.VMEM((HEAD_DIM, group_rows), BF),
            pltpu.VMEM((group_rows, heads * rows), BF),
            pltpu.VMEM((group_rows, heads * rows), BF),
            pltpu.VMEM((group, rows, heads * HEAD_DIM), F32),
            pltpu.VMEM((group_rows, HEAD_DIM), F32),
            pltpu.VMEM((group_rows, HEAD_DIM), F32),
            DMA,
            DMA((nz,)),
        ]
        + Gather.scratch(nz)
        + Scatter.scratch(nz, rows, width),
        compiler_params=params(10 + 2 * layer, 60),
        name="attention_backward",
    )(block, mats, cos_part, sin_part, key_at, query_at, queries, keys, values, peaks, shares)


def rope_tables(places):
    half_dim = HEAD_DIM // 2
    freq_steps = jnp.arange(half_dim, dtype=jnp.float32)
    inverse = jnp.exp(freq_steps * (-2.0 * math.log(10000.0) / HEAD_DIM))
    angles = places[:, None] * inverse[None, :]
    return jnp.cos(angles), jnp.sin(angles)


def pack_weights(master_set, layer, nctx):
    query_weight, key_weight, value_weight, out_weight, attn_gain, moe_gain, gate_weight, up_weight, down_weight = master_set
    rows = query_weight.shape[1]

    def columns(master):
        low = master[layer].astype(BF).reshape(rows, nctx, -1)
        return low.transpose(1, 0, 2)

    attn = jnp.concatenate(
        [columns(query_weight), columns(key_weight), columns(value_weight), columns(out_weight)], axis=-1
    )

    def experts(master):
        low = master[layer].astype(BF)
        return low.reshape(nctx, -1, rows, low.shape[-1])

    send = jnp.concatenate(
        [attn[:, None], experts(gate_weight), experts(up_weight), experts(down_weight)], axis=1
    )
    gains = jnp.stack([attn_gain[layer], moe_gain[layer]]).astype(BF).astype(F32)
    return send, jnp.pad(gains, ((0, 0), (0, 128 - rows)))


def norm_back(values, gain, grad):
    scale = lax.rsqrt(jnp.mean(values * values, axis=-1, keepdims=True) + EPSILON)
    unit = values * scale
    grad_gain = jnp.sum(grad * unit, axis=0)
    pulled = grad * gain
    return scale * (pulled - unit * jnp.mean(pulled * unit, axis=-1, keepdims=True)), grad_gain


def fast_body(nctx, nfs, *args):
    (tokens, cotangent, lengths, tile_order, routes, gates), master_set = args[:6], args[6:]
    nz = nctx // NX
    rows_here, model_width = tokens.shape[1], tokens.shape[2]
    group_rows = rows_here * nctx
    ctx = lax.axis_index("ctx")
    _, pos_all = layout(lengths[0], tile_order[0], group_rows)
    cos_half, sin_half = rope_tables(pos_all.astype(jnp.float32))
    cos_part = jnp.concatenate([cos_half] * 4, axis=1)
    sin_part = jnp.concatenate([-sin_half, sin_half] * 2, axis=1)
    row_ids = jnp.arange(rows_here, dtype=jnp.int32)
    first_at = (tile_order[0][:, None] * TILE + row_ids[None, :]).reshape(group_rows)
    key_at = first_at[:, None]
    query_at = jnp.stack(
        [(first_at - pos_all).reshape(nctx, rows_here), first_at.reshape(nctx, rows_here)], axis=1
    )
    q_width = 3 * HEAD_DIM
    kv_at, v_at, o_at = q_width, q_width + HEAD_DIM, q_width + 2 * HEAD_DIM

    expert_ids = jnp.arange(EXPERTS, dtype=jnp.int32)
    table = jnp.sum(
        jnp.where(routes[:, 0, :, :, None] == expert_ids, gates[:, 0, :, :, None], 0.0), axis=-2
    )
    packed = [pack_weights(master_set, layer, nctx) for layer in range(LAYERS)]
    rows = packed[0][0].shape[2]
    gains = jnp.broadcast_to(jnp.concatenate([gain for _, gain in packed])[None], (nctx, 2 * LAYERS, 128))
    shares = table.transpose(2, 0, 1).reshape(nctx, 2, LAYERS, rows_here).transpose(0, 2, 1, 3)
    shares = shares.reshape(nctx, 2 * LAYERS, rows_here)
    pad = jnp.zeros((nctx, 8 - 2 * LAYERS, 128), F32)
    small = jnp.concatenate([gains, pad, shares, pad], axis=1)
    mats_all, small_all = spread_weights(jnp.stack([send for send, _ in packed]), small, nfs)
    shares = lax.dynamic_index_in_dim(
        small_all.reshape(nctx, nfs, 16, 128), lax.axis_index("fsdp"), 1, keepdims=False
    )
    fetched = [
        (
            small_all[:, 2 * layer, :rows].reshape(-1),
            small_all[:, 2 * layer + 1, :rows].reshape(-1),
            shares[:, 8 + 2 * layer : 10 + 2 * layer].transpose(0, 2, 1),
        )
        for layer in range(LAYERS)
    ]

    hidden = tokens[0].astype(jnp.float32)
    records = []
    for layer in range(LAYERS):
        attn_gain, moe_gain, share = fetched[layer]
        normed = rms_norm(hidden, attn_gain).astype(BF)
        mixed, normed_all, queries, keys, values, peaks, sums, attended = attention_rows(
            normed, mats_all, layer, cos_part, sin_part, key_at, query_at, nz
        )
        middle = hidden + mixed

        moe_in = rms_norm(middle, moe_gain).astype(BF)
        moved, moe_all, gate_act, up_act = experts_forward(moe_in, share, mats_all, layer, nz)
        records.append((hidden, normed_all, queries, keys, values, peaks, sums, attended, middle, moe_all, gate_act, up_act))
        hidden = middle + moved

    output = hidden.astype(BF)
    grad = cotangent[0].astype(jnp.float32)
    layer_args, gain_grads = [None] * LAYERS, [None] * LAYERS
    for layer in reversed(range(LAYERS)):
        attn_gain, moe_gain, share = fetched[layer]
        hidden, normed_all, queries, keys, values, peaks, sums, attended, middle, moe_all, gate_act, up_act = records[layer]
        grad_moe_in, grad_all, d_gate, d_up, inner = experts_backward(grad.astype(BF), share, mats_all, layer, gate_act, up_act, nz)
        through, grad_moe_gain = norm_back(middle, moe_gain, grad_moe_in)
        grad_middle = grad + through

        grad_normed, middle_all, d_proj = attention_rows_back(
            grad_middle.astype(BF), mats_all, layer, cos_part, sin_part, key_at, query_at, queries, keys, values, peaks, sums, nz
        )
        through, grad_attn_gain = norm_back(hidden, attn_gain, grad_normed)
        grad = grad_middle + through

        layer_args[layer] = [
            part.reshape(group_rows, -1)
            for part in (normed_all, d_proj, middle_all, attended, moe_all, d_gate, d_up, grad_all, inner)
        ]
        gain_grads[layer] = [grad_attn_gain, grad_moe_gain]

    extra = jnp.stack([part for pair in gain_grads for part in pair])
    extra = extra.reshape(2 * LAYERS, nctx, nfs // NCORE, NCORE, rows).transpose(3, 2, 1, 0, 4)
    extra = jnp.pad(extra, ((0, 0), (0, 0), (0, 0), (0, 8 - 2 * LAYERS), (0, 128 - rows)))
    collected, gains_in = collect_grads(nctx, nfs, layer_args, extra)

    def attn_part(low, high):
        return jnp.stack(
            [
                c[:, 0, :, low:high].transpose(1, 0, 2).reshape(rows, -1).astype(F32)
                for c in collected
            ]
        )

    def expert_part(first):
        return jnp.stack(
            [
                c[:, first : first + 2].reshape((EXPERTS,) + c.shape[2:]).astype(F32)
                for c in collected
            ]
        )

    def gain_part(kind):
        return jnp.stack([jnp.sum(gains_in[:, 2 * layer + kind, :rows], axis=0) for layer in range(LAYERS)])

    return (
        output[None],
        grad[None],
        attn_part(0, kv_at),
        attn_part(kv_at, v_at),
        attn_part(v_at, o_at),
        attn_part(o_at, o_at + q_width),
        gain_part(0),
        gain_part(1),
        expert_part(1),
        expert_part(3),
        expert_part(5),
    )


def solution(mesh):
    placed = (
        P("fsdp", "ctx", None),
        P("fsdp", "ctx", None),
        P("fsdp", None),
        P("fsdp", None),
        P(None, "fsdp", "ctx", None),
        P(None, "fsdp", "ctx", None),
        P(None, ("ctx", "fsdp"), None),
        P(None, ("ctx", "fsdp"), None),
        P(None, ("ctx", "fsdp"), None),
        P(None, ("ctx", "fsdp"), None),
        P(None, ("ctx", "fsdp")),
        P(None, ("ctx", "fsdp")),
        P(None, None, ("ctx", "fsdp"), None),
        P(None, None, ("ctx", "fsdp"), None),
        P(None, None, ("ctx", "fsdp"), None),
    )
    nctx, nfs = mesh.shape["ctx"], mesh.shape["fsdp"]
    chosen = partial(fast_body, nctx, nfs) if (nctx, nfs) == (8, 4) else body
    return jax.shard_map(
        chosen,
        mesh=mesh,
        in_specs=placed,
        out_specs=(
            P("fsdp", "ctx", None),
            P("fsdp", "ctx", None),
            P(None, ("ctx", "fsdp"), None),
            P(None, ("ctx", "fsdp"), None),
            P(None, ("ctx", "fsdp"), None),
            P(None, ("ctx", "fsdp"), None),
            P(None, ("ctx", "fsdp")),
            P(None, ("ctx", "fsdp")),
            P(None, None, ("ctx", "fsdp"), None),
            P(None, None, ("ctx", "fsdp"), None),
            P(None, None, ("ctx", "fsdp"), None),
        ),
        check_vma=False,
    )
```

```python
from functools import partial
import functools
import math

import jax
import jax.numpy as jnp
from jax import lax
from jax.experimental import pallas as pl
from jax.experimental.pallas import tpu as pltpu
from jax.sharding import PartitionSpec as P

HEAD_DIM = 64
EXPERTS = 16
LAYERS = 2
TILE = 128
CAP = 80


EPSILON = 1e-06
NEGATIVE = -1e30


def layout(lengths, tile_order, group_rows):
    tile_count = tile_order.shape[0]
    row_ids = jnp.arange(group_rows, dtype=jnp.int32)
    in_tile = (row_ids // TILE)[:, None] == jnp.arange(tile_count, dtype=jnp.int32)[None, :]
    tile_of = jnp.sum(jnp.where(in_tile, tile_order[None, :], 0), axis=1, dtype=jnp.int32)
    anchor = tile_of * TILE + row_ids % TILE
    seq_ends = jnp.cumsum(lengths, dtype=jnp.int32)
    seq_starts = seq_ends - lengths
    segment = jnp.sum(
        (anchor[:, None] >= seq_ends[None, :]).astype(jnp.int32), axis=1, dtype=jnp.int32
    )
    picked = segment[:, None] == jnp.arange(lengths.shape[0], dtype=jnp.int32)[None, :]
    offset = jnp.sum(jnp.where(picked, seq_starts[None, :], 0), axis=1, dtype=jnp.int32)
    return (segment, anchor - offset)


def rms_norm(values, gain_vec):
    return (
        values * lax.rsqrt(jnp.mean(values * values, axis=-1, keepdims=True) + EPSILON) * gain_vec
    )


def rotate(values, places):
    half_dim = values.shape[-1] // 2
    freq_steps = jnp.arange(half_dim, dtype=jnp.float32)
    inverse = jnp.exp(freq_steps * (-2.0 * math.log(10000.0) / values.shape[-1]))
    angles = places[:, None] * inverse[None, :]
    cos_part = jnp.cos(angles)[:, None, :]
    sin_part = jnp.sin(angles)[:, None, :]
    first_half = values[..., :half_dim]
    second_half = values[..., half_dim:]
    return jnp.concatenate(
        [
            first_half * cos_part - second_half * sin_part,
            second_half * cos_part + first_half * sin_part,
        ],
        axis=-1,
    )


def rotate_back(grads_in, places):
    return jax.vjp(partial(rotate, places=places), jnp.zeros(grads_in.shape, jnp.float32))[1](
        grads_in
    )[0]


def mix_inner(gate_act, up_act):
    return jax.nn.silu(gate_act) * up_act


def split_halves(master):
    experts_here, rows_here, hidden_units = master.shape
    return (
        master.astype(jnp.bfloat16)
        .reshape(experts_here, rows_here, 2, hidden_units // 2)
        .transpose(0, 2, 1, 3)
        .reshape(2 * experts_here, rows_here, hidden_units // 2)
    )


def merge_halves(grads_in):
    halves_all, rows_here, half_units = grads_in.shape
    return (
        grads_in.reshape(halves_all // 2, 2, rows_here, half_units)
        .transpose(0, 2, 1, 3)
        .reshape(halves_all // 2, rows_here, 2 * half_units)
    )


def doubled(slots):
    return jnp.broadcast_to(slots[:, None], (slots.shape[0], 2) + slots.shape[1:]).reshape(
        (2 * slots.shape[0],) + slots.shape[1:]
    )


def fold_halves(parts):
    return jnp.sum(parts.reshape((parts.shape[0] // 2, 2) + parts.shape[1:]), axis=1)


def send_out(slots):
    return lax.all_to_all(slots, "ctx", split_axis=0, concat_axis=1, tiled=True)


def send_back(parts):
    return lax.all_to_all(
        parts.astype(jnp.bfloat16), "ctx", split_axis=1, concat_axis=0, tiled=True
    ).astype(parts.dtype)


def routing(route_ids, gate_share, rows_here):
    expert_ids = jnp.arange(EXPERTS, dtype=jnp.int32)
    chosen = (route_ids[:, :, None] == expert_ids[None, None, :]).astype(jnp.int32)
    member = jnp.sum(chosen, axis=1, dtype=jnp.int32)
    before = jnp.cumsum(member, axis=0, dtype=jnp.int32) - member
    rank_of = jnp.sum(chosen * before[:, None, :], axis=2, dtype=jnp.int32)
    slot_of = route_ids * CAP + rank_of
    token_ids = jnp.broadcast_to(jnp.arange(rows_here, dtype=jnp.int32)[:, None], route_ids.shape)
    flat_slots = slot_of.reshape(-1)
    slot_token = (
        jnp.full((EXPERTS * CAP,), rows_here, jnp.int32).at[flat_slots].set(token_ids.reshape(-1))
    )
    slot_share = jnp.zeros((EXPERTS * CAP,), jnp.float32).at[flat_slots].set(gate_share.reshape(-1))
    return (slot_of, slot_token, slot_share)


def key_block(key_rows, value_rows, token_meta, block_index, block_rows):
    seg_local, pos_local, seg_all, pos_all = token_meta
    first_row = block_index * block_rows
    key_part = lax.dynamic_slice_in_dim(key_rows, first_row, block_rows, 0)
    value_part = lax.dynamic_slice_in_dim(value_rows, first_row, block_rows, 0)
    seg_part = lax.dynamic_slice_in_dim(seg_all, first_row, block_rows, 0)
    pos_part = lax.dynamic_slice_in_dim(pos_all, first_row, block_rows, 0)
    visible = (seg_local[:, None] == seg_part[None, :]) & (pos_part[None, :] <= pos_local[:, None])
    return (key_part, value_part, visible)


def scores(queries, key_part, visible, score_scale):
    raw_scores = (
        jnp.einsum("qhgd,khd->hgqk", queries, key_part, preferred_element_type=jnp.float32)
        * score_scale
    )
    return jnp.where(visible[None, None], raw_scores, NEGATIVE)


def keep_same(running):
    return running


def attention_forward(queries, key_rows, value_rows, token_meta, block_rows, score_scale):
    block_count = key_rows.shape[0] // block_rows
    rows_here, heads_kv, groups = (queries.shape[0], queries.shape[1], queries.shape[2])

    def stat_step(block_index, running):
        key_part, value_part, visible = key_block(
            key_rows, value_rows, token_meta, block_index, block_rows
        )

        def stat_update(current):
            row_peak, denom_sum = current
            logits = scores(queries, key_part, visible, score_scale)
            new_peak = jnp.maximum(row_peak, jnp.max(logits, axis=-1))
            denom_sum = denom_sum * jnp.exp(row_peak - new_peak) + jnp.sum(
                jnp.exp(logits - new_peak[..., None]), axis=-1
            )
            return (new_peak, denom_sum)

        return lax.cond(jnp.any(visible), stat_update, keep_same, running)

    start_stats = (
        jnp.full((heads_kv, groups, rows_here), NEGATIVE, jnp.float32),
        jnp.zeros((heads_kv, groups, rows_here), jnp.float32),
    )
    row_peak, denom_sum = lax.fori_loop(0, block_count, stat_step, start_stats)

    def out_step(block_index, partial_sum):
        key_part, value_part, visible = key_block(
            key_rows, value_rows, token_meta, block_index, block_rows
        )

        def out_update(current):
            attn_probs = (
                jnp.exp(scores(queries, key_part, visible, score_scale) - row_peak[..., None])
                / denom_sum[..., None]
            )
            return current + jnp.einsum(
                "hgqk,khd->qhgd",
                attn_probs.astype(jnp.bfloat16),
                value_part,
                preferred_element_type=jnp.float32,
            )

        return lax.cond(jnp.any(visible), out_update, keep_same, partial_sum)

    attended = lax.fori_loop(
        0, block_count, out_step, jnp.zeros((rows_here, heads_kv, groups, HEAD_DIM), jnp.float32)
    )
    return ((row_peak, denom_sum), attended)


def attention_backward(
    queries, key_rows, value_rows, token_meta, softmax_stats, grad_attended, block_rows, score_scale
):
    row_peak, denom_sum = softmax_stats
    block_count = key_rows.shape[0] // block_rows

    def probs_for(key_part, visible):
        return (
            jnp.exp(scores(queries, key_part, visible, score_scale) - row_peak[..., None])
            / denom_sum[..., None]
        )

    def delta_step(block_index, partial_sum):
        key_part, value_part, visible = key_block(
            key_rows, value_rows, token_meta, block_index, block_rows
        )

        def delta_update(current):
            attn_probs = probs_for(key_part, visible)
            grad_probs = jnp.einsum(
                "qhgd,khd->hgqk", grad_attended, value_part, preferred_element_type=jnp.float32
            )
            return current + jnp.sum(attn_probs * grad_probs, axis=-1)

        return lax.cond(jnp.any(visible), delta_update, keep_same, partial_sum)

    delta_sum = lax.fori_loop(0, block_count, delta_step, jnp.zeros(denom_sum.shape, jnp.float32))

    def grad_step(block_index, running):
        key_part, value_part, visible = key_block(
            key_rows, value_rows, token_meta, block_index, block_rows
        )
        first_row = block_index * block_rows

        def grad_update(current):
            grad_queries, grad_keys, grad_values = current
            attn_probs = probs_for(key_part, visible)
            grad_probs = jnp.einsum(
                "qhgd,khd->hgqk", grad_attended, value_part, preferred_element_type=jnp.float32
            )
            grad_scores = (attn_probs * (grad_probs - delta_sum[..., None])).astype(jnp.bfloat16)
            grad_queries = grad_queries + jnp.einsum(
                "hgqk,khd->qhgd", grad_scores, key_part, preferred_element_type=jnp.float32
            )
            key_term = jnp.einsum(
                "hgqk,qhgd->khd", grad_scores, queries, preferred_element_type=jnp.float32
            )
            value_term = jnp.einsum(
                "hgqk,qhgd->khd",
                attn_probs.astype(jnp.bfloat16),
                grad_attended,
                preferred_element_type=jnp.float32,
            )
            grad_keys = lax.dynamic_update_slice_in_dim(
                grad_keys,
                lax.dynamic_slice_in_dim(grad_keys, first_row, block_rows, 0) + key_term,
                first_row,
                0,
            )
            grad_values = lax.dynamic_update_slice_in_dim(
                grad_values,
                lax.dynamic_slice_in_dim(grad_values, first_row, block_rows, 0) + value_term,
                first_row,
                0,
            )
            return (grad_queries, grad_keys, grad_values)

        return lax.cond(jnp.any(visible), grad_update, keep_same, running)

    start_grads = (
        jnp.zeros(queries.shape, jnp.float32),
        jnp.zeros(key_rows.shape, jnp.float32),
        jnp.zeros(value_rows.shape, jnp.float32),
    )
    return lax.fori_loop(0, block_count, grad_step, start_grads)


def fetch_layer(master_set, layer_index):
    (
        query_weight,
        key_weight,
        value_weight,
        out_weight,
        attn_gain,
        moe_gain,
        gate_weight,
        up_weight,
        down_weight,
    ) = master_set
    attn_set = (
        lax.all_gather(
            query_weight[layer_index].astype(jnp.bfloat16), ("ctx", "fsdp"), axis=0, tiled=True
        ),
        lax.all_gather(
            key_weight[layer_index].astype(jnp.bfloat16), ("ctx", "fsdp"), axis=0, tiled=True
        ),
        lax.all_gather(
            value_weight[layer_index].astype(jnp.bfloat16), ("ctx", "fsdp"), axis=0, tiled=True
        ),
        lax.all_gather(
            out_weight[layer_index].astype(jnp.bfloat16), ("ctx", "fsdp"), axis=0, tiled=True
        ),
        lax.all_gather(
            attn_gain[layer_index].astype(jnp.bfloat16), ("ctx", "fsdp"), axis=0, tiled=True
        ),
        lax.all_gather(
            moe_gain[layer_index].astype(jnp.bfloat16), ("ctx", "fsdp"), axis=0, tiled=True
        ),
    )
    row_set = (
        lax.all_gather(split_halves(gate_weight[layer_index]), "fsdp", axis=1, tiled=True),
        lax.all_gather(split_halves(up_weight[layer_index]), "fsdp", axis=1, tiled=True),
        lax.all_gather(split_halves(down_weight[layer_index]), "fsdp", axis=1, tiled=True),
    )
    expert_set = (
        lax.all_to_all(row_set[0], "ctx", split_axis=0, concat_axis=1, tiled=True),
        lax.all_to_all(row_set[1], "ctx", split_axis=0, concat_axis=1, tiled=True),
        lax.all_to_all(row_set[2], "ctx", split_axis=0, concat_axis=1, tiled=True),
    )
    return tuple(attn_set) + tuple(expert_set)


def layer_forward(hidden, weights, route_ids, gate_share, token_meta, places, block_rows):
    (
        query_full,
        key_full,
        value_full,
        out_full,
        attn_norm,
        moe_norm,
        gate_full,
        up_full,
        down_full,
    ) = weights
    rows_here, model_width = hidden.shape
    heads_all = query_full.shape[1] // HEAD_DIM
    heads_kv = key_full.shape[1] // HEAD_DIM
    groups = heads_all // heads_kv
    score_scale = HEAD_DIM ** (-0.5)
    normed = rms_norm(hidden, attn_norm.astype(jnp.float32)).astype(jnp.bfloat16)
    queries = rotate(
        jnp.dot(normed, query_full, preferred_element_type=jnp.float32).reshape(
            rows_here, heads_all, HEAD_DIM
        ),
        places,
    ).astype(jnp.bfloat16)
    key_new = (
        rotate(
            jnp.dot(normed, key_full, preferred_element_type=jnp.float32).reshape(
                rows_here, heads_kv, HEAD_DIM
            ),
            places,
        )
        .astype(jnp.bfloat16)
        .reshape(rows_here, heads_kv * HEAD_DIM)
    )
    value_new = jnp.dot(normed, value_full, preferred_element_type=jnp.float32).astype(jnp.bfloat16)
    key_rows, value_rows = (
        lax.all_gather(key_new, "ctx", axis=0, tiled=True),
        lax.all_gather(value_new, "ctx", axis=0, tiled=True),
    )
    key_rows = key_rows.reshape(-1, heads_kv, HEAD_DIM)
    value_rows = value_rows.reshape(-1, heads_kv, HEAD_DIM)
    queries = queries.reshape(rows_here, heads_kv, groups, HEAD_DIM)
    softmax_stats, attended = attention_forward(
        queries, key_rows, value_rows, token_meta, block_rows, score_scale
    )
    attended = attended.reshape(rows_here, heads_all * HEAD_DIM).astype(jnp.bfloat16)
    middle = hidden + jnp.einsum(
        "tx,dx->td", attended, out_full, preferred_element_type=jnp.float32
    )
    moe_in = rms_norm(middle, moe_norm.astype(jnp.float32)).astype(jnp.bfloat16)
    slot_of, slot_token, slot_share = routing(route_ids, gate_share, rows_here)
    padded = jnp.concatenate([moe_in, jnp.zeros((1, model_width), jnp.bfloat16)], axis=0)
    dispatched = jnp.take(padded, slot_token, axis=0).reshape(EXPERTS, CAP, model_width)
    owner_rows = send_out(doubled(dispatched))
    gate_act = jnp.einsum("ecd,edf->ecf", owner_rows, gate_full, preferred_element_type=jnp.float32)
    up_act = jnp.einsum("ecd,edf->ecf", owner_rows, up_full, preferred_element_type=jnp.float32)
    inner_act = mix_inner(gate_act, up_act).astype(jnp.bfloat16)
    expert_part = jnp.einsum(
        "ecf,edf->ecd", inner_act, down_full, preferred_element_type=jnp.float32
    )
    expert_out = fold_halves(send_back(expert_part))
    expert_out = expert_out.reshape(EXPERTS * CAP, model_width)
    moe_out = jnp.sum(jnp.take(expert_out, slot_of, axis=0) * gate_share[..., None], axis=1)
    record = (
        hidden,
        normed,
        queries,
        key_rows,
        value_rows,
        softmax_stats,
        attended,
        middle,
        moe_in,
        slot_of,
        slot_token,
        slot_share,
        owner_rows,
        gate_act,
        up_act,
        inner_act,
    )
    return (record, middle + moe_out)


def layer_backward(grad_hidden, record, weights, token_meta, places, block_rows):
    (
        hidden,
        normed,
        queries,
        key_rows,
        value_rows,
        softmax_stats,
        attended,
        middle,
        moe_in,
        slot_of,
        slot_token,
        slot_share,
        owner_rows,
        gate_act,
        up_act,
        inner_act,
    ) = record
    (
        query_full,
        key_full,
        value_full,
        out_full,
        attn_norm,
        moe_norm,
        gate_full,
        up_full,
        down_full,
    ) = weights
    rows_here, model_width = hidden.shape
    heads_kv, groups = (queries.shape[1], queries.shape[2])
    group_rows = key_rows.shape[0]
    score_scale = HEAD_DIM ** (-0.5)
    grad_padded = jnp.concatenate([grad_hidden, jnp.zeros((1, model_width), jnp.float32)], axis=0)
    grad_expert = (
        (jnp.take(grad_padded, slot_token, axis=0) * slot_share[:, None])
        .astype(jnp.bfloat16)
        .reshape(EXPERTS, CAP, model_width)
    )
    grad_owner = send_out(doubled(grad_expert))
    grad_down = jnp.einsum(
        "ecd,ecf->edf", grad_owner, inner_act, preferred_element_type=jnp.float32
    )
    grad_inner = jnp.einsum(
        "ecd,edf->ecf", grad_owner, down_full, preferred_element_type=jnp.float32
    )
    grad_gate_act, grad_up_act = jax.vjp(mix_inner, gate_act, up_act)[1](grad_inner)
    grad_gate_act = grad_gate_act.astype(jnp.bfloat16)
    grad_up_act = grad_up_act.astype(jnp.bfloat16)
    grad_gate = jnp.einsum(
        "ecd,ecf->edf", owner_rows, grad_gate_act, preferred_element_type=jnp.float32
    )
    grad_up = jnp.einsum(
        "ecd,ecf->edf", owner_rows, grad_up_act, preferred_element_type=jnp.float32
    )
    grad_owner_rows = jnp.einsum(
        "ecf,edf->ecd", grad_gate_act, gate_full, preferred_element_type=jnp.float32
    ) + jnp.einsum("ecf,edf->ecd", grad_up_act, up_full, preferred_element_type=jnp.float32)
    grad_dispatched = fold_halves(send_back(grad_owner_rows))
    home_set = (
        lax.all_to_all(
            grad_gate.astype(jnp.bfloat16), "ctx", split_axis=1, concat_axis=0, tiled=True
        ).astype(grad_gate.dtype),
        lax.all_to_all(
            grad_up.astype(jnp.bfloat16), "ctx", split_axis=1, concat_axis=0, tiled=True
        ).astype(grad_up.dtype),
        lax.all_to_all(
            grad_down.astype(jnp.bfloat16), "ctx", split_axis=1, concat_axis=0, tiled=True
        ).astype(grad_down.dtype),
    )
    summed_set = (
        lax.psum_scatter(
            home_set[0].astype(jnp.bfloat16), "fsdp", scatter_dimension=1, tiled=True
        ).astype(jnp.float32),
        lax.psum_scatter(
            home_set[1].astype(jnp.bfloat16), "fsdp", scatter_dimension=1, tiled=True
        ).astype(jnp.float32),
        lax.psum_scatter(
            home_set[2].astype(jnp.bfloat16), "fsdp", scatter_dimension=1, tiled=True
        ).astype(jnp.float32),
    )
    expert_grads = (
        merge_halves(summed_set[0]),
        merge_halves(summed_set[1]),
        merge_halves(summed_set[2]),
    )
    grad_moe_in = jnp.sum(
        jnp.take(grad_dispatched.reshape(EXPERTS * CAP, model_width), slot_of, axis=0), axis=1
    )
    grad_middle_part, grad_moe_norm = jax.vjp(rms_norm, middle, moe_norm.astype(jnp.float32))[1](
        grad_moe_in
    )
    grad_middle = grad_hidden + grad_middle_part
    grad_rounded = grad_middle.astype(jnp.bfloat16)
    grad_out_full = jnp.einsum(
        "td,tx->dx", grad_rounded, attended, preferred_element_type=jnp.float32
    )
    grad_attended = (
        jnp.dot(grad_rounded, out_full, preferred_element_type=jnp.float32)
        .astype(jnp.bfloat16)
        .reshape(rows_here, heads_kv, groups, HEAD_DIM)
    )
    grad_queries, grad_keys, grad_values = attention_backward(
        queries,
        key_rows,
        value_rows,
        token_meta,
        softmax_stats,
        grad_attended,
        block_rows,
        score_scale,
    )
    key_sums, value_sums = (
        lax.psum_scatter(
            grad_keys.reshape(group_rows, heads_kv * HEAD_DIM).astype(jnp.bfloat16),
            "ctx",
            scatter_dimension=0,
            tiled=True,
        ).astype(jnp.float32),
        lax.psum_scatter(
            grad_values.reshape(group_rows, heads_kv * HEAD_DIM).astype(jnp.bfloat16),
            "ctx",
            scatter_dimension=0,
            tiled=True,
        ).astype(jnp.float32),
    )
    grad_query_rows = (
        rotate_back(
            grad_queries.reshape(rows_here, heads_kv * groups, HEAD_DIM) * score_scale, places
        )
        .astype(jnp.bfloat16)
        .reshape(rows_here, heads_kv * groups * HEAD_DIM)
    )
    grad_key_rows = (
        rotate_back(key_sums.reshape(rows_here, heads_kv, HEAD_DIM) * score_scale, places)
        .astype(jnp.bfloat16)
        .reshape(rows_here, heads_kv * HEAD_DIM)
    )
    grad_value_rows = value_sums.astype(jnp.bfloat16)
    grad_query_full = jnp.einsum(
        "td,tx->dx", normed, grad_query_rows, preferred_element_type=jnp.float32
    )
    grad_key_full = jnp.einsum(
        "td,tx->dx", normed, grad_key_rows, preferred_element_type=jnp.float32
    )
    grad_value_full = jnp.einsum(
        "td,tx->dx", normed, grad_value_rows, preferred_element_type=jnp.float32
    )
    grad_normed = jnp.einsum(
        "tx,dx->td", grad_query_rows, query_full, preferred_element_type=jnp.float32
    )
    grad_normed = grad_normed + jnp.einsum(
        "tx,dx->td", grad_key_rows, key_full, preferred_element_type=jnp.float32
    )
    grad_normed = grad_normed + jnp.einsum(
        "tx,dx->td", grad_value_rows, value_full, preferred_element_type=jnp.float32
    )
    grad_hidden_part, grad_attn_norm = jax.vjp(rms_norm, hidden, attn_norm.astype(jnp.float32))[1](
        grad_normed
    )
    attn_grads = (
        lax.psum_scatter(grad_query_full, ("ctx", "fsdp"), scatter_dimension=0, tiled=True),
        lax.psum_scatter(grad_key_full, ("ctx", "fsdp"), scatter_dimension=0, tiled=True),
        lax.psum_scatter(grad_value_full, ("ctx", "fsdp"), scatter_dimension=0, tiled=True),
        lax.psum_scatter(grad_out_full, ("ctx", "fsdp"), scatter_dimension=0, tiled=True),
        lax.psum_scatter(grad_attn_norm, ("ctx", "fsdp"), scatter_dimension=0, tiled=True),
        lax.psum_scatter(grad_moe_norm, ("ctx", "fsdp"), scatter_dimension=0, tiled=True),
    )
    return (grad_middle + grad_hidden_part, attn_grads, expert_grads)


def body(
    tokens,
    cotangent,
    lengths,
    tile_order,
    routes,
    gates,
    query_weight,
    key_weight,
    value_weight,
    out_weight,
    attn_gain,
    moe_gain,
    gate_weight,
    up_weight,
    down_weight,
):
    rows_here = tokens.shape[1]
    group_rows = rows_here * lax.axis_size("ctx")
    seg_all, pos_all = layout(lengths[0], tile_order[0], group_rows)
    first_row = lax.axis_index("ctx") * rows_here
    seg_local = lax.dynamic_slice_in_dim(seg_all, first_row, rows_here, 0)
    pos_local = lax.dynamic_slice_in_dim(pos_all, first_row, rows_here, 0)
    token_meta = (seg_local, pos_local, seg_all, pos_all)
    places = pos_local.astype(jnp.float32)
    block_rows = math.gcd(group_rows, 512)
    master_set = (
        query_weight,
        key_weight,
        value_weight,
        out_weight,
        attn_gain,
        moe_gain,
        gate_weight,
        up_weight,
        down_weight,
    )
    hidden = tokens[0].astype(jnp.float32)
    records = []
    for layer_index in range(LAYERS):
        weights = fetch_layer(master_set, layer_index)
        record, hidden = layer_forward(
            hidden,
            weights,
            routes[layer_index, 0],
            gates[layer_index, 0],
            token_meta,
            places,
            block_rows,
        )
        records.append(record)
    grad_hidden = cotangent[0].astype(jnp.float32)
    attn_layers = []
    expert_layers = []
    for layer_index in reversed(range(LAYERS)):
        weights = fetch_layer(master_set, layer_index)
        grad_hidden, attn_grads, expert_grads = layer_backward(
            grad_hidden, records[layer_index], weights, token_meta, places, block_rows
        )
        attn_layers.insert(0, attn_grads)
        expert_layers.insert(0, expert_grads)
    grad_query_weight = jnp.stack([layer_grads[0] for layer_grads in attn_layers])
    grad_key_weight = jnp.stack([layer_grads[1] for layer_grads in attn_layers])
    grad_value_weight = jnp.stack([layer_grads[2] for layer_grads in attn_layers])
    grad_out_weight = jnp.stack([layer_grads[3] for layer_grads in attn_layers])
    grad_attn_gain = jnp.stack([layer_grads[4] for layer_grads in attn_layers])
    grad_moe_gain = jnp.stack([layer_grads[5] for layer_grads in attn_layers])
    grad_gate_weight = jnp.stack([layer_grads[0] for layer_grads in expert_layers])
    grad_up_weight = jnp.stack([layer_grads[1] for layer_grads in expert_layers])
    grad_down_weight = jnp.stack([layer_grads[2] for layer_grads in expert_layers])
    return (
        hidden.astype(jnp.bfloat16)[None],
        grad_hidden[None],
        grad_query_weight,
        grad_key_weight,
        grad_value_weight,
        grad_out_weight,
        grad_attn_gain,
        grad_moe_gain,
        grad_gate_weight,
        grad_up_weight,
        grad_down_weight,
    )


BF = jnp.bfloat16
F32 = jnp.float32
NX = 2
NCORE = 2
ANY = pl.BlockSpec(memory_space=pl.ANY)
VM = pl.BlockSpec(memory_space=pltpu.VMEM)
DMA = pltpu.SemaphoreType.DMA

NN = ((1,), (0,))
NT = ((1,), (1,))
TN = ((0,), (0,))


def dot(left, right, dims):
    return lax.dot_general(left, right, (dims, ((), ())), preferred_element_type=jnp.float32)


def remote(src, dst, send_sem, recv_sem, ctx, fsdp):
    return pltpu.make_async_remote_copy(
        src_ref=src,
        dst_ref=dst,
        send_sem=send_sem,
        recv_sem=recv_sem,
        device_id={"ctx": ctx, "fsdp": fsdp},
        device_id_type=pl.DeviceIdType.MESH,
    )


def greet(barrier, ctx, fsdp):
    pl.semaphore_signal(
        barrier, inc=1, device_id={"ctx": ctx, "fsdp": fsdp}, device_id_type=pl.DeviceIdType.MESH
    )


class Line:
    def __init__(self, nz):
        self.nz = nz
        self.ctx, self.fsdp = lax.axis_index("ctx"), lax.axis_index("fsdp")
        self.z, self.x = self.ctx // NX, self.ctx % NX
        self.mate = self.z * NX + 1 - self.x
        self.above = (self.z + 1) * NX + self.x
        self.below = (self.z - 1) * NX + self.x

    def greet(self, others=()):
        barrier = pltpu.get_barrier_semaphore()
        greet(barrier, self.mate, self.fsdp)
        for other in others:
            greet(barrier, self.ctx, other)

        @pl.when(self.z > 0)
        def _():
            greet(barrier, self.below, self.fsdp)

        @pl.when(self.z < self.nz - 1)
        def _():
            greet(barrier, self.above, self.fsdp)

        ends = jnp.where(self.z > 0, 1, 0) + jnp.where(self.z < self.nz - 1, 1, 0)
        pl.semaphore_wait(barrier, 1 + len(others) + ends)

    def near(self, i):
        z, nz = self.z, self.nz
        mid1 = jnp.where(i == 0, 1, jnp.where(i == 1, 0, i))
        mid2 = jnp.where(i == 0, 2, jnp.where(i == 1, 1, jnp.where(i == 2, 3, 0)))
        return jnp.where(z == 0, i, jnp.where(z == nz - 1, nz - 1 - i, jnp.where(z == 1, mid1, mid2)))

    def far(self, i):
        z, nz = self.z, self.nz
        mid1 = jnp.where(i == 0, 3, jnp.where(i == 1, 0, jnp.where(i == 2, 2, 1)))
        mid2 = jnp.where(i == 0, 0, jnp.where(i == 1, 3, jnp.where(i == 2, 1, 2)))
        return jnp.where(z == 0, nz - 1 - i, jnp.where(z == nz - 1, i, jnp.where(z == 1, mid1, mid2)))


EXTRA = 16


class Gather:
    @staticmethod
    def scratch(nz):
        return [DMA((10, nz))]

    def __init__(self, line, own_ref, all_ref, sems):
        self.line, self.own, self.all, self.sems = line, own_ref, all_ref, sems
        self.main = own_ref.shape[0] - EXTRA

    def block(self, row, column=None):
        column = self.line.x if column is None else column
        return self.all.at[row * NX + column, pl.ds(0, self.main)]

    def extras(self, row):
        return self.all.at[pl.ds(row * NX, NX), pl.ds(self.main, EXTRA)]

    def own_main(self):
        return self.own.at[pl.ds(0, self.main)]

    def move(self, kind, t, src, dst, ctx):
        return remote(src, dst, self.sems.at[kind, t], self.sems.at[kind + 1, t], ctx, self.line.fsdp)

    def up(self, t, src=None):
        block = self.block(self.line.z - t)
        return self.move(0, t, block if src is None else src, block, self.line.above)

    def down(self, t, src=None):
        block = self.block(self.line.z + t)
        return self.move(2, t, block if src is None else src, block, self.line.below)

    def across(self, row, src=None):
        block = self.block(row)
        return self.move(4, row, block if src is None else src, block, self.line.mate)

    def extra_up(self, t):
        return self.move(6, t, self.extras(self.line.z - t), self.extras(self.line.z - t), self.line.above)

    def extra_down(self, t):
        return self.move(8, t, self.extras(self.line.z + t), self.extras(self.line.z + t), self.line.below)

    def extra_across(self, column):
        own = self.own.at[pl.ds(self.main, EXTRA)]
        there = self.all.at[self.line.z * NX + column, pl.ds(self.main, EXTRA)]
        last = self.line.nz - 1
        return remote(own, there, self.sems.at[6, last], self.sems.at[7, last], self.line.mate, self.line.fsdp)

    def start(self):
        line = self.line
        self.extra_across(line.x).start()

        @pl.when(line.z < line.nz - 1)
        def _():
            self.up(0, self.own_main()).start()

        @pl.when(line.z > 0)
        def _():
            self.down(0, self.own_main()).start()

        self.across(line.z, self.own_main()).start()

    def start_extras(self):
        line = self.line
        self.extra_across(1 - line.x).wait_recv()

        @pl.when(line.z < line.nz - 1)
        def _():
            self.extra_up(0).start()

        @pl.when(line.z > 0)
        def _():
            self.extra_down(0).start()

    def forward(self, t):
        line = self.line

        @pl.when(line.z - 1 - t >= 0)
        def _():
            row = line.z - 1 - t
            self.move(0, t, self.own_main(), self.block(row), line.above).wait_recv()

            @pl.when(line.z < line.nz - 1)
            def _():
                self.up(t + 1).start()

            self.across(row).start()
            self.move(6, t, self.extras(row), self.extras(row), line.above).wait_recv()

            @pl.when(line.z < line.nz - 1)
            def _():
                self.extra_up(t + 1).start()

        @pl.when(line.z + 1 + t < line.nz)
        def _():
            row = line.z + 1 + t
            self.move(2, t, self.own_main(), self.block(row), line.below).wait_recv()

            @pl.when(line.z > 0)
            def _():
                self.down(t + 1).start()

            self.across(row).start()
            self.move(8, t, self.extras(row), self.extras(row), line.below).wait_recv()

            @pl.when(line.z > 0)
            def _():
                self.extra_down(t + 1).start()

    def wait_pair(self, row):
        self.move(4, row, self.own_main(), self.block(row, 1 - self.line.x), self.line.mate).wait_recv()

    def finish(self):
        line = self.line
        self.extra_across(line.x).wait_send()
        for t in range(line.nz - 1):

            @pl.when((line.z - t >= 0) & (line.z < line.nz - 1))
            def _():
                self.up(t).wait_send()
                self.extra_up(t).wait_send()

            @pl.when((line.z + t < line.nz) & (line.z > 0))
            def _():
                self.down(t).wait_send()
                self.extra_down(t).wait_send()

        for row in range(line.nz):
            self.across(row).wait_send()


class Scatter:
    @staticmethod
    def scratch(nz, rows, width):
        return [
            pltpu.VMEM((4, nz, rows - EXTRA, width), BF),
            pltpu.VMEM((4, nz, NX, EXTRA, width), BF),
            DMA((10, nz)),
            DMA((2,)),
        ]

    def __init__(self, line, part_ref, out_ref, work, extra, sems, mate_sems):
        self.line, self.part, self.out, self.sems, self.mate_sems = line, part_ref, out_ref, sems, mate_sems
        self.xin, self.acc, self.upin, self.downin = (work.at[i] for i in range(4))
        self.eacc, self.eup, self.edown, self.emate = (extra.at[i] for i in range(4))
        self.main = part_ref.shape[1] - EXTRA

    def move(self, kind, row, src, dst, ctx):
        return remote(src, dst, self.sems.at[kind, row], self.sems.at[kind + 1, row], ctx, self.line.fsdp)

    def across(self, row):
        mates = self.part.at[row * NX + 1 - self.line.x, pl.ds(0, self.main)]
        return self.move(0, row, mates, self.xin.at[row], self.line.mate)

    def up(self, row):
        return self.move(2, row, self.acc.at[row], self.upin.at[row], self.line.above)

    def down(self, row):
        return self.move(4, row, self.acc.at[row], self.downin.at[row], self.line.below)

    def extra_up(self, row):
        return self.move(6, row, self.eacc.at[row], self.eup.at[row], self.line.above)

    def extra_down(self, row):
        return self.move(8, row, self.eacc.at[row], self.edown.at[row], self.line.below)

    def extra_across(self):
        return remote(
            self.emate.at[0, 0], self.emate.at[1, 0], self.mate_sems.at[0], self.mate_sems.at[1], self.line.mate, self.line.fsdp
        )

    def extras(self, row):
        return self.part[pl.ds(row * NX, NX), pl.ds(self.main, EXTRA), :].astype(F32)

    def add(self, i):
        line = self.line
        row = line.far(i)

        @pl.when(row > line.z)
        def _():
            @pl.when(line.z == 0)
            def _():
                self.eacc[row] = self.extras(row).astype(BF)

            @pl.when(line.z > 0)
            def _():
                self.extra_up(row).wait_recv()
                self.eacc[row] = (self.extras(row) + self.eup[row].astype(F32)).astype(BF)

            self.extra_up(row).start()

        @pl.when(row < line.z)
        def _():
            @pl.when(line.z == line.nz - 1)
            def _():
                self.eacc[row] = self.extras(row).astype(BF)

            @pl.when(line.z < line.nz - 1)
            def _():
                self.extra_down(row).wait_recv()
                self.eacc[row] = (self.extras(row) + self.edown[row].astype(F32)).astype(BF)

            self.extra_down(row).start()

        self.across(row).wait_recv()
        mine = self.part[row * NX + line.x, 0 : self.main, :].astype(F32) + self.xin[row].astype(F32)

        @pl.when(row > line.z)
        def _():
            @pl.when(line.z == 0)
            def _():
                self.acc[row] = mine.astype(BF)

            @pl.when(line.z > 0)
            def _():
                self.up(row).wait_recv()
                self.acc[row] = (mine + self.upin[row].astype(F32)).astype(BF)

            self.up(row).start()

        @pl.when(row < line.z)
        def _():
            @pl.when(line.z == line.nz - 1)
            def _():
                self.acc[row] = mine.astype(BF)

            @pl.when(line.z < line.nz - 1)
            def _():
                self.down(row).wait_recv()
                self.acc[row] = (mine + self.downin[row].astype(F32)).astype(BF)

            self.down(row).start()

        @pl.when(row == line.z)
        def _():
            self.out[0 : self.main, :] = mine

    def extra_sum(self, column):
        at = self.line.z * NX + column
        return self.part[at, self.main : self.main + EXTRA, :].astype(F32)

    def finish(self):
        line = self.line
        self.out[self.main : self.main + EXTRA, :] = self.extra_sum(line.x)
        others = self.extra_sum(1 - line.x)

        def more(ref):
            self.out[self.main : self.main + EXTRA, :] += ref[line.z, line.x].astype(F32)

        @pl.when(line.z > 0)
        def _():
            self.extra_up(line.z).wait_recv()
            more(self.eup)

        @pl.when(line.z < line.nz - 1)
        def _():
            self.extra_down(line.z).wait_recv()
            more(self.edown)

        @pl.when(line.z == 0)
        def _():
            self.emate[0, 0] = (others + self.edown[line.z, 1 - line.x].astype(F32)).astype(BF)

        @pl.when(line.z == line.nz - 1)
        def _():
            self.emate[0, 0] = (others + self.eup[line.z, 1 - line.x].astype(F32)).astype(BF)

        @pl.when((line.z > 0) & (line.z < line.nz - 1))
        def _():
            self.emate[0, 0] = (
                others + self.eup[line.z, 1 - line.x].astype(F32) + self.edown[line.z, 1 - line.x].astype(F32)
            ).astype(BF)

        self.extra_across().start()

        @pl.when(line.z > 0)
        def _():
            self.up(line.z).wait_recv()
            self.out[0 : self.main, :] += self.upin[line.z].astype(F32)

        @pl.when(line.z < line.nz - 1)
        def _():
            self.down(line.z).wait_recv()
            self.out[0 : self.main, :] += self.downin[line.z].astype(F32)

        self.extra_across().wait_recv()
        self.out[self.main : self.main + EXTRA, :] += self.emate[1, 0].astype(F32)
        self.extra_across().wait_send()
        for row in range(line.nz):
            self.across(row).wait_send()

            @pl.when(row > line.z)
            def _():
                self.up(row).wait_send()
                self.extra_up(row).wait_send()

            @pl.when(row < line.z)
            def _():
                self.down(row).wait_send()
                self.extra_down(row).wait_send()


def params(collective, vmem_mib):
    return pltpu.CompilerParams(collective_id=collective, has_side_effects=True, vmem_limit_bytes=vmem_mib << 20)


def experts_kernel(nz, layer, x_ref, share_ref, mats_ref, o_ref, all_out, gate_out, up_out,
                   mats, blocks, part, gate, up, load_sem, save_sem, gsems, work, ework, ssems, msems):
    line = Line(nz)
    rows, width = x_ref.shape
    load = pltpu.make_async_copy(mats_ref.at[layer, pl.ds(1, 6)], mats, load_sem)
    load.start()
    line.greet()
    ring = Gather(line, x_ref, blocks, gsems)
    blocks[line.ctx] = x_ref[...]
    ring.start()
    load.wait()
    ring.start_extras()

    def saves(row):
        pair = pl.ds(row * NX, NX)
        return (
            pltpu.make_async_copy(blocks.at[pair], all_out.at[pair], save_sem.at[0, row]),
            pltpu.make_async_copy(gate.at[pair], gate_out.at[pair], save_sem.at[1, row]),
            pltpu.make_async_copy(up.at[pair], up_out.at[pair], save_sem.at[2, row]),
        )

    def step(i, carry):
        @pl.when(i < nz - 1)
        def _():
            ring.forward(i)

        row = line.near(i)
        ring.wait_pair(row)
        pair = pl.ds(row * NX, NX)
        block = blocks[pair].reshape(NX * rows, width)
        share = share_ref[pair].reshape(NX * rows, 2)
        total = None
        for e in range(2):
            gate_act = dot(block, mats[e], NN)
            up_act = dot(block, mats[2 + e], NN)
            units = gate_act.shape[1]
            gate[pair, :, pl.ds(e * units, units)] = gate_act.astype(BF).reshape(NX, rows, units)
            up[pair, :, pl.ds(e * units, units)] = up_act.astype(BF).reshape(NX, rows, units)
            inner = gate_act / (1.0 + jnp.exp(-gate_act)) * up_act * share[:, e : e + 1]
            term = dot(inner.astype(BF), mats[4 + e], NT)
            total = term if total is None else total + term
        part[pair] = total.astype(BF).reshape(NX, rows, width)
        for save in saves(row):
            save.start()
        return carry

    lax.fori_loop(0, nz, step, 0)
    sums = Scatter(line, part, o_ref, work, ework, ssems, msems)
    for i in range(nz):
        sums.across(line.far(i)).start()
    ring.finish()
    for i in range(nz):
        sums.add(i)
    sums.finish()
    for row in range(nz):
        for save in saves(row):
            save.wait()


def experts_forward(block, share, mats, layer, nz):
    rows, width = block.shape
    units = mats.shape[3]
    group = nz * NX
    acts = jax.ShapeDtypeStruct((group, rows, 2 * units), BF)
    return pl.pallas_call(
        functools.partial(experts_kernel, nz, layer),
        out_shape=(
            jax.ShapeDtypeStruct((rows, width), F32),
            jax.ShapeDtypeStruct((group, rows, width), BF),
            acts,
            acts,
        ),
        in_specs=[VM, VM, ANY],
        out_specs=(VM, ANY, ANY, ANY),
        scratch_shapes=[
            pltpu.VMEM((6, width, units), BF),
            pltpu.VMEM((group, rows, width), BF),
            pltpu.VMEM((group, rows, width), BF),
            pltpu.VMEM((group, rows, 2 * units), BF),
            pltpu.VMEM((group, rows, 2 * units), BF),
            DMA,
            DMA((3, nz)),
        ]
        + Gather.scratch(nz)
        + Scatter.scratch(nz, rows, width),
        compiler_params=params(5 + 2 * layer, 60),
        name="experts_forward",
    )(block, share, mats)


def experts_back_kernel(nz, layer, x_ref, share_ref, mats_ref, gate_ref, up_ref, o_ref, all_out, dgate_out, dup_out, inner_out,
                        mats, blocks, part, gate, up, inners, load_sem, save_sem, gsems, work, ework, ssems, msems):
    line = Line(nz)
    rows, width = x_ref.shape
    loads = (
        pltpu.make_async_copy(mats_ref.at[layer, pl.ds(1, 6)], mats, load_sem.at[0]),
        pltpu.make_async_copy(gate_ref, gate, load_sem.at[1]),
        pltpu.make_async_copy(up_ref, up, load_sem.at[2]),
    )
    for load in loads:
        load.start()
    line.greet()
    ring = Gather(line, x_ref, blocks, gsems)
    blocks[line.ctx] = x_ref[...]
    ring.start()
    for load in loads:
        load.wait()
    ring.start_extras()

    def saves(row):
        pair = pl.ds(row * NX, NX)
        return (
            pltpu.make_async_copy(blocks.at[pair], all_out.at[pair], save_sem.at[0, row]),
            pltpu.make_async_copy(gate.at[pair], dgate_out.at[pair], save_sem.at[1, row]),
            pltpu.make_async_copy(up.at[pair], dup_out.at[pair], save_sem.at[2, row]),
            pltpu.make_async_copy(inners.at[pair], inner_out.at[pair], save_sem.at[3, row]),
        )

    def step(i, carry):
        @pl.when(i < nz - 1)
        def _():
            ring.forward(i)

        row = line.near(i)
        ring.wait_pair(row)
        pair = pl.ds(row * NX, NX)
        block = blocks[pair].reshape(NX * rows, width)
        share = share_ref[pair].reshape(NX * rows, 2)
        total = None
        units = mats.shape[2]
        for e in range(2):
            part_of = pl.ds(e * units, units)
            gate_act = gate[pair, :, part_of].reshape(NX * rows, units).astype(F32)
            up_act = up[pair, :, part_of].reshape(NX * rows, units).astype(F32)
            grad_inner = dot(block, mats[4 + e], NN) * share[:, e : e + 1]
            sigmoid = 1.0 / (1.0 + jnp.exp(-gate_act))
            silu = gate_act * sigmoid
            d_gate = (grad_inner * up_act * (sigmoid + silu * (1.0 - sigmoid))).astype(BF)
            d_up = (grad_inner * silu).astype(BF)
            inners[pair, :, part_of] = (silu * up_act * share[:, e : e + 1]).astype(BF).reshape(NX, rows, units)
            gate[pair, :, part_of] = d_gate.reshape(NX, rows, units)
            up[pair, :, part_of] = d_up.reshape(NX, rows, units)
            term = dot(d_gate, mats[e], NT) + dot(d_up, mats[2 + e], NT)
            total = term if total is None else total + term
        part[pair] = total.astype(BF).reshape(NX, rows, width)
        for save in saves(row):
            save.start()
        return carry

    lax.fori_loop(0, nz, step, 0)
    sums = Scatter(line, part, o_ref, work, ework, ssems, msems)
    for i in range(nz):
        sums.across(line.far(i)).start()
    ring.finish()
    for i in range(nz):
        sums.add(i)
    sums.finish()
    for row in range(nz):
        for save in saves(row):
            save.wait()


def experts_backward(block, share, mats, layer, gate_act, up_act, nz):
    rows, width = block.shape
    units = mats.shape[3]
    group = nz * NX
    acts = jax.ShapeDtypeStruct((group, rows, 2 * units), BF)
    held = pltpu.VMEM((group, rows, 2 * units), BF)
    return pl.pallas_call(
        functools.partial(experts_back_kernel, nz, layer),
        out_shape=(
            jax.ShapeDtypeStruct((rows, width), F32),
            jax.ShapeDtypeStruct((group, rows, width), BF),
            acts,
            acts,
            acts,
        ),
        in_specs=[VM, VM, ANY, ANY, ANY],
        out_specs=(VM, ANY, ANY, ANY, ANY),
        scratch_shapes=[
            pltpu.VMEM((6, width, units), BF),
            pltpu.VMEM((group, rows, width), BF),
            pltpu.VMEM((group, rows, width), BF),
            held,
            held,
            held,
            DMA((3,)),
            DMA((4, nz)),
        ]
        + Gather.scratch(nz)
        + Scatter.scratch(nz, rows, width),
        compiler_params=params(6 + 2 * layer, 60),
        name="experts_backward",
    )(block, share, mats, gate_act, up_act)


def far_of(nz, z, i):
    mid1 = jnp.where(i == 0, 3, jnp.where(i == 1, 0, jnp.where(i == 2, 2, 1)))
    mid2 = jnp.where(i == 0, 0, jnp.where(i == 1, 3, jnp.where(i == 2, 1, 2)))
    return jnp.where(z == 0, nz - 1 - i, jnp.where(z == nz - 1, i, jnp.where(z == 1, mid1, mid2)))


class Exchange:
    @staticmethod
    def scratch(nz, blk, lead=()):
        return [
            pltpu.VMEM(lead + (2, 2, 2) + blk, BF),
            pltpu.VMEM(lead + (nz,) + blk, BF),
            DMA(lead + (2, nz, nz, 2)),
            DMA(lead + (2, nz)),
        ]

    def __init__(self, line, src_at, dst_at, passing, for_mate, zs, xs, lead=()):
        self.line, self.src_at, self.dst_at, self.lead = line, src_at, dst_at, lead
        self.passing, self.for_mate, self.zs, self.xs = passing, for_mate, zs, xs

    def held(self, way, src, dest, side, at):
        last = self.line.nz - 1
        slot = (dest - at - 1) + src if way == 0 else (at - dest - 1) + last - src
        return self.passing.at[self.lead + (way, slot, side)]

    def zsem(self, kind, src, dest, side):
        return self.zs.at[self.lead + (kind, src, dest, side)]

    def hop(self, way, src, dest, side, ref):
        line = self.line
        to = line.z + 1 if way == 0 else line.z - 1
        sems = self.zsem(0, src, dest, side), self.zsem(1, src, dest, side)
        target = to * NX + line.x

        @pl.when(dest == to)
        def _():
            land = self.dst_at(src * NX + line.x) if side == 0 else self.for_mate.at[self.lead + (src,)]
            remote(ref, land, *sems, target, line.fsdp).start()

        @pl.when(dest != to)
        def _():
            remote(ref, self.held(way, src, dest, side, to), *sems, target, line.fsdp).start()

    def to_mate(self, src, ref=None):
        line = self.line
        ref = self.for_mate.at[self.lead + (src,)] if ref is None else ref
        return remote(ref, self.dst_at(src * NX + line.x), self.xs.at[self.lead + (0, src)], self.xs.at[self.lead + (1, src)], line.mate, line.fsdp)

    def send(self, dest):
        line = self.line
        for side, column in ((0, line.x), (1, 1 - line.x)):
            ref = self.src_at(dest * NX + column)

            @pl.when(dest > line.z)
            def _():
                self.hop(0, line.z, dest, side, ref)

            @pl.when(dest < line.z)
            def _():
                self.hop(1, line.z, dest, side, ref)

        @pl.when(dest == line.z)
        def _():
            self.to_mate(line.z, self.src_at(line.mate)).start()

    def events(self, i):
        line = self.line
        found = []
        for k in range(1, line.nz):
            j = i - k
            for way in range(2):
                src = line.z - k if way == 0 else line.z + k
                dest = far_of(line.nz, src, j)
                here = (dest >= line.z) if way == 0 else (dest <= line.z)
                found.append((way, src, dest, (src >= 0) & (src < line.nz) & (j >= 0) & (j < line.nz - 1) & here))
        return found

    def handle(self, way, src, dest, arrived):
        line = self.line
        for side in range(2):
            wait = self.held(way, 0 if way == 0 else line.nz - 1, line.z + 1 if way == 0 else line.z - 1, side, line.z)
            remote(wait, wait, self.zsem(0, src, dest, side), self.zsem(1, src, dest, side), line.mate, line.fsdp).wait_recv()

            @pl.when(dest != line.z)
            def _():
                self.hop(way, src, dest, side, self.held(way, src, dest, side, line.z))

        @pl.when(dest == line.z)
        def _():
            self.to_mate(src).start()
            arrived(src * NX + line.x)

    def mate_arrived(self, src):
        line = self.line
        wait = self.for_mate.at[self.lead + (src,)]
        remote(wait, wait, self.xs.at[self.lead + (0, src)], self.xs.at[self.lead + (1, src)], line.mate, line.fsdp).wait_recv()

    def finish(self):
        line = self.line
        wait = self.for_mate.at[self.lead + (0,)]
        for src in range(line.nz):
            for dest in range(line.nz):
                if src != dest:
                    passes = (line.z >= src) & (line.z < dest) if src < dest else (line.z <= src) & (line.z > dest)

                    @pl.when(passes)
                    def _():
                        for side in range(2):
                            remote(wait, wait, self.zsem(0, src, dest, side), self.zsem(1, src, dest, side), line.mate, line.fsdp).wait_send()

            self.to_mate(src).wait_send()


LAG = 3


def weights_kernel(nctx, nfs, rows, w_ref, g_ref, o_ref, go_ref, passing, for_mate, zs, xs, own_sem, y_sem, c_sem, gown_sem, gp_sem, gy_sem, gc_sem):
    nz = nctx // NX
    line = Line(nz)
    ctx, fsdp = line.ctx, line.fsdp
    layers = w_ref.shape[0]
    spread = layers - 1
    y, core = fsdp // NCORE, fsdp % NCORE
    y_mate = (1 - y) * NCORE + core
    c_mate = y * NCORE + 1 - core
    y_c_mate = (1 - y) * NCORE + 1 - core
    barrier = pltpu.get_barrier_semaphore()
    for step in range(1, nctx):
        greet(barrier, (ctx + step) % nctx, fsdp)
    for other in (y_mate, c_mate):
        greet(barrier, ctx, other)
    pl.semaphore_wait(barrier, nctx + 1)

    def place(layer, s, f):
        return o_ref.at[layer, :, pl.ds(pl.multiple_of((s * nfs + f) * rows, rows), rows), :]

    def swap(layer):
        return Exchange(
            line,
            lambda to: w_ref.at[layer, to],
            lambda frm: place(layer, frm, fsdp),
            passing, for_mate, zs, xs,
            (layer,),
        )

    def over_y(layer, frm, f, ref=None):
        return remote(place(layer, frm, f) if ref is None else ref, place(layer, frm, f), y_sem.at[0, layer, frm], y_sem.at[1, layer, frm], ctx, y_mate)

    def over_c(layer, frm, f, k, ref=None):
        return remote(place(layer, frm, f) if ref is None else ref, place(layer, frm, f), c_sem.at[0, k, layer, frm], c_sem.at[1, k, layer, frm], ctx, c_mate)

    def own(layer):
        return pltpu.make_async_copy(w_ref.at[layer, ctx], place(layer, ctx, fsdp), own_sem.at[layer])

    def begin(layer):
        exchange = swap(layer)
        for i in range(nz - 1):
            exchange.send(line.far(i))
        exchange.send(line.z)
        if layer < spread:
            over_y(layer, ctx, fsdp, w_ref.at[layer, ctx]).start()
            over_c(layer, ctx, fsdp, 0, w_ref.at[layer, ctx]).start()
        own(layer).start()

    def arrived(layer, frm):
        @pl.when(layer < spread)
        def _():
            over_y(layer, frm, fsdp).start()
            over_c(layer, frm, fsdp, 0).start()

    def from_y(layer, frm):
        @pl.when(layer < spread)
        def _():
            over_y(layer, frm, y_mate).wait_recv()
            over_c(layer, frm, y_mate, 1).start()

    def take(layer, i):
        exchange = swap(layer)
        for way, src, dest, real in exchange.events(i):

            @pl.when(real)
            def _():
                exchange.handle(way, src, dest, lambda frm: arrived(layer, frm))

        def mine(late, then):
            @pl.when(i == late)
            def _():
                then(line.z)

            for way, src, dest, real in exchange.events(i - late):

                @pl.when(real & (dest == line.z))
                def _():
                    then(src)

        def mates(src):
            exchange.mate_arrived(src)
            arrived(layer, src * NX + 1 - line.x)

        mine(1, mates)
        mine(2, lambda src: from_y(layer, src * NX + line.x))
        mine(3, lambda src: from_y(layer, src * NX + 1 - line.x))

    def small(to):
        return remote(g_ref.at[to], go_ref.at[ctx * nfs + fsdp], gp_sem.at[0, to], gp_sem.at[1, ctx], to, fsdp)

    def small_in(frm):
        return remote(g_ref.at[ctx], go_ref.at[frm * nfs + fsdp], gp_sem.at[0, frm], gp_sem.at[1, frm], frm, fsdp)

    def small_y(frm, f):
        return remote(go_ref.at[frm * nfs + f], go_ref.at[frm * nfs + f], gy_sem.at[0, frm], gy_sem.at[1, frm], ctx, y_mate)

    def small_c(frm, f, k):
        return remote(go_ref.at[frm * nfs + f], go_ref.at[frm * nfs + f], gc_sem.at[0, k, frm], gc_sem.at[1, k, frm], ctx, c_mate)

    small_own = pltpu.make_async_copy(g_ref.at[ctx], go_ref.at[ctx * nfs + fsdp], gown_sem)
    small_own.start()
    for step in range(1, nctx):
        small((ctx + step) % nctx).start()
    steps = 2 * nz - 3 + 3

    def step(i, carry):
        for layer in range(layers):
            at = i - LAG * layer

            @pl.when(at == 0)
            def _():
                begin(layer)

        def each(layer, carry):
            at = i - LAG * layer

            @pl.when((at > 0) & (at <= steps))
            def _():
                take(layer, at)

            return carry

        lax.fori_loop(0, layers, each, 0)
        return carry

    lax.fori_loop(0, steps - 1 + LAG * (layers - 1), step, 0)
    small_own.wait()
    for k in range(nctx):
        if k:
            small_in((ctx + k) % nctx).wait_recv()
        small_y((ctx + k) % nctx, fsdp).start()
        small_c((ctx + k) % nctx, fsdp, 0).start()
    for k in range(nctx):
        small_y((ctx + k) % nctx, y_mate).wait_recv()
        small_c((ctx + k) % nctx, y_mate, 1).start()
    for frm in range(nctx):
        small_c(frm, c_mate, 0).wait_recv()
        small_c(frm, y_c_mate, 1).wait_recv()
        small_c(frm, fsdp, 0).wait_send()
        small_c(frm, y_mate, 1).wait_send()
        small_y(frm, fsdp).wait_send()
    for step_ in range(1, nctx):
        small((ctx + step_) % nctx).wait_send()

    def close(layer, carry):
        own(layer).wait()

        @pl.when(layer < spread)
        def _():
            for frm in range(nctx):
                over_c(layer, frm, c_mate, 0).wait_recv()
                over_c(layer, frm, y_c_mate, 1).wait_recv()
                over_c(layer, frm, fsdp, 0).wait_send()
                over_c(layer, frm, y_mate, 1).wait_send()
                over_y(layer, frm, fsdp).wait_send()

        swap(layer).finish()
        return carry

    lax.fori_loop(0, layers, close, 0)


def spread_weights(send, small, nfs):
    layers, nctx, mats, rows, width = send.shape
    return pl.pallas_call(
        functools.partial(weights_kernel, nctx, nfs, rows),
        out_shape=(
            jax.ShapeDtypeStruct((layers, mats, nctx * nfs * rows, width), send.dtype),
            jax.ShapeDtypeStruct((nctx * nfs,) + small.shape[1:], small.dtype),
        ),
        in_specs=[ANY, VM],
        out_specs=(ANY, ANY),
        scratch_shapes=Exchange.scratch(nctx // NX, (mats, rows, width), (layers,))
        + [
            DMA((layers,)),
            DMA((2, layers, nctx)),
            DMA((2, 2, layers, nctx)),
            DMA,
            DMA((2, nctx)),
            DMA((2, nctx)),
            DMA((2, 2, nctx)),
        ],
        compiler_params=params(3, 40),
        name="spread_weights",
    )(send, small)


class Spread:
    @staticmethod
    def scratch(nctx):
        return [DMA((2, nctx)), DMA((2, 2, nctx))]

    def __init__(self, line, mats, layer, nfs, y_sem, c_sem):
        self.line, self.mats, self.layer, self.nfs, self.y_sem, self.c_sem = line, mats, layer, nfs, y_sem, c_sem
        y, core = line.fsdp // NCORE, line.fsdp % NCORE
        self.y_mate = (1 - y) * NCORE + core
        self.c_mate = y * NCORE + 1 - core
        self.nctx = line.nz * NX
        self.rows = mats.shape[2] // (self.nctx * nfs)

    def place(self, frm, f):
        at = pl.multiple_of((frm * self.nfs + f) * self.rows, self.rows)
        return self.mats.at[self.layer, :, pl.ds(at, self.rows), :]

    def over_y(self, frm):
        place = self.place(frm, self.line.fsdp)
        return remote(place, place, self.y_sem.at[0, frm], self.y_sem.at[1, frm], self.line.ctx, self.y_mate)

    def over_c(self, frm, k):
        place = self.place(frm, self.y_mate if k else self.line.fsdp)
        return remote(place, place, self.c_sem.at[0, k, frm], self.c_sem.at[1, k, frm], self.line.ctx, self.c_mate)

    def start(self):
        for frm in range(self.nctx):
            self.over_y(frm).start()
            self.over_c(frm, 0).start()

    def take(self, frm):
        self.over_y(frm).wait_recv()
        self.over_c(frm, 1).start()

    def finish(self):
        for frm in range(self.nctx):
            self.over_y(frm).wait_send()
            for k in range(2):
                self.over_c(frm, k).wait()


def grads_kernel(nctx, nfs, rows, layers, *refs):
    count = 9 * layers
    ins, (e_ref, o_ref, eo_ref), refs = refs[:count], refs[count : count + 3], refs[count + 3 :]
    tall, dproj, attended, dgate, dup, inner, mine, cin, yin, e_cin, e_half, e_yin, e_full = refs[:13]
    tall_sem, wide_sem, own_sem, c_sem, y_sem, p_sem, eown_sem, ec_sem, ey_sem, ep_sem = refs[13:]
    nz = nctx // NX
    line = Line(nz)
    ctx, fsdp = line.ctx, line.fsdp
    y, core = fsdp // NCORE, fsdp % NCORE
    y_mate = (1 - y) * NCORE + core
    c_mate = y * NCORE + 1 - core
    mats, slab = mine.shape[1], mine.shape[2]
    proj = mine.shape[3] - attended.shape[2]
    units = dgate.shape[2] // 2
    items = layers * nz

    def layer_of(i):
        return layers - 1 - i // nz

    def row_of(i):
        return line.far(i % nz)

    def wide_loads(layer):
        _, dproj_in, _, attended_in, _, dgate_in, dup_in, _, inner_in = ins[9 * layer : 9 * layer + 9]
        pairs = ((dproj_in, dproj), (attended_in, attended), (dgate_in, dgate), (dup_in, dup), (inner_in, inner))
        return [pltpu.make_async_copy(src, dst.at[layer], wide_sem.at[k, layer]) for k, (src, dst) in enumerate(pairs)]

    def tall_loads(i, layer):
        normed_in, _, middle_in, _, moe_in, _, _, grad_in, _ = ins[9 * layer : 9 * layer + 9]
        lanes = pl.ds(pl.multiple_of(row_of(i) * slab, 128), slab)
        return [
            pltpu.make_async_copy(src.at[:, lanes], tall.at[i % 2, k], tall_sem.at[i % 2, k])
            for k, src in enumerate((normed_in, middle_in, moe_in, grad_in))
        ]

    def load(i):
        for layer in range(layers):

            @pl.when(layer_of(i) == layer)
            def _():
                for copy in tall_loads(i, layer):
                    copy.start()

    for layer in reversed(range(layers)):
        for copy in wide_loads(layer):
            copy.start()
        if layer == layers - 1:
            load(0)
    barrier = pltpu.get_barrier_semaphore()
    for step in range(1, nctx):
        greet(barrier, (ctx + step) % nctx, fsdp)
    for other in (y_mate, c_mate):
        greet(barrier, ctx, other)
    pl.semaphore_wait(barrier, nctx + 1)

    def span(side, f):
        return pl.ds(pl.multiple_of((side * nfs + f) * rows, rows), rows)

    def to_c(i, side, k):
        layer, s = layer_of(i), row_of(i) * NX + side
        f = (1 - y if k == 0 else y) * NCORE + 1 - core
        return remote(mine.at[i % 3, :, span(side, f), :], cin.at[layer, k, s], c_sem.at[0, layer, k, s], c_sem.at[1, layer, k, s], ctx, c_mate)

    def to_y(layer, s):
        return remote(cin.at[layer, 0, s], yin.at[layer, s], y_sem.at[0, layer, s], y_sem.at[1, layer, s], ctx, y_mate)

    def out(layer, s):
        return remote(cin.at[layer, 1, s], o_ref.at[layer, ctx], p_sem.at[0, layer, s], p_sem.at[1, layer, ctx], s, fsdp)

    def out_in(layer, s):
        return remote(cin.at[layer, 1, s], o_ref.at[layer, s], p_sem.at[0, layer, s], p_sem.at[1, layer, s], s, fsdp)

    def own(layer):
        return pltpu.make_async_copy(cin.at[layer, 1, ctx], o_ref.at[layer, ctx], own_sem.at[layer])

    e_to_c = remote(e_ref.at[1 - core], e_cin, ec_sem.at[0], ec_sem.at[1], ctx, c_mate)
    e_to_y = remote(e_half.at[1 - y], e_yin, ey_sem.at[0], ey_sem.at[1], ctx, y_mate)
    e_own = pltpu.make_async_copy(e_full.at[ctx], eo_ref.at[ctx], eown_sem)

    def e_out(s):
        return remote(e_full.at[s], eo_ref.at[ctx], ep_sem.at[0, s], ep_sem.at[1, ctx], s, fsdp)

    def e_out_in(s):
        return remote(e_full.at[s], eo_ref.at[s], ep_sem.at[0, s], ep_sem.at[1, s], s, fsdp)

    e_to_c.start()

    def compute(i):
        layer, slot, here = layer_of(i), i % 2, i % 3
        mine[here, 0, :, pl.ds(0, proj)] = dot(tall[slot, 0], dproj[layer], TN)[:, :proj].astype(BF)
        mine[here, 0, :, pl.ds(proj, mine.shape[3] - proj)] = dot(tall[slot, 1], attended[layer], TN).astype(BF)
        for e in range(2):
            part_of = pl.ds(e * units, units)
            mine[here, 1 + e] = dot(tall[slot, 2], dgate[layer, :, part_of], TN).astype(BF)
            mine[here, 3 + e] = dot(tall[slot, 2], dup[layer, :, part_of], TN).astype(BF)
            mine[here, 5 + e] = dot(tall[slot, 3], inner[layer, :, part_of], TN).astype(BF)

    def first(i, side):
        layer, s = layer_of(i), row_of(i) * NX + side
        to_c(i, side, 0).wait_recv()

        def one(m, _):
            term = mine[i % 3, m, span(side, y_mate), :].astype(F32)
            cin[layer, 0, s, m] = (term + cin[layer, 0, s, m].astype(F32)).astype(BF)
            return 0

        lax.fori_loop(0, mats, one, 0)
        to_y(layer, s).start()

    def second(i, side):
        layer, s = layer_of(i), row_of(i) * NX + side
        to_c(i, side, 1).wait_recv()
        to_y(layer, s).wait_recv()

        def one(m, _):
            term = mine[i % 3, m, span(side, fsdp), :].astype(F32) + yin[layer, s, m].astype(F32)
            cin[layer, 1, s, m] = (term + cin[layer, 1, s, m].astype(F32)).astype(BF)
            return 0

        lax.fori_loop(0, mats, one, 0)
        for k in range(2):
            to_c(i, side, k).wait_send()

        @pl.when(s != ctx)
        def _():
            out(layer, s).start()

        @pl.when(s == ctx)
        def _():
            own(layer).start()

    def step(i, carry):
        @pl.when(i < items)
        def _():
            for layer in range(layers):

                @pl.when(i == (layers - 1 - layer) * nz)
                def _():
                    for copy in wide_loads(layer):
                        copy.wait()

            for copy in tall_loads(i, 0):
                copy.wait()

            @pl.when(i + 1 < items)
            def _():
                load(i + 1)

            compute(i)
            for k in range(2):
                for side in range(NX):
                    to_c(i, side, k).start()

        @pl.when((i >= 1) & (i < items + 1))
        def _():
            for side in range(NX):
                first(i - 1, side)

        @pl.when(i >= 2)
        def _():
            for side in range(NX):
                second(i - 2, side)

        @pl.when(i == 1)
        def _():
            e_to_c.wait_recv()
            e_half[...] = e_ref[core] + e_cin[...]
            e_to_y.start()

        @pl.when(i == 3)
        def _():
            e_to_y.wait_recv()
            e_full[...] = e_half[y] + e_yin[...]
            e_own.start()
            for step_ in range(1, nctx):
                e_out((ctx + step_) % nctx).start()

        return carry

    lax.fori_loop(0, items + 2, step, 0)
    for layer in range(layers):
        own(layer).wait()
        for s in range(nctx):
            to_y(layer, s).wait_send()

            @pl.when(s != ctx)
            def _():
                out(layer, s).wait_send()
                out_in(layer, s).wait_recv()

    for s in range(nctx):

        @pl.when(s != ctx)
        def _():
            e_out(s).wait_send()
            e_out_in(s).wait_recv()

    e_to_c.wait_send()
    e_to_y.wait_send()
    e_own.wait()


def collect_grads(nctx, nfs, layer_args, extra):
    layers = len(layer_args)
    normed, dproj, middle, attended, moe, dgate, dup, grad, inner = layer_args[0]
    group_rows, width = normed.shape
    rows = width // (nctx * nfs)
    slab = NX * nfs * rows
    mats, cols = 7, dgate.shape[1] // 2
    blk = (mats, rows, cols)
    tile = extra.shape[3:]
    held = [pltpu.VMEM((layers,) + part.shape, BF) for part in (dproj, attended, dgate, dup, inner)]
    return pl.pallas_call(
        functools.partial(grads_kernel, nctx, nfs, rows, layers),
        out_shape=(jax.ShapeDtypeStruct((layers, nctx) + blk, BF), jax.ShapeDtypeStruct((nctx,) + tile, F32)),
        in_specs=[ANY] * (9 * layers) + [VM],
        out_specs=(ANY, ANY),
        scratch_shapes=[pltpu.VMEM((2, 4, group_rows, slab), BF)]
        + held
        + [
            pltpu.VMEM((3, mats, slab, cols), BF),
            pltpu.VMEM((layers, 2, nctx) + blk, BF),
            pltpu.VMEM((layers, nctx) + blk, BF),
            pltpu.VMEM((2, nctx) + tile, F32),
            pltpu.VMEM((2, nctx) + tile, F32),
            pltpu.VMEM((nctx,) + tile, F32),
            pltpu.VMEM((nctx,) + tile, F32),
            DMA((2, 4)),
            DMA((5, layers)),
            DMA((layers,)),
            DMA((2, layers, 2, nctx)),
            DMA((2, layers, nctx)),
            DMA((2, layers, nctx)),
            DMA,
            DMA((2,)),
            DMA((2,)),
            DMA((2, nctx)),
        ],
        compiler_params=params(4, 63),
        name="collect_grads",
    )(*[part for args in layer_args for part in args], extra)


def spin(values, cos_part, sin_part):
    lane = lax.broadcasted_iota(jnp.int32, values.shape, 1) % HEAD_DIM
    half_dim = HEAD_DIM // 2
    swapped = jnp.where(
        lane < half_dim,
        pltpu.roll(values, values.shape[1] - half_dim, 1),
        pltpu.roll(values, half_dim, 1),
    )
    return values * cos_part + swapped * sin_part


def attention_kernel(nz, nfs, layer, x_ref, mats_ref, cos_ref, sin_ref, key_at_ref, query_at_ref,
                     o_ref, all_out, q_ref, k_ref, v_ref, peak_ref, share_ref, att_ref, *refs):
    line = Line(nz)
    spread = None
    if layer == 0:
        mats_ref, refs = refs[0], refs[1:]
        spread = Spread(line, mats_ref, layer + 1, nfs, *refs[-2:])
        refs = refs[:-2]
    attn, out_w, blocks, part, v_turned, probs, load_sem, save_sem, gsems, work, ework, ssems, msems = refs
    rows, width = x_ref.shape
    pair_rows = NX * rows
    heads = q_ref.shape[1] // rows
    o_at = (heads + 2) * HEAD_DIM
    wide = -(-o_at // 128) * 128
    load = pltpu.make_async_copy(mats_ref.at[layer, 0], attn, load_sem)
    load.start()
    line.greet((spread.y_mate, spread.c_mate) if spread else ())
    if spread:
        spread.start()
    ring = Gather(line, x_ref, blocks, gsems)
    blocks[line.ctx] = x_ref[...]
    ring.start()
    load.wait()
    out_w[...] = attn[:, o_at:]
    ring.start_extras()

    def save(row):
        pair = pl.ds(row * NX, NX)
        return pltpu.make_async_copy(blocks.at[pair], all_out.at[pair], save_sem.at[row])

    def project(i, carry):
        @pl.when(i < nz - 1)
        def _():
            ring.forward(i)

        row = line.near(i)
        ring.wait_pair(row)
        pair = pl.ds(row * NX, NX)
        tall = pl.ds(pl.multiple_of(row * pair_rows, pair_rows), pair_rows)
        block = blocks[pair].reshape(pair_rows, width)
        save(row).start()
        proj = dot(block, attn[:, :wide], NN)
        cos_part, sin_part = cos_ref[tall, :], sin_ref[tall, :]
        first = spin(proj[:, :128], cos_part, sin_part)
        second = spin(proj[:, 128:256], cos_part, sin_part)
        values = proj[:, 256 : 256 + HEAD_DIM]
        for side in range(NX):
            at = slice(side * rows, (side + 1) * rows)
            q_ref[row * NX + side, 0:rows, :] = first[at, :HEAD_DIM].astype(BF)
            q_ref[row * NX + side, rows : 2 * rows, :] = first[at, HEAD_DIM:].astype(BF)
            q_ref[row * NX + side, 2 * rows : 3 * rows, :] = second[at, :HEAD_DIM].astype(BF)
        k_ref[tall, :] = second[:, HEAD_DIM:].astype(BF)
        v_ref[tall, :] = values.astype(BF)
        v_turned[:, tall] = values.T.astype(BF)
        return carry

    lax.fori_loop(0, nz, project, 0)
    ring.finish()
    sums = Scatter(line, part, o_ref, work, ework, ssems, msems)

    def attend(at):
        scores = dot(k_ref[...], q_ref[at], NT)
        key_at = key_at_ref[...]
        visible = (key_at >= query_at_ref[at, 0:1, :]) & (key_at <= query_at_ref[at, 1:2, :])
        for head in range(heads):
            lanes = slice(head * rows, (head + 1) * rows)
            raw = jnp.where(visible, scores[:, lanes] * HEAD_DIM**-0.5, NEGATIVE)
            peak = jnp.max(raw, axis=0, keepdims=True)
            powers = jnp.exp(raw - peak)
            peak_ref[at, :, lanes] = peak
            share_ref[at, :, lanes] = 1.0 / jnp.sum(powers, axis=0, keepdims=True)
            probs[:, lanes] = powers.astype(BF)
        turned = dot(v_turned[...], probs[...], NN) * share_ref[at]
        stacked = turned.T.astype(BF)
        for head in range(heads):
            att_ref[at, :, head * HEAD_DIM : (head + 1) * HEAD_DIM] = stacked[head * rows : (head + 1) * rows]
        part[at] = dot(att_ref[at], out_w[...], NT).astype(BF)

    def step(i, carry):
        row = line.far(i)
        attend(row * NX + 1 - line.x)
        sums.across(row).start()
        attend(row * NX + line.x)

        @pl.when(i > 0)
        def _():
            sums.add(i - 1)

        if spread:
            for side in range(NX):
                spread.take(i * NX + side)

        return carry

    lax.fori_loop(0, nz, step, 0)
    sums.add(nz - 1)
    sums.finish()
    for row in range(nz):
        save(row).wait()
    if spread:
        spread.finish()


def attention_rows(block, mats, layer, cos_part, sin_part, key_at, query_at, nz, nfs):
    rows, width = block.shape
    spreads = layer == 0
    group = nz * NX
    group_rows = group * rows
    heads = 3
    return pl.pallas_call(
        functools.partial(attention_kernel, nz, nfs, layer),
        out_shape=(
            jax.ShapeDtypeStruct((rows, width), F32),
            jax.ShapeDtypeStruct((group, rows, width), BF),
            jax.ShapeDtypeStruct((group, heads * rows, HEAD_DIM), BF),
            jax.ShapeDtypeStruct((group_rows, HEAD_DIM), BF),
            jax.ShapeDtypeStruct((group_rows, HEAD_DIM), BF),
            jax.ShapeDtypeStruct((group, 1, heads * rows), F32),
            jax.ShapeDtypeStruct((group, 1, heads * rows), F32),
            jax.ShapeDtypeStruct((group, rows, heads * HEAD_DIM), BF),
        )
        + ((jax.ShapeDtypeStruct(mats.shape, BF),) if spreads else ()),
        in_specs=[VM, ANY, VM, VM, VM, VM],
        out_specs=(VM, ANY, VM, VM, VM, VM, VM, VM) + ((ANY,) if spreads else ()),
        input_output_aliases={1: 8} if spreads else {},
        scratch_shapes=[
            pltpu.VMEM(mats.shape[2:], BF),
            pltpu.VMEM((width, heads * HEAD_DIM), BF),
            pltpu.VMEM((group, rows, width), BF),
            pltpu.VMEM((group, rows, width), BF),
            pltpu.VMEM((HEAD_DIM, group_rows), BF),
            pltpu.VMEM((group_rows, heads * rows), BF),
            DMA,
            DMA((nz,)),
        ]
        + Gather.scratch(nz)
        + Scatter.scratch(nz, rows, width)
        + (Spread.scratch(group) if spreads else []),
        compiler_params=params(9 + 2 * layer, 60),
        name="attention_forward",
    )(block, mats, cos_part, sin_part, key_at, query_at)


def attention_back_kernel(nz, layer, x_ref, mats_ref, cos_ref, sin_ref, key_at_ref, query_at_ref, q_ref, k_ref, v_ref, peak_ref, share_ref,
                          o_ref, all_out, dproj_ref,
                          attn, out_w, blocks, part, k_turned, probs, slopes, dq, dk, dv, load_sem, save_sem, gsems, work, ework, ssems, msems):
    line = Line(nz)
    rows, width = x_ref.shape
    pair_rows = NX * rows
    heads = q_ref.shape[1] // rows
    o_at = (heads + 2) * HEAD_DIM
    wide = dproj_ref.shape[2]
    scale = HEAD_DIM**-0.5
    load = pltpu.make_async_copy(mats_ref.at[layer, 0], attn, load_sem)
    load.start()
    line.greet()
    ring = Gather(line, x_ref, blocks, gsems)
    blocks[line.ctx] = x_ref[...]
    ring.start()
    k_turned[...] = k_ref[...].astype(F32).T.astype(BF)
    dk[...] = jnp.zeros(dk.shape, F32)
    dv[...] = jnp.zeros(dv.shape, F32)
    load.wait()
    out_w[...] = attn[:, o_at:]
    ring.start_extras()

    def save(row):
        pair = pl.ds(row * NX, NX)
        return pltpu.make_async_copy(blocks.at[pair], all_out.at[pair], save_sem.at[row])

    def back(at):
        d_att = dot(blocks[at], out_w[...], NN)
        d_heads = jnp.concatenate(
            [d_att[:, head * HEAD_DIM : (head + 1) * HEAD_DIM] for head in range(heads)], axis=0
        ).astype(BF)
        scores = dot(k_ref[...], q_ref[at], NT)
        d_probs = dot(v_ref[...], d_heads, NT)
        key_at = key_at_ref[...]
        visible = (key_at >= query_at_ref[at, 0:1, :]) & (key_at <= query_at_ref[at, 1:2, :])
        for head in range(heads):
            lanes = slice(head * rows, (head + 1) * rows)
            raw = jnp.where(visible, scores[:, lanes] * scale, NEGATIVE)
            prob = jnp.exp(raw - peak_ref[at, :, lanes]) * share_ref[at, :, lanes]
            grad = d_probs[:, lanes]
            delta = jnp.sum(prob * grad, axis=0, keepdims=True)
            probs[:, lanes] = prob.astype(BF)
            slopes[:, lanes] = (prob * (grad - delta)).astype(BF)
        dv[...] += dot(probs[...], d_heads, NN)
        dk[...] += dot(slopes[...], q_ref[at], NN)
        stacked = dot(k_turned[...], slopes[...], NN).T * scale
        for head in range(heads):
            dq[at, :, head * HEAD_DIM : (head + 1) * HEAD_DIM] = stacked[head * rows : (head + 1) * rows]

    def take(i, carry):
        @pl.when(i < nz - 1)
        def _():
            ring.forward(i)

        row = line.near(i)
        back(row * NX + line.x)
        ring.wait_pair(row)
        save(row).start()
        back(row * NX + 1 - line.x)
        return carry

    lax.fori_loop(0, nz, take, 0)
    ring.finish()
    sums = Scatter(line, part, o_ref, work, ework, ssems, msems)

    def project(at):
        tall = pl.ds(pl.multiple_of(at * rows, rows), rows)
        cos_part, sin_part = cos_ref[tall, :], -sin_ref[tall, :]
        block_dq = dq[at]
        second = jnp.concatenate([block_dq[:, 128:], dk[tall, :] * scale], axis=1)
        dproj_ref[at, :, 0:128] = spin(block_dq[:, :128], cos_part, sin_part).astype(BF)
        dproj_ref[at, :, 128:256] = spin(second, cos_part, sin_part).astype(BF)
        last = jnp.concatenate([dv[tall, :], jnp.zeros((rows, wide - 256 - HEAD_DIM), F32)], axis=1)
        dproj_ref[at, :, 256:wide] = last.astype(BF)
        part[at] = dot(dproj_ref[at], attn[:, :wide], NT).astype(BF)

    def step(i, carry):
        row = line.far(i)
        project(row * NX + 1 - line.x)
        sums.across(row).start()
        project(row * NX + line.x)

        @pl.when(i > 0)
        def _():
            sums.add(i - 1)

        return carry

    lax.fori_loop(0, nz, step, 0)
    sums.add(nz - 1)
    sums.finish()
    for row in range(nz):
        save(row).wait()


def attention_rows_back(block, mats, layer, cos_part, sin_part, key_at, query_at, queries, keys, values, peaks, shares, nz):
    rows, width = block.shape
    group = nz * NX
    group_rows = group * rows
    heads = 3
    wide = 384
    return pl.pallas_call(
        functools.partial(attention_back_kernel, nz, layer),
        out_shape=(
            jax.ShapeDtypeStruct((rows, width), F32),
            jax.ShapeDtypeStruct((group, rows, width), BF),
            jax.ShapeDtypeStruct((group, rows, wide), BF),
        ),
        in_specs=[VM, ANY] + [VM] * 9,
        out_specs=(VM, ANY, VM),
        scratch_shapes=[
            pltpu.VMEM(mats.shape[2:], BF),
            pltpu.VMEM((width, heads * HEAD_DIM), BF),
            pltpu.VMEM((group, rows, width), BF),
            pltpu.VMEM((group, rows, width), BF),
            pltpu.VMEM((HEAD_DIM, group_rows), BF),
            pltpu.VMEM((group_rows, heads * rows), BF),
            pltpu.VMEM((group_rows, heads * rows), BF),
            pltpu.VMEM((group, rows, heads * HEAD_DIM), F32),
            pltpu.VMEM((group_rows, HEAD_DIM), F32),
            pltpu.VMEM((group_rows, HEAD_DIM), F32),
            DMA,
            DMA((nz,)),
        ]
        + Gather.scratch(nz)
        + Scatter.scratch(nz, rows, width),
        compiler_params=params(10 + 2 * layer, 60),
        name="attention_backward",
    )(block, mats, cos_part, sin_part, key_at, query_at, queries, keys, values, peaks, shares)


def rope_tables(places):
    half_dim = HEAD_DIM // 2
    freq_steps = jnp.arange(half_dim, dtype=jnp.float32)
    inverse = jnp.exp(freq_steps * (-2.0 * math.log(10000.0) / HEAD_DIM))
    angles = places[:, None] * inverse[None, :]
    return jnp.cos(angles), jnp.sin(angles)


def pack_weights(master_set, layer, nctx):
    query_weight, key_weight, value_weight, out_weight, attn_gain, moe_gain, gate_weight, up_weight, down_weight = master_set
    rows = query_weight.shape[1]

    def columns(master):
        low = master[layer].astype(BF).reshape(rows, nctx, -1)
        return low.transpose(1, 0, 2)

    attn = jnp.concatenate(
        [columns(query_weight), columns(key_weight), columns(value_weight), columns(out_weight)], axis=-1
    )

    def experts(master):
        low = master[layer].astype(BF)
        return low.reshape(nctx, -1, rows, low.shape[-1])

    send = jnp.concatenate(
        [attn[:, None], experts(gate_weight), experts(up_weight), experts(down_weight)], axis=1
    )
    gains = jnp.stack([attn_gain[layer], moe_gain[layer]]).astype(BF).astype(F32)
    return send, jnp.pad(gains, ((0, 0), (0, 128 - rows)))


def norm_back(values, gain, grad):
    scale = lax.rsqrt(jnp.mean(values * values, axis=-1, keepdims=True) + EPSILON)
    unit = values * scale
    grad_gain = jnp.sum(grad * unit, axis=0)
    pulled = grad * gain
    return scale * (pulled - unit * jnp.mean(pulled * unit, axis=-1, keepdims=True)), grad_gain


def fast_body(nctx, nfs, *args):
    (tokens, cotangent, lengths, tile_order, routes, gates), master_set = args[:6], args[6:]
    nz = nctx // NX
    rows_here, model_width = tokens.shape[1], tokens.shape[2]
    group_rows = rows_here * nctx
    ctx = lax.axis_index("ctx")
    _, pos_all = layout(lengths[0], tile_order[0], group_rows)
    cos_half, sin_half = rope_tables(pos_all.astype(jnp.float32))
    cos_part = jnp.concatenate([cos_half] * 4, axis=1)
    sin_part = jnp.concatenate([-sin_half, sin_half] * 2, axis=1)
    row_ids = jnp.arange(rows_here, dtype=jnp.int32)
    first_at = (tile_order[0][:, None] * TILE + row_ids[None, :]).reshape(group_rows)
    key_at = first_at[:, None]
    query_at = jnp.stack(
        [(first_at - pos_all).reshape(nctx, rows_here), first_at.reshape(nctx, rows_here)], axis=1
    )
    q_width = 3 * HEAD_DIM
    kv_at, v_at, o_at = q_width, q_width + HEAD_DIM, q_width + 2 * HEAD_DIM

    expert_ids = jnp.arange(EXPERTS, dtype=jnp.int32)
    table = jnp.sum(
        jnp.where(routes[:, 0, :, :, None] == expert_ids, gates[:, 0, :, :, None], 0.0), axis=-2
    )
    packed = [pack_weights(master_set, layer, nctx) for layer in range(LAYERS)]
    rows = packed[0][0].shape[2]
    gains = jnp.broadcast_to(jnp.concatenate([gain for _, gain in packed])[None], (nctx, 2 * LAYERS, 128))
    shares = table.transpose(2, 0, 1).reshape(nctx, 2, LAYERS, rows_here).transpose(0, 2, 1, 3)
    shares = shares.reshape(nctx, 2 * LAYERS, rows_here)
    pad = jnp.zeros((nctx, 8 - 2 * LAYERS, 128), F32)
    small = jnp.concatenate([gains, pad, shares, pad], axis=1)
    mats_all, small_all = spread_weights(jnp.stack([send for send, _ in packed]), small, nfs)
    shares = lax.dynamic_index_in_dim(
        small_all.reshape(nctx, nfs, 16, 128), lax.axis_index("fsdp"), 1, keepdims=False
    )
    fetched = [
        (
            small_all[:, 2 * layer, :rows].reshape(-1),
            small_all[:, 2 * layer + 1, :rows].reshape(-1),
            shares[:, 8 + 2 * layer : 10 + 2 * layer].transpose(0, 2, 1),
        )
        for layer in range(LAYERS)
    ]

    hidden = tokens[0].astype(jnp.float32)
    records = []
    for layer in range(LAYERS):
        attn_gain, moe_gain, share = fetched[layer]
        normed = rms_norm(hidden, attn_gain).astype(BF)
        mixed, normed_all, queries, keys, values, peaks, sums, attended, *rest = attention_rows(
            normed, mats_all, layer, cos_part, sin_part, key_at, query_at, nz, nfs
        )
        mats_all = rest[0] if rest else mats_all
        middle = hidden + mixed

        moe_in = rms_norm(middle, moe_gain).astype(BF)
        moved, moe_all, gate_act, up_act = experts_forward(moe_in, share, mats_all, layer, nz)
        records.append((hidden, normed_all, queries, keys, values, peaks, sums, attended, middle, moe_all, gate_act, up_act))
        hidden = middle + moved

    output = hidden.astype(BF)
    grad = cotangent[0].astype(jnp.float32)
    layer_args, gain_grads = [None] * LAYERS, [None] * LAYERS
    for layer in reversed(range(LAYERS)):
        attn_gain, moe_gain, share = fetched[layer]
        hidden, normed_all, queries, keys, values, peaks, sums, attended, middle, moe_all, gate_act, up_act = records[layer]
        grad_moe_in, grad_all, d_gate, d_up, inner = experts_backward(grad.astype(BF), share, mats_all, layer, gate_act, up_act, nz)
        through, grad_moe_gain = norm_back(middle, moe_gain, grad_moe_in)
        grad_middle = grad + through

        grad_normed, middle_all, d_proj = attention_rows_back(
            grad_middle.astype(BF), mats_all, layer, cos_part, sin_part, key_at, query_at, queries, keys, values, peaks, sums, nz
        )
        through, grad_attn_gain = norm_back(hidden, attn_gain, grad_normed)
        grad = grad_middle + through

        layer_args[layer] = [
            part.reshape(group_rows, -1)
            for part in (normed_all, d_proj, middle_all, attended, moe_all, d_gate, d_up, grad_all, inner)
        ]
        gain_grads[layer] = [grad_attn_gain, grad_moe_gain]

    extra = jnp.stack([part for pair in gain_grads for part in pair])
    extra = extra.reshape(2 * LAYERS, nctx, nfs // NCORE, NCORE, rows).transpose(3, 2, 1, 0, 4)
    extra = jnp.pad(extra, ((0, 0), (0, 0), (0, 0), (0, 8 - 2 * LAYERS), (0, 128 - rows)))
    collected, gains_in = collect_grads(nctx, nfs, layer_args, extra)

    def attn_part(low, high):
        return jnp.stack(
            [
                c[:, 0, :, low:high].transpose(1, 0, 2).reshape(rows, -1).astype(F32)
                for c in collected
            ]
        )

    def expert_part(first):
        return jnp.stack(
            [
                c[:, first : first + 2].reshape((EXPERTS,) + c.shape[2:]).astype(F32)
                for c in collected
            ]
        )

    def gain_part(kind):
        return jnp.stack([jnp.sum(gains_in[:, 2 * layer + kind, :rows], axis=0) for layer in range(LAYERS)])

    return (
        output[None],
        grad[None],
        attn_part(0, kv_at),
        attn_part(kv_at, v_at),
        attn_part(v_at, o_at),
        attn_part(o_at, o_at + q_width),
        gain_part(0),
        gain_part(1),
        expert_part(1),
        expert_part(3),
        expert_part(5),
    )


def solution(mesh):
    placed = (
        P("fsdp", "ctx", None),
        P("fsdp", "ctx", None),
        P("fsdp", None),
        P("fsdp", None),
        P(None, "fsdp", "ctx", None),
        P(None, "fsdp", "ctx", None),
        P(None, ("ctx", "fsdp"), None),
        P(None, ("ctx", "fsdp"), None),
        P(None, ("ctx", "fsdp"), None),
        P(None, ("ctx", "fsdp"), None),
        P(None, ("ctx", "fsdp")),
        P(None, ("ctx", "fsdp")),
        P(None, None, ("ctx", "fsdp"), None),
        P(None, None, ("ctx", "fsdp"), None),
        P(None, None, ("ctx", "fsdp"), None),
    )
    nctx, nfs = mesh.shape["ctx"], mesh.shape["fsdp"]
    chosen = partial(fast_body, nctx, nfs) if (nctx, nfs) == (8, 4) else body
    return jax.shard_map(
        chosen,
        mesh=mesh,
        in_specs=placed,
        out_specs=(
            P("fsdp", "ctx", None),
            P("fsdp", "ctx", None),
            P(None, ("ctx", "fsdp"), None),
            P(None, ("ctx", "fsdp"), None),
            P(None, ("ctx", "fsdp"), None),
            P(None, ("ctx", "fsdp"), None),
            P(None, ("ctx", "fsdp")),
            P(None, ("ctx", "fsdp")),
            P(None, None, ("ctx", "fsdp"), None),
            P(None, None, ("ctx", "fsdp"), None),
            P(None, None, ("ctx", "fsdp"), None),
        ),
        check_vma=False,
    )
```

```python
from functools import partial
import functools
import math

import jax
import jax.numpy as jnp
from jax import lax
from jax.experimental import pallas as pl
from jax.experimental.pallas import tpu as pltpu
from jax.sharding import PartitionSpec as P

HEAD_DIM = 64
EXPERTS = 16
LAYERS = 2
TILE = 128
CAP = 80


EPSILON = 1e-06
NEGATIVE = -1e30


def layout(lengths, tile_order, group_rows):
    tile_count = tile_order.shape[0]
    row_ids = jnp.arange(group_rows, dtype=jnp.int32)
    in_tile = (row_ids // TILE)[:, None] == jnp.arange(tile_count, dtype=jnp.int32)[None, :]
    tile_of = jnp.sum(jnp.where(in_tile, tile_order[None, :], 0), axis=1, dtype=jnp.int32)
    anchor = tile_of * TILE + row_ids % TILE
    seq_ends = jnp.cumsum(lengths, dtype=jnp.int32)
    seq_starts = seq_ends - lengths
    segment = jnp.sum(
        (anchor[:, None] >= seq_ends[None, :]).astype(jnp.int32), axis=1, dtype=jnp.int32
    )
    picked = segment[:, None] == jnp.arange(lengths.shape[0], dtype=jnp.int32)[None, :]
    offset = jnp.sum(jnp.where(picked, seq_starts[None, :], 0), axis=1, dtype=jnp.int32)
    return (segment, anchor - offset)


def rms_norm(values, gain_vec):
    return (
        values * lax.rsqrt(jnp.mean(values * values, axis=-1, keepdims=True) + EPSILON) * gain_vec
    )


def rotate(values, places):
    half_dim = values.shape[-1] // 2
    freq_steps = jnp.arange(half_dim, dtype=jnp.float32)
    inverse = jnp.exp(freq_steps * (-2.0 * math.log(10000.0) / values.shape[-1]))
    angles = places[:, None] * inverse[None, :]
    cos_part = jnp.cos(angles)[:, None, :]
    sin_part = jnp.sin(angles)[:, None, :]
    first_half = values[..., :half_dim]
    second_half = values[..., half_dim:]
    return jnp.concatenate(
        [
            first_half * cos_part - second_half * sin_part,
            second_half * cos_part + first_half * sin_part,
        ],
        axis=-1,
    )


def rotate_back(grads_in, places):
    return jax.vjp(partial(rotate, places=places), jnp.zeros(grads_in.shape, jnp.float32))[1](
        grads_in
    )[0]


def mix_inner(gate_act, up_act):
    return jax.nn.silu(gate_act) * up_act


def split_halves(master):
    experts_here, rows_here, hidden_units = master.shape
    return (
        master.astype(jnp.bfloat16)
        .reshape(experts_here, rows_here, 2, hidden_units // 2)
        .transpose(0, 2, 1, 3)
        .reshape(2 * experts_here, rows_here, hidden_units // 2)
    )


def merge_halves(grads_in):
    halves_all, rows_here, half_units = grads_in.shape
    return (
        grads_in.reshape(halves_all // 2, 2, rows_here, half_units)
        .transpose(0, 2, 1, 3)
        .reshape(halves_all // 2, rows_here, 2 * half_units)
    )


def doubled(slots):
    return jnp.broadcast_to(slots[:, None], (slots.shape[0], 2) + slots.shape[1:]).reshape(
        (2 * slots.shape[0],) + slots.shape[1:]
    )


def fold_halves(parts):
    return jnp.sum(parts.reshape((parts.shape[0] // 2, 2) + parts.shape[1:]), axis=1)


def send_out(slots):
    return lax.all_to_all(slots, "ctx", split_axis=0, concat_axis=1, tiled=True)


def send_back(parts):
    return lax.all_to_all(
        parts.astype(jnp.bfloat16), "ctx", split_axis=1, concat_axis=0, tiled=True
    ).astype(parts.dtype)


def routing(route_ids, gate_share, rows_here):
    expert_ids = jnp.arange(EXPERTS, dtype=jnp.int32)
    chosen = (route_ids[:, :, None] == expert_ids[None, None, :]).astype(jnp.int32)
    member = jnp.sum(chosen, axis=1, dtype=jnp.int32)
    before = jnp.cumsum(member, axis=0, dtype=jnp.int32) - member
    rank_of = jnp.sum(chosen * before[:, None, :], axis=2, dtype=jnp.int32)
    slot_of = route_ids * CAP + rank_of
    token_ids = jnp.broadcast_to(jnp.arange(rows_here, dtype=jnp.int32)[:, None], route_ids.shape)
    flat_slots = slot_of.reshape(-1)
    slot_token = (
        jnp.full((EXPERTS * CAP,), rows_here, jnp.int32).at[flat_slots].set(token_ids.reshape(-1))
    )
    slot_share = jnp.zeros((EXPERTS * CAP,), jnp.float32).at[flat_slots].set(gate_share.reshape(-1))
    return (slot_of, slot_token, slot_share)


def key_block(key_rows, value_rows, token_meta, block_index, block_rows):
    seg_local, pos_local, seg_all, pos_all = token_meta
    first_row = block_index * block_rows
    key_part = lax.dynamic_slice_in_dim(key_rows, first_row, block_rows, 0)
    value_part = lax.dynamic_slice_in_dim(value_rows, first_row, block_rows, 0)
    seg_part = lax.dynamic_slice_in_dim(seg_all, first_row, block_rows, 0)
    pos_part = lax.dynamic_slice_in_dim(pos_all, first_row, block_rows, 0)
    visible = (seg_local[:, None] == seg_part[None, :]) & (pos_part[None, :] <= pos_local[:, None])
    return (key_part, value_part, visible)


def scores(queries, key_part, visible, score_scale):
    raw_scores = (
        jnp.einsum("qhgd,khd->hgqk", queries, key_part, preferred_element_type=jnp.float32)
        * score_scale
    )
    return jnp.where(visible[None, None], raw_scores, NEGATIVE)


def keep_same(running):
    return running


def attention_forward(queries, key_rows, value_rows, token_meta, block_rows, score_scale):
    block_count = key_rows.shape[0] // block_rows
    rows_here, heads_kv, groups = (queries.shape[0], queries.shape[1], queries.shape[2])

    def stat_step(block_index, running):
        key_part, value_part, visible = key_block(
            key_rows, value_rows, token_meta, block_index, block_rows
        )

        def stat_update(current):
            row_peak, denom_sum = current
            logits = scores(queries, key_part, visible, score_scale)
            new_peak = jnp.maximum(row_peak, jnp.max(logits, axis=-1))
            denom_sum = denom_sum * jnp.exp(row_peak - new_peak) + jnp.sum(
                jnp.exp(logits - new_peak[..., None]), axis=-1
            )
            return (new_peak, denom_sum)

        return lax.cond(jnp.any(visible), stat_update, keep_same, running)

    start_stats = (
        jnp.full((heads_kv, groups, rows_here), NEGATIVE, jnp.float32),
        jnp.zeros((heads_kv, groups, rows_here), jnp.float32),
    )
    row_peak, denom_sum = lax.fori_loop(0, block_count, stat_step, start_stats)

    def out_step(block_index, partial_sum):
        key_part, value_part, visible = key_block(
            key_rows, value_rows, token_meta, block_index, block_rows
        )

        def out_update(current):
            attn_probs = (
                jnp.exp(scores(queries, key_part, visible, score_scale) - row_peak[..., None])
                / denom_sum[..., None]
            )
            return current + jnp.einsum(
                "hgqk,khd->qhgd",
                attn_probs.astype(jnp.bfloat16),
                value_part,
                preferred_element_type=jnp.float32,
            )

        return lax.cond(jnp.any(visible), out_update, keep_same, partial_sum)

    attended = lax.fori_loop(
        0, block_count, out_step, jnp.zeros((rows_here, heads_kv, groups, HEAD_DIM), jnp.float32)
    )
    return ((row_peak, denom_sum), attended)


def attention_backward(
    queries, key_rows, value_rows, token_meta, softmax_stats, grad_attended, block_rows, score_scale
):
    row_peak, denom_sum = softmax_stats
    block_count = key_rows.shape[0] // block_rows

    def probs_for(key_part, visible):
        return (
            jnp.exp(scores(queries, key_part, visible, score_scale) - row_peak[..., None])
            / denom_sum[..., None]
        )

    def delta_step(block_index, partial_sum):
        key_part, value_part, visible = key_block(
            key_rows, value_rows, token_meta, block_index, block_rows
        )

        def delta_update(current):
            attn_probs = probs_for(key_part, visible)
            grad_probs = jnp.einsum(
                "qhgd,khd->hgqk", grad_attended, value_part, preferred_element_type=jnp.float32
            )
            return current + jnp.sum(attn_probs * grad_probs, axis=-1)

        return lax.cond(jnp.any(visible), delta_update, keep_same, partial_sum)

    delta_sum = lax.fori_loop(0, block_count, delta_step, jnp.zeros(denom_sum.shape, jnp.float32))

    def grad_step(block_index, running):
        key_part, value_part, visible = key_block(
            key_rows, value_rows, token_meta, block_index, block_rows
        )
        first_row = block_index * block_rows

        def grad_update(current):
            grad_queries, grad_keys, grad_values = current
            attn_probs = probs_for(key_part, visible)
            grad_probs = jnp.einsum(
                "qhgd,khd->hgqk", grad_attended, value_part, preferred_element_type=jnp.float32
            )
            grad_scores = (attn_probs * (grad_probs - delta_sum[..., None])).astype(jnp.bfloat16)
            grad_queries = grad_queries + jnp.einsum(
                "hgqk,khd->qhgd", grad_scores, key_part, preferred_element_type=jnp.float32
            )
            key_term = jnp.einsum(
                "hgqk,qhgd->khd", grad_scores, queries, preferred_element_type=jnp.float32
            )
            value_term = jnp.einsum(
                "hgqk,qhgd->khd",
                attn_probs.astype(jnp.bfloat16),
                grad_attended,
                preferred_element_type=jnp.float32,
            )
            grad_keys = lax.dynamic_update_slice_in_dim(
                grad_keys,
                lax.dynamic_slice_in_dim(grad_keys, first_row, block_rows, 0) + key_term,
                first_row,
                0,
            )
            grad_values = lax.dynamic_update_slice_in_dim(
                grad_values,
                lax.dynamic_slice_in_dim(grad_values, first_row, block_rows, 0) + value_term,
                first_row,
                0,
            )
            return (grad_queries, grad_keys, grad_values)

        return lax.cond(jnp.any(visible), grad_update, keep_same, running)

    start_grads = (
        jnp.zeros(queries.shape, jnp.float32),
        jnp.zeros(key_rows.shape, jnp.float32),
        jnp.zeros(value_rows.shape, jnp.float32),
    )
    return lax.fori_loop(0, block_count, grad_step, start_grads)


def fetch_layer(master_set, layer_index):
    (
        query_weight,
        key_weight,
        value_weight,
        out_weight,
        attn_gain,
        moe_gain,
        gate_weight,
        up_weight,
        down_weight,
    ) = master_set
    attn_set = (
        lax.all_gather(
            query_weight[layer_index].astype(jnp.bfloat16), ("ctx", "fsdp"), axis=0, tiled=True
        ),
        lax.all_gather(
            key_weight[layer_index].astype(jnp.bfloat16), ("ctx", "fsdp"), axis=0, tiled=True
        ),
        lax.all_gather(
            value_weight[layer_index].astype(jnp.bfloat16), ("ctx", "fsdp"), axis=0, tiled=True
        ),
        lax.all_gather(
            out_weight[layer_index].astype(jnp.bfloat16), ("ctx", "fsdp"), axis=0, tiled=True
        ),
        lax.all_gather(
            attn_gain[layer_index].astype(jnp.bfloat16), ("ctx", "fsdp"), axis=0, tiled=True
        ),
        lax.all_gather(
            moe_gain[layer_index].astype(jnp.bfloat16), ("ctx", "fsdp"), axis=0, tiled=True
        ),
    )
    row_set = (
        lax.all_gather(split_halves(gate_weight[layer_index]), "fsdp", axis=1, tiled=True),
        lax.all_gather(split_halves(up_weight[layer_index]), "fsdp", axis=1, tiled=True),
        lax.all_gather(split_halves(down_weight[layer_index]), "fsdp", axis=1, tiled=True),
    )
    expert_set = (
        lax.all_to_all(row_set[0], "ctx", split_axis=0, concat_axis=1, tiled=True),
        lax.all_to_all(row_set[1], "ctx", split_axis=0, concat_axis=1, tiled=True),
        lax.all_to_all(row_set[2], "ctx", split_axis=0, concat_axis=1, tiled=True),
    )
    return tuple(attn_set) + tuple(expert_set)


def layer_forward(hidden, weights, route_ids, gate_share, token_meta, places, block_rows):
    (
        query_full,
        key_full,
        value_full,
        out_full,
        attn_norm,
        moe_norm,
        gate_full,
        up_full,
        down_full,
    ) = weights
    rows_here, model_width = hidden.shape
    heads_all = query_full.shape[1] // HEAD_DIM
    heads_kv = key_full.shape[1] // HEAD_DIM
    groups = heads_all // heads_kv
    score_scale = HEAD_DIM ** (-0.5)
    normed = rms_norm(hidden, attn_norm.astype(jnp.float32)).astype(jnp.bfloat16)
    queries = rotate(
        jnp.dot(normed, query_full, preferred_element_type=jnp.float32).reshape(
            rows_here, heads_all, HEAD_DIM
        ),
        places,
    ).astype(jnp.bfloat16)
    key_new = (
        rotate(
            jnp.dot(normed, key_full, preferred_element_type=jnp.float32).reshape(
                rows_here, heads_kv, HEAD_DIM
            ),
            places,
        )
        .astype(jnp.bfloat16)
        .reshape(rows_here, heads_kv * HEAD_DIM)
    )
    value_new = jnp.dot(normed, value_full, preferred_element_type=jnp.float32).astype(jnp.bfloat16)
    key_rows, value_rows = (
        lax.all_gather(key_new, "ctx", axis=0, tiled=True),
        lax.all_gather(value_new, "ctx", axis=0, tiled=True),
    )
    key_rows = key_rows.reshape(-1, heads_kv, HEAD_DIM)
    value_rows = value_rows.reshape(-1, heads_kv, HEAD_DIM)
    queries = queries.reshape(rows_here, heads_kv, groups, HEAD_DIM)
    softmax_stats, attended = attention_forward(
        queries, key_rows, value_rows, token_meta, block_rows, score_scale
    )
    attended = attended.reshape(rows_here, heads_all * HEAD_DIM).astype(jnp.bfloat16)
    middle = hidden + jnp.einsum(
        "tx,dx->td", attended, out_full, preferred_element_type=jnp.float32
    )
    moe_in = rms_norm(middle, moe_norm.astype(jnp.float32)).astype(jnp.bfloat16)
    slot_of, slot_token, slot_share = routing(route_ids, gate_share, rows_here)
    padded = jnp.concatenate([moe_in, jnp.zeros((1, model_width), jnp.bfloat16)], axis=0)
    dispatched = jnp.take(padded, slot_token, axis=0).reshape(EXPERTS, CAP, model_width)
    owner_rows = send_out(doubled(dispatched))
    gate_act = jnp.einsum("ecd,edf->ecf", owner_rows, gate_full, preferred_element_type=jnp.float32)
    up_act = jnp.einsum("ecd,edf->ecf", owner_rows, up_full, preferred_element_type=jnp.float32)
    inner_act = mix_inner(gate_act, up_act).astype(jnp.bfloat16)
    expert_part = jnp.einsum(
        "ecf,edf->ecd", inner_act, down_full, preferred_element_type=jnp.float32
    )
    expert_out = fold_halves(send_back(expert_part))
    expert_out = expert_out.reshape(EXPERTS * CAP, model_width)
    moe_out = jnp.sum(jnp.take(expert_out, slot_of, axis=0) * gate_share[..., None], axis=1)
    record = (
        hidden,
        normed,
        queries,
        key_rows,
        value_rows,
        softmax_stats,
        attended,
        middle,
        moe_in,
        slot_of,
        slot_token,
        slot_share,
        owner_rows,
        gate_act,
        up_act,
        inner_act,
    )
    return (record, middle + moe_out)


def layer_backward(grad_hidden, record, weights, token_meta, places, block_rows):
    (
        hidden,
        normed,
        queries,
        key_rows,
        value_rows,
        softmax_stats,
        attended,
        middle,
        moe_in,
        slot_of,
        slot_token,
        slot_share,
        owner_rows,
        gate_act,
        up_act,
        inner_act,
    ) = record
    (
        query_full,
        key_full,
        value_full,
        out_full,
        attn_norm,
        moe_norm,
        gate_full,
        up_full,
        down_full,
    ) = weights
    rows_here, model_width = hidden.shape
    heads_kv, groups = (queries.shape[1], queries.shape[2])
    group_rows = key_rows.shape[0]
    score_scale = HEAD_DIM ** (-0.5)
    grad_padded = jnp.concatenate([grad_hidden, jnp.zeros((1, model_width), jnp.float32)], axis=0)
    grad_expert = (
        (jnp.take(grad_padded, slot_token, axis=0) * slot_share[:, None])
        .astype(jnp.bfloat16)
        .reshape(EXPERTS, CAP, model_width)
    )
    grad_owner = send_out(doubled(grad_expert))
    grad_down = jnp.einsum(
        "ecd,ecf->edf", grad_owner, inner_act, preferred_element_type=jnp.float32
    )
    grad_inner = jnp.einsum(
        "ecd,edf->ecf", grad_owner, down_full, preferred_element_type=jnp.float32
    )
    grad_gate_act, grad_up_act = jax.vjp(mix_inner, gate_act, up_act)[1](grad_inner)
    grad_gate_act = grad_gate_act.astype(jnp.bfloat16)
    grad_up_act = grad_up_act.astype(jnp.bfloat16)
    grad_gate = jnp.einsum(
        "ecd,ecf->edf", owner_rows, grad_gate_act, preferred_element_type=jnp.float32
    )
    grad_up = jnp.einsum(
        "ecd,ecf->edf", owner_rows, grad_up_act, preferred_element_type=jnp.float32
    )
    grad_owner_rows = jnp.einsum(
        "ecf,edf->ecd", grad_gate_act, gate_full, preferred_element_type=jnp.float32
    ) + jnp.einsum("ecf,edf->ecd", grad_up_act, up_full, preferred_element_type=jnp.float32)
    grad_dispatched = fold_halves(send_back(grad_owner_rows))
    home_set = (
        lax.all_to_all(
            grad_gate.astype(jnp.bfloat16), "ctx", split_axis=1, concat_axis=0, tiled=True
        ).astype(grad_gate.dtype),
        lax.all_to_all(
            grad_up.astype(jnp.bfloat16), "ctx", split_axis=1, concat_axis=0, tiled=True
        ).astype(grad_up.dtype),
        lax.all_to_all(
            grad_down.astype(jnp.bfloat16), "ctx", split_axis=1, concat_axis=0, tiled=True
        ).astype(grad_down.dtype),
    )
    summed_set = (
        lax.psum_scatter(
            home_set[0].astype(jnp.bfloat16), "fsdp", scatter_dimension=1, tiled=True
        ).astype(jnp.float32),
        lax.psum_scatter(
            home_set[1].astype(jnp.bfloat16), "fsdp", scatter_dimension=1, tiled=True
        ).astype(jnp.float32),
        lax.psum_scatter(
            home_set[2].astype(jnp.bfloat16), "fsdp", scatter_dimension=1, tiled=True
        ).astype(jnp.float32),
    )
    expert_grads = (
        merge_halves(summed_set[0]),
        merge_halves(summed_set[1]),
        merge_halves(summed_set[2]),
    )
    grad_moe_in = jnp.sum(
        jnp.take(grad_dispatched.reshape(EXPERTS * CAP, model_width), slot_of, axis=0), axis=1
    )
    grad_middle_part, grad_moe_norm = jax.vjp(rms_norm, middle, moe_norm.astype(jnp.float32))[1](
        grad_moe_in
    )
    grad_middle = grad_hidden + grad_middle_part
    grad_rounded = grad_middle.astype(jnp.bfloat16)
    grad_out_full = jnp.einsum(
        "td,tx->dx", grad_rounded, attended, preferred_element_type=jnp.float32
    )
    grad_attended = (
        jnp.dot(grad_rounded, out_full, preferred_element_type=jnp.float32)
        .astype(jnp.bfloat16)
        .reshape(rows_here, heads_kv, groups, HEAD_DIM)
    )
    grad_queries, grad_keys, grad_values = attention_backward(
        queries,
        key_rows,
        value_rows,
        token_meta,
        softmax_stats,
        grad_attended,
        block_rows,
        score_scale,
    )
    key_sums, value_sums = (
        lax.psum_scatter(
            grad_keys.reshape(group_rows, heads_kv * HEAD_DIM).astype(jnp.bfloat16),
            "ctx",
            scatter_dimension=0,
            tiled=True,
        ).astype(jnp.float32),
        lax.psum_scatter(
            grad_values.reshape(group_rows, heads_kv * HEAD_DIM).astype(jnp.bfloat16),
            "ctx",
            scatter_dimension=0,
            tiled=True,
        ).astype(jnp.float32),
    )
    grad_query_rows = (
        rotate_back(
            grad_queries.reshape(rows_here, heads_kv * groups, HEAD_DIM) * score_scale, places
        )
        .astype(jnp.bfloat16)
        .reshape(rows_here, heads_kv * groups * HEAD_DIM)
    )
    grad_key_rows = (
        rotate_back(key_sums.reshape(rows_here, heads_kv, HEAD_DIM) * score_scale, places)
        .astype(jnp.bfloat16)
        .reshape(rows_here, heads_kv * HEAD_DIM)
    )
    grad_value_rows = value_sums.astype(jnp.bfloat16)
    grad_query_full = jnp.einsum(
        "td,tx->dx", normed, grad_query_rows, preferred_element_type=jnp.float32
    )
    grad_key_full = jnp.einsum(
        "td,tx->dx", normed, grad_key_rows, preferred_element_type=jnp.float32
    )
    grad_value_full = jnp.einsum(
        "td,tx->dx", normed, grad_value_rows, preferred_element_type=jnp.float32
    )
    grad_normed = jnp.einsum(
        "tx,dx->td", grad_query_rows, query_full, preferred_element_type=jnp.float32
    )
    grad_normed = grad_normed + jnp.einsum(
        "tx,dx->td", grad_key_rows, key_full, preferred_element_type=jnp.float32
    )
    grad_normed = grad_normed + jnp.einsum(
        "tx,dx->td", grad_value_rows, value_full, preferred_element_type=jnp.float32
    )
    grad_hidden_part, grad_attn_norm = jax.vjp(rms_norm, hidden, attn_norm.astype(jnp.float32))[1](
        grad_normed
    )
    attn_grads = (
        lax.psum_scatter(grad_query_full, ("ctx", "fsdp"), scatter_dimension=0, tiled=True),
        lax.psum_scatter(grad_key_full, ("ctx", "fsdp"), scatter_dimension=0, tiled=True),
        lax.psum_scatter(grad_value_full, ("ctx", "fsdp"), scatter_dimension=0, tiled=True),
        lax.psum_scatter(grad_out_full, ("ctx", "fsdp"), scatter_dimension=0, tiled=True),
        lax.psum_scatter(grad_attn_norm, ("ctx", "fsdp"), scatter_dimension=0, tiled=True),
        lax.psum_scatter(grad_moe_norm, ("ctx", "fsdp"), scatter_dimension=0, tiled=True),
    )
    return (grad_middle + grad_hidden_part, attn_grads, expert_grads)


def body(
    tokens,
    cotangent,
    lengths,
    tile_order,
    routes,
    gates,
    query_weight,
    key_weight,
    value_weight,
    out_weight,
    attn_gain,
    moe_gain,
    gate_weight,
    up_weight,
    down_weight,
):
    rows_here = tokens.shape[1]
    group_rows = rows_here * lax.axis_size("ctx")
    seg_all, pos_all = layout(lengths[0], tile_order[0], group_rows)
    first_row = lax.axis_index("ctx") * rows_here
    seg_local = lax.dynamic_slice_in_dim(seg_all, first_row, rows_here, 0)
    pos_local = lax.dynamic_slice_in_dim(pos_all, first_row, rows_here, 0)
    token_meta = (seg_local, pos_local, seg_all, pos_all)
    places = pos_local.astype(jnp.float32)
    block_rows = math.gcd(group_rows, 512)
    master_set = (
        query_weight,
        key_weight,
        value_weight,
        out_weight,
        attn_gain,
        moe_gain,
        gate_weight,
        up_weight,
        down_weight,
    )
    hidden = tokens[0].astype(jnp.float32)
    records = []
    for layer_index in range(LAYERS):
        weights = fetch_layer(master_set, layer_index)
        record, hidden = layer_forward(
            hidden,
            weights,
            routes[layer_index, 0],
            gates[layer_index, 0],
            token_meta,
            places,
            block_rows,
        )
        records.append(record)
    grad_hidden = cotangent[0].astype(jnp.float32)
    attn_layers = []
    expert_layers = []
    for layer_index in reversed(range(LAYERS)):
        weights = fetch_layer(master_set, layer_index)
        grad_hidden, attn_grads, expert_grads = layer_backward(
            grad_hidden, records[layer_index], weights, token_meta, places, block_rows
        )
        attn_layers.insert(0, attn_grads)
        expert_layers.insert(0, expert_grads)
    grad_query_weight = jnp.stack([layer_grads[0] for layer_grads in attn_layers])
    grad_key_weight = jnp.stack([layer_grads[1] for layer_grads in attn_layers])
    grad_value_weight = jnp.stack([layer_grads[2] for layer_grads in attn_layers])
    grad_out_weight = jnp.stack([layer_grads[3] for layer_grads in attn_layers])
    grad_attn_gain = jnp.stack([layer_grads[4] for layer_grads in attn_layers])
    grad_moe_gain = jnp.stack([layer_grads[5] for layer_grads in attn_layers])
    grad_gate_weight = jnp.stack([layer_grads[0] for layer_grads in expert_layers])
    grad_up_weight = jnp.stack([layer_grads[1] for layer_grads in expert_layers])
    grad_down_weight = jnp.stack([layer_grads[2] for layer_grads in expert_layers])
    return (
        hidden.astype(jnp.bfloat16)[None],
        grad_hidden[None],
        grad_query_weight,
        grad_key_weight,
        grad_value_weight,
        grad_out_weight,
        grad_attn_gain,
        grad_moe_gain,
        grad_gate_weight,
        grad_up_weight,
        grad_down_weight,
    )


BF = jnp.bfloat16
F32 = jnp.float32
NX = 2
NCORE = 2
ANY = pl.BlockSpec(memory_space=pl.ANY)
VM = pl.BlockSpec(memory_space=pltpu.VMEM)
DMA = pltpu.SemaphoreType.DMA

NN = ((1,), (0,))
NT = ((1,), (1,))
TN = ((0,), (0,))


def dot(left, right, dims):
    return lax.dot_general(left, right, (dims, ((), ())), preferred_element_type=jnp.float32)


def remote(src, dst, send_sem, recv_sem, ctx, fsdp):
    return pltpu.make_async_remote_copy(
        src_ref=src,
        dst_ref=dst,
        send_sem=send_sem,
        recv_sem=recv_sem,
        device_id={"ctx": ctx, "fsdp": fsdp},
        device_id_type=pl.DeviceIdType.MESH,
    )


def greet(barrier, ctx, fsdp):
    pl.semaphore_signal(
        barrier, inc=1, device_id={"ctx": ctx, "fsdp": fsdp}, device_id_type=pl.DeviceIdType.MESH
    )


class Line:
    def __init__(self, nz):
        self.nz = nz
        self.ctx, self.fsdp = lax.axis_index("ctx"), lax.axis_index("fsdp")
        self.z, self.x = self.ctx // NX, self.ctx % NX
        self.mate = self.z * NX + 1 - self.x
        self.above = (self.z + 1) * NX + self.x
        self.below = (self.z - 1) * NX + self.x

    def greet(self, others=()):
        barrier = pltpu.get_barrier_semaphore()
        greet(barrier, self.mate, self.fsdp)
        for other in others:
            greet(barrier, self.ctx, other)

        @pl.when(self.z > 0)
        def _():
            greet(barrier, self.below, self.fsdp)

        @pl.when(self.z < self.nz - 1)
        def _():
            greet(barrier, self.above, self.fsdp)

        ends = jnp.where(self.z > 0, 1, 0) + jnp.where(self.z < self.nz - 1, 1, 0)
        pl.semaphore_wait(barrier, 1 + len(others) + ends)

    def near(self, i):
        z, nz = self.z, self.nz
        mid1 = jnp.where(i == 0, 1, jnp.where(i == 1, 0, i))
        mid2 = jnp.where(i == 0, 2, jnp.where(i == 1, 1, jnp.where(i == 2, 3, 0)))
        return jnp.where(z == 0, i, jnp.where(z == nz - 1, nz - 1 - i, jnp.where(z == 1, mid1, mid2)))

    def far(self, i):
        z, nz = self.z, self.nz
        mid1 = jnp.where(i == 0, 3, jnp.where(i == 1, 0, jnp.where(i == 2, 2, 1)))
        mid2 = jnp.where(i == 0, 0, jnp.where(i == 1, 3, jnp.where(i == 2, 1, 2)))
        return jnp.where(z == 0, nz - 1 - i, jnp.where(z == nz - 1, i, jnp.where(z == 1, mid1, mid2)))


EXTRA = 16


class Gather:
    @staticmethod
    def scratch(nz):
        return [DMA((10, nz))]

    def __init__(self, line, own_ref, all_ref, sems):
        self.line, self.own, self.all, self.sems = line, own_ref, all_ref, sems
        self.main = own_ref.shape[0] - EXTRA

    def block(self, row, column=None):
        column = self.line.x if column is None else column
        return self.all.at[row * NX + column, pl.ds(0, self.main)]

    def extras(self, row):
        return self.all.at[pl.ds(row * NX, NX), pl.ds(self.main, EXTRA)]

    def own_main(self):
        return self.own.at[pl.ds(0, self.main)]

    def move(self, kind, t, src, dst, ctx):
        return remote(src, dst, self.sems.at[kind, t], self.sems.at[kind + 1, t], ctx, self.line.fsdp)

    def up(self, t, src=None):
        block = self.block(self.line.z - t)
        return self.move(0, t, block if src is None else src, block, self.line.above)

    def down(self, t, src=None):
        block = self.block(self.line.z + t)
        return self.move(2, t, block if src is None else src, block, self.line.below)

    def across(self, row, src=None):
        block = self.block(row)
        return self.move(4, row, block if src is None else src, block, self.line.mate)

    def extra_up(self, t):
        return self.move(6, t, self.extras(self.line.z - t), self.extras(self.line.z - t), self.line.above)

    def extra_down(self, t):
        return self.move(8, t, self.extras(self.line.z + t), self.extras(self.line.z + t), self.line.below)

    def extra_across(self, column):
        own = self.own.at[pl.ds(self.main, EXTRA)]
        there = self.all.at[self.line.z * NX + column, pl.ds(self.main, EXTRA)]
        last = self.line.nz - 1
        return remote(own, there, self.sems.at[6, last], self.sems.at[7, last], self.line.mate, self.line.fsdp)

    def start(self):
        line = self.line
        self.extra_across(line.x).start()

        @pl.when(line.z < line.nz - 1)
        def _():
            self.up(0, self.own_main()).start()

        @pl.when(line.z > 0)
        def _():
            self.down(0, self.own_main()).start()

        self.across(line.z, self.own_main()).start()

    def start_extras(self):
        line = self.line
        self.extra_across(1 - line.x).wait_recv()

        @pl.when(line.z < line.nz - 1)
        def _():
            self.extra_up(0).start()

        @pl.when(line.z > 0)
        def _():
            self.extra_down(0).start()

    def forward(self, t):
        line = self.line

        @pl.when(line.z - 1 - t >= 0)
        def _():
            row = line.z - 1 - t
            self.move(0, t, self.own_main(), self.block(row), line.above).wait_recv()

            @pl.when(line.z < line.nz - 1)
            def _():
                self.up(t + 1).start()

            self.across(row).start()
            self.move(6, t, self.extras(row), self.extras(row), line.above).wait_recv()

            @pl.when(line.z < line.nz - 1)
            def _():
                self.extra_up(t + 1).start()

        @pl.when(line.z + 1 + t < line.nz)
        def _():
            row = line.z + 1 + t
            self.move(2, t, self.own_main(), self.block(row), line.below).wait_recv()

            @pl.when(line.z > 0)
            def _():
                self.down(t + 1).start()

            self.across(row).start()
            self.move(8, t, self.extras(row), self.extras(row), line.below).wait_recv()

            @pl.when(line.z > 0)
            def _():
                self.extra_down(t + 1).start()

    def wait_pair(self, row):
        self.move(4, row, self.own_main(), self.block(row, 1 - self.line.x), self.line.mate).wait_recv()

    def finish(self):
        line = self.line
        self.extra_across(line.x).wait_send()
        for t in range(line.nz - 1):

            @pl.when((line.z - t >= 0) & (line.z < line.nz - 1))
            def _():
                self.up(t).wait_send()
                self.extra_up(t).wait_send()

            @pl.when((line.z + t < line.nz) & (line.z > 0))
            def _():
                self.down(t).wait_send()
                self.extra_down(t).wait_send()

        for row in range(line.nz):
            self.across(row).wait_send()


class Scatter:
    @staticmethod
    def scratch(nz, rows, width):
        return [
            pltpu.VMEM((4, nz, rows - EXTRA, width), BF),
            pltpu.VMEM((4, nz, NX, EXTRA, width), BF),
            DMA((10, nz)),
            DMA((2,)),
        ]

    def __init__(self, line, part_ref, out_ref, work, extra, sems, mate_sems):
        self.line, self.part, self.out, self.sems, self.mate_sems = line, part_ref, out_ref, sems, mate_sems
        self.xin, self.acc, self.upin, self.downin = (work.at[i] for i in range(4))
        self.eacc, self.eup, self.edown, self.emate = (extra.at[i] for i in range(4))
        self.main = part_ref.shape[1] - EXTRA

    def move(self, kind, row, src, dst, ctx):
        return remote(src, dst, self.sems.at[kind, row], self.sems.at[kind + 1, row], ctx, self.line.fsdp)

    def across(self, row):
        mates = self.part.at[row * NX + 1 - self.line.x, pl.ds(0, self.main)]
        return self.move(0, row, mates, self.xin.at[row], self.line.mate)

    def up(self, row):
        return self.move(2, row, self.acc.at[row], self.upin.at[row], self.line.above)

    def down(self, row):
        return self.move(4, row, self.acc.at[row], self.downin.at[row], self.line.below)

    def extra_up(self, row):
        return self.move(6, row, self.eacc.at[row], self.eup.at[row], self.line.above)

    def extra_down(self, row):
        return self.move(8, row, self.eacc.at[row], self.edown.at[row], self.line.below)

    def extra_across(self):
        return remote(
            self.emate.at[0, 0], self.emate.at[1, 0], self.mate_sems.at[0], self.mate_sems.at[1], self.line.mate, self.line.fsdp
        )

    def extras(self, row):
        return self.part[pl.ds(row * NX, NX), pl.ds(self.main, EXTRA), :].astype(F32)

    def add(self, i):
        line = self.line
        row = line.far(i)

        @pl.when(row > line.z)
        def _():
            @pl.when(line.z == 0)
            def _():
                self.eacc[row] = self.extras(row).astype(BF)

            @pl.when(line.z > 0)
            def _():
                self.extra_up(row).wait_recv()
                self.eacc[row] = (self.extras(row) + self.eup[row].astype(F32)).astype(BF)

            self.extra_up(row).start()

        @pl.when(row < line.z)
        def _():
            @pl.when(line.z == line.nz - 1)
            def _():
                self.eacc[row] = self.extras(row).astype(BF)

            @pl.when(line.z < line.nz - 1)
            def _():
                self.extra_down(row).wait_recv()
                self.eacc[row] = (self.extras(row) + self.edown[row].astype(F32)).astype(BF)

            self.extra_down(row).start()

        self.across(row).wait_recv()
        mine = self.part[row * NX + line.x, 0 : self.main, :].astype(F32) + self.xin[row].astype(F32)

        @pl.when(row > line.z)
        def _():
            @pl.when(line.z == 0)
            def _():
                self.acc[row] = mine.astype(BF)

            @pl.when(line.z > 0)
            def _():
                self.up(row).wait_recv()
                self.acc[row] = (mine + self.upin[row].astype(F32)).astype(BF)

            self.up(row).start()

        @pl.when(row < line.z)
        def _():
            @pl.when(line.z == line.nz - 1)
            def _():
                self.acc[row] = mine.astype(BF)

            @pl.when(line.z < line.nz - 1)
            def _():
                self.down(row).wait_recv()
                self.acc[row] = (mine + self.downin[row].astype(F32)).astype(BF)

            self.down(row).start()

        @pl.when(row == line.z)
        def _():
            self.out[0 : self.main, :] = mine

    def extra_sum(self, column):
        at = self.line.z * NX + column
        return self.part[at, self.main : self.main + EXTRA, :].astype(F32)

    def finish(self):
        line = self.line
        self.out[self.main : self.main + EXTRA, :] = self.extra_sum(line.x)
        others = self.extra_sum(1 - line.x)

        def more(ref):
            self.out[self.main : self.main + EXTRA, :] += ref[line.z, line.x].astype(F32)

        @pl.when(line.z > 0)
        def _():
            self.extra_up(line.z).wait_recv()
            more(self.eup)

        @pl.when(line.z < line.nz - 1)
        def _():
            self.extra_down(line.z).wait_recv()
            more(self.edown)

        @pl.when(line.z == 0)
        def _():
            self.emate[0, 0] = (others + self.edown[line.z, 1 - line.x].astype(F32)).astype(BF)

        @pl.when(line.z == line.nz - 1)
        def _():
            self.emate[0, 0] = (others + self.eup[line.z, 1 - line.x].astype(F32)).astype(BF)

        @pl.when((line.z > 0) & (line.z < line.nz - 1))
        def _():
            self.emate[0, 0] = (
                others + self.eup[line.z, 1 - line.x].astype(F32) + self.edown[line.z, 1 - line.x].astype(F32)
            ).astype(BF)

        self.extra_across().start()

        @pl.when(line.z > 0)
        def _():
            self.up(line.z).wait_recv()
            self.out[0 : self.main, :] += self.upin[line.z].astype(F32)

        @pl.when(line.z < line.nz - 1)
        def _():
            self.down(line.z).wait_recv()
            self.out[0 : self.main, :] += self.downin[line.z].astype(F32)

        self.extra_across().wait_recv()
        self.out[self.main : self.main + EXTRA, :] += self.emate[1, 0].astype(F32)
        self.extra_across().wait_send()
        for row in range(line.nz):
            self.across(row).wait_send()

            @pl.when(row > line.z)
            def _():
                self.up(row).wait_send()
                self.extra_up(row).wait_send()

            @pl.when(row < line.z)
            def _():
                self.down(row).wait_send()
                self.extra_down(row).wait_send()


def normed_rows(values_ref, gain_ref):
    values = values_ref[...]
    scale = lax.rsqrt(jnp.mean(values * values, axis=1, keepdims=True) + EPSILON)
    return (values * scale * gain_ref[...]).astype(BF)


def norm_back_rows(grad_ref, values_ref, gain_ref, sums_ref, gain_out):
    values, sums = values_ref[...], sums_ref[...]
    scale = lax.rsqrt(jnp.mean(values * values, axis=1, keepdims=True) + EPSILON)
    unit = values * scale
    gain_out[...] = jnp.sum(sums * unit, axis=0, keepdims=True)
    pulled = sums * gain_ref[...]
    sums_ref[...] = grad_ref[...] + scale * (pulled - unit * jnp.mean(pulled * unit, axis=1, keepdims=True))


def params(collective, vmem_mib):
    return pltpu.CompilerParams(collective_id=collective, has_side_effects=True, vmem_limit_bytes=vmem_mib << 20)


def experts_kernel(nz, layer, x_ref, gain_ref, share_ref, mats_ref, o_ref, all_out, gate_out, up_out,
                   mats, blocks, part, gate, up, load_sem, save_sem, gsems, work, ework, ssems, msems):
    line = Line(nz)
    rows, width = x_ref.shape
    load = pltpu.make_async_copy(mats_ref.at[layer, pl.ds(1, 6)], mats, load_sem)
    load.start()
    blocks[line.ctx] = normed_rows(x_ref, gain_ref)
    line.greet()
    ring = Gather(line, blocks.at[line.ctx], blocks, gsems)
    ring.start()
    load.wait()
    ring.start_extras()

    def saves(row):
        pair = pl.ds(row * NX, NX)
        return (
            pltpu.make_async_copy(blocks.at[pair], all_out.at[pair], save_sem.at[0, row]),
            pltpu.make_async_copy(gate.at[pair], gate_out.at[pair], save_sem.at[1, row]),
            pltpu.make_async_copy(up.at[pair], up_out.at[pair], save_sem.at[2, row]),
        )

    def step(i, carry):
        @pl.when(i < nz - 1)
        def _():
            ring.forward(i)

        row = line.near(i)
        ring.wait_pair(row)
        pair = pl.ds(row * NX, NX)
        block = blocks[pair].reshape(NX * rows, width)
        share = share_ref[pair].reshape(NX * rows, 2)
        total = None
        for e in range(2):
            gate_act = dot(block, mats[e], NN)
            up_act = dot(block, mats[2 + e], NN)
            units = gate_act.shape[1]
            gate[pair, :, pl.ds(e * units, units)] = gate_act.astype(BF).reshape(NX, rows, units)
            up[pair, :, pl.ds(e * units, units)] = up_act.astype(BF).reshape(NX, rows, units)
            inner = gate_act / (1.0 + jnp.exp(-gate_act)) * up_act * share[:, e : e + 1]
            term = dot(inner.astype(BF), mats[4 + e], NT)
            total = term if total is None else total + term
        part[pair] = total.astype(BF).reshape(NX, rows, width)
        for save in saves(row):
            save.start()
        return carry

    lax.fori_loop(0, nz, step, 0)
    sums = Scatter(line, part, o_ref, work, ework, ssems, msems)
    for i in range(nz):
        sums.across(line.far(i)).start()
    ring.finish()
    for i in range(nz):
        sums.add(i)
    sums.finish()
    o_ref[...] += x_ref[...]
    for row in range(nz):
        for save in saves(row):
            save.wait()


def experts_forward(block, gain, share, mats, layer, nz):
    rows, width = block.shape
    units = mats.shape[3]
    group = nz * NX
    acts = jax.ShapeDtypeStruct((group, rows, 2 * units), BF)
    return pl.pallas_call(
        functools.partial(experts_kernel, nz, layer),
        out_shape=(
            jax.ShapeDtypeStruct((rows, width), F32),
            jax.ShapeDtypeStruct((group, rows, width), BF),
            acts,
            acts,
        ),
        in_specs=[VM, VM, VM, ANY],
        out_specs=(VM, ANY, ANY, ANY),
        scratch_shapes=[
            pltpu.VMEM((6, width, units), BF),
            pltpu.VMEM((group, rows, width), BF),
            pltpu.VMEM((group, rows, width), BF),
            pltpu.VMEM((group, rows, 2 * units), BF),
            pltpu.VMEM((group, rows, 2 * units), BF),
            DMA,
            DMA((3, nz)),
        ]
        + Gather.scratch(nz)
        + Scatter.scratch(nz, rows, width),
        compiler_params=params(5 + 2 * layer, 60),
        name="experts_forward",
    )(block, gain, share, mats)


def experts_back_kernel(nz, layer, x_ref, values_ref, gain_ref, share_ref, mats_ref, gate_ref, up_ref, o_ref, gain_out, all_out, dgate_out, dup_out, inner_out,
                        mats, blocks, part, gate, up, inners, load_sem, save_sem, gsems, work, ework, ssems, msems):
    line = Line(nz)
    rows, width = x_ref.shape
    loads = (
        pltpu.make_async_copy(mats_ref.at[layer, pl.ds(1, 6)], mats, load_sem.at[0]),
        pltpu.make_async_copy(gate_ref, gate, load_sem.at[1]),
        pltpu.make_async_copy(up_ref, up, load_sem.at[2]),
    )
    for load in loads:
        load.start()
    blocks[line.ctx] = x_ref[...].astype(BF)
    line.greet()
    ring = Gather(line, blocks.at[line.ctx], blocks, gsems)
    ring.start()
    for load in loads:
        load.wait()
    ring.start_extras()

    def saves(row):
        pair = pl.ds(row * NX, NX)
        return (
            pltpu.make_async_copy(blocks.at[pair], all_out.at[pair], save_sem.at[0, row]),
            pltpu.make_async_copy(gate.at[pair], dgate_out.at[pair], save_sem.at[1, row]),
            pltpu.make_async_copy(up.at[pair], dup_out.at[pair], save_sem.at[2, row]),
            pltpu.make_async_copy(inners.at[pair], inner_out.at[pair], save_sem.at[3, row]),
        )

    def step(i, carry):
        @pl.when(i < nz - 1)
        def _():
            ring.forward(i)

        row = line.near(i)
        ring.wait_pair(row)
        pair = pl.ds(row * NX, NX)
        block = blocks[pair].reshape(NX * rows, width)
        share = share_ref[pair].reshape(NX * rows, 2)
        total = None
        units = mats.shape[2]
        for e in range(2):
            part_of = pl.ds(e * units, units)
            gate_act = gate[pair, :, part_of].reshape(NX * rows, units).astype(F32)
            up_act = up[pair, :, part_of].reshape(NX * rows, units).astype(F32)
            grad_inner = dot(block, mats[4 + e], NN) * share[:, e : e + 1]
            sigmoid = 1.0 / (1.0 + jnp.exp(-gate_act))
            silu = gate_act * sigmoid
            d_gate = (grad_inner * up_act * (sigmoid + silu * (1.0 - sigmoid))).astype(BF)
            d_up = (grad_inner * silu).astype(BF)
            inners[pair, :, part_of] = (silu * up_act * share[:, e : e + 1]).astype(BF).reshape(NX, rows, units)
            gate[pair, :, part_of] = d_gate.reshape(NX, rows, units)
            up[pair, :, part_of] = d_up.reshape(NX, rows, units)
            term = dot(d_gate, mats[e], NT) + dot(d_up, mats[2 + e], NT)
            total = term if total is None else total + term
        part[pair] = total.astype(BF).reshape(NX, rows, width)
        for save in saves(row):
            save.start()
        return carry

    lax.fori_loop(0, nz, step, 0)
    sums = Scatter(line, part, o_ref, work, ework, ssems, msems)
    for i in range(nz):
        sums.across(line.far(i)).start()
    ring.finish()
    for i in range(nz):
        sums.add(i)
    sums.finish()
    norm_back_rows(x_ref, values_ref, gain_ref, o_ref, gain_out)
    for row in range(nz):
        for save in saves(row):
            save.wait()


def experts_backward(block, values, gain, share, mats, layer, gate_act, up_act, nz):
    rows, width = block.shape
    units = mats.shape[3]
    group = nz * NX
    acts = jax.ShapeDtypeStruct((group, rows, 2 * units), BF)
    held = pltpu.VMEM((group, rows, 2 * units), BF)
    return pl.pallas_call(
        functools.partial(experts_back_kernel, nz, layer),
        out_shape=(
            jax.ShapeDtypeStruct((rows, width), F32),
            jax.ShapeDtypeStruct((1, width), F32),
            jax.ShapeDtypeStruct((group, rows, width), BF),
            acts,
            acts,
            acts,
        ),
        in_specs=[VM, VM, VM, VM, ANY, ANY, ANY],
        out_specs=(VM, VM, ANY, ANY, ANY, ANY),
        scratch_shapes=[
            pltpu.VMEM((6, width, units), BF),
            pltpu.VMEM((group, rows, width), BF),
            pltpu.VMEM((group, rows, width), BF),
            held,
            held,
            held,
            DMA((3,)),
            DMA((4, nz)),
        ]
        + Gather.scratch(nz)
        + Scatter.scratch(nz, rows, width),
        compiler_params=params(6 + 2 * layer, 60),
        name="experts_backward",
    )(block, values, gain, share, mats, gate_act, up_act)


def far_of(nz, z, i):
    mid1 = jnp.where(i == 0, 3, jnp.where(i == 1, 0, jnp.where(i == 2, 2, 1)))
    mid2 = jnp.where(i == 0, 0, jnp.where(i == 1, 3, jnp.where(i == 2, 1, 2)))
    return jnp.where(z == 0, nz - 1 - i, jnp.where(z == nz - 1, i, jnp.where(z == 1, mid1, mid2)))


class Exchange:
    @staticmethod
    def scratch(nz, blk, lead=()):
        return [
            pltpu.VMEM(lead + (2, 2, 2) + blk, BF),
            pltpu.VMEM(lead + (nz,) + blk, BF),
            DMA(lead + (2, nz, nz, 2)),
            DMA(lead + (2, nz)),
        ]

    def __init__(self, line, src_at, dst_at, passing, for_mate, zs, xs, lead=()):
        self.line, self.src_at, self.dst_at, self.lead = line, src_at, dst_at, lead
        self.passing, self.for_mate, self.zs, self.xs = passing, for_mate, zs, xs

    def held(self, way, src, dest, side, at):
        last = self.line.nz - 1
        slot = (dest - at - 1) + src if way == 0 else (at - dest - 1) + last - src
        return self.passing.at[self.lead + (way, slot, side)]

    def zsem(self, kind, src, dest, side):
        return self.zs.at[self.lead + (kind, src, dest, side)]

    def hop(self, way, src, dest, side, ref):
        line = self.line
        to = line.z + 1 if way == 0 else line.z - 1
        sems = self.zsem(0, src, dest, side), self.zsem(1, src, dest, side)
        target = to * NX + line.x

        @pl.when(dest == to)
        def _():
            land = self.dst_at(src * NX + line.x) if side == 0 else self.for_mate.at[self.lead + (src,)]
            remote(ref, land, *sems, target, line.fsdp).start()

        @pl.when(dest != to)
        def _():
            remote(ref, self.held(way, src, dest, side, to), *sems, target, line.fsdp).start()

    def to_mate(self, src, ref=None):
        line = self.line
        ref = self.for_mate.at[self.lead + (src,)] if ref is None else ref
        return remote(ref, self.dst_at(src * NX + line.x), self.xs.at[self.lead + (0, src)], self.xs.at[self.lead + (1, src)], line.mate, line.fsdp)

    def send(self, dest):
        line = self.line
        for side, column in ((0, line.x), (1, 1 - line.x)):
            ref = self.src_at(dest * NX + column)

            @pl.when(dest > line.z)
            def _():
                self.hop(0, line.z, dest, side, ref)

            @pl.when(dest < line.z)
            def _():
                self.hop(1, line.z, dest, side, ref)

        @pl.when(dest == line.z)
        def _():
            self.to_mate(line.z, self.src_at(line.mate)).start()

    def events(self, i):
        line = self.line
        found = []
        for k in range(1, line.nz):
            j = i - k
            for way in range(2):
                src = line.z - k if way == 0 else line.z + k
                dest = far_of(line.nz, src, j)
                here = (dest >= line.z) if way == 0 else (dest <= line.z)
                found.append((way, src, dest, (src >= 0) & (src < line.nz) & (j >= 0) & (j < line.nz - 1) & here))
        return found

    def handle(self, way, src, dest, arrived):
        line = self.line
        for side in range(2):
            wait = self.held(way, 0 if way == 0 else line.nz - 1, line.z + 1 if way == 0 else line.z - 1, side, line.z)
            remote(wait, wait, self.zsem(0, src, dest, side), self.zsem(1, src, dest, side), line.mate, line.fsdp).wait_recv()

            @pl.when(dest != line.z)
            def _():
                self.hop(way, src, dest, side, self.held(way, src, dest, side, line.z))

        @pl.when(dest == line.z)
        def _():
            self.to_mate(src).start()
            arrived(src * NX + line.x)

    def mate_arrived(self, src):
        line = self.line
        wait = self.for_mate.at[self.lead + (src,)]
        remote(wait, wait, self.xs.at[self.lead + (0, src)], self.xs.at[self.lead + (1, src)], line.mate, line.fsdp).wait_recv()

    def finish(self):
        line = self.line
        wait = self.for_mate.at[self.lead + (0,)]
        for src in range(line.nz):
            for dest in range(line.nz):
                if src != dest:
                    passes = (line.z >= src) & (line.z < dest) if src < dest else (line.z <= src) & (line.z > dest)

                    @pl.when(passes)
                    def _():
                        for side in range(2):
                            remote(wait, wait, self.zsem(0, src, dest, side), self.zsem(1, src, dest, side), line.mate, line.fsdp).wait_send()

            self.to_mate(src).wait_send()


LAG = 3


def weights_kernel(nctx, nfs, rows, attn_ref, gate_ref, up_ref, down_ref, g_ref, o_ref, go_ref, w_ref, stage, stage_sem, passing, for_mate, zs, xs, own_sem, y_sem, c_sem, gown_sem, gp_sem, gy_sem, gc_sem):
    nz = nctx // NX
    line = Line(nz)
    ctx, fsdp = line.ctx, line.fsdp
    layers = w_ref.shape[0]
    spread = layers - 1
    y, core = fsdp // NCORE, fsdp % NCORE
    y_mate = (1 - y) * NCORE + core
    c_mate = y * NCORE + 1 - core
    y_c_mate = (1 - y) * NCORE + 1 - core

    def load(layer):
        return [
            pltpu.make_async_copy(src.at[layer], stage.at[layer, k], stage_sem.at[layer, k])
            for k, src in enumerate((gate_ref, up_ref, down_ref))
        ]

    for layer in range(layers):
        for copy in load(layer):
            copy.start()

    def pack(layer):
        for copy in load(layer):
            copy.wait()

        def one(to, carry):
            w_ref[layer, to, 0] = attn_ref[layer, to]
            for k in range(3):
                for e in range(2):
                    w_ref[layer, to, 1 + 2 * k + e] = stage[layer, k, 2 * to + e].astype(BF)
            return carry

        lax.fori_loop(0, nctx, one, 0)

    pack(0)
    barrier = pltpu.get_barrier_semaphore()
    for step in range(1, nctx):
        greet(barrier, (ctx + step) % nctx, fsdp)
    for other in (y_mate, c_mate):
        greet(barrier, ctx, other)
    pl.semaphore_wait(barrier, nctx + 1)

    def place(layer, s, f):
        return o_ref.at[layer, :, pl.ds(pl.multiple_of((s * nfs + f) * rows, rows), rows), :]

    def swap(layer):
        return Exchange(
            line,
            lambda to: w_ref.at[layer, to],
            lambda frm: place(layer, frm, fsdp),
            passing, for_mate, zs, xs,
            (layer,),
        )

    def over_y(layer, frm, f, ref=None):
        return remote(place(layer, frm, f) if ref is None else ref, place(layer, frm, f), y_sem.at[0, layer, frm], y_sem.at[1, layer, frm], ctx, y_mate)

    def over_c(layer, frm, f, k, ref=None):
        return remote(place(layer, frm, f) if ref is None else ref, place(layer, frm, f), c_sem.at[0, k, layer, frm], c_sem.at[1, k, layer, frm], ctx, c_mate)

    def own(layer):
        return pltpu.make_async_copy(w_ref.at[layer, ctx], place(layer, ctx, fsdp), own_sem.at[layer])

    def begin(layer):
        if layer:
            pack(layer)
        exchange = swap(layer)
        for i in range(nz - 1):
            exchange.send(line.far(i))
        exchange.send(line.z)
        if layer < spread:
            over_y(layer, ctx, fsdp, w_ref.at[layer, ctx]).start()
            over_c(layer, ctx, fsdp, 0, w_ref.at[layer, ctx]).start()
        own(layer).start()

    def arrived(layer, frm):
        @pl.when(layer < spread)
        def _():
            over_y(layer, frm, fsdp).start()
            over_c(layer, frm, fsdp, 0).start()

    def from_y(layer, frm):
        @pl.when(layer < spread)
        def _():
            over_y(layer, frm, y_mate).wait_recv()
            over_c(layer, frm, y_mate, 1).start()

    def take(layer, i):
        exchange = swap(layer)
        for way, src, dest, real in exchange.events(i):

            @pl.when(real)
            def _():
                exchange.handle(way, src, dest, lambda frm: arrived(layer, frm))

        def mine(late, then):
            @pl.when(i == late)
            def _():
                then(line.z)

            for way, src, dest, real in exchange.events(i - late):

                @pl.when(real & (dest == line.z))
                def _():
                    then(src)

        def mates(src):
            exchange.mate_arrived(src)
            arrived(layer, src * NX + 1 - line.x)

        mine(1, mates)
        mine(2, lambda src: from_y(layer, src * NX + line.x))
        mine(3, lambda src: from_y(layer, src * NX + 1 - line.x))

    def small(to):
        return remote(g_ref.at[to], go_ref.at[ctx * nfs + fsdp], gp_sem.at[0, to], gp_sem.at[1, ctx], to, fsdp)

    def small_in(frm):
        return remote(g_ref.at[ctx], go_ref.at[frm * nfs + fsdp], gp_sem.at[0, frm], gp_sem.at[1, frm], frm, fsdp)

    def small_y(frm, f):
        return remote(go_ref.at[frm * nfs + f], go_ref.at[frm * nfs + f], gy_sem.at[0, frm], gy_sem.at[1, frm], ctx, y_mate)

    def small_c(frm, f, k):
        return remote(go_ref.at[frm * nfs + f], go_ref.at[frm * nfs + f], gc_sem.at[0, k, frm], gc_sem.at[1, k, frm], ctx, c_mate)

    small_own = pltpu.make_async_copy(g_ref.at[ctx], go_ref.at[ctx * nfs + fsdp], gown_sem)
    small_own.start()
    for step in range(1, nctx):
        small((ctx + step) % nctx).start()
    steps = 2 * nz - 3 + 3

    def step(i, carry):
        for layer in range(layers):
            at = i - LAG * layer

            @pl.when(at == 0)
            def _():
                begin(layer)

        def each(layer, carry):
            at = i - LAG * layer

            @pl.when((at > 0) & (at <= steps))
            def _():
                take(layer, at)

            return carry

        lax.fori_loop(0, layers, each, 0)
        return carry

    lax.fori_loop(0, steps - 1 + LAG * (layers - 1), step, 0)
    small_own.wait()
    for k in range(nctx):
        if k:
            small_in((ctx + k) % nctx).wait_recv()
        small_y((ctx + k) % nctx, fsdp).start()
        small_c((ctx + k) % nctx, fsdp, 0).start()
    for k in range(nctx):
        small_y((ctx + k) % nctx, y_mate).wait_recv()
        small_c((ctx + k) % nctx, y_mate, 1).start()
    for frm in range(nctx):
        small_c(frm, c_mate, 0).wait_recv()
        small_c(frm, y_c_mate, 1).wait_recv()
        small_c(frm, fsdp, 0).wait_send()
        small_c(frm, y_mate, 1).wait_send()
        small_y(frm, fsdp).wait_send()
    for step_ in range(1, nctx):
        small((ctx + step_) % nctx).wait_send()

    def close(layer, carry):
        own(layer).wait()

        @pl.when(layer < spread)
        def _():
            for frm in range(nctx):
                over_c(layer, frm, c_mate, 0).wait_recv()
                over_c(layer, frm, y_c_mate, 1).wait_recv()
                over_c(layer, frm, fsdp, 0).wait_send()
                over_c(layer, frm, y_mate, 1).wait_send()
                over_y(layer, frm, fsdp).wait_send()

        swap(layer).finish()
        return carry

    lax.fori_loop(0, layers, close, 0)


def spread_weights(attn, gate, up, down, small, nfs):
    layers, nctx, rows, width = attn.shape
    mats = 7
    return pl.pallas_call(
        functools.partial(weights_kernel, nctx, nfs, rows),
        out_shape=(
            jax.ShapeDtypeStruct((layers, mats, nctx * nfs * rows, width), BF),
            jax.ShapeDtypeStruct((nctx * nfs,) + small.shape[1:], small.dtype),
        ),
        in_specs=[VM, ANY, ANY, ANY, VM],
        out_specs=(ANY, ANY),
        scratch_shapes=[
            pltpu.VMEM((layers, nctx, mats, rows, width), BF),
            pltpu.VMEM((layers, 3) + gate.shape[1:], F32),
            DMA((layers, 3)),
        ]
        + Exchange.scratch(nctx // NX, (mats, rows, width), (layers,))
        + [
            DMA((layers,)),
            DMA((2, layers, nctx)),
            DMA((2, 2, layers, nctx)),
            DMA,
            DMA((2, nctx)),
            DMA((2, nctx)),
            DMA((2, 2, nctx)),
        ],
        compiler_params=params(3, 63),
        name="spread_weights",
    )(attn, gate, up, down, small)


class Spread:
    @staticmethod
    def scratch(nctx):
        return [DMA((2, nctx)), DMA((2, 2, nctx))]

    def __init__(self, line, mats, layer, nfs, y_sem, c_sem):
        self.line, self.mats, self.layer, self.nfs, self.y_sem, self.c_sem = line, mats, layer, nfs, y_sem, c_sem
        y, core = line.fsdp // NCORE, line.fsdp % NCORE
        self.y_mate = (1 - y) * NCORE + core
        self.c_mate = y * NCORE + 1 - core
        self.nctx = line.nz * NX
        self.rows = mats.shape[2] // (self.nctx * nfs)

    def place(self, frm, f):
        at = pl.multiple_of((frm * self.nfs + f) * self.rows, self.rows)
        return self.mats.at[self.layer, :, pl.ds(at, self.rows), :]

    def over_y(self, frm):
        place = self.place(frm, self.line.fsdp)
        return remote(place, place, self.y_sem.at[0, frm], self.y_sem.at[1, frm], self.line.ctx, self.y_mate)

    def over_c(self, frm, k):
        place = self.place(frm, self.y_mate if k else self.line.fsdp)
        return remote(place, place, self.c_sem.at[0, k, frm], self.c_sem.at[1, k, frm], self.line.ctx, self.c_mate)

    def start(self):
        for frm in range(self.nctx):
            self.over_y(frm).start()
            self.over_c(frm, 0).start()

    def take(self, frm):
        self.over_y(frm).wait_recv()
        self.over_c(frm, 1).start()

    def finish(self):
        for frm in range(self.nctx):
            self.over_y(frm).wait_send()
            for k in range(2):
                self.over_c(frm, k).wait()


def grads_kernel(nctx, nfs, rows, layers, *refs):
    count = 9 * layers
    ins, (e_ref, o_ref, eo_ref), refs = refs[:count], refs[count : count + 3], refs[count + 3 :]
    tall, dproj, attended, dgate, dup, inner, mine, cin, yin, e_cin, e_half, e_yin, e_full = refs[:13]
    tall_sem, wide_sem, own_sem, c_sem, y_sem, p_sem, eown_sem, ec_sem, ey_sem, ep_sem = refs[13:]
    nz = nctx // NX
    line = Line(nz)
    ctx, fsdp = line.ctx, line.fsdp
    y, core = fsdp // NCORE, fsdp % NCORE
    y_mate = (1 - y) * NCORE + core
    c_mate = y * NCORE + 1 - core
    mats, slab = mine.shape[1], mine.shape[2]
    proj = mine.shape[3] - attended.shape[2]
    units = dgate.shape[2] // 2
    items = layers * nz

    def layer_of(i):
        return layers - 1 - i // nz

    def row_of(i):
        return line.far(i % nz)

    def wide_loads(layer):
        _, dproj_in, _, attended_in, _, dgate_in, dup_in, _, inner_in = ins[9 * layer : 9 * layer + 9]
        pairs = ((dproj_in, dproj), (attended_in, attended), (dgate_in, dgate), (dup_in, dup), (inner_in, inner))
        return [pltpu.make_async_copy(src, dst.at[layer], wide_sem.at[k, layer]) for k, (src, dst) in enumerate(pairs)]

    def tall_loads(i, layer):
        normed_in, _, middle_in, _, moe_in, _, _, grad_in, _ = ins[9 * layer : 9 * layer + 9]
        lanes = pl.ds(pl.multiple_of(row_of(i) * slab, 128), slab)
        return [
            pltpu.make_async_copy(src.at[:, lanes], tall.at[i % 2, k], tall_sem.at[i % 2, k])
            for k, src in enumerate((normed_in, middle_in, moe_in, grad_in))
        ]

    def load(i):
        for layer in range(layers):

            @pl.when(layer_of(i) == layer)
            def _():
                for copy in tall_loads(i, layer):
                    copy.start()

    for layer in reversed(range(layers)):
        for copy in wide_loads(layer):
            copy.start()
        if layer == layers - 1:
            load(0)
    barrier = pltpu.get_barrier_semaphore()
    for step in range(1, nctx):
        greet(barrier, (ctx + step) % nctx, fsdp)
    for other in (y_mate, c_mate):
        greet(barrier, ctx, other)
    pl.semaphore_wait(barrier, nctx + 1)

    def span(side, f):
        return pl.ds(pl.multiple_of((side * nfs + f) * rows, rows), rows)

    def to_c(i, side, k):
        layer, s = layer_of(i), row_of(i) * NX + side
        f = (1 - y if k == 0 else y) * NCORE + 1 - core
        return remote(mine.at[i % 3, :, span(side, f), :], cin.at[layer, k, s], c_sem.at[0, layer, k, s], c_sem.at[1, layer, k, s], ctx, c_mate)

    def to_y(layer, s):
        return remote(cin.at[layer, 0, s], yin.at[layer, s], y_sem.at[0, layer, s], y_sem.at[1, layer, s], ctx, y_mate)

    def out(layer, s):
        return remote(cin.at[layer, 1, s], o_ref.at[layer, ctx], p_sem.at[0, layer, s], p_sem.at[1, layer, ctx], s, fsdp)

    def out_in(layer, s):
        return remote(cin.at[layer, 1, s], o_ref.at[layer, s], p_sem.at[0, layer, s], p_sem.at[1, layer, s], s, fsdp)

    def own(layer):
        return pltpu.make_async_copy(cin.at[layer, 1, ctx], o_ref.at[layer, ctx], own_sem.at[layer])

    e_to_c = remote(e_ref.at[1 - core], e_cin, ec_sem.at[0], ec_sem.at[1], ctx, c_mate)
    e_to_y = remote(e_half.at[1 - y], e_yin, ey_sem.at[0], ey_sem.at[1], ctx, y_mate)
    e_own = pltpu.make_async_copy(e_full.at[ctx], eo_ref.at[ctx], eown_sem)

    def e_out(s):
        return remote(e_full.at[s], eo_ref.at[ctx], ep_sem.at[0, s], ep_sem.at[1, ctx], s, fsdp)

    def e_out_in(s):
        return remote(e_full.at[s], eo_ref.at[s], ep_sem.at[0, s], ep_sem.at[1, s], s, fsdp)

    e_to_c.start()

    def compute(i):
        layer, slot, here = layer_of(i), i % 2, i % 3
        mine[here, 0, :, pl.ds(0, proj)] = dot(tall[slot, 0], dproj[layer], TN)[:, :proj].astype(BF)
        mine[here, 0, :, pl.ds(proj, mine.shape[3] - proj)] = dot(tall[slot, 1], attended[layer], TN).astype(BF)
        for e in range(2):
            part_of = pl.ds(e * units, units)
            mine[here, 1 + e] = dot(tall[slot, 2], dgate[layer, :, part_of], TN).astype(BF)
            mine[here, 3 + e] = dot(tall[slot, 2], dup[layer, :, part_of], TN).astype(BF)
            mine[here, 5 + e] = dot(tall[slot, 3], inner[layer, :, part_of], TN).astype(BF)

    def first(i, side):
        layer, s = layer_of(i), row_of(i) * NX + side
        to_c(i, side, 0).wait_recv()

        def one(m, _):
            term = mine[i % 3, m, span(side, y_mate), :].astype(F32)
            cin[layer, 0, s, m] = (term + cin[layer, 0, s, m].astype(F32)).astype(BF)
            return 0

        lax.fori_loop(0, mats, one, 0)
        to_y(layer, s).start()

    def second(i, side):
        layer, s = layer_of(i), row_of(i) * NX + side
        to_c(i, side, 1).wait_recv()
        to_y(layer, s).wait_recv()

        def one(m, _):
            term = mine[i % 3, m, span(side, fsdp), :].astype(F32) + yin[layer, s, m].astype(F32)
            cin[layer, 1, s, m] = (term + cin[layer, 1, s, m].astype(F32)).astype(BF)
            return 0

        lax.fori_loop(0, mats, one, 0)
        for k in range(2):
            to_c(i, side, k).wait_send()

        @pl.when(s != ctx)
        def _():
            out(layer, s).start()

        @pl.when(s == ctx)
        def _():
            own(layer).start()

    def step(i, carry):
        @pl.when(i < items)
        def _():
            for layer in range(layers):

                @pl.when(i == (layers - 1 - layer) * nz)
                def _():
                    for copy in wide_loads(layer):
                        copy.wait()

            for copy in tall_loads(i, 0):
                copy.wait()

            @pl.when(i + 1 < items)
            def _():
                load(i + 1)

            compute(i)
            for k in range(2):
                for side in range(NX):
                    to_c(i, side, k).start()

        @pl.when((i >= 1) & (i < items + 1))
        def _():
            for side in range(NX):
                first(i - 1, side)

        @pl.when(i >= 2)
        def _():
            for side in range(NX):
                second(i - 2, side)

        @pl.when(i == 1)
        def _():
            e_to_c.wait_recv()
            e_half[...] = e_ref[core] + e_cin[...]
            e_to_y.start()

        @pl.when(i == 3)
        def _():
            e_to_y.wait_recv()
            e_full[...] = e_half[y] + e_yin[...]
            e_own.start()
            for step_ in range(1, nctx):
                e_out((ctx + step_) % nctx).start()

        return carry

    lax.fori_loop(0, items + 2, step, 0)
    for layer in range(layers):
        own(layer).wait()
        for s in range(nctx):
            to_y(layer, s).wait_send()

            @pl.when(s != ctx)
            def _():
                out(layer, s).wait_send()
                out_in(layer, s).wait_recv()

    for s in range(nctx):

        @pl.when(s != ctx)
        def _():
            e_out(s).wait_send()
            e_out_in(s).wait_recv()

    e_to_c.wait_send()
    e_to_y.wait_send()
    e_own.wait()


def collect_grads(nctx, nfs, layer_args, extra):
    layers = len(layer_args)
    normed, dproj, middle, attended, moe, dgate, dup, grad, inner = layer_args[0]
    group_rows, width = normed.shape
    rows = width // (nctx * nfs)
    slab = NX * nfs * rows
    mats, cols = 7, dgate.shape[1] // 2
    blk = (mats, rows, cols)
    tile = extra.shape[3:]
    held = [pltpu.VMEM((layers,) + part.shape, BF) for part in (dproj, attended, dgate, dup, inner)]
    return pl.pallas_call(
        functools.partial(grads_kernel, nctx, nfs, rows, layers),
        out_shape=(jax.ShapeDtypeStruct((layers, nctx) + blk, BF), jax.ShapeDtypeStruct((nctx,) + tile, F32)),
        in_specs=[ANY] * (9 * layers) + [VM],
        out_specs=(ANY, ANY),
        scratch_shapes=[pltpu.VMEM((2, 4, group_rows, slab), BF)]
        + held
        + [
            pltpu.VMEM((3, mats, slab, cols), BF),
            pltpu.VMEM((layers, 2, nctx) + blk, BF),
            pltpu.VMEM((layers, nctx) + blk, BF),
            pltpu.VMEM((2, nctx) + tile, F32),
            pltpu.VMEM((2, nctx) + tile, F32),
            pltpu.VMEM((nctx,) + tile, F32),
            pltpu.VMEM((nctx,) + tile, F32),
            DMA((2, 4)),
            DMA((5, layers)),
            DMA((layers,)),
            DMA((2, layers, 2, nctx)),
            DMA((2, layers, nctx)),
            DMA((2, layers, nctx)),
            DMA,
            DMA((2,)),
            DMA((2,)),
            DMA((2, nctx)),
        ],
        compiler_params=params(4, 63),
        name="collect_grads",
    )(*[part for args in layer_args for part in args], extra)


def spin(values, cos_part, sin_part):
    lane = lax.broadcasted_iota(jnp.int32, values.shape, 1) % HEAD_DIM
    half_dim = HEAD_DIM // 2
    swapped = jnp.where(
        lane < half_dim,
        pltpu.roll(values, values.shape[1] - half_dim, 1),
        pltpu.roll(values, half_dim, 1),
    )
    return values * cos_part + swapped * sin_part


def attention_kernel(nz, nfs, layer, x_ref, gain_ref, mats_ref, cos_ref, sin_ref, key_at_ref, query_at_ref,
                     o_ref, all_out, q_ref, k_ref, v_ref, peak_ref, share_ref, att_ref, *refs):
    line = Line(nz)
    spread = None
    if layer == 0:
        mats_ref, refs = refs[0], refs[1:]
        spread = Spread(line, mats_ref, layer + 1, nfs, *refs[-2:])
        refs = refs[:-2]
    attn, out_w, blocks, part, v_turned, probs, load_sem, save_sem, gsems, work, ework, ssems, msems = refs
    rows, width = x_ref.shape
    pair_rows = NX * rows
    heads = q_ref.shape[1] // rows
    o_at = (heads + 2) * HEAD_DIM
    wide = -(-o_at // 128) * 128
    load = pltpu.make_async_copy(mats_ref.at[layer, 0], attn, load_sem)
    load.start()
    blocks[line.ctx] = normed_rows(x_ref, gain_ref)
    line.greet((spread.y_mate, spread.c_mate) if spread else ())
    if spread:
        spread.start()
    ring = Gather(line, blocks.at[line.ctx], blocks, gsems)
    ring.start()
    load.wait()
    out_w[...] = attn[:, o_at:]
    ring.start_extras()

    def save(row):
        pair = pl.ds(row * NX, NX)
        return pltpu.make_async_copy(blocks.at[pair], all_out.at[pair], save_sem.at[row])

    def project(i, carry):
        @pl.when(i < nz - 1)
        def _():
            ring.forward(i)

        row = line.near(i)
        ring.wait_pair(row)
        pair = pl.ds(row * NX, NX)
        tall = pl.ds(pl.multiple_of(row * pair_rows, pair_rows), pair_rows)
        block = blocks[pair].reshape(pair_rows, width)
        save(row).start()
        proj = dot(block, attn[:, :wide], NN)
        cos_part, sin_part = cos_ref[tall, :], sin_ref[tall, :]
        first = spin(proj[:, :128], cos_part, sin_part)
        second = spin(proj[:, 128:256], cos_part, sin_part)
        values = proj[:, 256 : 256 + HEAD_DIM]
        for side in range(NX):
            at = slice(side * rows, (side + 1) * rows)
            q_ref[row * NX + side, 0:rows, :] = first[at, :HEAD_DIM].astype(BF)
            q_ref[row * NX + side, rows : 2 * rows, :] = first[at, HEAD_DIM:].astype(BF)
            q_ref[row * NX + side, 2 * rows : 3 * rows, :] = second[at, :HEAD_DIM].astype(BF)
        k_ref[tall, :] = second[:, HEAD_DIM:].astype(BF)
        v_ref[tall, :] = values.astype(BF)
        v_turned[:, tall] = values.T.astype(BF)
        return carry

    lax.fori_loop(0, nz, project, 0)
    ring.finish()
    sums = Scatter(line, part, o_ref, work, ework, ssems, msems)

    def attend(at):
        scores = dot(k_ref[...], q_ref[at], NT)
        key_at = key_at_ref[...]
        visible = (key_at >= query_at_ref[at, 0:1, :]) & (key_at <= query_at_ref[at, 1:2, :])
        for head in range(heads):
            lanes = slice(head * rows, (head + 1) * rows)
            raw = jnp.where(visible, scores[:, lanes] * HEAD_DIM**-0.5, NEGATIVE)
            peak = jnp.max(raw, axis=0, keepdims=True)
            powers = jnp.exp(raw - peak)
            peak_ref[at, :, lanes] = peak
            share_ref[at, :, lanes] = 1.0 / jnp.sum(powers, axis=0, keepdims=True)
            probs[:, lanes] = powers.astype(BF)
        turned = dot(v_turned[...], probs[...], NN) * share_ref[at]
        stacked = turned.T.astype(BF)
        for head in range(heads):
            att_ref[at, :, head * HEAD_DIM : (head + 1) * HEAD_DIM] = stacked[head * rows : (head + 1) * rows]
        part[at] = dot(att_ref[at], out_w[...], NT).astype(BF)

    def step(i, carry):
        row = line.far(i)
        attend(row * NX + 1 - line.x)
        sums.across(row).start()
        attend(row * NX + line.x)

        @pl.when(i > 0)
        def _():
            sums.add(i - 1)

        if spread:
            for side in range(NX):
                spread.take(i * NX + side)

        return carry

    lax.fori_loop(0, nz, step, 0)
    sums.add(nz - 1)
    sums.finish()
    o_ref[...] += x_ref[...]
    for row in range(nz):
        save(row).wait()
    if spread:
        spread.finish()


def attention_rows(block, gain, mats, layer, cos_part, sin_part, key_at, query_at, nz, nfs):
    rows, width = block.shape
    spreads = layer == 0
    group = nz * NX
    group_rows = group * rows
    heads = 3
    return pl.pallas_call(
        functools.partial(attention_kernel, nz, nfs, layer),
        out_shape=(
            jax.ShapeDtypeStruct((rows, width), F32),
            jax.ShapeDtypeStruct((group, rows, width), BF),
            jax.ShapeDtypeStruct((group, heads * rows, HEAD_DIM), BF),
            jax.ShapeDtypeStruct((group_rows, HEAD_DIM), BF),
            jax.ShapeDtypeStruct((group_rows, HEAD_DIM), BF),
            jax.ShapeDtypeStruct((group, 1, heads * rows), F32),
            jax.ShapeDtypeStruct((group, 1, heads * rows), F32),
            jax.ShapeDtypeStruct((group, rows, heads * HEAD_DIM), BF),
        )
        + ((jax.ShapeDtypeStruct(mats.shape, BF),) if spreads else ()),
        in_specs=[VM, VM, ANY, VM, VM, VM, VM],
        out_specs=(VM, ANY, VM, VM, VM, VM, VM, VM) + ((ANY,) if spreads else ()),
        input_output_aliases={2: 8} if spreads else {},
        scratch_shapes=[
            pltpu.VMEM(mats.shape[2:], BF),
            pltpu.VMEM((width, heads * HEAD_DIM), BF),
            pltpu.VMEM((group, rows, width), BF),
            pltpu.VMEM((group, rows, width), BF),
            pltpu.VMEM((HEAD_DIM, group_rows), BF),
            pltpu.VMEM((group_rows, heads * rows), BF),
            DMA,
            DMA((nz,)),
        ]
        + Gather.scratch(nz)
        + Scatter.scratch(nz, rows, width)
        + (Spread.scratch(group) if spreads else []),
        compiler_params=params(9 + 2 * layer, 60),
        name="attention_forward",
    )(block, gain, mats, cos_part, sin_part, key_at, query_at)


def attention_back_kernel(nz, layer, x_ref, values_ref, gain_ref, mats_ref, cos_ref, sin_ref, key_at_ref, query_at_ref, q_ref, k_ref, v_ref, peak_ref, share_ref,
                          o_ref, gain_out, all_out, dproj_ref,
                          attn, out_w, blocks, part, k_turned, probs, slopes, dq, dk, dv, load_sem, save_sem, gsems, work, ework, ssems, msems):
    line = Line(nz)
    rows, width = x_ref.shape
    pair_rows = NX * rows
    heads = q_ref.shape[1] // rows
    o_at = (heads + 2) * HEAD_DIM
    wide = dproj_ref.shape[2]
    scale = HEAD_DIM**-0.5
    load = pltpu.make_async_copy(mats_ref.at[layer, 0], attn, load_sem)
    load.start()
    blocks[line.ctx] = x_ref[...].astype(BF)
    line.greet()
    ring = Gather(line, blocks.at[line.ctx], blocks, gsems)
    ring.start()
    k_turned[...] = k_ref[...].astype(F32).T.astype(BF)
    dk[...] = jnp.zeros(dk.shape, F32)
    dv[...] = jnp.zeros(dv.shape, F32)
    load.wait()
    out_w[...] = attn[:, o_at:]
    ring.start_extras()

    def save(row):
        pair = pl.ds(row * NX, NX)
        return pltpu.make_async_copy(blocks.at[pair], all_out.at[pair], save_sem.at[row])

    def back(at):
        d_att = dot(blocks[at], out_w[...], NN)
        d_heads = jnp.concatenate(
            [d_att[:, head * HEAD_DIM : (head + 1) * HEAD_DIM] for head in range(heads)], axis=0
        ).astype(BF)
        scores = dot(k_ref[...], q_ref[at], NT)
        d_probs = dot(v_ref[...], d_heads, NT)
        key_at = key_at_ref[...]
        visible = (key_at >= query_at_ref[at, 0:1, :]) & (key_at <= query_at_ref[at, 1:2, :])
        for head in range(heads):
            lanes = slice(head * rows, (head + 1) * rows)
            raw = jnp.where(visible, scores[:, lanes] * scale, NEGATIVE)
            prob = jnp.exp(raw - peak_ref[at, :, lanes]) * share_ref[at, :, lanes]
            grad = d_probs[:, lanes]
            delta = jnp.sum(prob * grad, axis=0, keepdims=True)
            probs[:, lanes] = prob.astype(BF)
            slopes[:, lanes] = (prob * (grad - delta)).astype(BF)
        dv[...] += dot(probs[...], d_heads, NN)
        dk[...] += dot(slopes[...], q_ref[at], NN)
        stacked = dot(k_turned[...], slopes[...], NN).T * scale
        for head in range(heads):
            dq[at, :, head * HEAD_DIM : (head + 1) * HEAD_DIM] = stacked[head * rows : (head + 1) * rows]

    def take(i, carry):
        @pl.when(i < nz - 1)
        def _():
            ring.forward(i)

        row = line.near(i)
        back(row * NX + line.x)
        ring.wait_pair(row)
        save(row).start()
        back(row * NX + 1 - line.x)
        return carry

    lax.fori_loop(0, nz, take, 0)
    ring.finish()
    sums = Scatter(line, part, o_ref, work, ework, ssems, msems)

    def project(at):
        tall = pl.ds(pl.multiple_of(at * rows, rows), rows)
        cos_part, sin_part = cos_ref[tall, :], -sin_ref[tall, :]
        block_dq = dq[at]
        second = jnp.concatenate([block_dq[:, 128:], dk[tall, :] * scale], axis=1)
        dproj_ref[at, :, 0:128] = spin(block_dq[:, :128], cos_part, sin_part).astype(BF)
        dproj_ref[at, :, 128:256] = spin(second, cos_part, sin_part).astype(BF)
        last = jnp.concatenate([dv[tall, :], jnp.zeros((rows, wide - 256 - HEAD_DIM), F32)], axis=1)
        dproj_ref[at, :, 256:wide] = last.astype(BF)
        part[at] = dot(dproj_ref[at], attn[:, :wide], NT).astype(BF)

    def step(i, carry):
        row = line.far(i)
        project(row * NX + 1 - line.x)
        sums.across(row).start()
        project(row * NX + line.x)

        @pl.when(i > 0)
        def _():
            sums.add(i - 1)

        return carry

    lax.fori_loop(0, nz, step, 0)
    sums.add(nz - 1)
    sums.finish()
    norm_back_rows(x_ref, values_ref, gain_ref, o_ref, gain_out)
    for row in range(nz):
        save(row).wait()


def attention_rows_back(block, values_in, gain, mats, layer, cos_part, sin_part, key_at, query_at, queries, keys, values, peaks, shares, nz):
    rows, width = block.shape
    group = nz * NX
    group_rows = group * rows
    heads = 3
    wide = 384
    return pl.pallas_call(
        functools.partial(attention_back_kernel, nz, layer),
        out_shape=(
            jax.ShapeDtypeStruct((rows, width), F32),
            jax.ShapeDtypeStruct((1, width), F32),
            jax.ShapeDtypeStruct((group, rows, width), BF),
            jax.ShapeDtypeStruct((group, rows, wide), BF),
        ),
        in_specs=[VM, VM, VM, ANY] + [VM] * 9,
        out_specs=(VM, VM, ANY, VM),
        scratch_shapes=[
            pltpu.VMEM(mats.shape[2:], BF),
            pltpu.VMEM((width, heads * HEAD_DIM), BF),
            pltpu.VMEM((group, rows, width), BF),
            pltpu.VMEM((group, rows, width), BF),
            pltpu.VMEM((HEAD_DIM, group_rows), BF),
            pltpu.VMEM((group_rows, heads * rows), BF),
            pltpu.VMEM((group_rows, heads * rows), BF),
            pltpu.VMEM((group, rows, heads * HEAD_DIM), F32),
            pltpu.VMEM((group_rows, HEAD_DIM), F32),
            pltpu.VMEM((group_rows, HEAD_DIM), F32),
            DMA,
            DMA((nz,)),
        ]
        + Gather.scratch(nz)
        + Scatter.scratch(nz, rows, width),
        compiler_params=params(10 + 2 * layer, 60),
        name="attention_backward",
    )(block, values_in, gain, mats, cos_part, sin_part, key_at, query_at, queries, keys, values, peaks, shares)


def rope_tables(places):
    half_dim = HEAD_DIM // 2
    freq_steps = jnp.arange(half_dim, dtype=jnp.float32)
    inverse = jnp.exp(freq_steps * (-2.0 * math.log(10000.0) / HEAD_DIM))
    angles = places[:, None] * inverse[None, :]
    return jnp.cos(angles), jnp.sin(angles)


def pack_weights(master_set, nctx):
    query_weight, key_weight, value_weight, out_weight, attn_gain, moe_gain = master_set[:6]
    layers, rows = query_weight.shape[:2]

    def columns(master):
        return master.astype(BF).reshape(layers, rows, nctx, -1).transpose(0, 2, 1, 3)

    attn = jnp.concatenate(
        [columns(query_weight), columns(key_weight), columns(value_weight), columns(out_weight)], axis=-1
    )
    gains = jnp.stack([attn_gain, moe_gain], axis=1).reshape(2 * layers, rows).astype(BF).astype(F32)
    return attn, jnp.pad(gains, ((0, 0), (0, 128 - rows)))


def fast_body(nctx, nfs, *args):
    (tokens, cotangent, lengths, tile_order, routes, gates), master_set = args[:6], args[6:]
    nz = nctx // NX
    rows_here, model_width = tokens.shape[1], tokens.shape[2]
    group_rows = rows_here * nctx
    ctx = lax.axis_index("ctx")
    _, pos_all = layout(lengths[0], tile_order[0], group_rows)
    cos_half, sin_half = rope_tables(pos_all.astype(jnp.float32))
    cos_part = jnp.concatenate([cos_half] * 4, axis=1)
    sin_part = jnp.concatenate([-sin_half, sin_half] * 2, axis=1)
    row_ids = jnp.arange(rows_here, dtype=jnp.int32)
    first_at = (tile_order[0][:, None] * TILE + row_ids[None, :]).reshape(group_rows)
    key_at = first_at[:, None]
    query_at = jnp.stack(
        [(first_at - pos_all).reshape(nctx, rows_here), first_at.reshape(nctx, rows_here)], axis=1
    )
    q_width = 3 * HEAD_DIM
    kv_at, v_at, o_at = q_width, q_width + HEAD_DIM, q_width + 2 * HEAD_DIM

    expert_ids = jnp.arange(EXPERTS, dtype=jnp.int32)
    table = jnp.sum(
        jnp.where(routes[:, 0, :, :, None] == expert_ids, gates[:, 0, :, :, None], 0.0), axis=-2
    )
    attn, gains = pack_weights(master_set, nctx)
    rows = attn.shape[2]
    gains = jnp.broadcast_to(gains[None], (nctx, 2 * LAYERS, 128))
    shares = table.transpose(2, 0, 1).reshape(nctx, 2, LAYERS, rows_here).transpose(0, 2, 1, 3)
    shares = shares.reshape(nctx, 2 * LAYERS, rows_here)
    pad = jnp.zeros((nctx, 8 - 2 * LAYERS, 128), F32)
    small = jnp.concatenate([gains, pad, shares, pad], axis=1)
    mats_all, small_all = spread_weights(attn, *master_set[6:], small, nfs)
    shares = lax.dynamic_index_in_dim(
        small_all.reshape(nctx, nfs, 16, 128), lax.axis_index("fsdp"), 1, keepdims=False
    )
    fetched = [
        (
            small_all[:, 2 * layer, :rows].reshape(1, -1),
            small_all[:, 2 * layer + 1, :rows].reshape(1, -1),
            shares[:, 8 + 2 * layer : 10 + 2 * layer].transpose(0, 2, 1),
        )
        for layer in range(LAYERS)
    ]

    hidden = tokens[0].astype(jnp.float32)
    records = []
    for layer in range(LAYERS):
        attn_gain, moe_gain, share = fetched[layer]
        middle, normed_all, queries, keys, values, peaks, sums, attended, *rest = attention_rows(
            hidden, attn_gain, mats_all, layer, cos_part, sin_part, key_at, query_at, nz, nfs
        )
        mats_all = rest[0] if rest else mats_all
        moved, moe_all, gate_act, up_act = experts_forward(middle, moe_gain, share, mats_all, layer, nz)
        records.append((hidden, normed_all, queries, keys, values, peaks, sums, attended, middle, moe_all, gate_act, up_act))
        hidden = moved

    output = hidden.astype(BF)
    grad = cotangent[0].astype(jnp.float32)
    layer_args, gain_grads = [None] * LAYERS, [None] * LAYERS
    for layer in reversed(range(LAYERS)):
        attn_gain, moe_gain, share = fetched[layer]
        hidden, normed_all, queries, keys, values, peaks, sums, attended, middle, moe_all, gate_act, up_act = records[layer]
        grad_middle, grad_moe_gain, grad_all, d_gate, d_up, inner = experts_backward(
            grad, middle, moe_gain, share, mats_all, layer, gate_act, up_act, nz
        )
        grad, grad_attn_gain, middle_all, d_proj = attention_rows_back(
            grad_middle, hidden, attn_gain, mats_all, layer, cos_part, sin_part, key_at, query_at, queries, keys, values, peaks, sums, nz
        )
        layer_args[layer] = [
            part.reshape(group_rows, -1)
            for part in (normed_all, d_proj, middle_all, attended, moe_all, d_gate, d_up, grad_all, inner)
        ]
        gain_grads[layer] = [grad_attn_gain, grad_moe_gain]

    extra = jnp.stack([part for pair in gain_grads for part in pair])
    extra = extra.reshape(2 * LAYERS, nctx, nfs // NCORE, NCORE, rows).transpose(3, 2, 1, 0, 4)
    extra = jnp.pad(extra, ((0, 0), (0, 0), (0, 0), (0, 8 - 2 * LAYERS), (0, 128 - rows)))
    collected, gains_in = collect_grads(nctx, nfs, layer_args, extra)

    def attn_part(low, high):
        part = collected[:, :, 0, :, low:high].transpose(0, 2, 1, 3)
        return part.reshape(LAYERS, rows, -1).astype(F32)

    def expert_part(first):
        part = collected[:, :, first : first + 2]
        return part.reshape((LAYERS, EXPERTS) + part.shape[3:]).astype(F32)

    gain_sums = jnp.sum(gains_in[:, : 2 * LAYERS, :rows], axis=0).reshape(LAYERS, 2, rows)

    def gain_part(kind):
        return gain_sums[:, kind]

    return (
        output[None],
        grad[None],
        attn_part(0, kv_at),
        attn_part(kv_at, v_at),
        attn_part(v_at, o_at),
        attn_part(o_at, o_at + q_width),
        gain_part(0),
        gain_part(1),
        expert_part(1),
        expert_part(3),
        expert_part(5),
    )


def solution(mesh):
    placed = (
        P("fsdp", "ctx", None),
        P("fsdp", "ctx", None),
        P("fsdp", None),
        P("fsdp", None),
        P(None, "fsdp", "ctx", None),
        P(None, "fsdp", "ctx", None),
        P(None, ("ctx", "fsdp"), None),
        P(None, ("ctx", "fsdp"), None),
        P(None, ("ctx", "fsdp"), None),
        P(None, ("ctx", "fsdp"), None),
        P(None, ("ctx", "fsdp")),
        P(None, ("ctx", "fsdp")),
        P(None, None, ("ctx", "fsdp"), None),
        P(None, None, ("ctx", "fsdp"), None),
        P(None, None, ("ctx", "fsdp"), None),
    )
    nctx, nfs = mesh.shape["ctx"], mesh.shape["fsdp"]
    chosen = partial(fast_body, nctx, nfs) if (nctx, nfs) == (8, 4) else body
    return jax.shard_map(
        chosen,
        mesh=mesh,
        in_specs=placed,
        out_specs=(
            P("fsdp", "ctx", None),
            P("fsdp", "ctx", None),
            P(None, ("ctx", "fsdp"), None),
            P(None, ("ctx", "fsdp"), None),
            P(None, ("ctx", "fsdp"), None),
            P(None, ("ctx", "fsdp"), None),
            P(None, ("ctx", "fsdp")),
            P(None, ("ctx", "fsdp")),
            P(None, None, ("ctx", "fsdp"), None),
            P(None, None, ("ctx", "fsdp"), None),
            P(None, None, ("ctx", "fsdp"), None),
        ),
        check_vma=False,
    )
```
